32 devices in a mesh: dp: 8 (over z, x), expert: 4 (over y, core).
Axes of the slice: x: 2, y: 2, z: 4, core: 2. Of those that a mesh axis runs over, the one named last changes fastest.
Arguments:
- tokens: bfloat16 [32768, 768], P(('dp', 'expert')), may hold values from -6 to 6
- prev_scores: float32 [32768, 8], P(('dp', 'expert')), may hold values from -6 to 6
- segments: int32 [32, 1024], P(('dp', 'expert')), may hold values from 0 to 7, never falling along the last dimension, each value on 1 to 512 neighbouring positions
- routes: int32 [32768, 2], P(('dp', 'expert')), may hold values from 0 to 7, all different within a row; in each aligned block of 1024 rows (0 to 1023, 1024 to 2047, ...) at most 256 rows name the same one
- wqkv: bfloat16 [768, 2304], P('dp'), may hold values from -0.21875 to 0.21875
- wo: bfloat16 [768, 768], P('dp'), may hold values from -1.75 to 1.75
- router: bfloat16 [768, 8], P('dp'), may hold values from -0.125 to 0.125
- const_gate: bfloat16 [768, 4], P('dp'), may hold values from -0.21875 to 0.21875
- const_vec: bfloat16 [768, 2], P('dp'), may hold values from -5 to 5
- gain1: bfloat16 [768], P('dp'), may hold values from 0.5 to 1.5
- gain2: bfloat16 [768], P('dp'), may hold values from 0.5 to 1.5
- gate_mix: bfloat16 [8, 8], replicated, may hold values from -0.8984375 to 0.8984375
- w_in: bfloat16 [4, 768, 4096], P('expert'), may hold values from -0.21875 to 0.21875
- w_out: bfloat16 [4, 2048, 768], P('expert'), may hold values from -0.125 to 0.125
- cotangent: bfloat16 [32768, 768], P(('dp', 'expert')), may hold values from -6 to 6
Outputs:
- mixed: bfloat16 [32768, 768], P(('dp', 'expert'))
- grad_tokens: float32 [32768, 768], P(('dp', 'expert'))
- grad_prev: float32 [32768, 8], P(('dp', 'expert'))
- grad_wqkv: float32 [768, 2304], P('dp')
- grad_wo: float32 [768, 768], P('dp')
- grad_router: float32 [768, 8], P('dp')
- grad_const_gate: float32 [768, 4], P('dp')
- grad_const_vec: float32 [768, 2], P('dp')
- grad_gain1: float32 [768], P('dp')
- grad_gain2: float32 [768], P('dp')
- grad_gate_mix: float32 [8, 8], replicated
- grad_w_in: float32 [4, 768, 4096], P('expert', 'dp')
- grad_w_out: float32 [4, 2048, 768], P('expert', 'dp')
The draws below stay inside these ranges and needn't reach their ends.
Inputs may be any that keep to these rules, and one draw needn't show every extreme that they name: `routes`: each token names two different experts. Within the tokens of one device (aligned blocks of 1024 rows), no expert is named by more than 256 tokens, and some expert reaches 256. `segments`: within a sequence the numbers never fall; a document has at most 512 positions, and one has exactly that many.
All inputs are finite; a program needn't handle non-finite values.
Results may differ from the reference program's by a relative error of at most 0.014.
The reference program's roundings to bfloat16 on the way count: a program that leaves them out, or rounds other values in their place, can miss the bound.
Values may be sent and summed in bfloat16 or wider, within the bound.
A program may use at most 256 MiB of HBM per device.

```python
import math
from functools import partial
import jax
import jax.numpy as jnp
import numpy as np
from jax import lax

D = 768
HEADS = 12
HEAD_DIM = 64
FF = 2048
SEQ_LEN = 1024
EXPERTS = 4
KINDS = 8
TOK_DEV = 1024
SEQ_TOTAL = 32
TOKENS = 32768
CAP = 256
N_DP = 8
N_EXPERT = 4


def block_levels(key, shape, split, smallest, high):
    def one(position, parts):
        draws = jax.random.uniform(jax.random.fold_in(jax.random.fold_in(key, 6), position), (parts,), jnp.float32, smallest / len(split), high / len(split))
        return jnp.repeat(jnp.exp(draws), shape[position] // parts).reshape((-1,) + (1,) * (len(shape) - position - 1))

    loudness = one(*split[0])
    for cut in split[1:]:
        loudness = loudness * one(*cut)
    return loudness


def length_profile(number_of, total, most, lean):
    portions = [(1 << 20) // math.isqrt(standing ** lean) + 1 for standing in range(2, number_of + 1)]
    rest, holding = total - most - (number_of - 1), [1] * (number_of - 1)
    while rest > 0:
        movable = [i for i in range(number_of - 1) if holding[i] < most]
        whole, budget = sum([portions[i] for i in movable]), rest
        for i in movable:
            extra = min(most - holding[i], max(1, budget * portions[i] // whole), rest)
            holding[i] = holding[i] + extra
            rest = rest - extra
    return np.array([most] + holding)


def ragged(stream_key, number_of, total, most, slope):
    if number_of == 2:
        one = jax.random.randint(stream_key, (), max(1, total - most), min(most, total - 1) + 1)
        return jnp.stack([one, total - one])
    sizes = jnp.asarray(length_profile(number_of, total, most, slope), jnp.int32)
    twos = (number_of - 1) // 2
    giver, sink = sizes[1:1 + 2 * twos:2], sizes[2:2 + 2 * twos:2]
    room = jnp.minimum(giver - 1, most - sink)
    moved = jax.random.randint(jax.random.fold_in(stream_key, 1), (twos,), 0, 1 << 20) % (room + 1)
    sizes = sizes.at[1:1 + 2 * twos:2].set(giver - moved).at[2:2 + 2 * twos:2].set(sink + moved)
    return sizes[jax.random.permutation(jax.random.fold_in(stream_key, 2), number_of)]


def routed_block(stream_key, own, number, rows, number_of, top, limit, lean):
    order = jax.random.permutation(stream_key, number_of)
    heavy_load, common = portions_of(number_of, rows * top, limit, lean, True), portions_of(number_of, rows * top, limit, lean, False)
    places = jnp.arange(number_of)

    def named(tallies, rotation):
        used = int((tallies > 0).sum())
        fixed = max(1, used // 4)
        moved = fixed + (places - fixed + rotation * (used - fixed)) % max(1, number_of - fixed)
        return jnp.zeros((number_of,), jnp.int32).at[order[jnp.where(places < fixed, places, moved)]].set(jnp.asarray(tallies, jnp.int32))

    tallies = jnp.where(number % 4 == 0, named(heavy_load, number // 4), named(common, number - number // 4 - 1))
    mixed = jax.random.permutation(jax.random.fold_in(own, 3), number_of)
    donor, taker = mixed[0:number_of // 2 * 2:2], mixed[1:number_of // 2 * 2:2]
    slack = jnp.minimum(tallies[donor] - 1, limit - tallies[taker]) // 2
    slack = jnp.where((donor == order[0]) | (taker == order[0]) | (tallies[taker] == 0), 0, jnp.maximum(slack, 0))
    moved = jax.random.randint(jax.random.fold_in(own, 4), (number_of // 2,), 0, 1 << 20) % (slack + 1)
    tallies = tallies.at[donor].add(-moved).at[taker].add(moved)
    members = jnp.searchsorted(jnp.cumsum(tallies), jnp.arange(rows * top), side="right").astype(jnp.int32)
    table = members.reshape(top, rows).T
    table = table[jax.random.permutation(jax.random.fold_in(own, 1), rows)]
    rotation = jax.random.randint(jax.random.fold_in(own, 2), (rows, 1), 0, top)
    return jnp.take_along_axis(table, (jnp.arange(top)[None, :] + rotation) % top, axis=1)


def portions_of(number_of, total, most, slope, full):
    portions = [(1 << 20) // math.isqrt(standing ** slope) + 1 for standing in range(1, number_of + 1)]
    largest = most if full else min(most, max(-(-total // number_of), total * portions[0] // sum(portions)))
    least = 1 if total - largest >= number_of - 1 else 0
    counts, spare = [largest] + [least] * (number_of - 1), total - largest - least * (number_of - 1)
    while spare > 0:
        movable = [i for i in range(1, number_of) if counts[i] < largest] or [i for i in range(1, number_of) if counts[i] < most]
        whole, budget = sum([portions[i] for i in movable]), spare
        for i in movable:
            more = min(most - counts[i], max(1, budget * portions[i] // whole), spare)
            counts[i] = counts[i] + more
            spare = spare - more
    return np.array(counts)


def centred(stream_key, shape, scale, bound, cuts=(), kind=jnp.bfloat16):
    level = block_levels(stream_key, shape, cuts, -0.22, 0.18) if cuts else 1.0
    drawn = jax.random.normal(stream_key, shape, jnp.float32) * scale * level
    return jnp.minimum(jnp.maximum(drawn, -bound), bound).astype(kind)


def setup_inputs(seed: int = 0) -> dict:
    streams_of = jax.random.split(jax.random.key(seed), 16)
    tokens = centred(streams_of[0], (TOKENS, D), 1.0, 6.0, ((0, 32),))
    prev_scores = centred(streams_of[1], (TOKENS, KINDS), 1.0, 6.0, ((0, 32),), jnp.float32)
    segments = jax.vmap(lambda own: jnp.searchsorted(jnp.cumsum(ragged(own, 8, SEQ_LEN, SEQ_LEN // 2, 2)), jnp.arange(SEQ_LEN), side="right"))(jax.random.split(streams_of[2], SEQ_TOTAL)).reshape((SEQ_TOTAL, SEQ_LEN)).astype(jnp.int32)
    routes_keys = jax.random.split(jax.random.fold_in(streams_of[3], 1), TOKENS // TOK_DEV)
    routes_turns = jax.random.permutation(jax.random.fold_in(streams_of[3], 3), TOKENS // TOK_DEV)
    routes = jax.vmap(lambda own, number: routed_block(jax.random.fold_in(streams_of[3], 2), own, number, TOK_DEV, KINDS, 2, CAP, 2))(routes_keys, routes_turns).reshape((TOKENS, 2))
    wqkv = centred(streams_of[4], (D, 3 * D), D ** -0.5, 0.21875, ((0, 8),))
    wo = centred(streams_of[5], (D, D), (D // 64) ** -0.5, 1.75, ((0, 8),))
    router = centred(streams_of[6], (D, KINDS), (3 * D) ** -0.5, 0.125, ((0, 8),))
    const_gate = centred(streams_of[7], (D, 4), D ** -0.5, 0.21875, ((0, 8),))
    const_vec = centred(streams_of[8], (D, 2), 1.0, 5.0, ((0, 8),))
    gain1 = jnp.clip(1.0 + 0.1 * jax.random.normal(streams_of[9], (D,), jnp.float32), 0.5, 1.5).astype(jnp.bfloat16)
    gain2 = jnp.clip(1.0 + 0.1 * jax.random.normal(streams_of[10], (D,), jnp.float32), 0.5, 1.5).astype(jnp.bfloat16)
    gate_mix = centred(streams_of[11], (KINDS, KINDS), 0.15, 0.8984375)
    w_in = centred(streams_of[12], (EXPERTS, D, 2 * FF), D ** -0.5, 0.21875, ((0, 4),))
    w_out = centred(streams_of[13], (EXPERTS, FF, D), FF ** -0.5, 0.125, ((0, 4),))
    cotangent = centred(streams_of[14], (TOKENS, D), 1.0, 6.0, ((0, 32),))
    return {"tokens": tokens, "prev_scores": prev_scores, "segments": segments, "routes": routes, "wqkv": wqkv, "wo": wo, "router": router, "const_gate": const_gate, "const_vec": const_vec, "gain1": gain1, "gain2": gain2, "gate_mix": gate_mix, "w_in": w_in, "w_out": w_out, "cotangent": cotangent}


NORM_EPSILON = 1e-06
HIGHEST_PRECISION = lax.Precision.HIGHEST
NEGATIVE = -1e+30

@jax.custom_vjp
def low(v):
    return lax.optimization_barrier(v.astype(jnp.bfloat16)).astype(jnp.float32)

@jax.custom_vjp
def low_back(v):
    return v

def low_keep(v):
    return (low(v), None)

def low_pass(kept, grad):
    return (grad,)

def back_keep(v):
    return (v, None)

def back_low(kept, grad):
    return (low(grad),)
low.defvjp(low_keep, low_pass)
low_back.defvjp(back_keep, back_low)

def matmul(left, right):
    return jnp.dot(left, right, precision=HIGHEST_PRECISION)

def rms_norm(values, gain):
    return values * lax.rsqrt(lax.optimization_barrier(jnp.mean(values * values, axis=-1, keepdims=True)) + NORM_EPSILON) * gain

def rotate(values, cosines, sine_table):
    half_width = values.shape[-1] // 2
    front_half = values[..., :half_width]
    back_half = values[..., half_width:]
    return jnp.concatenate([front_half * cosines - back_half * sine_table, back_half * cosines + front_half * sine_table], axis=-1)

def pair_softmax(picked):
    weights = jnp.exp(picked - lax.optimization_barrier(jnp.max(picked, axis=-1, keepdims=True)))
    return weights / lax.optimization_barrier(jnp.sum(weights, axis=-1, keepdims=True))

def attend_block(q_block, key_rows, value_rows, seg_block, seg_keys, row_start):
    scores = low_back(jnp.einsum('qhd,khd->hqk', q_block, key_rows, precision=HIGHEST_PRECISION))
    row_ids = row_start + jnp.arange(q_block.shape[0], dtype=jnp.int32)
    col_ids = jnp.arange(key_rows.shape[0], dtype=jnp.int32)
    allowed = (col_ids[None, :] <= row_ids[:, None]) & (seg_block[:, None] == seg_keys[None, :])
    scores = jnp.where(allowed[None], scores, NEGATIVE)
    row_max = lax.optimization_barrier(jnp.max(scores, axis=-1, keepdims=True))
    expd = jnp.exp(scores - row_max)
    prob_rows = expd / lax.optimization_barrier(jnp.sum(expd, axis=-1, keepdims=True))
    return jnp.einsum('hqk,khd->qhd', low(prob_rows), value_rows, precision=HIGHEST_PRECISION)

def attend_sequence(packed):
    q_seq, k_seq, v_seq, seg_seq = packed
    block_rows = min(512, SEQ_LEN)
    pieces = []
    for row_start in range(0, SEQ_LEN, block_rows):
        block_fn = jax.checkpoint(partial(attend_block, row_start=row_start))
        pieces.append(block_fn(q_seq[row_start:row_start + block_rows], k_seq, v_seq, seg_seq[row_start:row_start + block_rows], seg_seq))
    return jnp.concatenate(pieces, axis=0)

def expert_rows(packed):
    rows_in, front_weight, back_weight = packed
    gate_up = low_back(matmul(rows_in, front_weight))
    gate_part = gate_up[:, :FF]
    up_part = gate_up[:, FF:]
    hidden_act = low(gate_part * jax.nn.sigmoid(gate_part) * up_part)
    return low(low_back(matmul(hidden_act, back_weight)))

def buffer_rows(routes):
    dev_count = N_DP * N_EXPERT
    per_dev = routes.reshape(dev_count, -1).astype(jnp.int32)
    onehot = (per_dev[:, :, None] == jnp.arange(KINDS, dtype=jnp.int32)[None, None, :]).astype(jnp.int32)
    earlier = jnp.cumsum(onehot, axis=1) - onehot
    slot_ids = lax.optimization_barrier(jnp.sum(earlier * onehot, axis=2)).astype(jnp.int32)
    device_ids = jnp.arange(dev_count, dtype=jnp.int32)[:, None]
    is_ffn = per_dev < EXPERTS
    target = jnp.where(is_ffn, per_dev * (dev_count * CAP) + device_ids * CAP + slot_ids, EXPERTS * dev_count * CAP)
    return target.reshape(-1).astype(jnp.int32)

def layer(tokens, prev_scores, wqkv, wo, router, const_gate, const_vec, gain1, gain2, gate_mix, w_in, w_out, routes, segments):
    attn_in = low(rms_norm(tokens, gain1))
    qkv_proj = low_back(matmul(attn_in, wqkv)).reshape(TOKENS, 3, HEADS, HEAD_DIM)
    positions = (jnp.arange(TOKENS, dtype=jnp.int32) % SEQ_LEN).astype(jnp.float32)
    frequency = 10000.0 ** (-jnp.arange(HEAD_DIM // 2).astype(jnp.float32) / (HEAD_DIM // 2))
    angles = positions[:, None, None] * frequency[None, None, :]
    cosines = jnp.cos(angles)
    sine_table = jnp.sin(angles)
    queries = low(rotate(qkv_proj[:, 0], cosines, sine_table) * HEAD_DIM ** (-0.5))
    key_rows = low(rotate(qkv_proj[:, 1], cosines, sine_table))
    value_rows = low(qkv_proj[:, 2])
    seq_shape = (SEQ_TOTAL, SEQ_LEN, HEADS, HEAD_DIM)
    attended = lax.map(attend_sequence, (queries.reshape(seq_shape), key_rows.reshape(seq_shape), value_rows.reshape(seq_shape), segments))
    attn_out = low(low_back(attended.reshape(TOKENS, D)))
    resid_mid = tokens + low_back(matmul(attn_out, wo))
    ffn_norm = rms_norm(resid_mid, gain2)
    ffn_in = low(ffn_norm)
    logits = low_back(matmul(ffn_in, router) + matmul(prev_scores, gate_mix))
    route_hot = (routes[:, :, None] == jnp.arange(KINDS, dtype=jnp.int32)[None, None, :]).astype(jnp.float32)
    gates = pair_softmax(lax.optimization_barrier(jnp.sum(logits[:, None, :] * route_hot, axis=-1)))
    mix_logits = low_back(matmul(ffn_in, const_gate))
    alpha_one = pair_softmax(mix_logits[:, 0:2])
    alpha_two = pair_softmax(mix_logits[:, 2:4])
    const_one = alpha_one[:, 0:1] * ffn_norm + alpha_one[:, 1:2] * const_vec[:, 0][None, :]
    const_two = alpha_two[:, 0:1] * ffn_norm + alpha_two[:, 1:2] * const_vec[:, 1][None, :]
    target = buffer_rows(routes)
    assign_count = TOKENS * 2
    owner = jnp.full((EXPERTS * N_DP * N_EXPERT * CAP,), assign_count, jnp.int32)
    owner = owner.at[target].set(jnp.arange(assign_count, dtype=jnp.int32), mode='drop')
    owner_token = jnp.where(owner == assign_count, TOKENS, owner // 2).astype(jnp.int32)
    ffn_padded = jnp.concatenate([ffn_in, jnp.zeros((1, D), jnp.float32)], axis=0)
    gathered = low_back(ffn_padded[owner_token]).reshape(EXPERTS, N_DP * N_EXPERT * CAP, D)
    outputs = lax.map(jax.checkpoint(expert_rows), (gathered, w_in, w_out))
    out_padded = jnp.concatenate([outputs.reshape(-1, D), jnp.zeros((1, D), jnp.float32)], axis=0)
    ffn_rows = out_padded[target].reshape(TOKENS, 2, D)
    is_ffn = (routes < EXPERTS).astype(jnp.float32)[:, :, None]
    is_copy = (routes == EXPERTS + 1).astype(jnp.float32)[:, :, None]
    is_one = (routes == EXPERTS + 2).astype(jnp.float32)[:, :, None]
    is_two = (routes == EXPERTS + 3).astype(jnp.float32)[:, :, None]
    branch = ffn_rows * is_ffn + ffn_norm[:, None, :] * is_copy + const_one[:, None, :] * is_one + const_two[:, None, :] * is_two
    return resid_mid + lax.optimization_barrier(jnp.sum(gates[:, :, None] * branch, axis=1))

def reference(tokens, prev_scores, segments, routes, wqkv, wo, router, const_gate, const_vec, gain1, gain2, gate_mix, w_in, w_out, cotangent):
    floats = [arr.astype(jnp.float32) for arr in (tokens, prev_scores, wqkv, wo, router, const_gate, const_vec, gain1, gain2, gate_mix, w_in, w_out)]

    def forward(*params):
        return layer(*params, routes, segments)
    output, pull = jax.vjp(forward, *floats)
    grads = pull(cotangent.astype(jnp.float32))
    return (output.astype(jnp.bfloat16), grads[0], grads[1], grads[2], grads[3], grads[4], grads[5], grads[6], grads[7], grads[8], grads[9], grads[10], grads[11])
```

```python
import jax
import jax.numpy as jnp
from jax import lax
from jax.sharding import PartitionSpec as P

HEADS = 12
HEAD_DIM = 64
CAP = 256


NORM_EPSILON = 1e-06
HIGHEST_PRECISION = lax.Precision.HIGHEST
NEGATIVE = -1e30


def rotate(values, cosines, sine_table):
    half_width = values.shape[-1] // 2
    front_half = values[..., :half_width]
    back_half = values[..., half_width:]
    return jnp.concatenate(
        [
            front_half * cosines - back_half * sine_table,
            back_half * cosines + front_half * sine_table,
        ],
        axis=-1,
    )


def pair_softmax(picked):
    weights = jnp.exp(picked - jnp.max(picked, axis=-1, keepdims=True))
    return weights / jnp.sum(weights, axis=-1, keepdims=True)


def pair_softmax_back(weights, upstream):
    return weights * (upstream - jnp.sum(weights * upstream, axis=-1, keepdims=True))


def norm_back(upstream, normed, inverse):
    return inverse * (upstream - normed * jnp.mean(upstream * normed, axis=-1, keepdims=True))


def masked_scores(q_block, key_rows, seg_rows, seg_keys, row_start):
    scores = jnp.einsum("qhd,khd->hqk", q_block, key_rows, preferred_element_type=jnp.float32)
    row_ids = row_start + jnp.arange(q_block.shape[0], dtype=jnp.int32)
    col_ids = jnp.arange(key_rows.shape[0], dtype=jnp.int32)
    allowed = (col_ids[None, :] <= row_ids[:, None]) & (seg_rows[:, None] == seg_keys[None, :])
    return jnp.where(allowed[None], scores, NEGATIVE)


def per_device(
    tokens,
    prev_scores,
    segments,
    routes,
    wqkv,
    wo,
    router,
    const_gate,
    const_vec,
    gain1,
    gain2,
    gate_mix,
    w_in,
    w_out,
    cotangent,
):
    kinds_in = router.shape[1]
    small = jnp.concatenate(
        [router, const_gate, const_vec, gain1[:, None], gain2[:, None]], axis=1
    )
    packed = jnp.concatenate(
        [wqkv, wo, jnp.pad(small, ((0, 0), (0, 128 - small.shape[1])))], axis=1
    )
    whole = lax.all_gather(packed, "dp", axis=0, tiled=True)
    qkv_cols = wqkv.shape[1]
    wqkv_full = whole[:, :qkv_cols]
    wo_full = whole[:, qkv_cols : qkv_cols + wo.shape[1]]
    small_full = whole[:, qkv_cols + wo.shape[1] :]
    router_full = small_full[:, :kinds_in]
    cgate_full = small_full[:, kinds_in : kinds_in + 4]
    cvec_full = small_full[:, kinds_in + 4 : kinds_in + 6]
    gain_attn = small_full[:, kinds_in + 6]
    gain_ffn = small_full[:, kinds_in + 7]
    tok_count, model_width = tokens.shape
    seq_count, seq_len = segments.shape
    head_count = HEADS
    head_size = HEAD_DIM
    kind_count = router.shape[1]
    experts = w_in.shape[0] * lax.axis_size("expert")
    hidden_width = w_out.shape[1]
    capacity = CAP
    scale = head_size ** (-0.5)
    resid_in = tokens.astype(jnp.float32)
    inverse_one = lax.rsqrt(jnp.mean(resid_in * resid_in, axis=-1, keepdims=True) + NORM_EPSILON)
    normed_one = resid_in * inverse_one
    gain_one = gain_attn.astype(jnp.float32)
    attn_in = (normed_one * gain_one).astype(jnp.bfloat16)
    qkv_proj = jnp.dot(attn_in, wqkv_full, preferred_element_type=jnp.float32).reshape(
        tok_count, 3, head_count, head_size
    )
    positions = (jnp.arange(tok_count, dtype=jnp.int32) % seq_len).astype(jnp.float32)
    frequency = 10000.0 ** (-jnp.arange(head_size // 2).astype(jnp.float32) / (head_size // 2))
    angles = positions[:, None, None] * frequency[None, None, :]
    cosines = jnp.cos(angles)
    sine_table = jnp.sin(angles)
    queries = (rotate(qkv_proj[:, 0], cosines, sine_table) * scale).astype(jnp.bfloat16)
    key_rows = rotate(qkv_proj[:, 1], cosines, sine_table).astype(jnp.bfloat16)
    value_rows = qkv_proj[:, 2].astype(jnp.bfloat16)
    seq_shape = (seq_count, seq_len, head_count, head_size)
    query_seqs = queries.reshape(seq_shape)
    key_seqs = key_rows.reshape(seq_shape)
    value_seqs = value_rows.reshape(seq_shape)
    block_rows = min(512, seq_len)
    per_seq = seq_len // block_rows
    block_count = seq_count * per_seq

    def block_inputs(block_index):
        seq_index = block_index // per_seq
        row_start = block_index % per_seq * block_rows
        seg_keys = segments[seq_index]
        q_block = lax.dynamic_slice_in_dim(query_seqs[seq_index], row_start, block_rows, 0)
        seg_rows = lax.dynamic_slice_in_dim(seg_keys, row_start, block_rows, 0)
        scores = masked_scores(q_block, key_seqs[seq_index], seg_rows, seg_keys, row_start)
        return (seq_index, row_start, q_block, scores)

    def forward_block(block_index):
        seq_index, row_start, q_block, scores = block_inputs(block_index)
        row_max = jnp.max(scores, axis=-1, keepdims=True)
        expd = jnp.exp(scores - row_max)
        row_total = jnp.sum(expd, axis=-1, keepdims=True)
        prob_rows = (expd / row_total).astype(jnp.bfloat16)
        attended = jnp.einsum(
            "hqk,khd->qhd", prob_rows, value_seqs[seq_index], preferred_element_type=jnp.float32
        )
        return (attended, row_max + jnp.log(row_total))

    attended, log_totals = lax.map(forward_block, jnp.arange(block_count, dtype=jnp.int32))
    attn_out = attended.reshape(tok_count, model_width).astype(jnp.bfloat16)
    resid_mid = resid_in + jnp.dot(attn_out, wo_full, preferred_element_type=jnp.float32)
    inverse_two = lax.rsqrt(jnp.mean(resid_mid * resid_mid, axis=-1, keepdims=True) + NORM_EPSILON)
    normed_two = resid_mid * inverse_two
    gain_two = gain_ffn.astype(jnp.float32)
    ffn_norm = normed_two * gain_two
    ffn_in = ffn_norm.astype(jnp.bfloat16)
    mix_matrix = gate_mix.astype(jnp.float32)
    logits = jnp.dot(ffn_in, router_full, preferred_element_type=jnp.float32) + jnp.dot(
        prev_scores, mix_matrix, precision=HIGHEST_PRECISION
    )
    route_hot = (
        routes[:, :, None] == jnp.arange(kind_count, dtype=jnp.int32)[None, None, :]
    ).astype(jnp.float32)
    gates = pair_softmax(jnp.sum(logits[:, None, :] * route_hot, axis=-1))
    mix_logits = jnp.dot(ffn_in, cgate_full, preferred_element_type=jnp.float32)
    alpha_one = pair_softmax(mix_logits[:, 0:2])
    alpha_two = pair_softmax(mix_logits[:, 2:4])
    const_values = cvec_full.astype(jnp.float32)
    const_one = alpha_one[:, 0:1] * ffn_norm + alpha_one[:, 1:2] * const_values[:, 0][None, :]
    const_two = alpha_two[:, 0:1] * ffn_norm + alpha_two[:, 1:2] * const_values[:, 1][None, :]
    flat_routes = routes.reshape(-1)
    assign_count = flat_routes.shape[0]
    route_onehot = (
        flat_routes[:, None] == jnp.arange(kind_count, dtype=jnp.int32)[None, :]
    ).astype(jnp.int32)
    earlier = jnp.cumsum(route_onehot, axis=0) - route_onehot
    slot_ids = jnp.sum(earlier * route_onehot, axis=1)
    target = jnp.where(flat_routes < experts, flat_routes * capacity + slot_ids, experts * capacity)
    slot_owner = jnp.full((experts * capacity,), assign_count, jnp.int32)
    slot_owner = slot_owner.at[target].set(jnp.arange(assign_count, dtype=jnp.int32), mode="drop")
    owner_token = jnp.where(slot_owner == assign_count, tok_count, slot_owner // 2)
    ffn_padded = jnp.concatenate([ffn_in, jnp.zeros((1, model_width), jnp.bfloat16)], axis=0)
    send_rows = ffn_padded[owner_token].reshape(experts, capacity, model_width)
    recv_rows = lax.all_to_all(send_rows, "expert", split_axis=0, concat_axis=1, tiled=True)
    gate_up = jnp.einsum("erd,edf->erf", recv_rows, w_in, preferred_element_type=jnp.float32)
    gate_part = gate_up[..., :hidden_width]
    up_part = gate_up[..., hidden_width:]
    sigmoid_gate = jax.nn.sigmoid(gate_part)
    hidden_act = (gate_part * sigmoid_gate * up_part).astype(jnp.bfloat16)
    expert_out = jnp.einsum(
        "erf,efd->erd", hidden_act, w_out, preferred_element_type=jnp.float32
    ).astype(jnp.bfloat16)
    returned = lax.all_to_all(expert_out, "expert", split_axis=1, concat_axis=0, tiled=True)
    out_padded = jnp.concatenate(
        [
            returned.reshape(experts * capacity, model_width),
            jnp.zeros((1, model_width), jnp.bfloat16),
        ],
        axis=0,
    )
    ffn_rows = out_padded[target].astype(jnp.float32).reshape(tok_count, 2, model_width)
    is_ffn = (routes < experts).astype(jnp.float32)
    is_copy = (routes == experts + 1).astype(jnp.float32)
    is_one = (routes == experts + 2).astype(jnp.float32)
    is_two = (routes == experts + 3).astype(jnp.float32)
    branch = (
        ffn_rows * is_ffn[:, :, None]
        + ffn_norm[:, None, :] * is_copy[:, :, None]
        + const_one[:, None, :] * is_one[:, :, None]
        + const_two[:, None, :] * is_two[:, :, None]
    )
    mixed = (resid_mid + jnp.sum(gates[:, :, None] * branch, axis=1)).astype(jnp.bfloat16)
    upstream = cotangent.astype(jnp.float32)
    gate_grad = jnp.sum(branch * upstream[:, None, :], axis=-1)
    weighted = (
        (gates[:, :, None] * upstream[:, None, :])
        .reshape(assign_count, model_width)
        .astype(jnp.bfloat16)
    )
    weighted_padded = jnp.concatenate([weighted, jnp.zeros((1, model_width), jnp.bfloat16)], axis=0)
    slot_grads = weighted_padded[slot_owner].reshape(experts, capacity, model_width)
    grad_sent = lax.all_to_all(slot_grads, "expert", split_axis=0, concat_axis=1, tiled=True)
    hidden_grad = jnp.einsum("erd,efd->erf", grad_sent, w_out, preferred_element_type=jnp.float32)
    gate_grad_h = hidden_grad * up_part * sigmoid_gate * (1.0 + gate_part * (1.0 - sigmoid_gate))
    up_grad = hidden_grad * gate_part * sigmoid_gate
    front_grad = jnp.concatenate([gate_grad_h, up_grad], axis=-1).astype(jnp.bfloat16)
    rows_grad = jnp.einsum(
        "erf,edf->erd", front_grad, w_in, preferred_element_type=jnp.float32
    ).astype(jnp.bfloat16)
    back_rows = lax.all_to_all(rows_grad, "expert", split_axis=1, concat_axis=0, tiled=True)
    back_padded = jnp.concatenate(
        [
            back_rows.reshape(experts * capacity, model_width),
            jnp.zeros((1, model_width), jnp.bfloat16),
        ],
        axis=0,
    )
    ffn_in_grad = jnp.sum(
        back_padded[target].astype(jnp.float32).reshape(tok_count, 2, model_width), axis=1
    )
    weight_one = jnp.sum(gates * is_one, axis=1)
    weight_two = jnp.sum(gates * is_two, axis=1)
    weight_copy = jnp.sum(gates * is_copy, axis=1)
    dot_norm = jnp.sum(upstream * ffn_norm, axis=-1)
    dot_vecs = jnp.dot(cotangent, cvec_full, preferred_element_type=jnp.float32)
    alpha_grad_one = weight_one[:, None] * jnp.stack([dot_norm, dot_vecs[:, 0]], axis=1)
    alpha_grad_two = weight_two[:, None] * jnp.stack([dot_norm, dot_vecs[:, 1]], axis=1)
    mix_grad = jnp.concatenate(
        [
            pair_softmax_back(alpha_one, alpha_grad_one),
            pair_softmax_back(alpha_two, alpha_grad_two),
        ],
        axis=1,
    ).astype(jnp.bfloat16)
    grad_cgate = jnp.einsum("td,tk->dk", ffn_in, mix_grad, preferred_element_type=jnp.float32)
    vec_weights = jnp.stack([weight_one * alpha_one[:, 1], weight_two * alpha_two[:, 1]], axis=1)
    grad_cvec = jnp.einsum("td,tk->dk", upstream, vec_weights, precision=HIGHEST_PRECISION)
    picked_grad = pair_softmax_back(gates, gate_grad)
    logit_grad = jnp.sum(route_hot * picked_grad[:, :, None], axis=1).astype(jnp.bfloat16)
    grad_router = jnp.einsum("td,tk->dk", ffn_in, logit_grad, preferred_element_type=jnp.float32)
    logit_wide = logit_grad.astype(jnp.float32)
    grad_mix = jnp.einsum("tk,tj->kj", prev_scores, logit_wide, precision=HIGHEST_PRECISION)
    grad_prev = jnp.einsum("tj,kj->tk", logit_grad, gate_mix, preferred_element_type=jnp.float32)
    norm_grad_two = (
        ffn_in_grad
        + jnp.einsum("tk,dk->td", logit_grad, router_full, preferred_element_type=jnp.float32)
        + jnp.einsum("tk,dk->td", mix_grad, cgate_full, preferred_element_type=jnp.float32)
        + (weight_copy + weight_one * alpha_one[:, 0] + weight_two * alpha_two[:, 0])[:, None]
        * upstream
    )
    grad_gain2 = jnp.sum(norm_grad_two * normed_two, axis=0)
    mid_grad = upstream + norm_back(norm_grad_two * gain_two, normed_two, inverse_two)
    proj_grad = mid_grad.astype(jnp.bfloat16)
    grad_wo = jnp.einsum("td,te->de", attn_out, proj_grad, preferred_element_type=jnp.float32)
    attn_grad = jnp.einsum(
        "te,de->td", proj_grad, wo_full, preferred_element_type=jnp.float32
    ).astype(jnp.bfloat16)
    attn_grad_seqs = attn_grad.reshape(seq_shape)

    def backward_block(packed):
        block_index, log_total = packed
        seq_index, row_start, q_block, scores = block_inputs(block_index)
        prob_rows = jnp.exp(scores - log_total)
        out_grad_block = lax.dynamic_slice_in_dim(
            attn_grad_seqs[seq_index], row_start, block_rows, 0
        )
        prob_grad = jnp.einsum(
            "qhd,khd->hqk",
            out_grad_block,
            value_seqs[seq_index],
            preferred_element_type=jnp.float32,
        )
        row_delta = jnp.sum(prob_rows * prob_grad, axis=-1, keepdims=True)
        score_grad = (prob_rows * (prob_grad - row_delta)).astype(jnp.bfloat16)
        query_grad = jnp.einsum(
            "hqk,khd->qhd", score_grad, key_seqs[seq_index], preferred_element_type=jnp.float32
        )
        key_grad = jnp.einsum(
            "hqk,qhd->khd", score_grad, q_block, preferred_element_type=jnp.float32
        )
        value_grad = jnp.einsum(
            "hqk,qhd->khd",
            prob_rows.astype(jnp.bfloat16),
            out_grad_block,
            preferred_element_type=jnp.float32,
        )
        return (query_grad, key_grad, value_grad)

    query_grad, key_grad, value_grad = lax.map(
        backward_block, (jnp.arange(block_count, dtype=jnp.int32), log_totals)
    )
    query_grad = query_grad.reshape(tok_count, head_count, head_size)
    key_grad = jnp.sum(
        key_grad.reshape(seq_count, per_seq, seq_len, head_count, head_size), axis=1
    ).reshape(tok_count, head_count, head_size)
    value_grad = jnp.sum(
        value_grad.reshape(seq_count, per_seq, seq_len, head_count, head_size), axis=1
    ).reshape(tok_count, head_count, head_size)
    query_back = rotate(query_grad * scale, cosines, -sine_table)
    key_back = rotate(key_grad, cosines, -sine_table)
    qkv_grad = (
        jnp.stack([query_back, key_back, value_grad], axis=1)
        .reshape(tok_count, 3 * model_width)
        .astype(jnp.bfloat16)
    )
    grad_wqkv = jnp.einsum("td,tf->df", attn_in, qkv_grad, preferred_element_type=jnp.float32)
    attn_in_grad = jnp.einsum("tf,df->td", qkv_grad, wqkv_full, preferred_element_type=jnp.float32)
    grad_gain1 = jnp.sum(attn_in_grad * normed_one, axis=0)
    grad_tokens = mid_grad + norm_back(attn_in_grad * gain_one, normed_one, inverse_one)
    grad_w_out = jnp.einsum(
        "erf,erd->efd", hidden_act, grad_sent, preferred_element_type=jnp.float32
    ).astype(jnp.bfloat16)
    grad_w_in = jnp.einsum(
        "erd,erf->edf", recv_rows, front_grad, preferred_element_type=jnp.float32
    ).astype(jnp.bfloat16)
    out_share = lax.psum_scatter(grad_w_out, "dp", scatter_dimension=1, tiled=True).astype(
        jnp.float32
    )
    in_share = lax.psum_scatter(grad_w_in, "dp", scatter_dimension=1, tiled=True).astype(
        jnp.float32
    )
    large = jnp.concatenate([grad_wqkv, grad_wo], axis=1).astype(jnp.bfloat16)
    large_share = lax.psum_scatter(large, "dp", scatter_dimension=0, tiled=True)
    minor = jnp.concatenate(
        [grad_router, grad_cgate, grad_cvec, grad_gain1[:, None], grad_gain2[:, None]], axis=1
    )
    minor_share = lax.psum_scatter(minor, "dp", scatter_dimension=0, tiled=True)
    summed = lax.psum((large_share.astype(jnp.float32), minor_share), "expert")
    grad_gate_mix = lax.psum(grad_mix, ("dp", "expert"))
    shares = (
        summed[0][:, : wqkv.shape[1]],
        summed[0][:, wqkv.shape[1] :],
        summed[1][:, :kinds_in],
        summed[1][:, kinds_in : kinds_in + 4],
        summed[1][:, kinds_in + 4 : kinds_in + 6],
        summed[1][:, kinds_in + 6],
        summed[1][:, kinds_in + 7],
    )
    return (
        mixed,
        grad_tokens,
        grad_prev,
        shares[0],
        shares[1],
        shares[2],
        shares[3],
        shares[4],
        shares[5],
        shares[6],
        grad_gate_mix,
        in_share,
        out_share,
    )


def solution(mesh):
    in_specs = (
        P(("dp", "expert"), None),
        P(("dp", "expert"), None),
        P(("dp", "expert"), None),
        P(("dp", "expert"), None),
        P("dp", None),
        P("dp", None),
        P("dp", None),
        P("dp", None),
        P("dp", None),
        P("dp"),
        P("dp"),
        P(),
        P("expert", None, None),
        P("expert", None, None),
        P(("dp", "expert"), None),
    )
    out_specs = (
        P(("dp", "expert"), None),
        P(("dp", "expert"), None),
        P(("dp", "expert"), None),
        P("dp", None),
        P("dp", None),
        P("dp", None),
        P("dp", None),
        P("dp", None),
        P("dp"),
        P("dp"),
        P(),
        P("expert", "dp", None),
        P("expert", "dp", None),
    )
    return jax.shard_map(
        per_device, mesh=mesh, in_specs=in_specs, out_specs=out_specs, check_vma=False
    )
```

```python
import functools

import jax
import jax.numpy as jnp
from jax import lax
from jax.experimental import pallas as pl
from jax.experimental.pallas import tpu as pltpu
from jax.sharding import PartitionSpec as P

HEADS = 12
HEAD_DIM = 64
CAP = 256
DOC_MAX = 512
NORM_EPSILON = 1e-06
HIGHEST_PRECISION = lax.Precision.HIGHEST
NEGATIVE = -1e30
F32 = jnp.float32
BF16 = jnp.bfloat16
BLOCK = 256
GROUP = 4
GROUP_LANES = GROUP * HEAD_DIM
LANES = 128
VMEM_BYTES = 62 * 1024 * 1024


def nn(left, right):
    return jnp.dot(left, right, preferred_element_type=F32)


def nt(left, right):
    return lax.dot_general(left, right, (((1,), (1,)), ((), ())), preferred_element_type=F32)


def tn(left, right):
    return lax.dot_general(left, right, (((0,), (0,)), ((), ())), preferred_element_type=F32)


def iota(shape, axis):
    return lax.broadcasted_iota(jnp.int32, shape, axis)


def split_low(values):
    high = values.astype(BF16)
    return high, (values - high.astype(F32)).astype(BF16)


def inverse_rms(values):
    return lax.rsqrt(jnp.mean(values * values, axis=-1, keepdims=True) + NORM_EPSILON)


def norm_back(upstream, normed, inverse):
    return inverse * (upstream - normed * jnp.mean(upstream * normed, axis=-1, keepdims=True))


def turn(values, cosines, signed_sines):
    pieces = []
    for start in range(0, values.shape[1], LANES):
        part = values[:, start : start + LANES]
        front = iota(part.shape, 1) % HEAD_DIM < HEAD_DIM // 2
        swapped = jnp.where(
            front,
            pltpu.roll(part, LANES - HEAD_DIM // 2, 1),
            pltpu.roll(part, HEAD_DIM // 2, 1),
        )
        pieces.append(part * cosines + swapped * signed_sines)
    return jnp.concatenate(pieces, axis=1)


def head_mask(head):
    return (iota((1, GROUP_LANES), 1) // HEAD_DIM == head).astype(F32).astype(BF16)


def params(**extra):
    return pltpu.CompilerParams(vmem_limit_bytes=VMEM_BYTES, **extra)


def whole_block(shape):
    return pl.BlockSpec(shape, lambda *_: (0,) * len(shape))


def cost(flops, moved):
    return pl.CostEstimate(flops=int(flops), bytes_accessed=int(moved), transcendentals=0)


def send_cotangent_kernel(experts, cot_ref, target_ref, out_ref):
    tokens = cot_ref.shape[0]

    @pl.loop(0, experts)
    def _(expert):
        slots = iota((CAP, tokens), 0) + expert * CAP
        hot = (target_ref[0:1, :] == slots) | (target_ref[1:2, :] == slots)
        out_ref[expert] = nn(hot.astype(F32).astype(BF16), cot_ref[...]).astype(BF16)


def attend_kernel(
    gain_row, tok_ref, wq_ref, wk_ref, wv_ref, small_ref, cos_ref, sin_ref, segc_ref, segr_ref,
    qkv_ref, attn_in_ref, out_ref, lse_ref, gain_ref, bias_ref, log_ref,
):
    step = pl.program_id(0)
    tokens = tok_ref.shape[0]
    blocks = tokens // BLOCK
    reach = DOC_MAX // BLOCK

    @pl.when(step == 0)
    def _():
        gain_ref[...] = small_ref[...].astype(F32).T[gain_row : gain_row + 1, :]
        log_ref[...] = jnp.zeros_like(log_ref)

        @pl.loop(0, blocks)
        def _(block):
            rows = pl.ds(pl.multiple_of(block * BLOCK, BLOCK), BLOCK)
            values = tok_ref[rows, :].astype(F32)
            attn_in_ref[rows, :] = (values * inverse_rms(values) * gain_ref[...]).astype(BF16)

    @pl.loop(0, blocks)
    def _(block):
        rows = pl.ds(pl.multiple_of(block * BLOCK, BLOCK), BLOCK)
        normed = attn_in_ref[rows, :]
        cosines = cos_ref[rows, :]
        sines = sin_ref[rows, :]
        query = turn(nn(normed, wq_ref[...]), cosines, sines) * HEAD_DIM**-0.5
        qkv_ref[0, rows, :] = query.astype(BF16)
        qkv_ref[1, rows, :] = turn(nn(normed, wk_ref[...]), cosines, sines).astype(BF16)
        qkv_ref[2, rows, :] = nn(normed, wv_ref[...]).astype(BF16)

    for block in range(blocks):
        first = max(0, block - reach) * BLOCK
        last = (block + 1) * BLOCK
        span = last - first
        rows = slice(block * BLOCK, last)
        row_ids = iota((BLOCK, span), 0) + block * BLOCK
        col_ids = iota((BLOCK, span), 1) + first
        seen = (col_ids <= row_ids) & (segc_ref[rows, :] == segr_ref[0:1, first:last])
        bias_ref[:, 0:span] = jnp.where(seen, 0.0, NEGATIVE)
        attended = []
        logs = log_ref[rows, :]
        for head in range(GROUP):
            mask = head_mask(head)
            scores = nt(qkv_ref[0, rows, :] * mask, qkv_ref[1, first:last, :]) + bias_ref[:, 0:span]
            top = jnp.max(scores, axis=1, keepdims=True)
            weights = jnp.exp(scores - top).astype(BF16)
            value = qkv_ref[2, first:last, :] * mask + (1 - mask)
            mixed = nn(weights, value)
            own = iota(mixed.shape, 1) // HEAD_DIM == head
            total = jnp.max(jnp.where(own, 0.0, mixed), axis=1, keepdims=True)
            attended.append(jnp.where(own, mixed / total, 0.0))
            logs = jnp.where(
                iota(logs.shape, 1) == step * GROUP + head, top + jnp.log(total), logs
            )
        log_ref[rows, :] = logs
        out_ref[rows, :] = (attended[0] + attended[1] + attended[2] + attended[3]).astype(BF16)

    @pl.when(step == pl.num_programs(0) - 1)
    def _():
        lse_ref[...] = log_ref[...].T[0 : lse_ref.shape[0], :]


def middle_kernel(
    kinds, ao_ref, wo_ref, tok_ref, small_ref, prev_ref, routes_ref, target_ref,
    resid_ref, scal_ref, send_ref, ffn_ref, first_ref, second_ref,
):
    tokens, width = tok_ref.shape
    gain = small_ref[...].astype(F32).T[kinds + 7 : kinds + 8, :]

    @pl.loop(0, tokens // BLOCK)
    def _(block):
        rows = pl.ds(pl.multiple_of(block * BLOCK, BLOCK), BLOCK)
        resid = tok_ref[rows, :].astype(F32) + nn(ao_ref[rows, :], wo_ref[...])
        resid_ref[rows, :] = resid
        inverse = inverse_rms(resid)
        low = (resid * inverse * gain).astype(BF16)
        ffn_ref[rows, :] = low
        logits = nn(low, small_ref[...]) + prev_ref[rows, :]
        lane = iota(logits.shape, 1)

        def pick(index):
            return jnp.sum(jnp.where(lane == index, logits, 0.0), axis=1, keepdims=True)

        def pair(left, right):
            top = jnp.maximum(left, right)
            left = jnp.exp(left - top)
            right = jnp.exp(right - top)
            total = left + right
            return left / total, right / total

        gates = pair(pick(routes_ref[rows, 0:1]), pick(routes_ref[rows, 1:2]))
        one = pair(pick(kinds), pick(kinds + 1))
        two = pair(pick(kinds + 2), pick(kinds + 3))
        scal = jnp.zeros_like(logits)
        for index, value in enumerate(gates + one + two + (inverse,)):
            scal = jnp.where(lane == index, value, scal)
        scal_ref[rows, :] = scal
        for gate, ref in zip(gates, (first_ref, second_ref)):
            high, rest = split_low(gate)
            ref[rows, :] = jnp.where(
                lane == 0, high.astype(F32), jnp.where(lane == 1, rest.astype(F32), 0.0)
            ).astype(BF16)

    @pl.loop(0, send_ref.shape[0])
    def _(expert):
        slots = iota((CAP, tokens), 0) + expert * CAP
        hot_one = (target_ref[0:1, :] == slots).astype(F32)
        hot_two = (target_ref[1:2, :] == slots).astype(F32)
        send_ref[expert, :, 0:width] = nn((hot_one + hot_two).astype(BF16), ffn_ref[...]).astype(
            BF16
        )
        send_ref[expert, :, width:] = (
            nn(hot_one.astype(BF16), first_ref[...]) + nn(hot_two.astype(BF16), second_ref[...])
        ).astype(BF16)


def expert_kernel(
    recv_ref, cot_ref, wg_ref, wu_ref, wo_ref, front_ref, ret_ref, out_acc, row_acc,
):
    step = pl.program_id(0)
    total, width = out_acc.shape
    tile = 512

    @pl.when(step == 0)
    def _():
        out_acc[...] = jnp.zeros_like(out_acc)
        row_acc[...] = jnp.zeros_like(row_acc)

    @pl.loop(0, total // tile)
    def _(block):
        rows = pl.ds(pl.multiple_of(block * tile, tile), tile)
        token = recv_ref[rows, 0:width]
        extra = recv_ref[rows, width:].astype(F32)
        gate_weight = extra[:, 0:1] + extra[:, 1:2]
        gate = nn(token, wg_ref[...])
        up = nn(token, wu_ref[...])
        grad = nt(cot_ref[rows, :], wo_ref[...]) * gate_weight
        sig = jax.nn.sigmoid(gate)
        act = gate * sig
        hidden = act * up
        out_acc[rows, :] += nn(hidden.astype(BF16), wo_ref[...])
        front_ref[2, rows, :] = (hidden * gate_weight).astype(BF16)
        gate_grad = (grad * up * sig * (1.0 + gate * (1.0 - sig))).astype(BF16)
        up_grad = (grad * act).astype(BF16)
        front_ref[0, rows, :] = gate_grad
        front_ref[1, rows, :] = up_grad
        row_acc[rows, :] += nt(gate_grad, wg_ref[...]) + nt(up_grad, wu_ref[...])

    @pl.when(step == pl.num_programs(0) - 1)
    def _():
        @pl.loop(0, total // CAP)
        def _(peer):
            rows = pl.ds(pl.multiple_of(peer * CAP, CAP), CAP)
            ret_ref[peer, 0:CAP, :] = out_acc[rows, :].astype(BF16)
            ret_ref[peer, CAP:, :] = row_acc[rows, :].astype(BF16)


def expert_grad_kernel(recv_ref, cot_ref, front_ref, gate_ref, up_ref, wout_ref, turned_ref):
    step = pl.program_id(0)
    width = turned_ref.shape[0]

    @pl.when(step == 0)
    def _():
        turned_ref[...] = recv_ref[:, 0:width].T

    wout_ref[...] = tn(front_ref[2], cot_ref[...]).astype(BF16)
    gate_ref[...] = nn(turned_ref[...], front_ref[0]).astype(BF16)
    up_ref[...] = nn(turned_ref[...], front_ref[1]).astype(BF16)


def combine_kernel(
    kinds, experts, ret_ref, target_ref, routes_ref, scal_ref, resid_ref, cot_ref, ao_ref,
    small_ref, wo_ref, mix_ref, prevt_ref, ind_ref,
    mixed_ref, prev_ref, mid_ref, proj_ref, attn_ref, delta_ref, minor_ref, vec_ref, gain_ref,
    gmix_ref, rows_ref,
):
    step = pl.program_id(0)

    @pl.when(step == 0)
    def _():
        rows_ref[...] = small_ref[...].astype(F32).T
        minor_ref[...] = jnp.zeros_like(minor_ref)
        vec_ref[...] = jnp.zeros_like(vec_ref)
        gain_ref[...] = jnp.zeros_like(gain_ref)
        gmix_ref[...] = jnp.zeros_like(gmix_ref)

    width = resid_ref.shape[1]
    slots = experts * CAP
    resid = resid_ref[...]
    cot = cot_ref[...]
    upstream = cot.astype(F32)
    scal = scal_ref[...]
    routes = (routes_ref[:, 0:1], routes_ref[:, 1:2])
    targets = (target_ref[:, 0:1], target_ref[:, 1:2])
    gates = (scal[:, 0:1], scal[:, 1:2])
    one_keep, one_vec = scal[:, 2:3], scal[:, 3:4]
    two_keep, two_vec = scal[:, 4:5], scal[:, 5:6]
    inverse = scal[:, 6:7]
    gain = rows_ref[kinds + 7 : kinds + 8, :]
    vec_one = rows_ref[kinds + 4 : kinds + 5, :]
    vec_two = rows_ref[kinds + 5 : kinds + 6, :]
    normed = resid * inverse
    ffn_norm = normed * gain
    low = ffn_norm.astype(BF16)
    slot_ids = iota((BLOCK, slots), 1)
    hots = [(target == slot_ids).astype(F32) for target in targets]
    outs = ret_ref[:, 0:CAP, :].reshape(slots, width)
    backs = ret_ref[:, CAP:, :].reshape(slots, width)
    branches = [nn(hot.astype(BF16), outs) for hot in hots]
    back = nn((hots[0] + hots[1]).astype(BF16), backs)

    def weight(kind):
        return sum(
            jnp.where(route == kind, gate, 0.0) for route, gate in zip(routes, gates)
        )

    weight_copy = weight(experts + 1)
    weight_one = weight(experts + 2)
    weight_two = weight(experts + 3)
    keep = weight_copy + weight_one * one_keep + weight_two * two_keep
    mixed_ref[...] = (
        resid
        + gates[0] * branches[0]
        + gates[1] * branches[1]
        + keep * ffn_norm
        + (weight_one * one_vec) * vec_one
        + (weight_two * two_vec) * vec_two
    ).astype(BF16)
    dot_norm = jnp.sum(upstream * ffn_norm, axis=1, keepdims=True)
    dot_one = jnp.sum(upstream * vec_one, axis=1, keepdims=True)
    dot_two = jnp.sum(upstream * vec_two, axis=1, keepdims=True)
    grads = []
    for route, branch in zip(routes, branches):
        grads.append(
            jnp.sum(branch * upstream, axis=1, keepdims=True)
            + jnp.where(route == experts + 1, dot_norm, 0.0)
            + jnp.where(route == experts + 2, one_keep * dot_norm + one_vec * dot_one, 0.0)
            + jnp.where(route == experts + 3, two_keep * dot_norm + two_vec * dot_two, 0.0)
        )
    mean_grad = gates[0] * grads[0] + gates[1] * grads[1]
    lane = iota((BLOCK, LANES), 1)
    wide = jnp.zeros((BLOCK, LANES), F32)
    for route, gate, grad in zip(routes, gates, grads):
        wide = jnp.where(lane == route, gate * (grad - mean_grad), wide)
    for index, keep_part, vec_part, grad_weight, dot in (
        (kinds, one_keep, one_vec, weight_one, dot_one),
        (kinds + 2, two_keep, two_vec, weight_two, dot_two),
    ):
        keep_grad = grad_weight * dot_norm
        vec_grad = grad_weight * dot
        both = keep_part * keep_grad + vec_part * vec_grad
        wide = jnp.where(lane == index, keep_part * (keep_grad - both), wide)
        wide = jnp.where(lane == index + 1, vec_part * (vec_grad - both), wide)
    wide_low = wide.astype(BF16)
    wide_back = wide_low.astype(F32)
    minor_ref[...] += nn(wide_back.T.astype(BF16), low)
    share = jnp.where(lane == 0, weight_one * one_vec, 0.0)
    share = jnp.where(lane == 1, weight_two * two_vec, share)
    high, rest = split_low(share.T)
    vec_ref[...] += nn(high, cot) + nn(rest, cot)
    prev_ref[...] = nn(wide_low, mix_ref[...])[:, 0:kinds]
    gmix_ref[...] += jnp.dot(
        prevt_ref[...], wide_back, precision=HIGHEST_PRECISION, preferred_element_type=F32
    )
    grad_two = back + nt(wide_low, small_ref[...]) + keep * upstream
    gain_ref[...] += jnp.sum(grad_two * normed, axis=0, keepdims=True)
    mid = upstream + norm_back(grad_two * gain, normed, inverse)
    mid_ref[...] = mid
    proj = mid.astype(BF16)
    proj_ref[...] = proj
    attn = nt(proj, wo_ref[...]).astype(BF16)
    attn_ref[...] = attn
    high, rest = split_low(attn.astype(F32) * ao_ref[...].astype(F32))
    delta_ref[...] = nt(ind_ref[...], high) + nt(ind_ref[...], rest)


def attend_back_kernel(
    gain_row, qkv_ref, grad_ref, lse_ref, delta_ref, cos_ref, sin_ref, segc_ref, segr_ref,
    wq_ref, wk_ref, wv_ref, attn_in_ref, ao_ref, proj_ref, tok_ref, mid_ref, small_ref,
    weight_ref, gtok_ref, gain_ref, dq_ref, dk_ref, dv_ref, bias_ref, in_t_ref, ao_t_ref, acc_ref,
):
    step = pl.program_id(0)
    tokens = tok_ref.shape[0]
    blocks = tokens // BLOCK
    reach = DOC_MAX // BLOCK

    @pl.when(step == 0)
    def _():
        in_t_ref[...] = attn_in_ref[...].T
        ao_t_ref[...] = ao_ref[...].T
        acc_ref[...] = jnp.zeros_like(acc_ref)

    dq_ref[...] = jnp.zeros_like(dq_ref)
    for block in range(blocks):
        first = block * BLOCK
        last = min(blocks, block + reach + 1) * BLOCK
        span = last - first
        keys = slice(first, first + BLOCK)
        key_ids = iota((BLOCK, span), 0) + first
        row_ids = iota((BLOCK, span), 1) + first
        seen = (key_ids <= row_ids) & (segc_ref[keys, :] == segr_ref[0:1, first:last])
        bias_ref[:, 0:span] = jnp.where(seen, 0.0, NEGATIVE)
        key = qkv_ref[1, keys, :]
        value = qkv_ref[2, keys, :]
        key_grad = None
        for head in range(GROUP):
            mask = head_mask(head)
            index = step * GROUP + head
            query = qkv_ref[0, first:last, :] * mask
            upstream = grad_ref[first:last, :] * mask
            scores = nt(key, query) + bias_ref[:, 0:span]
            probs = jnp.exp(scores - lse_ref[pl.ds(index, 1), first:last])
            prob_grad = nt(value, upstream)
            score_grad = (probs * (prob_grad - delta_ref[pl.ds(index, 1), first:last])).astype(BF16)
            dv = nn(probs.astype(BF16), upstream)
            dk = nn(score_grad, query)
            dq_ref[first:last, :] += tn(score_grad, key * mask)
            key_grad = dk if key_grad is None else key_grad + dk
            value_grad = dv if head == 0 else value_grad + dv
        dk_ref[keys, :] = key_grad
        dv_ref[keys, :] = value_grad.astype(BF16)

    @pl.loop(0, blocks)
    def _(block):
        rows = pl.ds(pl.multiple_of(block * BLOCK, BLOCK), BLOCK)
        cosines = cos_ref[rows, :]
        sines = -sin_ref[rows, :]
        dq = turn(dq_ref[rows, :] * HEAD_DIM**-0.5, cosines, sines)
        dk = turn(dk_ref[rows, :], cosines, sines)
        dq_ref[rows, :] = dq
        dk_ref[rows, :] = dk
        acc_ref[rows, :] += (
            nt(dq.astype(BF16), wq_ref[...])
            + nt(dk.astype(BF16), wk_ref[...])
            + nt(dv_ref[rows, :], wv_ref[...])
        )

    halves = GROUP_LANES // LANES
    for index, (turned, grads) in enumerate(
        ((in_t_ref, dq_ref), (in_t_ref, dk_ref), (in_t_ref, dv_ref), (ao_t_ref, proj_ref))
    ):
        product = nn(turned[...], grads[...].astype(BF16)).astype(BF16)
        for half in range(halves):
            weight_ref[index * halves + half] = product[:, half * LANES : (half + 1) * LANES]

    @pl.when(step == pl.num_programs(0) - 1)
    def _():
        gain = small_ref[...].astype(F32).T[gain_row : gain_row + 1, :]
        gain_ref[...] = jnp.zeros_like(gain_ref)

        @pl.loop(0, blocks)
        def _(block):
            rows = pl.ds(pl.multiple_of(block * BLOCK, BLOCK), BLOCK)
            values = tok_ref[rows, :].astype(F32)
            inverse = inverse_rms(values)
            normed = values * inverse
            grad = acc_ref[rows, :]
            gain_ref[...] += jnp.sum(grad * normed, axis=0, keepdims=True)
            gtok_ref[rows, :] = mid_ref[rows, :] + norm_back(grad * gain, normed, inverse)


def take(values, index, axis=0):
    index = jnp.clip(index, 0, values.shape[axis] - 1)
    return lax.dynamic_index_in_dim(values, index, axis, keepdims=False)


def add_low(left, right):
    return (left.astype(F32) + right.astype(F32)).astype(BF16)


def split_parts(values):
    return values.reshape(4, 2, values.shape[0] // 8, *values.shape[1:])


def cross(values):
    here = lax.axis_index("dp") % 2
    sent = lax.ppermute(take(values, 1 - here, 1), "dp", [(d, d ^ 1) for d in range(8)])
    return take(values, here, 1), sent


def meet(pair):
    return add_low(*pair)


def line_sum(kept):
    here = lax.axis_index("dp") // 2
    rising = falling = None
    for step in range(1, 4):
        up = take(kept, 4 - step + here)
        down = take(kept, here + step - 4)
        if rising is not None:
            up = add_low(up, rising)
            down = add_low(down, falling)
        spots = [(z, x) for z in range(step) for x in range(2)]
        rising = lax.ppermute(up, "dp", [(2 * z + x, 2 * z + 2 + x) for z, x in spots])
        falling = lax.ppermute(down, "dp", [(6 - 2 * z + x, 4 - 2 * z + x) for z, x in spots])
    return take(kept, here).astype(F32) + rising.astype(F32) + falling.astype(F32)


def fold(values, bit):
    side = lax.axis_index("expert") // bit % 2
    both = values.reshape(2, values.shape[0] // 2, *values.shape[1:])
    sent = lax.ppermute(take(both, 1 - side), "expert", [(e, e ^ bit) for e in range(4)])
    return add_low(take(both, side), sent)


def unfold(values, bit):
    side = lax.axis_index("expert") // bit % 2
    other = lax.ppermute(values, "expert", [(e, e ^ bit) for e in range(4)])
    first = jnp.where(side == 0, values, other)
    second = jnp.where(side == 0, other, values)
    return jnp.concatenate([first, second], axis=0)


def per_device(
    tokens, prev_scores, segments, routes, wqkv, wo, router, const_gate, const_vec, gain1, gain2,
    gate_mix, w_in, w_out, cotangent,
):
    tok_count, width = tokens.shape
    kinds = router.shape[1]
    experts = w_in.shape[0] * lax.axis_size("expert")
    ff = w_out.shape[1]
    qkv_cols = wqkv.shape[1]
    parts = lax.axis_size("dp")
    by_hand = parts == 8 and experts == 4
    small = jnp.concatenate(
        [router, const_gate, const_vec, gain1[:, None], gain2[:, None]], axis=1
    )
    packed = jnp.concatenate(
        [wqkv, wo, jnp.pad(small, ((0, 0), (0, LANES - small.shape[1])))], axis=1
    )
    whole = lax.all_gather(packed, "dp", axis=0, tiled=True)

    seq_len = segments.shape[1]
    positions = (jnp.arange(tok_count, dtype=jnp.int32) % seq_len).astype(F32)
    half = HEAD_DIM // 2
    frequency = 10000.0 ** (-jnp.arange(half).astype(F32) / half)
    angles = positions[:, None] * frequency[None, :]
    cosines = jnp.tile(jnp.cos(angles), (1, LANES // half))
    sines = jnp.tile(jnp.sin(angles), (1, LANES // half))
    signs = jnp.where(jnp.arange(LANES) % HEAD_DIM < half, -1.0, 1.0).astype(F32)
    sines = sines * signs[None, :]
    seg_col = segments.reshape(tok_count, 1)
    seg_row = segments.reshape(1, tok_count)

    names = jnp.arange(kinds, dtype=jnp.int32)
    hot = [routes[:, i : i + 1] == names[None, :] for i in range(2)]
    named = (hot[0] | hot[1]).astype(BF16)
    ids = jnp.arange(tok_count, dtype=jnp.int32)
    before = (ids[:, None] > ids[None, :]).astype(BF16)
    earlier = jnp.dot(before, named, preferred_element_type=F32)
    slots = [jnp.sum(jnp.where(h, earlier, 0.0), axis=1).astype(jnp.int32) for h in hot]
    targets = [
        jnp.where(routes[:, i] < experts, routes[:, i] * CAP + slots[i], experts * CAP)
        for i in range(2)
    ]
    target_row = jnp.stack(targets, axis=0)
    target_col = jnp.stack(targets, axis=1)
    prev_mix = jnp.dot(prev_scores, gate_mix.astype(F32), precision=HIGHEST_PRECISION)
    prev_mix = jnp.pad(prev_mix, ((0, 0), (0, LANES - kinds)))

    def swap(values):
        return lax.all_to_all(values, "expert", split_axis=0, concat_axis=0, tiled=True)

    cot_send = pl.pallas_call(
        functools.partial(send_cotangent_kernel, experts),
        out_shape=jax.ShapeDtypeStruct((experts, CAP, width), BF16),
        compiler_params=params(),
        cost_estimate=cost(2 * experts * CAP * tok_count * width, 4 * tok_count * width),
        name="send_cotangent",
    )(cotangent, target_row)
    cot_rows = swap(cot_send).reshape(experts * CAP, width)

    groups = HEADS // GROUP
    tiles = qkv_cols // 3 // GROUP_LANES
    weight_specs = [
        pl.BlockSpec((width, GROUP_LANES), functools.partial(lambda o, i: (0, o + i), part * tiles))
        for part in range(3)
    ]
    small_spec = pl.BlockSpec((width, LANES), lambda *_: (0, (qkv_cols + width) // LANES))
    wo_spec = pl.BlockSpec((width, width), lambda *_: (0, qkv_cols // width))
    table = whole_block((tok_count, LANES))
    full = whole_block((tok_count, width))
    group_spec = pl.BlockSpec((tok_count, GROUP_LANES), lambda i: (0, i))
    qkv_spec = pl.BlockSpec((3, tok_count, GROUP_LANES), lambda i: (0, 0, i))
    seg_specs = [whole_block((tok_count, 1)), whole_block((1, tok_count))]
    span = DOC_MAX + BLOCK
    head_rows = 16
    lse_spec = whole_block((head_rows, tok_count))
    qkv, attn_in, attn_out, lse = pl.pallas_call(
        functools.partial(attend_kernel, kinds + 6),
        grid=(groups,),
        in_specs=[full, *weight_specs, small_spec, table, table, *seg_specs],
        out_specs=[qkv_spec, full, group_spec, lse_spec],
        out_shape=[
            jax.ShapeDtypeStruct((3, tok_count, width), BF16),
            jax.ShapeDtypeStruct((tok_count, width), BF16),
            jax.ShapeDtypeStruct((tok_count, width), BF16),
            jax.ShapeDtypeStruct((head_rows, tok_count), F32),
        ],
        scratch_shapes=[
            pltpu.VMEM((1, width), F32),
            pltpu.VMEM((BLOCK, span), F32),
            pltpu.VMEM((tok_count, LANES), F32),
        ],
        compiler_params=params(),
        cost_estimate=cost(12e9, 16e6),
        name="attend",
    )(tokens, whole, whole, whole, whole, cosines, sines, seg_col, seg_row)

    payload = width + LANES
    resid_mid, scal, send = pl.pallas_call(
        functools.partial(middle_kernel, kinds),
        grid=(1,),
        in_specs=[
            full, wo_spec, full, small_spec, table, whole_block((tok_count, 2)),
            whole_block((2, tok_count)),
        ],
        out_specs=[full, table, whole_block((experts, CAP, payload))],
        out_shape=[
            jax.ShapeDtypeStruct((tok_count, width), F32),
            jax.ShapeDtypeStruct((tok_count, LANES), F32),
            jax.ShapeDtypeStruct((experts, CAP, payload), BF16),
        ],
        scratch_shapes=[
            pltpu.VMEM((tok_count, width), BF16),
            pltpu.VMEM((tok_count, LANES), BF16),
            pltpu.VMEM((tok_count, LANES), BF16),
        ],
        compiler_params=params(),
        cost_estimate=cost(3.5e9, 10e6),
        name="middle",
    )(attn_out, whole, tokens, whole, prev_mix, routes, target_row)
    recv = swap(send).reshape(experts * CAP, payload)

    slot_count = experts * CAP
    ff_tile = 256
    ff_tiles = ff // ff_tile
    w_in_one = w_in.reshape(width, 2 * ff)
    w_out_one = w_out.reshape(ff, width)
    slot_full = whole_block((slot_count, width))
    recv_full = whole_block((slot_count, payload))
    front_spec = pl.BlockSpec((3, slot_count, ff_tile), lambda j: (0, 0, j))
    front, ret = pl.pallas_call(
        expert_kernel,
        grid=(ff_tiles,),
        in_specs=[
            recv_full,
            slot_full,
            pl.BlockSpec((width, ff_tile), lambda j: (0, j)),
            pl.BlockSpec((width, ff_tile), lambda j: (0, ff_tiles + j)),
            pl.BlockSpec((ff_tile, width), lambda j: (j, 0)),
        ],
        out_specs=[front_spec, whole_block((experts, 2 * CAP, width))],
        out_shape=[
            jax.ShapeDtypeStruct((3, slot_count, ff), BF16),
            jax.ShapeDtypeStruct((experts, 2 * CAP, width), BF16),
        ],
        scratch_shapes=[pltpu.VMEM((slot_count, width), F32)] * 2,
        compiler_params=params(),
        cost_estimate=cost(12 * slot_count * width * ff, 26e6),
        name="expert",
    )(recv, cot_rows, w_in_one, w_in_one, w_out_one)
    returned = swap(ret)
    expert_grads = pl.pallas_call(
        expert_grad_kernel,
        grid=(ff_tiles,),
        in_specs=[recv_full, slot_full, front_spec],
        out_specs=[
            pl.BlockSpec((width, ff_tile), lambda j: (0, j)),
            pl.BlockSpec((width, ff_tile), lambda j: (0, j)),
            pl.BlockSpec((ff_tile, width), lambda j: (j, 0)),
        ],
        out_shape=[
            jax.ShapeDtypeStruct((width, ff), BF16),
            jax.ShapeDtypeStruct((width, ff), BF16),
            jax.ShapeDtypeStruct((ff, width), BF16),
        ],
        scratch_shapes=[pltpu.VMEM((width, slot_count), BF16)],
        compiler_params=params(),
        cost_estimate=cost(6 * slot_count * width * ff, 24e6),
        name="expert_grad",
    )(recv, cot_rows, front)
    returned, *expert_grads = lax.optimization_barrier((returned, *expert_grads))
    crossed = [cross(split_parts(grad)) for grad in expert_grads] if by_hand else None

    mix_turned = jnp.pad(gate_mix.T, ((0, LANES - kinds), (0, LANES - kinds)))
    indicator = (
        jnp.arange(width)[None, :] // HEAD_DIM == jnp.arange(head_rows)[:, None]
    ).astype(BF16)
    token_block = pl.BlockSpec((BLOCK, width), lambda i: (i, 0))
    table_block = pl.BlockSpec((BLOCK, LANES), lambda i: (i, 0))
    two_block = pl.BlockSpec((BLOCK, 2), lambda i: (i, 0))
    (
        mixed, grad_prev, mid_grad, proj_grad, attn_grad, delta, minor, vec, gain2_row, grad_mix,
    ) = pl.pallas_call(
        functools.partial(combine_kernel, kinds, experts),
        grid=(tok_count // BLOCK,),
        in_specs=[
            whole_block((experts, 2 * CAP, width)), two_block, two_block, table_block,
            token_block, token_block, token_block, small_spec, wo_spec,
            whole_block((LANES, LANES)),
            pl.BlockSpec((kinds, BLOCK), lambda i: (0, i)),
            whole_block((head_rows, width)),
        ],
        out_specs=[
            token_block, pl.BlockSpec((BLOCK, kinds), lambda i: (i, 0)), token_block, token_block,
            token_block, pl.BlockSpec((head_rows, BLOCK), lambda i: (0, i)),
            whole_block((LANES, width)), whole_block((LANES, width)), whole_block((1, width)),
            whole_block((kinds, LANES)),
        ],
        out_shape=[
            jax.ShapeDtypeStruct((tok_count, width), BF16),
            jax.ShapeDtypeStruct((tok_count, kinds), F32),
            jax.ShapeDtypeStruct((tok_count, width), F32),
            jax.ShapeDtypeStruct((tok_count, width), BF16),
            jax.ShapeDtypeStruct((tok_count, width), BF16),
            jax.ShapeDtypeStruct((head_rows, tok_count), F32),
            jax.ShapeDtypeStruct((LANES, width), F32),
            jax.ShapeDtypeStruct((LANES, width), F32),
            jax.ShapeDtypeStruct((1, width), F32),
            jax.ShapeDtypeStruct((kinds, LANES), F32),
        ],
        scratch_shapes=[pltpu.VMEM((LANES, width), F32)],
        compiler_params=params(),
        cost_estimate=cost(7e9, 20e6),
        name="combine",
    )(
        returned, target_col, routes, scal, resid_mid, cotangent, attn_out, whole, whole,
        mix_turned, prev_scores.T, indicator,
    )

    halves = GROUP_LANES // LANES
    weights, grad_tokens, gain1_row = pl.pallas_call(
        functools.partial(attend_back_kernel, kinds + 6),
        grid=(groups,),
        in_specs=[
            qkv_spec, group_spec, lse_spec, lse_spec, table, table, *seg_specs, *weight_specs,
            full, full, group_spec, full, full, small_spec,
        ],
        out_specs=[
            pl.BlockSpec((4 * halves, width, LANES), lambda i: (i, 0, 0)), full,
            whole_block((1, width)),
        ],
        out_shape=[
            jax.ShapeDtypeStruct((4 * halves * groups, width, LANES), BF16),
            jax.ShapeDtypeStruct((tok_count, width), F32),
            jax.ShapeDtypeStruct((1, width), F32),
        ],
        scratch_shapes=[
            pltpu.VMEM((tok_count, GROUP_LANES), F32),
            pltpu.VMEM((tok_count, GROUP_LANES), F32),
            pltpu.VMEM((tok_count, GROUP_LANES), BF16),
            pltpu.VMEM((BLOCK, span), F32),
            pltpu.VMEM((width, tok_count), BF16),
            pltpu.VMEM((width, tok_count), BF16),
            pltpu.VMEM((tok_count, width), F32),
        ],
        compiler_params=params(),
        cost_estimate=cost(28e9, 25e6),
        name="attend_back",
    )(
        qkv, attn_grad, lse, delta, cosines, sines, seg_col, seg_row, whole, whole, whole,
        attn_in, attn_out, proj_grad, tokens, mid_grad, whole,
    )

    minor_rows = jnp.concatenate([minor[: kinds + 4], vec[:2], gain1_row, gain2_row], axis=0)
    minor_all = jnp.concatenate(
        [minor_rows, jnp.pad(grad_mix[:, :kinds], ((0, 0), (0, width - kinds)))], axis=0
    )
    rows = width // parts
    if by_hand:
        crossed, weights = lax.optimization_barrier((crossed, weights))
        kept = [meet(halves_of) for halves_of in crossed]
        shares = [line_sum(part) for part in kept]
        weight_part = fold(weights, 1)
        weight_part = fold(weight_part, 2)
        weight_part = weight_part.reshape(-1, parts, rows, LANES).transpose(1, 0, 2, 3)
        weight_part = line_sum(meet(cross(weight_part.reshape(4, 2, -1, rows, LANES))))
        weight_sum = unfold(unfold(weight_part.astype(BF16), 2), 1)
        for bit in (1, 2, 4):
            minor_all += lax.ppermute(minor_all, "dp", [(d, d ^ bit) for d in range(8)])
        for bit in (1, 2):
            minor_all += lax.ppermute(minor_all, "expert", [(e, e ^ bit) for e in range(4)])
    else:
        shares = [
            lax.psum_scatter(grad, "dp", scatter_dimension=0, tiled=True).astype(F32)
            for grad in expert_grads
        ]
        weight_part = lax.psum_scatter(weights, "expert", scatter_dimension=0, tiled=True)
        weight_part = lax.psum_scatter(weight_part, "dp", scatter_dimension=1, tiled=True)
        weight_sum = lax.all_gather(weight_part, "expert", axis=0, tiled=True)
        minor_all = lax.psum(minor_all, ("dp", "expert"))
    grad_gate_mix = minor_all[kinds + 8 :, :kinds]
    minor_sum = lax.dynamic_slice_in_dim(
        minor_all[: kinds + 8], lax.axis_index("dp") * rows, rows, 1
    ).T
    weight_sum = weight_sum.reshape(groups, 4, -1, rows, LANES)
    weight_sum = weight_sum.transpose(3, 1, 0, 2, 4).reshape(rows, 4 * width).astype(F32)
    return (
        mixed,
        grad_tokens,
        grad_prev,
        weight_sum[:, :qkv_cols],
        weight_sum[:, qkv_cols:],
        minor_sum[:, :kinds],
        minor_sum[:, kinds : kinds + 4],
        minor_sum[:, kinds + 4 : kinds + 6],
        minor_sum[:, kinds + 6],
        minor_sum[:, kinds + 7],
        grad_gate_mix,
        jnp.concatenate([shares[0], shares[1]], axis=1)[None],
        shares[2][None],
    )


def solution(mesh):
    rows = P(("dp", "expert"), None)
    in_specs = (
        rows, rows, rows, rows,
        P("dp", None), P("dp", None), P("dp", None), P("dp", None), P("dp", None), P("dp"), P("dp"),
        P(), P("expert", None, None), P("expert", None, None), rows,
    )
    out_specs = (
        rows, rows, rows,
        P("dp", None), P("dp", None), P("dp", None), P("dp", None), P("dp", None), P("dp"), P("dp"),
        P(), P("expert", "dp", None), P("expert", "dp", None),
    )
    return jax.shard_map(
        per_device, mesh=mesh, in_specs=in_specs, out_specs=out_specs, check_vma=False
    )
```

```python
import functools

import jax
import jax.numpy as jnp
from jax import lax
from jax.experimental import pallas as pl
from jax.experimental.pallas import tpu as pltpu
from jax.sharding import PartitionSpec as P

HEADS = 12
HEAD_DIM = 64
CAP = 256
DOC_MAX = 512
NORM_EPSILON = 1e-06
HIGHEST_PRECISION = lax.Precision.HIGHEST
NEGATIVE = -1e30
F32 = jnp.float32
BF16 = jnp.bfloat16
BLOCK = 256
GROUP = 4
GROUP_LANES = GROUP * HEAD_DIM
LANES = 128
MESH = pl.DeviceIdType.MESH
VMEM_BYTES = 62 * 1024 * 1024


def nn(left, right):
    return jnp.dot(left, right, preferred_element_type=F32)


def nt(left, right):
    return lax.dot_general(left, right, (((1,), (1,)), ((), ())), preferred_element_type=F32)


def tn(left, right):
    return lax.dot_general(left, right, (((0,), (0,)), ((), ())), preferred_element_type=F32)


def iota(shape, axis):
    return lax.broadcasted_iota(jnp.int32, shape, axis)


def split_low(values):
    high = values.astype(BF16)
    return high, (values - high.astype(F32)).astype(BF16)


def inverse_rms(values):
    return lax.rsqrt(jnp.mean(values * values, axis=-1, keepdims=True) + NORM_EPSILON)


def norm_back(upstream, normed, inverse):
    return inverse * (upstream - normed * jnp.mean(upstream * normed, axis=-1, keepdims=True))


def turn(values, cosines, signed_sines):
    pieces = []
    for start in range(0, values.shape[1], LANES):
        part = values[:, start : start + LANES]
        front = iota(part.shape, 1) % HEAD_DIM < HEAD_DIM // 2
        swapped = jnp.where(
            front,
            pltpu.roll(part, LANES - HEAD_DIM // 2, 1),
            pltpu.roll(part, HEAD_DIM // 2, 1),
        )
        pieces.append(part * cosines + swapped * signed_sines)
    return jnp.concatenate(pieces, axis=1)


def head_mask(head):
    return (iota((1, GROUP_LANES), 1) // HEAD_DIM == head).astype(F32).astype(BF16)


def params(**extra):
    return pltpu.CompilerParams(vmem_limit_bytes=VMEM_BYTES, **extra)


def whole_block(shape):
    return pl.BlockSpec(shape, lambda *_: (0,) * len(shape))


def cost(flops, moved):
    return pl.CostEstimate(flops=int(flops), bytes_accessed=int(moved), transcendentals=0)


def send_cotangent_kernel(experts, cot_ref, target_ref, out_ref):
    tokens = cot_ref.shape[0]

    @pl.loop(0, experts)
    def _(expert):
        slots = iota((CAP, tokens), 0) + expert * CAP
        hot = (target_ref[0:1, :] == slots) | (target_ref[1:2, :] == slots)
        out_ref[expert] = nn(hot.astype(F32).astype(BF16), cot_ref[...]).astype(BF16)


def attend_kernel(
    gain_row, tok_ref, wq_ref, wk_ref, wv_ref, small_ref, cos_ref, sin_ref, segc_ref, segr_ref,
    qkv_ref, attn_in_ref, out_ref, lse_ref, gain_ref, bias_ref, log_ref,
):
    step = pl.program_id(0)
    tokens = tok_ref.shape[0]
    blocks = tokens // BLOCK
    reach = DOC_MAX // BLOCK

    @pl.when(step == 0)
    def _():
        gain_ref[...] = small_ref[...].astype(F32).T[gain_row : gain_row + 1, :]
        log_ref[...] = jnp.zeros_like(log_ref)

        @pl.loop(0, blocks)
        def _(block):
            rows = pl.ds(pl.multiple_of(block * BLOCK, BLOCK), BLOCK)
            values = tok_ref[rows, :].astype(F32)
            attn_in_ref[rows, :] = (values * inverse_rms(values) * gain_ref[...]).astype(BF16)

    @pl.loop(0, blocks)
    def _(block):
        rows = pl.ds(pl.multiple_of(block * BLOCK, BLOCK), BLOCK)
        normed = attn_in_ref[rows, :]
        cosines = cos_ref[rows, :]
        sines = sin_ref[rows, :]
        query = turn(nn(normed, wq_ref[...]), cosines, sines) * HEAD_DIM**-0.5
        qkv_ref[0, rows, :] = query.astype(BF16)
        qkv_ref[1, rows, :] = turn(nn(normed, wk_ref[...]), cosines, sines).astype(BF16)
        qkv_ref[2, rows, :] = nn(normed, wv_ref[...]).astype(BF16)

    for block in range(blocks):
        first = max(0, block - reach) * BLOCK
        last = (block + 1) * BLOCK
        span = last - first
        rows = slice(block * BLOCK, last)
        row_ids = iota((BLOCK, span), 0) + block * BLOCK
        col_ids = iota((BLOCK, span), 1) + first
        seen = (col_ids <= row_ids) & (segc_ref[rows, :] == segr_ref[0:1, first:last])
        bias_ref[:, 0:span] = jnp.where(seen, 0.0, NEGATIVE)
        attended = []
        logs = log_ref[rows, :]
        for head in range(GROUP):
            mask = head_mask(head)
            scores = nt(qkv_ref[0, rows, :] * mask, qkv_ref[1, first:last, :]) + bias_ref[:, 0:span]
            top = jnp.max(scores, axis=1, keepdims=True)
            weights = jnp.exp(scores - top).astype(BF16)
            value = qkv_ref[2, first:last, :] * mask + (1 - mask)
            mixed = nn(weights, value)
            own = iota(mixed.shape, 1) // HEAD_DIM == head
            total = jnp.max(jnp.where(own, 0.0, mixed), axis=1, keepdims=True)
            attended.append(jnp.where(own, mixed / total, 0.0))
            logs = jnp.where(
                iota(logs.shape, 1) == step * GROUP + head, top + jnp.log(total), logs
            )
        log_ref[rows, :] = logs
        out_ref[rows, :] = (attended[0] + attended[1] + attended[2] + attended[3]).astype(BF16)

    @pl.when(step == pl.num_programs(0) - 1)
    def _():
        lse_ref[...] = log_ref[...].T[0 : lse_ref.shape[0], :]


def middle_kernel(
    kinds, ao_ref, wo_ref, tok_ref, small_ref, prev_ref, routes_ref, target_ref,
    resid_ref, scal_ref, send_ref, ffn_ref, first_ref, second_ref,
):
    tokens, width = tok_ref.shape
    gain = small_ref[...].astype(F32).T[kinds + 7 : kinds + 8, :]

    @pl.loop(0, tokens // BLOCK)
    def _(block):
        rows = pl.ds(pl.multiple_of(block * BLOCK, BLOCK), BLOCK)
        resid = tok_ref[rows, :].astype(F32) + nn(ao_ref[rows, :], wo_ref[...])
        resid_ref[rows, :] = resid
        inverse = inverse_rms(resid)
        low = (resid * inverse * gain).astype(BF16)
        ffn_ref[rows, :] = low
        logits = nn(low, small_ref[...]) + prev_ref[rows, :]
        lane = iota(logits.shape, 1)

        def pick(index):
            return jnp.sum(jnp.where(lane == index, logits, 0.0), axis=1, keepdims=True)

        def pair(left, right):
            top = jnp.maximum(left, right)
            left = jnp.exp(left - top)
            right = jnp.exp(right - top)
            total = left + right
            return left / total, right / total

        gates = pair(pick(routes_ref[rows, 0:1]), pick(routes_ref[rows, 1:2]))
        one = pair(pick(kinds), pick(kinds + 1))
        two = pair(pick(kinds + 2), pick(kinds + 3))
        scal = jnp.zeros_like(logits)
        for index, value in enumerate(gates + one + two + (inverse,)):
            scal = jnp.where(lane == index, value, scal)
        scal_ref[rows, :] = scal
        for gate, ref in zip(gates, (first_ref, second_ref)):
            high, rest = split_low(gate)
            ref[rows, :] = jnp.where(
                lane == 0, high.astype(F32), jnp.where(lane == 1, rest.astype(F32), 0.0)
            ).astype(BF16)

    @pl.loop(0, send_ref.shape[0])
    def _(expert):
        slots = iota((CAP, tokens), 0) + expert * CAP
        hot_one = (target_ref[0:1, :] == slots).astype(F32)
        hot_two = (target_ref[1:2, :] == slots).astype(F32)
        send_ref[expert, :, 0:width] = nn((hot_one + hot_two).astype(BF16), ffn_ref[...]).astype(
            BF16
        )
        send_ref[expert, :, width:] = (
            nn(hot_one.astype(BF16), first_ref[...]) + nn(hot_two.astype(BF16), second_ref[...])
        ).astype(BF16)


def expert_kernel(
    recv_ref, cot_ref, wg_ref, wu_ref, wo_ref, front_ref, ret_ref, out_acc, row_acc,
):
    step = pl.program_id(0)
    total, width = out_acc.shape
    tile = 512

    @pl.when(step == 0)
    def _():
        out_acc[...] = jnp.zeros_like(out_acc)
        row_acc[...] = jnp.zeros_like(row_acc)

    @pl.loop(0, total // tile)
    def _(block):
        rows = pl.ds(pl.multiple_of(block * tile, tile), tile)
        token = recv_ref[rows, 0:width]
        extra = recv_ref[rows, width:].astype(F32)
        gate_weight = extra[:, 0:1] + extra[:, 1:2]
        gate = nn(token, wg_ref[...])
        up = nn(token, wu_ref[...])
        grad = nt(cot_ref[rows, :], wo_ref[...]) * gate_weight
        sig = jax.nn.sigmoid(gate)
        act = gate * sig
        hidden = act * up
        out_acc[rows, :] += nn(hidden.astype(BF16), wo_ref[...])
        front_ref[2, rows, :] = (hidden * gate_weight).astype(BF16)
        gate_grad = (grad * up * sig * (1.0 + gate * (1.0 - sig))).astype(BF16)
        up_grad = (grad * act).astype(BF16)
        front_ref[0, rows, :] = gate_grad
        front_ref[1, rows, :] = up_grad
        row_acc[rows, :] += nt(gate_grad, wg_ref[...]) + nt(up_grad, wu_ref[...])

    @pl.when(step == pl.num_programs(0) - 1)
    def _():
        @pl.loop(0, total // CAP)
        def _(peer):
            rows = pl.ds(pl.multiple_of(peer * CAP, CAP), CAP)
            ret_ref[peer, 0:CAP, :] = out_acc[rows, :].astype(BF16)
            ret_ref[peer, CAP:, :] = row_acc[rows, :].astype(BF16)


def expert_grad_kernel(recv_ref, cot_ref, front_ref, gate_ref, up_ref, wout_ref, turned_ref):
    step = pl.program_id(0)
    width = turned_ref.shape[0]

    @pl.when(step == 0)
    def _():
        turned_ref[...] = recv_ref[:, 0:width].T

    wout_ref[...] = tn(front_ref[2], cot_ref[...]).astype(BF16)
    gate_ref[...] = nn(turned_ref[...], front_ref[0]).astype(BF16)
    up_ref[...] = nn(turned_ref[...], front_ref[1]).astype(BF16)


def combine_kernel(
    kinds, experts, ret_ref, target_ref, routes_ref, scal_ref, resid_ref, cot_ref, ao_ref,
    small_ref, wo_ref, mix_ref, prevt_ref, ind_ref,
    mixed_ref, prev_ref, mid_ref, proj_ref, attn_ref, delta_ref, minor_ref, vec_ref, gain_ref,
    gmix_ref, rows_ref,
):
    step = pl.program_id(0)

    @pl.when(step == 0)
    def _():
        rows_ref[...] = small_ref[...].astype(F32).T
        minor_ref[...] = jnp.zeros_like(minor_ref)
        vec_ref[...] = jnp.zeros_like(vec_ref)
        gain_ref[...] = jnp.zeros_like(gain_ref)
        gmix_ref[...] = jnp.zeros_like(gmix_ref)

    width = resid_ref.shape[1]
    slots = experts * CAP
    resid = resid_ref[...]
    cot = cot_ref[...]
    upstream = cot.astype(F32)
    scal = scal_ref[...]
    routes = (routes_ref[:, 0:1], routes_ref[:, 1:2])
    targets = (target_ref[:, 0:1], target_ref[:, 1:2])
    gates = (scal[:, 0:1], scal[:, 1:2])
    one_keep, one_vec = scal[:, 2:3], scal[:, 3:4]
    two_keep, two_vec = scal[:, 4:5], scal[:, 5:6]
    inverse = scal[:, 6:7]
    gain = rows_ref[kinds + 7 : kinds + 8, :]
    vec_one = rows_ref[kinds + 4 : kinds + 5, :]
    vec_two = rows_ref[kinds + 5 : kinds + 6, :]
    normed = resid * inverse
    ffn_norm = normed * gain
    low = ffn_norm.astype(BF16)
    slot_ids = iota((BLOCK, slots), 1)
    hots = [(target == slot_ids).astype(F32) for target in targets]
    outs = ret_ref[:, 0:CAP, :].reshape(slots, width)
    backs = ret_ref[:, CAP:, :].reshape(slots, width)
    branches = [nn(hot.astype(BF16), outs) for hot in hots]
    back = nn((hots[0] + hots[1]).astype(BF16), backs)

    def weight(kind):
        return sum(
            jnp.where(route == kind, gate, 0.0) for route, gate in zip(routes, gates)
        )

    weight_copy = weight(experts + 1)
    weight_one = weight(experts + 2)
    weight_two = weight(experts + 3)
    keep = weight_copy + weight_one * one_keep + weight_two * two_keep
    mixed_ref[...] = (
        resid
        + gates[0] * branches[0]
        + gates[1] * branches[1]
        + keep * ffn_norm
        + (weight_one * one_vec) * vec_one
        + (weight_two * two_vec) * vec_two
    ).astype(BF16)
    dot_norm = jnp.sum(upstream * ffn_norm, axis=1, keepdims=True)
    dot_one = jnp.sum(upstream * vec_one, axis=1, keepdims=True)
    dot_two = jnp.sum(upstream * vec_two, axis=1, keepdims=True)
    grads = []
    for route, branch in zip(routes, branches):
        grads.append(
            jnp.sum(branch * upstream, axis=1, keepdims=True)
            + jnp.where(route == experts + 1, dot_norm, 0.0)
            + jnp.where(route == experts + 2, one_keep * dot_norm + one_vec * dot_one, 0.0)
            + jnp.where(route == experts + 3, two_keep * dot_norm + two_vec * dot_two, 0.0)
        )
    mean_grad = gates[0] * grads[0] + gates[1] * grads[1]
    lane = iota((BLOCK, LANES), 1)
    wide = jnp.zeros((BLOCK, LANES), F32)
    for route, gate, grad in zip(routes, gates, grads):
        wide = jnp.where(lane == route, gate * (grad - mean_grad), wide)
    for index, keep_part, vec_part, grad_weight, dot in (
        (kinds, one_keep, one_vec, weight_one, dot_one),
        (kinds + 2, two_keep, two_vec, weight_two, dot_two),
    ):
        keep_grad = grad_weight * dot_norm
        vec_grad = grad_weight * dot
        both = keep_part * keep_grad + vec_part * vec_grad
        wide = jnp.where(lane == index, keep_part * (keep_grad - both), wide)
        wide = jnp.where(lane == index + 1, vec_part * (vec_grad - both), wide)
    wide_low = wide.astype(BF16)
    wide_back = wide_low.astype(F32)
    minor_ref[...] += nn(wide_back.T.astype(BF16), low)
    share = jnp.where(lane == 0, weight_one * one_vec, 0.0)
    share = jnp.where(lane == 1, weight_two * two_vec, share)
    high, rest = split_low(share.T)
    vec_ref[...] += nn(high, cot) + nn(rest, cot)
    prev_ref[...] = nn(wide_low, mix_ref[...])[:, 0:kinds]
    gmix_ref[...] += jnp.dot(
        prevt_ref[...], wide_back, precision=HIGHEST_PRECISION, preferred_element_type=F32
    )
    grad_two = back + nt(wide_low, small_ref[...]) + keep * upstream
    gain_ref[...] += jnp.sum(grad_two * normed, axis=0, keepdims=True)
    mid = upstream + norm_back(grad_two * gain, normed, inverse)
    mid_ref[...] = mid
    proj = mid.astype(BF16)
    proj_ref[...] = proj
    attn = nt(proj, wo_ref[...]).astype(BF16)
    attn_ref[...] = attn
    high, rest = split_low(attn.astype(F32) * ao_ref[...].astype(F32))
    delta_ref[...] = nt(ind_ref[...], high) + nt(ind_ref[...], rest)


def attend_back_kernel(
    gain_row, qkv_ref, grad_ref, lse_ref, delta_ref, cos_ref, sin_ref, segc_ref, segr_ref,
    wq_ref, wk_ref, wv_ref, attn_in_ref, ao_ref, proj_ref, tok_ref, mid_ref, small_ref,
    weight_ref, gtok_ref, gain_ref, dq_ref, dk_ref, dv_ref, bias_ref, in_t_ref, ao_t_ref, acc_ref,
):
    step = pl.program_id(0)
    tokens = tok_ref.shape[0]
    blocks = tokens // BLOCK
    reach = DOC_MAX // BLOCK

    @pl.when(step == 0)
    def _():
        in_t_ref[...] = attn_in_ref[...].T
        ao_t_ref[...] = ao_ref[...].T
        acc_ref[...] = jnp.zeros_like(acc_ref)

    dq_ref[...] = jnp.zeros_like(dq_ref)
    for block in range(blocks):
        first = block * BLOCK
        last = min(blocks, block + reach + 1) * BLOCK
        span = last - first
        keys = slice(first, first + BLOCK)
        key_ids = iota((BLOCK, span), 0) + first
        row_ids = iota((BLOCK, span), 1) + first
        seen = (key_ids <= row_ids) & (segc_ref[keys, :] == segr_ref[0:1, first:last])
        bias_ref[:, 0:span] = jnp.where(seen, 0.0, NEGATIVE)
        key = qkv_ref[1, keys, :]
        value = qkv_ref[2, keys, :]
        key_grad = None
        for head in range(GROUP):
            mask = head_mask(head)
            index = step * GROUP + head
            query = qkv_ref[0, first:last, :] * mask
            upstream = grad_ref[first:last, :] * mask
            scores = nt(key, query) + bias_ref[:, 0:span]
            probs = jnp.exp(scores - lse_ref[pl.ds(index, 1), first:last])
            prob_grad = nt(value, upstream)
            score_grad = (probs * (prob_grad - delta_ref[pl.ds(index, 1), first:last])).astype(BF16)
            dv = nn(probs.astype(BF16), upstream)
            dk = nn(score_grad, query)
            dq_ref[first:last, :] += tn(score_grad, key * mask)
            key_grad = dk if key_grad is None else key_grad + dk
            value_grad = dv if head == 0 else value_grad + dv
        dk_ref[keys, :] = key_grad
        dv_ref[keys, :] = value_grad.astype(BF16)

    @pl.loop(0, blocks)
    def _(block):
        rows = pl.ds(pl.multiple_of(block * BLOCK, BLOCK), BLOCK)
        cosines = cos_ref[rows, :]
        sines = -sin_ref[rows, :]
        dq = turn(dq_ref[rows, :] * HEAD_DIM**-0.5, cosines, sines)
        dk = turn(dk_ref[rows, :], cosines, sines)
        dq_ref[rows, :] = dq
        dk_ref[rows, :] = dk
        acc_ref[rows, :] += (
            nt(dq.astype(BF16), wq_ref[...])
            + nt(dk.astype(BF16), wk_ref[...])
            + nt(dv_ref[rows, :], wv_ref[...])
        )

    halves = GROUP_LANES // LANES
    for index, (turned, grads) in enumerate(
        ((in_t_ref, dq_ref), (in_t_ref, dk_ref), (in_t_ref, dv_ref), (ao_t_ref, proj_ref))
    ):
        product = nn(turned[...], grads[...].astype(BF16)).astype(BF16)
        for half in range(halves):
            weight_ref[index * halves + half] = product[:, half * LANES : (half + 1) * LANES]

    @pl.when(step == pl.num_programs(0) - 1)
    def _():
        gain = small_ref[...].astype(F32).T[gain_row : gain_row + 1, :]
        gain_ref[...] = jnp.zeros_like(gain_ref)

        @pl.loop(0, blocks)
        def _(block):
            rows = pl.ds(pl.multiple_of(block * BLOCK, BLOCK), BLOCK)
            values = tok_ref[rows, :].astype(F32)
            inverse = inverse_rms(values)
            normed = values * inverse
            grad = acc_ref[rows, :]
            gain_ref[...] += jnp.sum(grad * normed, axis=0, keepdims=True)
            gtok_ref[rows, :] = mid_ref[rows, :] + norm_back(grad * gain, normed, inverse)


def take(values, index, axis=0):
    index = jnp.clip(index, 0, values.shape[axis] - 1)
    return lax.dynamic_index_in_dim(values, index, axis, keepdims=False)


def add_low(left, right):
    return (left.astype(F32) + right.astype(F32)).astype(BF16)


def split_parts(values):
    return values.reshape(4, 2, values.shape[0] // 8, *values.shape[1:])


def cross(values):
    here = lax.axis_index("dp") % 2
    sent = lax.ppermute(take(values, 1 - here, 1), "dp", [(d, d ^ 1) for d in range(8)])
    return take(values, here, 1), sent


def meet(pair):
    return add_low(*pair)


def greet(targets):
    barrier = pltpu.get_barrier_semaphore()
    for present, target in targets:
        @pl.when(present)
        def _():
            pl.semaphore_signal(barrier, inc=1, device_id=target, device_id_type=MESH)
    pl.semaphore_wait(barrier, sum(present.astype(jnp.int32) for present, _ in targets))


def gather_kernel(part_ref, out_ref, send_sem, recv_sem, local_sem):
    me = lax.axis_index("dp")
    owner = lax.axis_index("expert")
    here, side = me // 2, me % 2
    core = owner % 2
    up = ((2 * jnp.minimum(here + 1, 3) + side), here < 3)
    down = ((2 * jnp.maximum(here - 1, 0) + side), here > 0)
    across = 2 * here + 1 - side
    partner = owner + 1 - 2 * core
    always = here >= 0
    routes = (
        (up[1], {"dp": up[0]}),
        (down[1], {"dp": down[0]}),
        (always, {"dp": across}),
        (always, {"expert": partner}),
    )
    greet(routes)

    def copy(index, half, route, source=None):
        return pltpu.make_async_remote_copy(
            src_ref=out_ref.at[index, half] if source is None else source,
            dst_ref=out_ref.at[index, half],
            send_sem=send_sem.at[route, index],
            recv_sem=recv_sem.at[half, index],
            device_id=routes[route][1],
            device_id_type=MESH,
        )

    def arrive(index, half):
        copy(index, half, 2).wait_recv()

    local = pltpu.make_async_copy(part_ref, out_ref.at[me], local_sem)
    local.start()
    for route in range(3):
        @pl.when(routes[route][0])
        def _():
            copy(me, core, route, part_ref.at[core]).start()
    for distance in range(1, 5):
        for toward, forward, present in (
            (here - distance, 0, here >= distance),
            (here + distance, 1, here + distance <= 3),
        ):
            index = 2 * jnp.clip(toward, 0, 3) + side

            @pl.when(present)
            def _():
                arrive(index, core)
                copy(index, core, 2).start()
                copy(index, core, 3).start()

            @pl.when(present & routes[forward][0])
            def _():
                copy(index, core, forward).start()
        for sign in (-1, 1):
            if distance == 1 and sign == 1:
                continue
            toward = here + sign * (distance - 1)
            index = 2 * jnp.clip(toward, 0, 3) + 1 - side

            @pl.when((toward >= 0) & (toward <= 3))
            def _():
                arrive(index, core)
                copy(index, core, 3).start()
    for offset in range(1, 8):
        index = (me + offset) % 8
        arrive(index, 1 - core)
        copy(index, core, 3).wait_send()
    local.wait()
    for route in range(3):
        @pl.when(routes[route][0])
        def _():
            copy(me, core, route, part_ref.at[core]).wait_send()
    for distance in range(1, 4):
        for toward, forward, present in (
            (here - distance, 0, here >= distance),
            (here + distance, 1, here + distance <= 3),
        ):
            index = 2 * jnp.clip(toward, 0, 3) + side

            @pl.when(present)
            def _():
                copy(index, core, 2).wait_send()

            @pl.when(present & routes[forward][0])
            def _():
                copy(index, core, forward).wait_send()


def gather_parts(packed):
    rows, columns = packed.shape
    whole = pl.pallas_call(
        gather_kernel,
        in_specs=[pl.BlockSpec(memory_space=pltpu.VMEM)],
        out_specs=pl.BlockSpec(memory_space=pl.ANY),
        out_shape=jax.ShapeDtypeStruct((8, 2, rows // 2, columns), BF16),
        scratch_shapes=[
            pltpu.SemaphoreType.DMA((4, 8)),
            pltpu.SemaphoreType.DMA((2, 8)),
            pltpu.SemaphoreType.DMA,
        ],
        compiler_params=params(collective_id=0, has_side_effects=True),
        cost_estimate=cost(10e9, 10e6),
        name="gather_parts",
    )(packed.reshape(2, rows // 2, columns))
    return whole.reshape(8 * rows, columns)


def add_planes(target, left, right):
    @pl.loop(0, target.shape[0])
    def _(index):
        total = left[index].astype(F32) + right[index].astype(F32)
        target[index] = total.astype(target.dtype)


def reduce_kernel(
    gate_ref, up_ref, pair_ref, weight_ref, minor_ref,
    gate_out, up_out, down_out, weight_out, minor_out,
    gate_in, up_in, down_in, line_in, gate_stage, up_stage, down_stage, line_stage,
    pair_in, down_ref, core_in, core_sum, side_in, side_sum, cross_in, line_ref, line_sum_ref,
    small_in, small_sum, piece_send, piece_recv, other_send, other_recv,
):
    me = lax.axis_index("dp")
    owner = lax.axis_index("expert")
    here, flank = me // 2, me % 2
    core, side = owner % 2, owner // 2
    rising = {"dp": 2 * jnp.minimum(here + 1, 3) + flank}
    falling = {"dp": 2 * jnp.maximum(here - 1, 0) + flank}
    across = {"dp": me + 1 - 2 * flank}
    partner = {"expert": owner + 1 - 2 * core}
    beside = {"expert": owner + 2 - 4 * side}
    always = here >= 0
    greet(((here < 3, rising), (here > 0, falling), (always, across), (always, partner),
           (always, beside)))
    pieces = (
        (gate_ref, gate_in, gate_stage),
        (up_ref, up_in, up_stage),
        (down_ref, down_in, down_stage),
        (line_ref, line_in, line_stage),
    )
    def piece_copy(piece, turn_index, way, source):
        return pltpu.make_async_remote_copy(
            src_ref=source,
            dst_ref=pieces[piece][1].at[way, turn_index],
            send_sem=piece_send.at[piece, turn_index, way],
            recv_sem=piece_recv.at[piece, turn_index, way],
            device_id=(rising, falling)[way],
            device_id_type=MESH,
        )

    def other_copy(index, source, target, device):
        return pltpu.make_async_remote_copy(
            src_ref=source, dst_ref=target, send_sem=other_send.at[index],
            recv_sem=other_recv.at[index], device_id=device, device_id_type=MESH,
        )

    def direct(piece, turn_index):
        own = pieces[piece][0]

        @pl.when(here == 0)
        def _():
            piece_copy(piece, turn_index, 0, own.at[3 - turn_index]).start()

        @pl.when(here == 3)
        def _():
            piece_copy(piece, turn_index, 1, own.at[turn_index]).start()

    def relayed(turn_index):
        return (
            (0, (here > 0) & (here < 3 - turn_index), 3 - turn_index),
            (1, (here < 3) & (here > turn_index), turn_index),
        )

    def relay(piece, turn_index):
        own, landed, stage = pieces[piece]
        for way, present, chunk in relayed(turn_index):
            @pl.when(present)
            def _():
                copy = piece_copy(piece, turn_index, way, stage.at[way, turn_index])
                copy.wait_recv()
                add_planes(
                    stage.at[way, turn_index], own.at[chunk], landed.at[way, turn_index]
                )
                copy.start()

    def finish(piece, target):
        own, landed, stage = pieces[piece]
        lower = jnp.minimum(3 - here, 2)
        upper = jnp.minimum(here, 2)

        @pl.when(here > 0)
        def _():
            piece_copy(piece, lower, 0, stage.at[0, 0]).wait_recv()

        @pl.when(here < 3)
        def _():
            piece_copy(piece, upper, 1, stage.at[0, 0]).wait_recv()

        @pl.when(here == 0)
        def _():
            add_planes(target, own.at[here], landed.at[1, upper])

        @pl.when(here == 3)
        def _():
            add_planes(target, own.at[here], landed.at[0, lower])

        @pl.when((here > 0) & (here < 3))
        def _():
            @pl.loop(0, target.shape[0])
            def _(index):
                total = (
                    own[here, index].astype(F32)
                    + landed[0, lower, index].astype(F32)
                    + landed[1, upper, index].astype(F32)
                )
                target[index] = total.astype(target.dtype)

    def drain(piece):
        own, _, stage = pieces[piece]
        for turn_index in range(3):
            @pl.when(here == 0)
            def _():
                piece_copy(piece, turn_index, 0, own.at[3 - turn_index]).wait_send()

            @pl.when(here == 3)
            def _():
                piece_copy(piece, turn_index, 1, own.at[turn_index]).wait_send()
        for turn_index in range(2):
            for way, present, _ in relayed(turn_index):
                @pl.when(present)
                def _():
                    piece_copy(
                        piece, turn_index, way, stage.at[way, turn_index]
                    ).wait_send()

    half = core_in.shape[0]
    quarter = half // 2
    core_weight = other_copy(0, weight_ref.at[pl.ds(half * (1 - core), half)], core_in, partner)
    core_small = other_copy(1, minor_ref, small_in.at[0], partner)
    side_weight = other_copy(2, core_sum.at[pl.ds(quarter * (1 - side), quarter)], side_in, beside)
    side_small = other_copy(3, small_sum.at[0], small_in.at[1], beside)
    cross_weight = [
        other_copy(4 + z, side_sum.at[:, 2 * z + 1 - flank], cross_in.at[z], across)
        for z in range(4)
    ]
    cross_small = other_copy(8, small_sum.at[1], small_in.at[2], across)
    rise_small = other_copy(9, small_sum.at[3], small_in.at[3], rising)
    fall_small = other_copy(10, small_sum.at[4], small_in.at[4], falling)
    mine = half * core + quarter * side
    own_part = weight_out.at[pl.ds(mine, quarter)]
    own_half = weight_out.at[pl.ds(half * core, half)]
    side_back = other_copy(11, own_part, own_part, beside)
    core_back = other_copy(12, own_half, own_half, partner)

    pair_copies = [
        other_copy(13 + z, pair_ref.at[z, 1 - flank], pair_in.at[z], across) for z in range(4)
    ]
    core_weight.start()
    core_small.start()
    for copy in pair_copies:
        copy.start()
    for turn_index in range(2):
        for piece in (0, 1):
            direct(piece, turn_index)
    core_weight.wait_recv()
    core_small.wait_recv()
    add_planes(core_sum, weight_ref.at[pl.ds(half * core, half)], core_in)
    small_sum[0] = minor_ref[...] + small_in[0]
    side_weight.start()
    side_small.start()
    for piece in (0, 1):
        relay(piece, 0)
    for z, copy in enumerate(pair_copies):
        copy.wait_recv()
        add_planes(down_ref.at[z], pair_ref.at[z, flank], pair_in.at[z])
    for turn_index in range(2):
        direct(2, turn_index)
    side_weight.wait_recv()
    side_small.wait_recv()
    add_planes(side_sum, core_sum.at[pl.ds(quarter * side, quarter)], side_in)
    small_sum[1] = small_sum[0] + small_in[1]
    for copy in cross_weight:
        copy.start()
    cross_small.start()
    for piece in (0, 1):
        relay(piece, 1)
    relay(2, 0)
    for copy in cross_weight:
        copy.wait_recv()
    cross_small.wait_recv()
    for z in range(4):
        add_planes(line_ref.at[z], side_sum.at[:, 2 * z + flank], cross_in.at[z])
    small_sum[2] = small_sum[1] + small_in[2]
    small_sum[3] = small_sum[2]
    small_sum[4] = small_sum[2]
    for turn_index in range(3):
        direct(3, turn_index)

    @pl.when(here == 0)
    def _():
        rise_small.start()

    @pl.when(here == 3)
    def _():
        fall_small.start()

    for piece in (0, 1, 2):
        direct(piece, 2)
    relay(2, 1)
    for turn_index in range(2):
        relay(3, turn_index)

    @pl.when(here > 0)
    def _():
        rise_small.wait_recv()
        small_sum[3] = small_sum[2] + small_in[3]

    @pl.when((here > 0) & (here < 3))
    def _():
        rise_small.start()

    @pl.when(here < 3)
    def _():
        fall_small.wait_recv()
        small_sum[4] = small_sum[2] + small_in[4]

    @pl.when((here > 0) & (here < 3))
    def _():
        fall_small.start()

    minor_out[...] = small_sum[3] + small_sum[4] - small_sum[2]
    finish(3, line_sum_ref)
    for index in range(quarter):
        weight_out[mine + index] = line_sum_ref[index]
    side_back.start()
    finish(0, gate_out)
    side_back.wait_recv()
    core_back.start()
    finish(1, up_out)
    finish(2, down_out)
    core_back.wait_recv()
    for piece in range(4):
        drain(piece)
    for copy in (core_weight, core_small, side_weight, side_small, *cross_weight, cross_small,
                 side_back, core_back, *pair_copies):
        copy.wait_send()

    @pl.when(here < 3)
    def _():
        rise_small.wait_send()

    @pl.when(here > 0)
    def _():
        fall_small.wait_send()


def reduce_parts(kept, down, weights, minor):
    gate, up = kept
    kept = [piece.reshape(4, piece.shape[1] // 8, 8, piece.shape[2]) for piece in kept]
    pair = down.reshape(4, 2, down.shape[0] // 64, 8, down.shape[1])
    blocks, width, lanes = weights.shape
    rows = width // 8
    plane = (rows, lanes)
    chunks = [piece.shape[1:] for piece in kept] + [pair.shape[2:]]
    line = (blocks // 4,) + plane
    low = [pltpu.VMEM((2, 3) + chunk, BF16) for chunk in chunks + [line]]
    stages = [pltpu.VMEM((2, 2) + chunk, BF16) for chunk in chunks + [line]]
    outs = pl.pallas_call(
        reduce_kernel,
        in_specs=[pl.BlockSpec(memory_space=pltpu.VMEM)] * 5,
        out_specs=[pl.BlockSpec(memory_space=pltpu.VMEM)] * 5,
        out_shape=[jax.ShapeDtypeStruct(chunk, F32) for chunk in chunks]
        + [
            jax.ShapeDtypeStruct((blocks,) + plane, BF16),
            jax.ShapeDtypeStruct(minor.shape, F32),
        ],
        scratch_shapes=[
            *low,
            *stages,
            pltpu.VMEM((4,) + chunks[2], BF16),
            pltpu.VMEM((4,) + chunks[2], BF16),
            pltpu.VMEM((blocks // 2, 8) + plane, BF16),
            pltpu.VMEM((blocks // 2, 8) + plane, BF16),
            pltpu.VMEM((blocks // 4, 8) + plane, BF16),
            pltpu.VMEM((blocks // 4, 8) + plane, BF16),
            pltpu.VMEM((4,) + line, BF16),
            pltpu.VMEM((4,) + line, BF16),
            pltpu.VMEM(line, BF16),
            pltpu.VMEM((5,) + minor.shape, F32),
            pltpu.VMEM((5,) + minor.shape, F32),
            pltpu.SemaphoreType.DMA((4, 3, 2)),
            pltpu.SemaphoreType.DMA((4, 3, 2)),
            pltpu.SemaphoreType.DMA((17,)),
            pltpu.SemaphoreType.DMA((17,)),
        ],
        compiler_params=params(collective_id=1, has_side_effects=True),
        name="reduce_parts",
    )(*kept, pair, weights.reshape(blocks, 8, rows, lanes), minor)
    shapes = (gate.shape[1:], up.shape[1:], (down.shape[0] // 8, down.shape[1]))
    shares = [out.reshape(shape) for out, shape in zip(outs, shapes)]
    return shares, outs[3], outs[4]


def per_device(
    tokens, prev_scores, segments, routes, wqkv, wo, router, const_gate, const_vec, gain1, gain2,
    gate_mix, w_in, w_out, cotangent,
):
    tok_count, width = tokens.shape
    kinds = router.shape[1]
    experts = w_in.shape[0] * lax.axis_size("expert")
    ff = w_out.shape[1]
    qkv_cols = wqkv.shape[1]
    parts = lax.axis_size("dp")
    by_hand = parts == 8 and experts == 4
    small = jnp.concatenate(
        [router, const_gate, const_vec, gain1[:, None], gain2[:, None]], axis=1
    )
    packed = jnp.concatenate(
        [wqkv, wo, jnp.pad(small, ((0, 0), (0, LANES - small.shape[1])))], axis=1
    )
    if by_hand:
        whole = gather_parts(packed)
    else:
        whole = lax.all_gather(packed, "dp", axis=0, tiled=True)

    seq_len = segments.shape[1]
    positions = (jnp.arange(tok_count, dtype=jnp.int32) % seq_len).astype(F32)
    half = HEAD_DIM // 2
    frequency = 10000.0 ** (-jnp.arange(half).astype(F32) / half)
    angles = positions[:, None] * frequency[None, :]
    cosines = jnp.tile(jnp.cos(angles), (1, LANES // half))
    sines = jnp.tile(jnp.sin(angles), (1, LANES // half))
    signs = jnp.where(jnp.arange(LANES) % HEAD_DIM < half, -1.0, 1.0).astype(F32)
    sines = sines * signs[None, :]
    seg_col = segments.reshape(tok_count, 1)
    seg_row = segments.reshape(1, tok_count)

    names = jnp.arange(kinds, dtype=jnp.int32)
    hot = [routes[:, i : i + 1] == names[None, :] for i in range(2)]
    named = (hot[0] | hot[1]).astype(BF16)
    ids = jnp.arange(tok_count, dtype=jnp.int32)
    before = (ids[:, None] > ids[None, :]).astype(BF16)
    earlier = jnp.dot(before, named, preferred_element_type=F32)
    slots = [jnp.sum(jnp.where(h, earlier, 0.0), axis=1).astype(jnp.int32) for h in hot]
    targets = [
        jnp.where(routes[:, i] < experts, routes[:, i] * CAP + slots[i], experts * CAP)
        for i in range(2)
    ]
    target_row = jnp.stack(targets, axis=0)
    target_col = jnp.stack(targets, axis=1)
    prev_mix = jnp.dot(prev_scores, gate_mix.astype(F32), precision=HIGHEST_PRECISION)
    prev_mix = jnp.pad(prev_mix, ((0, 0), (0, LANES - kinds)))

    def swap(values):
        return lax.all_to_all(values, "expert", split_axis=0, concat_axis=0, tiled=True)

    cot_send = pl.pallas_call(
        functools.partial(send_cotangent_kernel, experts),
        out_shape=jax.ShapeDtypeStruct((experts, CAP, width), BF16),
        compiler_params=params(),
        cost_estimate=cost(2 * experts * CAP * tok_count * width, 4 * tok_count * width),
        name="send_cotangent",
    )(cotangent, target_row)
    cot_rows = swap(cot_send).reshape(experts * CAP, width)

    groups = HEADS // GROUP
    tiles = qkv_cols // 3 // GROUP_LANES
    weight_specs = [
        pl.BlockSpec((width, GROUP_LANES), functools.partial(lambda o, i: (0, o + i), part * tiles))
        for part in range(3)
    ]
    small_spec = pl.BlockSpec((width, LANES), lambda *_: (0, (qkv_cols + width) // LANES))
    wo_spec = pl.BlockSpec((width, width), lambda *_: (0, qkv_cols // width))
    table = whole_block((tok_count, LANES))
    full = whole_block((tok_count, width))
    group_spec = pl.BlockSpec((tok_count, GROUP_LANES), lambda i: (0, i))
    qkv_spec = pl.BlockSpec((3, tok_count, GROUP_LANES), lambda i: (0, 0, i))
    seg_specs = [whole_block((tok_count, 1)), whole_block((1, tok_count))]
    span = DOC_MAX + BLOCK
    head_rows = 16
    lse_spec = whole_block((head_rows, tok_count))
    qkv, attn_in, attn_out, lse = pl.pallas_call(
        functools.partial(attend_kernel, kinds + 6),
        grid=(groups,),
        in_specs=[full, *weight_specs, small_spec, table, table, *seg_specs],
        out_specs=[qkv_spec, full, group_spec, lse_spec],
        out_shape=[
            jax.ShapeDtypeStruct((3, tok_count, width), BF16),
            jax.ShapeDtypeStruct((tok_count, width), BF16),
            jax.ShapeDtypeStruct((tok_count, width), BF16),
            jax.ShapeDtypeStruct((head_rows, tok_count), F32),
        ],
        scratch_shapes=[
            pltpu.VMEM((1, width), F32),
            pltpu.VMEM((BLOCK, span), F32),
            pltpu.VMEM((tok_count, LANES), F32),
        ],
        compiler_params=params(),
        cost_estimate=cost(12e9, 16e6),
        name="attend",
    )(tokens, whole, whole, whole, whole, cosines, sines, seg_col, seg_row)

    payload = width + LANES
    resid_mid, scal, send = pl.pallas_call(
        functools.partial(middle_kernel, kinds),
        grid=(1,),
        in_specs=[
            full, wo_spec, full, small_spec, table, whole_block((tok_count, 2)),
            whole_block((2, tok_count)),
        ],
        out_specs=[full, table, whole_block((experts, CAP, payload))],
        out_shape=[
            jax.ShapeDtypeStruct((tok_count, width), F32),
            jax.ShapeDtypeStruct((tok_count, LANES), F32),
            jax.ShapeDtypeStruct((experts, CAP, payload), BF16),
        ],
        scratch_shapes=[
            pltpu.VMEM((tok_count, width), BF16),
            pltpu.VMEM((tok_count, LANES), BF16),
            pltpu.VMEM((tok_count, LANES), BF16),
        ],
        compiler_params=params(),
        cost_estimate=cost(3.5e9, 10e6),
        name="middle",
    )(attn_out, whole, tokens, whole, prev_mix, routes, target_row)
    recv = swap(send).reshape(experts * CAP, payload)

    slot_count = experts * CAP
    ff_tile = 256
    ff_tiles = ff // ff_tile
    w_in_one = w_in.reshape(width, 2 * ff)
    w_out_one = w_out.reshape(ff, width)
    slot_full = whole_block((slot_count, width))
    recv_full = whole_block((slot_count, payload))
    front_spec = pl.BlockSpec((3, slot_count, ff_tile), lambda j: (0, 0, j))
    front, ret = pl.pallas_call(
        expert_kernel,
        grid=(ff_tiles,),
        in_specs=[
            recv_full,
            slot_full,
            pl.BlockSpec((width, ff_tile), lambda j: (0, j)),
            pl.BlockSpec((width, ff_tile), lambda j: (0, ff_tiles + j)),
            pl.BlockSpec((ff_tile, width), lambda j: (j, 0)),
        ],
        out_specs=[front_spec, whole_block((experts, 2 * CAP, width))],
        out_shape=[
            jax.ShapeDtypeStruct((3, slot_count, ff), BF16),
            jax.ShapeDtypeStruct((experts, 2 * CAP, width), BF16),
        ],
        scratch_shapes=[pltpu.VMEM((slot_count, width), F32)] * 2,
        compiler_params=params(),
        cost_estimate=cost(12 * slot_count * width * ff, 26e6),
        name="expert",
    )(recv, cot_rows, w_in_one, w_in_one, w_out_one)
    returned = swap(ret)
    expert_grads = pl.pallas_call(
        expert_grad_kernel,
        grid=(ff_tiles,),
        in_specs=[recv_full, slot_full, front_spec],
        out_specs=[
            pl.BlockSpec((width, ff_tile), lambda j: (0, j)),
            pl.BlockSpec((width, ff_tile), lambda j: (0, j)),
            pl.BlockSpec((ff_tile, width), lambda j: (j, 0)),
        ],
        out_shape=[
            jax.ShapeDtypeStruct((width, ff), BF16),
            jax.ShapeDtypeStruct((width, ff), BF16),
            jax.ShapeDtypeStruct((ff, width), BF16),
        ],
        scratch_shapes=[pltpu.VMEM((width, slot_count), BF16)],
        compiler_params=params(),
        cost_estimate=cost(6 * slot_count * width * ff, 24e6),
        name="expert_grad",
    )(recv, cot_rows, front)
    returned, *expert_grads = lax.optimization_barrier((returned, *expert_grads))
    crossed = [cross(split_parts(grad)) for grad in expert_grads[:2]] if by_hand else None

    mix_turned = jnp.pad(gate_mix.T, ((0, LANES - kinds), (0, LANES - kinds)))
    indicator = (
        jnp.arange(width)[None, :] // HEAD_DIM == jnp.arange(head_rows)[:, None]
    ).astype(BF16)
    token_block = pl.BlockSpec((BLOCK, width), lambda i: (i, 0))
    table_block = pl.BlockSpec((BLOCK, LANES), lambda i: (i, 0))
    two_block = pl.BlockSpec((BLOCK, 2), lambda i: (i, 0))
    (
        mixed, grad_prev, mid_grad, proj_grad, attn_grad, delta, minor, vec, gain2_row, grad_mix,
    ) = pl.pallas_call(
        functools.partial(combine_kernel, kinds, experts),
        grid=(tok_count // BLOCK,),
        in_specs=[
            whole_block((experts, 2 * CAP, width)), two_block, two_block, table_block,
            token_block, token_block, token_block, small_spec, wo_spec,
            whole_block((LANES, LANES)),
            pl.BlockSpec((kinds, BLOCK), lambda i: (0, i)),
            whole_block((head_rows, width)),
        ],
        out_specs=[
            token_block, pl.BlockSpec((BLOCK, kinds), lambda i: (i, 0)), token_block, token_block,
            token_block, pl.BlockSpec((head_rows, BLOCK), lambda i: (0, i)),
            whole_block((LANES, width)), whole_block((LANES, width)), whole_block((1, width)),
            whole_block((kinds, LANES)),
        ],
        out_shape=[
            jax.ShapeDtypeStruct((tok_count, width), BF16),
            jax.ShapeDtypeStruct((tok_count, kinds), F32),
            jax.ShapeDtypeStruct((tok_count, width), F32),
            jax.ShapeDtypeStruct((tok_count, width), BF16),
            jax.ShapeDtypeStruct((tok_count, width), BF16),
            jax.ShapeDtypeStruct((head_rows, tok_count), F32),
            jax.ShapeDtypeStruct((LANES, width), F32),
            jax.ShapeDtypeStruct((LANES, width), F32),
            jax.ShapeDtypeStruct((1, width), F32),
            jax.ShapeDtypeStruct((kinds, LANES), F32),
        ],
        scratch_shapes=[pltpu.VMEM((LANES, width), F32)],
        compiler_params=params(),
        cost_estimate=cost(1e6, 1e5),
        name="combine",
    )(
        returned, target_col, routes, scal, resid_mid, cotangent, attn_out, whole, whole,
        mix_turned, prev_scores.T, indicator,
    )

    halves = GROUP_LANES // LANES
    weights, grad_tokens, gain1_row = pl.pallas_call(
        functools.partial(attend_back_kernel, kinds + 6),
        grid=(groups,),
        in_specs=[
            qkv_spec, group_spec, lse_spec, lse_spec, table, table, *seg_specs, *weight_specs,
            full, full, group_spec, full, full, small_spec,
        ],
        out_specs=[
            pl.BlockSpec((4 * halves, width, LANES), lambda i: (i, 0, 0)), full,
            whole_block((1, width)),
        ],
        out_shape=[
            jax.ShapeDtypeStruct((4 * halves * groups, width, LANES), BF16),
            jax.ShapeDtypeStruct((tok_count, width), F32),
            jax.ShapeDtypeStruct((1, width), F32),
        ],
        scratch_shapes=[
            pltpu.VMEM((tok_count, GROUP_LANES), F32),
            pltpu.VMEM((tok_count, GROUP_LANES), F32),
            pltpu.VMEM((tok_count, GROUP_LANES), BF16),
            pltpu.VMEM((BLOCK, span), F32),
            pltpu.VMEM((width, tok_count), BF16),
            pltpu.VMEM((width, tok_count), BF16),
            pltpu.VMEM((tok_count, width), F32),
        ],
        compiler_params=params(),
        cost_estimate=cost(1e6, 1e5),
        name="attend_back",
    )(
        qkv, attn_grad, lse, delta, cosines, sines, seg_col, seg_row, whole, whole, whole,
        attn_in, attn_out, proj_grad, tokens, mid_grad, whole,
    )

    minor_rows = jnp.concatenate([minor[: kinds + 4], vec[:2], gain1_row, gain2_row], axis=0)
    minor_all = jnp.concatenate(
        [minor_rows, jnp.pad(grad_mix[:, :kinds], ((0, 0), (0, width - kinds)))], axis=0
    )
    rows = width // parts
    if by_hand:
        crossed, weights = lax.optimization_barrier((crossed, weights))
        kept = [meet(halves_of) for halves_of in crossed]
        shares, weight_sum, minor_all = reduce_parts(
            kept, expert_grads[2], weights, minor_all
        )
    else:
        shares = [
            lax.psum_scatter(grad, "dp", scatter_dimension=0, tiled=True).astype(F32)
            for grad in expert_grads
        ]
        weight_part = lax.psum_scatter(weights, "expert", scatter_dimension=0, tiled=True)
        weight_part = lax.psum_scatter(weight_part, "dp", scatter_dimension=1, tiled=True)
        weight_sum = lax.all_gather(weight_part, "expert", axis=0, tiled=True)
        minor_all = lax.psum(minor_all, ("dp", "expert"))
    grad_gate_mix = minor_all[kinds + 8 :, :kinds]
    minor_sum = lax.dynamic_slice_in_dim(
        minor_all[: kinds + 8], lax.axis_index("dp") * rows, rows, 1
    ).T
    weight_sum = weight_sum.reshape(groups, 4, -1, rows, LANES)
    weight_sum = weight_sum.transpose(3, 1, 0, 2, 4).reshape(rows, 4 * width).astype(F32)
    return (
        mixed,
        grad_tokens,
        grad_prev,
        weight_sum[:, :qkv_cols],
        weight_sum[:, qkv_cols:],
        minor_sum[:, :kinds],
        minor_sum[:, kinds : kinds + 4],
        minor_sum[:, kinds + 4 : kinds + 6],
        minor_sum[:, kinds + 6],
        minor_sum[:, kinds + 7],
        grad_gate_mix,
        jnp.concatenate([shares[0], shares[1]], axis=1)[None],
        shares[2][None],
    )


def solution(mesh):
    rows = P(("dp", "expert"), None)
    in_specs = (
        rows, rows, rows, rows,
        P("dp", None), P("dp", None), P("dp", None), P("dp", None), P("dp", None), P("dp"), P("dp"),
        P(), P("expert", None, None), P("expert", None, None), rows,
    )
    out_specs = (
        rows, rows, rows,
        P("dp", None), P("dp", None), P("dp", None), P("dp", None), P("dp", None), P("dp"), P("dp"),
        P(), P("expert", "dp", None), P("expert", "dp", None),
    )
    return jax.shard_map(
        per_device, mesh=mesh, in_specs=in_specs, out_specs=out_specs, check_vma=False
    )
```

```python
import functools

import jax
import jax.numpy as jnp
from jax import lax
from jax.experimental import pallas as pl
from jax.experimental.pallas import tpu as pltpu
from jax.sharding import PartitionSpec as P

HEADS = 12
HEAD_DIM = 64
CAP = 256
DOC_MAX = 512
NORM_EPSILON = 1e-06
HIGHEST_PRECISION = lax.Precision.HIGHEST
NEGATIVE = -1e30
F32 = jnp.float32
BF16 = jnp.bfloat16
BLOCK = 256
GROUP = 4
GROUP_LANES = GROUP * HEAD_DIM
LANES = 128
MESH = pl.DeviceIdType.MESH
VMEM_BYTES = 62 * 1024 * 1024


def nn(left, right):
    return jnp.dot(left, right, preferred_element_type=F32)


def nt(left, right):
    return lax.dot_general(left, right, (((1,), (1,)), ((), ())), preferred_element_type=F32)


def tn(left, right):
    return lax.dot_general(left, right, (((0,), (0,)), ((), ())), preferred_element_type=F32)


def iota(shape, axis):
    return lax.broadcasted_iota(jnp.int32, shape, axis)


def split_low(values):
    high = values.astype(BF16)
    return high, (values - high.astype(F32)).astype(BF16)


def inverse_rms(values):
    return lax.rsqrt(jnp.mean(values * values, axis=-1, keepdims=True) + NORM_EPSILON)


def norm_back(upstream, normed, inverse):
    return inverse * (upstream - normed * jnp.mean(upstream * normed, axis=-1, keepdims=True))


def turn(values, cosines, signed_sines):
    pieces = []
    for start in range(0, values.shape[1], LANES):
        part = values[:, start : start + LANES]
        front = iota(part.shape, 1) % HEAD_DIM < HEAD_DIM // 2
        swapped = jnp.where(
            front,
            pltpu.roll(part, LANES - HEAD_DIM // 2, 1),
            pltpu.roll(part, HEAD_DIM // 2, 1),
        )
        pieces.append(part * cosines + swapped * signed_sines)
    return jnp.concatenate(pieces, axis=1)


def head_mask(head):
    return (iota((1, GROUP_LANES), 1) // HEAD_DIM == head).astype(F32).astype(BF16)


def params(**extra):
    return pltpu.CompilerParams(vmem_limit_bytes=VMEM_BYTES, **extra)


def whole_block(shape):
    return pl.BlockSpec(shape, lambda *_: (0,) * len(shape))


def cost(flops, moved):
    return pl.CostEstimate(flops=int(flops), bytes_accessed=int(moved), transcendentals=0)


def send_cotangent_kernel(experts, cot_ref, target_ref, out_ref):
    tokens = cot_ref.shape[0]

    @pl.loop(0, experts)
    def _(expert):
        slots = iota((CAP, tokens), 0) + expert * CAP
        hot = (target_ref[0:1, :] == slots) | (target_ref[1:2, :] == slots)
        out_ref[expert] = nn(hot.astype(F32).astype(BF16), cot_ref[...]).astype(BF16)


def attend_kernel(
    gain_row, tok_ref, wq_ref, wk_ref, wv_ref, small_ref, cos_ref, sin_ref, segc_ref, segr_ref,
    qkv_ref, attn_in_ref, out_ref, lse_ref, gain_ref, bias_ref, log_ref,
):
    step = pl.program_id(0)
    tokens = tok_ref.shape[0]
    blocks = tokens // BLOCK
    reach = DOC_MAX // BLOCK

    @pl.when(step == 0)
    def _():
        gain_ref[...] = small_ref[...].astype(F32).T[gain_row : gain_row + 1, :]
        log_ref[...] = jnp.zeros_like(log_ref)

        @pl.loop(0, blocks)
        def _(block):
            rows = pl.ds(pl.multiple_of(block * BLOCK, BLOCK), BLOCK)
            values = tok_ref[rows, :].astype(F32)
            attn_in_ref[rows, :] = (values * inverse_rms(values) * gain_ref[...]).astype(BF16)

    @pl.loop(0, blocks)
    def _(block):
        rows = pl.ds(pl.multiple_of(block * BLOCK, BLOCK), BLOCK)
        normed = attn_in_ref[rows, :]
        cosines = cos_ref[rows, :]
        sines = sin_ref[rows, :]
        query = turn(nn(normed, wq_ref[...]), cosines, sines) * HEAD_DIM**-0.5
        qkv_ref[0, rows, :] = query.astype(BF16)
        qkv_ref[1, rows, :] = turn(nn(normed, wk_ref[...]), cosines, sines).astype(BF16)
        qkv_ref[2, rows, :] = nn(normed, wv_ref[...]).astype(BF16)

    for block in range(blocks):
        first = max(0, block - reach) * BLOCK
        last = (block + 1) * BLOCK
        span = last - first
        rows = slice(block * BLOCK, last)
        row_ids = iota((BLOCK, span), 0) + block * BLOCK
        col_ids = iota((BLOCK, span), 1) + first
        seen = (col_ids <= row_ids) & (segc_ref[rows, :] == segr_ref[0:1, first:last])
        bias_ref[:, 0:span] = jnp.where(seen, 0.0, NEGATIVE)
        attended = []
        logs = log_ref[rows, :]
        for head in range(GROUP):
            mask = head_mask(head)
            scores = nt(qkv_ref[0, rows, :] * mask, qkv_ref[1, first:last, :]) + bias_ref[:, 0:span]
            top = jnp.max(scores, axis=1, keepdims=True)
            weights = jnp.exp(scores - top).astype(BF16)
            value = qkv_ref[2, first:last, :] * mask + (1 - mask)
            mixed = nn(weights, value)
            own = iota(mixed.shape, 1) // HEAD_DIM == head
            total = jnp.max(jnp.where(own, 0.0, mixed), axis=1, keepdims=True)
            attended.append(jnp.where(own, mixed / total, 0.0))
            logs = jnp.where(
                iota(logs.shape, 1) == step * GROUP + head, top + jnp.log(total), logs
            )
        log_ref[rows, :] = logs
        out_ref[rows, :] = (attended[0] + attended[1] + attended[2] + attended[3]).astype(BF16)

    @pl.when(step == pl.num_programs(0) - 1)
    def _():
        lse_ref[...] = log_ref[...].T[0 : lse_ref.shape[0], :]


def middle_kernel(
    kinds, ao_ref, wo_ref, tok_ref, small_ref, prev_ref, routes_ref, target_ref,
    resid_ref, scal_ref, send_ref, ffn_ref, first_ref, second_ref,
):
    tokens, width = tok_ref.shape
    gain = small_ref[...].astype(F32).T[kinds + 7 : kinds + 8, :]

    @pl.loop(0, tokens // BLOCK)
    def _(block):
        rows = pl.ds(pl.multiple_of(block * BLOCK, BLOCK), BLOCK)
        resid = tok_ref[rows, :].astype(F32) + nn(ao_ref[rows, :], wo_ref[...])
        resid_ref[rows, :] = resid
        inverse = inverse_rms(resid)
        low = (resid * inverse * gain).astype(BF16)
        ffn_ref[rows, :] = low
        logits = nn(low, small_ref[...]) + prev_ref[rows, :]
        lane = iota(logits.shape, 1)

        def pick(index):
            return jnp.sum(jnp.where(lane == index, logits, 0.0), axis=1, keepdims=True)

        def pair(left, right):
            top = jnp.maximum(left, right)
            left = jnp.exp(left - top)
            right = jnp.exp(right - top)
            total = left + right
            return left / total, right / total

        gates = pair(pick(routes_ref[rows, 0:1]), pick(routes_ref[rows, 1:2]))
        one = pair(pick(kinds), pick(kinds + 1))
        two = pair(pick(kinds + 2), pick(kinds + 3))
        scal = jnp.zeros_like(logits)
        for index, value in enumerate(gates + one + two + (inverse,)):
            scal = jnp.where(lane == index, value, scal)
        scal_ref[rows, :] = scal
        for gate, ref in zip(gates, (first_ref, second_ref)):
            high, rest = split_low(gate)
            ref[rows, :] = jnp.where(
                lane == 0, high.astype(F32), jnp.where(lane == 1, rest.astype(F32), 0.0)
            ).astype(BF16)

    @pl.loop(0, send_ref.shape[0])
    def _(expert):
        slots = iota((CAP, tokens), 0) + expert * CAP
        hot_one = (target_ref[0:1, :] == slots).astype(F32)
        hot_two = (target_ref[1:2, :] == slots).astype(F32)
        send_ref[expert, :, 0:width] = nn((hot_one + hot_two).astype(BF16), ffn_ref[...]).astype(
            BF16
        )
        send_ref[expert, :, width:] = (
            nn(hot_one.astype(BF16), first_ref[...]) + nn(hot_two.astype(BF16), second_ref[...])
        ).astype(BF16)


def expert_kernel(
    recv_ref, cot_ref, wg_ref, wu_ref, wo_ref, front_ref, ret_ref, out_acc, row_acc,
):
    step = pl.program_id(0)
    total, width = out_acc.shape
    tile = 512

    @pl.when(step == 0)
    def _():
        out_acc[...] = jnp.zeros_like(out_acc)
        row_acc[...] = jnp.zeros_like(row_acc)

    @pl.loop(0, total // tile)
    def _(block):
        rows = pl.ds(pl.multiple_of(block * tile, tile), tile)
        token = recv_ref[rows, 0:width]
        extra = recv_ref[rows, width:].astype(F32)
        gate_weight = extra[:, 0:1] + extra[:, 1:2]
        gate = nn(token, wg_ref[...])
        up = nn(token, wu_ref[...])
        grad = nt(cot_ref[rows, :], wo_ref[...]) * gate_weight
        sig = jax.nn.sigmoid(gate)
        act = gate * sig
        hidden = act * up
        out_acc[rows, :] += nn(hidden.astype(BF16), wo_ref[...])
        front_ref[2, rows, :] = (hidden * gate_weight).astype(BF16)
        gate_grad = (grad * up * sig * (1.0 + gate * (1.0 - sig))).astype(BF16)
        up_grad = (grad * act).astype(BF16)
        front_ref[0, rows, :] = gate_grad
        front_ref[1, rows, :] = up_grad
        row_acc[rows, :] += nt(gate_grad, wg_ref[...]) + nt(up_grad, wu_ref[...])

    @pl.when(step == pl.num_programs(0) - 1)
    def _():
        @pl.loop(0, total // CAP)
        def _(peer):
            rows = pl.ds(pl.multiple_of(peer * CAP, CAP), CAP)
            ret_ref[peer, 0:CAP, :] = out_acc[rows, :].astype(BF16)
            ret_ref[peer, CAP:, :] = row_acc[rows, :].astype(BF16)


def expert_grad_kernel(recv_ref, cot_ref, front_ref, gate_ref, up_ref, wout_ref, turned_ref):
    step = pl.program_id(0)
    width = turned_ref.shape[0]

    @pl.when(step == 0)
    def _():
        turned_ref[...] = recv_ref[:, 0:width].T

    wout_ref[...] = tn(front_ref[2], cot_ref[...]).astype(BF16)
    gate_ref[...] = nn(turned_ref[...], front_ref[0]).astype(BF16)
    up_ref[...] = nn(turned_ref[...], front_ref[1]).astype(BF16)


def combine_kernel(
    kinds, experts, ret_ref, target_ref, routes_ref, scal_ref, resid_ref, cot_ref, ao_ref,
    small_ref, wo_ref, mix_ref, prevt_ref, ind_ref,
    mixed_ref, prev_ref, mid_ref, proj_ref, attn_ref, delta_ref, minor_ref, vec_ref, gain_ref,
    gmix_ref, rows_ref,
):
    step = pl.program_id(0)

    @pl.when(step == 0)
    def _():
        rows_ref[...] = small_ref[...].astype(F32).T
        minor_ref[...] = jnp.zeros_like(minor_ref)
        vec_ref[...] = jnp.zeros_like(vec_ref)
        gain_ref[...] = jnp.zeros_like(gain_ref)
        gmix_ref[...] = jnp.zeros_like(gmix_ref)

    width = resid_ref.shape[1]
    slots = experts * CAP
    resid = resid_ref[...]
    cot = cot_ref[...]
    upstream = cot.astype(F32)
    scal = scal_ref[...]
    routes = (routes_ref[:, 0:1], routes_ref[:, 1:2])
    targets = (target_ref[:, 0:1], target_ref[:, 1:2])
    gates = (scal[:, 0:1], scal[:, 1:2])
    one_keep, one_vec = scal[:, 2:3], scal[:, 3:4]
    two_keep, two_vec = scal[:, 4:5], scal[:, 5:6]
    inverse = scal[:, 6:7]
    gain = rows_ref[kinds + 7 : kinds + 8, :]
    vec_one = rows_ref[kinds + 4 : kinds + 5, :]
    vec_two = rows_ref[kinds + 5 : kinds + 6, :]
    normed = resid * inverse
    ffn_norm = normed * gain
    low = ffn_norm.astype(BF16)
    slot_ids = iota((BLOCK, slots), 1)
    hots = [(target == slot_ids).astype(F32) for target in targets]
    outs = ret_ref[:, 0:CAP, :].reshape(slots, width)
    backs = ret_ref[:, CAP:, :].reshape(slots, width)
    branches = [nn(hot.astype(BF16), outs) for hot in hots]
    back = nn((hots[0] + hots[1]).astype(BF16), backs)

    def weight(kind):
        return sum(
            jnp.where(route == kind, gate, 0.0) for route, gate in zip(routes, gates)
        )

    weight_copy = weight(experts + 1)
    weight_one = weight(experts + 2)
    weight_two = weight(experts + 3)
    keep = weight_copy + weight_one * one_keep + weight_two * two_keep
    mixed_ref[...] = (
        resid
        + gates[0] * branches[0]
        + gates[1] * branches[1]
        + keep * ffn_norm
        + (weight_one * one_vec) * vec_one
        + (weight_two * two_vec) * vec_two
    ).astype(BF16)
    dot_norm = jnp.sum(upstream * ffn_norm, axis=1, keepdims=True)
    dot_one = jnp.sum(upstream * vec_one, axis=1, keepdims=True)
    dot_two = jnp.sum(upstream * vec_two, axis=1, keepdims=True)
    grads = []
    for route, branch in zip(routes, branches):
        grads.append(
            jnp.sum(branch * upstream, axis=1, keepdims=True)
            + jnp.where(route == experts + 1, dot_norm, 0.0)
            + jnp.where(route == experts + 2, one_keep * dot_norm + one_vec * dot_one, 0.0)
            + jnp.where(route == experts + 3, two_keep * dot_norm + two_vec * dot_two, 0.0)
        )
    mean_grad = gates[0] * grads[0] + gates[1] * grads[1]
    lane = iota((BLOCK, LANES), 1)
    wide = jnp.zeros((BLOCK, LANES), F32)
    for route, gate, grad in zip(routes, gates, grads):
        wide = jnp.where(lane == route, gate * (grad - mean_grad), wide)
    for index, keep_part, vec_part, grad_weight, dot in (
        (kinds, one_keep, one_vec, weight_one, dot_one),
        (kinds + 2, two_keep, two_vec, weight_two, dot_two),
    ):
        keep_grad = grad_weight * dot_norm
        vec_grad = grad_weight * dot
        both = keep_part * keep_grad + vec_part * vec_grad
        wide = jnp.where(lane == index, keep_part * (keep_grad - both), wide)
        wide = jnp.where(lane == index + 1, vec_part * (vec_grad - both), wide)
    wide_low = wide.astype(BF16)
    wide_back = wide_low.astype(F32)
    minor_ref[...] += nn(wide_back.T.astype(BF16), low)
    share = jnp.where(lane == 0, weight_one * one_vec, 0.0)
    share = jnp.where(lane == 1, weight_two * two_vec, share)
    high, rest = split_low(share.T)
    vec_ref[...] += nn(high, cot) + nn(rest, cot)
    prev_ref[...] = nn(wide_low, mix_ref[...])[:, 0:kinds]
    gmix_ref[...] += jnp.dot(
        prevt_ref[...], wide_back, precision=HIGHEST_PRECISION, preferred_element_type=F32
    )
    grad_two = back + nt(wide_low, small_ref[...]) + keep * upstream
    gain_ref[...] += jnp.sum(grad_two * normed, axis=0, keepdims=True)
    mid = upstream + norm_back(grad_two * gain, normed, inverse)
    mid_ref[...] = mid
    proj = mid.astype(BF16)
    proj_ref[...] = proj
    attn = nt(proj, wo_ref[...]).astype(BF16)
    attn_ref[...] = attn
    high, rest = split_low(attn.astype(F32) * ao_ref[...].astype(F32))
    delta_ref[...] = nt(ind_ref[...], high) + nt(ind_ref[...], rest)


def attend_back_kernel(
    gain_row, qkv_ref, grad_ref, lse_ref, delta_ref, cos_ref, sin_ref, segc_ref, segr_ref,
    wq_ref, wk_ref, wv_ref, attn_in_ref, ao_ref, proj_ref, tok_ref, mid_ref, small_ref,
    weight_ref, gtok_ref, gain_ref, dq_ref, dk_ref, dv_ref, bias_ref, in_t_ref, ao_t_ref, acc_ref,
):
    step = pl.program_id(0)
    tokens = tok_ref.shape[0]
    blocks = tokens // BLOCK
    reach = DOC_MAX // BLOCK

    @pl.when(step == 0)
    def _():
        in_t_ref[...] = attn_in_ref[...].T
        ao_t_ref[...] = ao_ref[...].T
        acc_ref[...] = jnp.zeros_like(acc_ref)

    dq_ref[...] = jnp.zeros_like(dq_ref)
    for block in range(blocks):
        first = block * BLOCK
        last = min(blocks, block + reach + 1) * BLOCK
        span = last - first
        keys = slice(first, first + BLOCK)
        key_ids = iota((BLOCK, span), 0) + first
        row_ids = iota((BLOCK, span), 1) + first
        seen = (key_ids <= row_ids) & (segc_ref[keys, :] == segr_ref[0:1, first:last])
        bias_ref[:, 0:span] = jnp.where(seen, 0.0, NEGATIVE)
        key = qkv_ref[1, keys, :]
        value = qkv_ref[2, keys, :]
        key_grad = None
        for head in range(GROUP):
            mask = head_mask(head)
            index = step * GROUP + head
            query = qkv_ref[0, first:last, :] * mask
            upstream = grad_ref[first:last, :] * mask
            scores = nt(key, query) + bias_ref[:, 0:span]
            probs = jnp.exp(scores - lse_ref[pl.ds(index, 1), first:last])
            prob_grad = nt(value, upstream)
            score_grad = (probs * (prob_grad - delta_ref[pl.ds(index, 1), first:last])).astype(BF16)
            dv = nn(probs.astype(BF16), upstream)
            dk = nn(score_grad, query)
            dq_ref[first:last, :] += tn(score_grad, key * mask)
            key_grad = dk if key_grad is None else key_grad + dk
            value_grad = dv if head == 0 else value_grad + dv
        dk_ref[keys, :] = key_grad
        dv_ref[keys, :] = value_grad.astype(BF16)

    @pl.loop(0, blocks)
    def _(block):
        rows = pl.ds(pl.multiple_of(block * BLOCK, BLOCK), BLOCK)
        cosines = cos_ref[rows, :]
        sines = -sin_ref[rows, :]
        dq = turn(dq_ref[rows, :] * HEAD_DIM**-0.5, cosines, sines)
        dk = turn(dk_ref[rows, :], cosines, sines)
        dq_ref[rows, :] = dq
        dk_ref[rows, :] = dk
        acc_ref[rows, :] += (
            nt(dq.astype(BF16), wq_ref[...])
            + nt(dk.astype(BF16), wk_ref[...])
            + nt(dv_ref[rows, :], wv_ref[...])
        )

    halves = GROUP_LANES // LANES
    for index, (turned, grads) in enumerate(
        ((in_t_ref, dq_ref), (in_t_ref, dk_ref), (in_t_ref, dv_ref), (ao_t_ref, proj_ref))
    ):
        product = nn(turned[...], grads[...].astype(BF16)).astype(BF16)
        for half in range(halves):
            weight_ref[index * halves + half] = product[:, half * LANES : (half + 1) * LANES]

    @pl.when(step == pl.num_programs(0) - 1)
    def _():
        gain = small_ref[...].astype(F32).T[gain_row : gain_row + 1, :]
        gain_ref[...] = jnp.zeros_like(gain_ref)

        @pl.loop(0, blocks)
        def _(block):
            rows = pl.ds(pl.multiple_of(block * BLOCK, BLOCK), BLOCK)
            values = tok_ref[rows, :].astype(F32)
            inverse = inverse_rms(values)
            normed = values * inverse
            grad = acc_ref[rows, :]
            gain_ref[...] += jnp.sum(grad * normed, axis=0, keepdims=True)
            gtok_ref[rows, :] = mid_ref[rows, :] + norm_back(grad * gain, normed, inverse)


def take(values, index, axis=0):
    index = jnp.clip(index, 0, values.shape[axis] - 1)
    return lax.dynamic_index_in_dim(values, index, axis, keepdims=False)


def add_low(left, right):
    return (left.astype(F32) + right.astype(F32)).astype(BF16)


def split_parts(values):
    return values.reshape(4, 2, values.shape[0] // 8, *values.shape[1:])


def cross(values):
    here = lax.axis_index("dp") % 2
    sent = lax.ppermute(take(values, 1 - here, 1), "dp", [(d, d ^ 1) for d in range(8)])
    return take(values, here, 1), sent


def meet(pair):
    return add_low(*pair)


def greet(targets):
    barrier = pltpu.get_barrier_semaphore()
    for present, target in targets:
        @pl.when(present)
        def _():
            pl.semaphore_signal(barrier, inc=1, device_id=target, device_id_type=MESH)
    pl.semaphore_wait(barrier, sum(present.astype(jnp.int32) for present, _ in targets))


def gather_kernel(part_ref, out_ref, send_sem, recv_sem, local_sem):
    me = lax.axis_index("dp")
    owner = lax.axis_index("expert")
    here, side = me // 2, me % 2
    core = owner % 2
    up = ((2 * jnp.minimum(here + 1, 3) + side), here < 3)
    down = ((2 * jnp.maximum(here - 1, 0) + side), here > 0)
    across = 2 * here + 1 - side
    partner = owner + 1 - 2 * core
    always = here >= 0
    routes = (
        (up[1], {"dp": up[0]}),
        (down[1], {"dp": down[0]}),
        (always, {"dp": across}),
        (always, {"expert": partner}),
    )
    greet(routes)

    def copy(index, half, route, source=None):
        return pltpu.make_async_remote_copy(
            src_ref=out_ref.at[index, half] if source is None else source,
            dst_ref=out_ref.at[index, half],
            send_sem=send_sem.at[route, index],
            recv_sem=recv_sem.at[half, index],
            device_id=routes[route][1],
            device_id_type=MESH,
        )

    def arrive(index, half):
        copy(index, half, 2).wait_recv()

    local = pltpu.make_async_copy(part_ref, out_ref.at[me], local_sem)
    local.start()
    for route in range(3):
        @pl.when(routes[route][0])
        def _():
            copy(me, core, route, part_ref.at[core]).start()
    for distance in range(1, 5):
        for toward, forward, present in (
            (here - distance, 0, here >= distance),
            (here + distance, 1, here + distance <= 3),
        ):
            index = 2 * jnp.clip(toward, 0, 3) + side

            @pl.when(present)
            def _():
                arrive(index, core)
                copy(index, core, 2).start()
                copy(index, core, 3).start()

            @pl.when(present & routes[forward][0])
            def _():
                copy(index, core, forward).start()
        for sign in (-1, 1):
            if distance == 1 and sign == 1:
                continue
            toward = here + sign * (distance - 1)
            index = 2 * jnp.clip(toward, 0, 3) + 1 - side

            @pl.when((toward >= 0) & (toward <= 3))
            def _():
                arrive(index, core)
                copy(index, core, 3).start()
    for offset in range(1, 8):
        index = (me + offset) % 8
        arrive(index, 1 - core)
        copy(index, core, 3).wait_send()
    local.wait()
    for route in range(3):
        @pl.when(routes[route][0])
        def _():
            copy(me, core, route, part_ref.at[core]).wait_send()
    for distance in range(1, 4):
        for toward, forward, present in (
            (here - distance, 0, here >= distance),
            (here + distance, 1, here + distance <= 3),
        ):
            index = 2 * jnp.clip(toward, 0, 3) + side

            @pl.when(present)
            def _():
                copy(index, core, 2).wait_send()

            @pl.when(present & routes[forward][0])
            def _():
                copy(index, core, forward).wait_send()


def gather_parts(packed):
    rows, columns = packed.shape
    whole = pl.pallas_call(
        gather_kernel,
        in_specs=[pl.BlockSpec(memory_space=pltpu.VMEM)],
        out_specs=pl.BlockSpec(memory_space=pl.ANY),
        out_shape=jax.ShapeDtypeStruct((8, 2, rows // 2, columns), BF16),
        scratch_shapes=[
            pltpu.SemaphoreType.DMA((4, 8)),
            pltpu.SemaphoreType.DMA((2, 8)),
            pltpu.SemaphoreType.DMA,
        ],
        compiler_params=params(collective_id=0, has_side_effects=True),
        cost_estimate=cost(10e9, 10e6),
        name="gather_parts",
    )(packed.reshape(2, rows // 2, columns))
    return whole.reshape(8 * rows, columns)


def add_planes(target, left, right):
    @pl.loop(0, target.shape[0])
    def _(index):
        total = left[index].astype(F32) + right[index].astype(F32)
        target[index] = total.astype(target.dtype)


def reduce_kernel(
    gate_ref, up_ref, pair_ref, weight_ref, minor_ref,
    gate_out, up_out, down_out, weight_out, minor_out,
    gate_in, up_in, down_in, line_in, gate_stage, up_stage, down_stage, line_stage,
    pair_in, down_ref, core_in, core_sum, side_in, side_sum, cross_in, line_ref, line_sum_ref,
    small_in, small_sum, piece_send, piece_recv, other_send, other_recv,
):
    me = lax.axis_index("dp")
    owner = lax.axis_index("expert")
    here, flank = me // 2, me % 2
    core, side = owner % 2, owner // 2
    rising = {"dp": 2 * jnp.minimum(here + 1, 3) + flank}
    falling = {"dp": 2 * jnp.maximum(here - 1, 0) + flank}
    across = {"dp": me + 1 - 2 * flank}
    partner = {"expert": owner + 1 - 2 * core}
    beside = {"expert": owner + 2 - 4 * side}
    always = here >= 0
    greet(((here < 3, rising), (here > 0, falling), (always, across), (always, partner),
           (always, beside)))
    pieces = (
        (gate_ref, gate_in, gate_stage),
        (up_ref, up_in, up_stage),
        (down_ref, down_in, down_stage),
        (line_ref, line_in, line_stage),
    )
    def piece_copy(piece, turn_index, way, source):
        return pltpu.make_async_remote_copy(
            src_ref=source,
            dst_ref=pieces[piece][1].at[way, turn_index],
            send_sem=piece_send.at[piece, turn_index, way],
            recv_sem=piece_recv.at[piece, turn_index, way],
            device_id=(rising, falling)[way],
            device_id_type=MESH,
        )

    def other_copy(index, source, target, device):
        return pltpu.make_async_remote_copy(
            src_ref=source, dst_ref=target, send_sem=other_send.at[index],
            recv_sem=other_recv.at[index], device_id=device, device_id_type=MESH,
        )

    def direct(piece, turn_index):
        own = pieces[piece][0]

        @pl.when(here == 0)
        def _():
            piece_copy(piece, turn_index, 0, own.at[3 - turn_index]).start()

        @pl.when(here == 3)
        def _():
            piece_copy(piece, turn_index, 1, own.at[turn_index]).start()

    def relayed(turn_index):
        return (
            (0, (here > 0) & (here < 3 - turn_index), 3 - turn_index),
            (1, (here < 3) & (here > turn_index), turn_index),
        )

    def relay(piece, turn_index):
        own, landed, stage = pieces[piece]
        for way, present, chunk in relayed(turn_index):
            @pl.when(present)
            def _():
                copy = piece_copy(piece, turn_index, way, stage.at[way, turn_index])
                copy.wait_recv()
                add_planes(
                    stage.at[way, turn_index], own.at[chunk], landed.at[way, turn_index]
                )
                copy.start()

    def finish(piece, target):
        own, landed, stage = pieces[piece]
        lower = jnp.minimum(3 - here, 2)
        upper = jnp.minimum(here, 2)

        @pl.when(here > 0)
        def _():
            piece_copy(piece, lower, 0, stage.at[0, 0]).wait_recv()

        @pl.when(here < 3)
        def _():
            piece_copy(piece, upper, 1, stage.at[0, 0]).wait_recv()

        @pl.when(here == 0)
        def _():
            add_planes(target, own.at[here], landed.at[1, upper])

        @pl.when(here == 3)
        def _():
            add_planes(target, own.at[here], landed.at[0, lower])

        @pl.when((here > 0) & (here < 3))
        def _():
            @pl.loop(0, target.shape[0])
            def _(index):
                total = (
                    own[here, index].astype(F32)
                    + landed[0, lower, index].astype(F32)
                    + landed[1, upper, index].astype(F32)
                )
                target[index] = total.astype(target.dtype)

    def drain(piece):
        own, _, stage = pieces[piece]
        for turn_index in range(3):
            @pl.when(here == 0)
            def _():
                piece_copy(piece, turn_index, 0, own.at[3 - turn_index]).wait_send()

            @pl.when(here == 3)
            def _():
                piece_copy(piece, turn_index, 1, own.at[turn_index]).wait_send()
        for turn_index in range(2):
            for way, present, _ in relayed(turn_index):
                @pl.when(present)
                def _():
                    piece_copy(
                        piece, turn_index, way, stage.at[way, turn_index]
                    ).wait_send()

    half = core_in.shape[0]
    quarter = half // 2
    core_weight = other_copy(0, weight_ref.at[pl.ds(half * (1 - core), half)], core_in, partner)
    core_small = other_copy(1, minor_ref, small_in.at[0], partner)
    side_weight = other_copy(2, core_sum.at[pl.ds(quarter * (1 - side), quarter)], side_in, beside)
    side_small = other_copy(3, small_sum.at[0], small_in.at[1], beside)
    cross_weight = [
        other_copy(4 + z, side_sum.at[:, 2 * z + 1 - flank], cross_in.at[z], across)
        for z in range(4)
    ]
    cross_small = other_copy(8, small_sum.at[1], small_in.at[2], across)
    rise_small = other_copy(9, small_sum.at[3], small_in.at[3], rising)
    fall_small = other_copy(10, small_sum.at[4], small_in.at[4], falling)
    mine = half * core + quarter * side
    own_part = weight_out.at[pl.ds(mine, quarter)]
    own_half = weight_out.at[pl.ds(half * core, half)]
    side_back = other_copy(11, own_part, own_part, beside)
    core_back = other_copy(12, own_half, own_half, partner)

    pair_copies = [
        other_copy(13 + z, pair_ref.at[z, 1 - flank], pair_in.at[z], across) for z in range(4)
    ]
    core_weight.start()
    core_small.start()
    for copy in pair_copies:
        copy.start()
    for turn_index in range(2):
        for piece in (0, 1):
            direct(piece, turn_index)
    core_weight.wait_recv()
    core_small.wait_recv()
    add_planes(core_sum, weight_ref.at[pl.ds(half * core, half)], core_in)
    small_sum[0] = minor_ref[...] + small_in[0]
    side_weight.start()
    side_small.start()
    for piece in (0, 1):
        relay(piece, 0)
    for z, copy in enumerate(pair_copies):
        copy.wait_recv()
        add_planes(down_ref.at[z], pair_ref.at[z, flank], pair_in.at[z])
    for turn_index in range(2):
        direct(2, turn_index)
    side_weight.wait_recv()
    side_small.wait_recv()
    add_planes(side_sum, core_sum.at[pl.ds(quarter * side, quarter)], side_in)
    small_sum[1] = small_sum[0] + small_in[1]
    for copy in cross_weight:
        copy.start()
    cross_small.start()
    for piece in (0, 1):
        relay(piece, 1)
    relay(2, 0)
    for copy in cross_weight:
        copy.wait_recv()
    cross_small.wait_recv()
    for z in range(4):
        add_planes(line_ref.at[z], side_sum.at[:, 2 * z + flank], cross_in.at[z])
    small_sum[2] = small_sum[1] + small_in[2]
    small_sum[3] = small_sum[2]
    small_sum[4] = small_sum[2]
    for turn_index in range(3):
        direct(3, turn_index)

    @pl.when(here == 0)
    def _():
        rise_small.start()

    @pl.when(here == 3)
    def _():
        fall_small.start()

    for piece in (0, 1, 2):
        direct(piece, 2)
    relay(2, 1)
    for turn_index in range(2):
        relay(3, turn_index)

    @pl.when(here > 0)
    def _():
        rise_small.wait_recv()
        small_sum[3] = small_sum[2] + small_in[3]

    @pl.when((here > 0) & (here < 3))
    def _():
        rise_small.start()

    @pl.when(here < 3)
    def _():
        fall_small.wait_recv()
        small_sum[4] = small_sum[2] + small_in[4]

    @pl.when((here > 0) & (here < 3))
    def _():
        fall_small.start()

    minor_out[...] = small_sum[3] + small_sum[4] - small_sum[2]
    finish(3, line_sum_ref)
    for index in range(quarter):
        weight_out[mine + index] = line_sum_ref[index]
    side_back.start()
    finish(0, gate_out)
    side_back.wait_recv()
    core_back.start()
    finish(1, up_out)
    finish(2, down_out)
    core_back.wait_recv()
    for piece in range(4):
        drain(piece)
    for copy in (core_weight, core_small, side_weight, side_small, *cross_weight, cross_small,
                 side_back, core_back, *pair_copies):
        copy.wait_send()

    @pl.when(here < 3)
    def _():
        rise_small.wait_send()

    @pl.when(here > 0)
    def _():
        fall_small.wait_send()


def reduce_parts(kept, down, weights, minor):
    gate, up = kept
    kept = [piece.reshape(4, piece.shape[1] // 8, 8, piece.shape[2]) for piece in kept]
    pair = down.reshape(4, 2, down.shape[0] // 64, 8, down.shape[1])
    blocks, width, lanes = weights.shape
    rows = width // 8
    plane = (rows, lanes)
    chunks = [piece.shape[1:] for piece in kept] + [pair.shape[2:]]
    line = (blocks // 4,) + plane
    low = [pltpu.VMEM((2, 3) + chunk, BF16) for chunk in chunks + [line]]
    stages = [pltpu.VMEM((2, 2) + chunk, BF16) for chunk in chunks + [line]]
    outs = pl.pallas_call(
        reduce_kernel,
        in_specs=[pl.BlockSpec(memory_space=pltpu.VMEM)] * 5,
        out_specs=[pl.BlockSpec(memory_space=pltpu.VMEM)] * 5,
        out_shape=[jax.ShapeDtypeStruct(chunk, F32) for chunk in chunks]
        + [
            jax.ShapeDtypeStruct((blocks,) + plane, BF16),
            jax.ShapeDtypeStruct(minor.shape, F32),
        ],
        scratch_shapes=[
            *low,
            *stages,
            pltpu.VMEM((4,) + chunks[2], BF16),
            pltpu.VMEM((4,) + chunks[2], BF16),
            pltpu.VMEM((blocks // 2, 8) + plane, BF16),
            pltpu.VMEM((blocks // 2, 8) + plane, BF16),
            pltpu.VMEM((blocks // 4, 8) + plane, BF16),
            pltpu.VMEM((blocks // 4, 8) + plane, BF16),
            pltpu.VMEM((4,) + line, BF16),
            pltpu.VMEM((4,) + line, BF16),
            pltpu.VMEM(line, BF16),
            pltpu.VMEM((5,) + minor.shape, F32),
            pltpu.VMEM((5,) + minor.shape, F32),
            pltpu.SemaphoreType.DMA((4, 3, 2)),
            pltpu.SemaphoreType.DMA((4, 3, 2)),
            pltpu.SemaphoreType.DMA((17,)),
            pltpu.SemaphoreType.DMA((17,)),
        ],
        compiler_params=params(collective_id=1, has_side_effects=True),
        name="reduce_parts",
    )(*kept, pair, weights.reshape(blocks, 8, rows, lanes), minor)
    shapes = (gate.shape[1:], up.shape[1:], (down.shape[0] // 8, down.shape[1]))
    shares = [out.reshape(shape) for out, shape in zip(outs, shapes)]
    return shares, outs[3], outs[4]


FF_TILE = 256


def exchange_kernel(
    send_ref, cot_ref, win_ref, wout_ref,
    gate_out, up_out, down_out, return_out,
    recv, cot, gate_w, up_w, down_w, front, turned, out_acc, row_acc, ret, gate_g, up_g, down_g,
    token_send, token_recv, back_send, back_recv, load_sem, weight_sem, store_sem, own_sem,
):
    me = lax.axis_index("expert")
    core, side = me % 2, me // 2
    partner = me + 1 - 2 * core
    beside = me + 2 - 4 * side
    corner = partner + 2 - 4 * side
    peers = (me, beside, corner, partner)
    always = me >= 0
    width = out_acc.shape[1]
    ff = down_w.shape[0]
    tiles = ff // FF_TILE
    greet([(always, {"expert": peer}) for peer in peers[1:]])

    def token_copy(slot):
        return pltpu.make_async_remote_copy(
            src_ref=send_ref.at[peers[slot]], dst_ref=recv.at[slot],
            send_sem=token_send.at[slot], recv_sem=token_recv.at[slot],
            device_id={"expert": peers[slot]}, device_id_type=MESH,
        )

    def back_copy(slot):
        return pltpu.make_async_remote_copy(
            src_ref=ret.at[slot], dst_ref=return_out.at[me],
            send_sem=back_send.at[slot], recv_sem=back_recv.at[slot],
            device_id={"expert": peers[slot]}, device_id_type=MESH,
        )

    def tile_slice(tile):
        return pl.ds(pl.multiple_of(tile * FF_TILE, FF_TILE), FF_TILE)

    def weight_copies(tile):
        cols = tile_slice(tile)
        shifted = pl.ds(pl.multiple_of(ff + tile * FF_TILE, FF_TILE), FF_TILE)
        return (
            pltpu.make_async_copy(
                win_ref.at[:, cols], gate_w.at[:, cols], weight_sem.at[0, tile]
            ),
            pltpu.make_async_copy(
                win_ref.at[:, shifted], up_w.at[:, cols], weight_sem.at[1, tile]
            ),
            pltpu.make_async_copy(
                wout_ref.at[cols, :], down_w.at[cols, :], weight_sem.at[2, tile]
            ),
        )

    def grad_copies(tile):
        cols = tile_slice(tile)
        return (
            pltpu.make_async_copy(gate_g.at[:, cols], gate_out.at[:, cols], store_sem.at[0, tile]),
            pltpu.make_async_copy(up_g.at[:, cols], up_out.at[:, cols], store_sem.at[1, tile]),
            pltpu.make_async_copy(down_g.at[cols, :], down_out.at[cols, :], store_sem.at[2, tile]),
        )

    for slot in (1, 2, 3):
        token_copy(slot).start()
    loads = [pltpu.make_async_copy(send_ref.at[me], recv.at[0], load_sem.at[0])] + [
        pltpu.make_async_copy(cot_ref.at[peers[slot]], cot.at[slot], load_sem.at[1 + slot])
        for slot in range(4)
    ]
    for load in loads:
        load.start()

    @pl.loop(0, tiles)
    def _(tile):
        for copy in weight_copies(tile):
            copy.start()

    for load in loads:
        load.wait()

    def work(slot):
        extra = recv[slot, :, width:].astype(F32)
        gate_weight = extra[:, 0:1] + extra[:, 1:2]
        out_acc[...] = jnp.zeros_like(out_acc)
        row_acc[...] = jnp.zeros_like(row_acc)

        @pl.loop(0, tiles)
        def _(tile):
            cols = tile_slice(tile)
            if slot == 0:
                for copy in weight_copies(tile):
                    copy.wait()
            token = recv[slot, :, 0:width]
            gate = nn(token, gate_w[:, cols])
            up = nn(token, up_w[:, cols])
            grad = nt(cot[slot], down_w[cols, :]) * gate_weight
            sig = jax.nn.sigmoid(gate)
            act = gate * sig
            hidden = act * up
            out_acc[...] += nn(hidden.astype(BF16), down_w[cols, :])
            front[2, slot, :, cols] = (hidden * gate_weight).astype(BF16)
            gate_grad = (grad * up * sig * (1.0 + gate * (1.0 - sig))).astype(BF16)
            up_grad = (grad * act).astype(BF16)
            front[0, slot, :, cols] = gate_grad
            front[1, slot, :, cols] = up_grad
            row_acc[...] += nt(gate_grad, gate_w[:, cols]) + nt(up_grad, up_w[:, cols])

        ret[slot, 0:CAP, :] = out_acc[...].astype(BF16)
        ret[slot, CAP:, :] = row_acc[...].astype(BF16)
        turned[:, slot * CAP : (slot + 1) * CAP] = recv[slot, :, 0:width].T

    own_back = pltpu.make_async_copy(ret.at[0], return_out.at[me], own_sem)
    work(0)
    own_back.start()
    for slot in (1, 2, 3):
        token_copy(slot).wait_recv()
        work(slot)
        back_copy(slot).start()
    total = 4 * CAP

    @pl.loop(0, tiles)
    def _(tile):
        cols = tile_slice(tile)
        hidden = front[2, :, :, cols].reshape(total, FF_TILE)
        down_g[cols, :] = tn(hidden, cot[...].reshape(total, width)).astype(BF16)
        gate_g[:, cols] = nn(turned[...], front[0, :, :, cols].reshape(total, FF_TILE)).astype(BF16)
        up_g[:, cols] = nn(turned[...], front[1, :, :, cols].reshape(total, FF_TILE)).astype(BF16)
        for copy in grad_copies(tile):
            copy.start()

    for slot in (1, 2, 3):
        token_copy(slot).wait_send()
        back_copy(slot).wait_recv()
        back_copy(slot).wait_send()
    own_back.wait()

    @pl.loop(0, tiles)
    def _(tile):
        for copy in grad_copies(tile):
            copy.wait()


def exchange_experts(send, cot_rows, w_in, w_out):
    peers, cap, payload = send.shape
    ff, width = w_out.shape
    anywhere = pl.BlockSpec(memory_space=pl.ANY)
    tiles = ff // FF_TILE
    *grads, returned = pl.pallas_call(
        exchange_kernel,
        in_specs=[anywhere] * 4,
        out_specs=[anywhere] * 4,
        out_shape=[
            jax.ShapeDtypeStruct((width, ff), BF16),
            jax.ShapeDtypeStruct((width, ff), BF16),
            jax.ShapeDtypeStruct((ff, width), BF16),
            jax.ShapeDtypeStruct((peers, 2 * cap, width), BF16),
        ],
        scratch_shapes=[
            pltpu.VMEM((peers, cap, payload), BF16),
            pltpu.VMEM((peers, cap, width), BF16),
            pltpu.VMEM((width, ff), BF16),
            pltpu.VMEM((width, ff), BF16),
            pltpu.VMEM((ff, width), BF16),
            pltpu.VMEM((3, peers, cap, ff), BF16),
            pltpu.VMEM((width, peers * cap), BF16),
            pltpu.VMEM((cap, width), F32),
            pltpu.VMEM((cap, width), F32),
            pltpu.VMEM((peers, 2 * cap, width), BF16),
            pltpu.VMEM((width, ff), BF16),
            pltpu.VMEM((width, ff), BF16),
            pltpu.VMEM((ff, width), BF16),
            pltpu.SemaphoreType.DMA((4,)),
            pltpu.SemaphoreType.DMA((4,)),
            pltpu.SemaphoreType.DMA((4,)),
            pltpu.SemaphoreType.DMA((4,)),
            pltpu.SemaphoreType.DMA((5,)),
            pltpu.SemaphoreType.DMA((3, tiles)),
            pltpu.SemaphoreType.DMA((3, tiles)),
            pltpu.SemaphoreType.DMA,
        ],
        compiler_params=params(collective_id=2, has_side_effects=True),
        cost_estimate=cost(18 * peers * cap * width * ff, 40e6),
        name="exchange_experts",
    )(send, cot_rows.reshape(peers, cap, width), w_in, w_out)
    return grads, returned


def plain_experts(send, cot_rows, w_in_one, w_out_one, swap):
    experts, _, payload = send.shape
    ff, width = w_out_one.shape
    recv = swap(send).reshape(experts * CAP, payload)

    slot_count = experts * CAP
    ff_tile = 256
    ff_tiles = ff // ff_tile
    slot_full = whole_block((slot_count, width))
    recv_full = whole_block((slot_count, payload))
    front_spec = pl.BlockSpec((3, slot_count, ff_tile), lambda j: (0, 0, j))
    front, ret = pl.pallas_call(
        expert_kernel,
        grid=(ff_tiles,),
        in_specs=[
            recv_full,
            slot_full,
            pl.BlockSpec((width, ff_tile), lambda j: (0, j)),
            pl.BlockSpec((width, ff_tile), lambda j: (0, ff_tiles + j)),
            pl.BlockSpec((ff_tile, width), lambda j: (j, 0)),
        ],
        out_specs=[front_spec, whole_block((experts, 2 * CAP, width))],
        out_shape=[
            jax.ShapeDtypeStruct((3, slot_count, ff), BF16),
            jax.ShapeDtypeStruct((experts, 2 * CAP, width), BF16),
        ],
        scratch_shapes=[pltpu.VMEM((slot_count, width), F32)] * 2,
        compiler_params=params(),
        cost_estimate=cost(12 * slot_count * width * ff, 26e6),
        name="expert",
    )(recv, cot_rows, w_in_one, w_in_one, w_out_one)
    returned = swap(ret)
    expert_grads = pl.pallas_call(
        expert_grad_kernel,
        grid=(ff_tiles,),
        in_specs=[recv_full, slot_full, front_spec],
        out_specs=[
            pl.BlockSpec((width, ff_tile), lambda j: (0, j)),
            pl.BlockSpec((width, ff_tile), lambda j: (0, j)),
            pl.BlockSpec((ff_tile, width), lambda j: (j, 0)),
        ],
        out_shape=[
            jax.ShapeDtypeStruct((width, ff), BF16),
            jax.ShapeDtypeStruct((width, ff), BF16),
            jax.ShapeDtypeStruct((ff, width), BF16),
        ],
        scratch_shapes=[pltpu.VMEM((width, slot_count), BF16)],
        compiler_params=params(),
        cost_estimate=cost(6 * slot_count * width * ff, 24e6),
        name="expert_grad",
    )(recv, cot_rows, front)
    return expert_grads, returned


def per_device(
    tokens, prev_scores, segments, routes, wqkv, wo, router, const_gate, const_vec, gain1, gain2,
    gate_mix, w_in, w_out, cotangent,
):
    tok_count, width = tokens.shape
    kinds = router.shape[1]
    experts = w_in.shape[0] * lax.axis_size("expert")
    ff = w_out.shape[1]
    qkv_cols = wqkv.shape[1]
    parts = lax.axis_size("dp")
    by_hand = parts == 8 and experts == 4
    small = jnp.concatenate(
        [router, const_gate, const_vec, gain1[:, None], gain2[:, None]], axis=1
    )
    packed = jnp.concatenate(
        [wqkv, wo, jnp.pad(small, ((0, 0), (0, LANES - small.shape[1])))], axis=1
    )
    if by_hand:
        whole = gather_parts(packed)
    else:
        whole = lax.all_gather(packed, "dp", axis=0, tiled=True)

    seq_len = segments.shape[1]
    positions = (jnp.arange(tok_count, dtype=jnp.int32) % seq_len).astype(F32)
    half = HEAD_DIM // 2
    frequency = 10000.0 ** (-jnp.arange(half).astype(F32) / half)
    angles = positions[:, None] * frequency[None, :]
    cosines = jnp.tile(jnp.cos(angles), (1, LANES // half))
    sines = jnp.tile(jnp.sin(angles), (1, LANES // half))
    signs = jnp.where(jnp.arange(LANES) % HEAD_DIM < half, -1.0, 1.0).astype(F32)
    sines = sines * signs[None, :]
    seg_col = segments.reshape(tok_count, 1)
    seg_row = segments.reshape(1, tok_count)

    names = jnp.arange(kinds, dtype=jnp.int32)
    hot = [routes[:, i : i + 1] == names[None, :] for i in range(2)]
    named = (hot[0] | hot[1]).astype(BF16)
    ids = jnp.arange(tok_count, dtype=jnp.int32)
    before = (ids[:, None] > ids[None, :]).astype(BF16)
    earlier = jnp.dot(before, named, preferred_element_type=F32)
    slots = [jnp.sum(jnp.where(h, earlier, 0.0), axis=1).astype(jnp.int32) for h in hot]
    targets = [
        jnp.where(routes[:, i] < experts, routes[:, i] * CAP + slots[i], experts * CAP)
        for i in range(2)
    ]
    target_row = jnp.stack(targets, axis=0)
    target_col = jnp.stack(targets, axis=1)
    prev_mix = jnp.dot(prev_scores, gate_mix.astype(F32), precision=HIGHEST_PRECISION)
    prev_mix = jnp.pad(prev_mix, ((0, 0), (0, LANES - kinds)))

    def swap(values):
        return lax.all_to_all(values, "expert", split_axis=0, concat_axis=0, tiled=True)

    cot_send = pl.pallas_call(
        functools.partial(send_cotangent_kernel, experts),
        out_shape=jax.ShapeDtypeStruct((experts, CAP, width), BF16),
        compiler_params=params(),
        cost_estimate=cost(2 * experts * CAP * tok_count * width, 4 * tok_count * width),
        name="send_cotangent",
    )(cotangent, target_row)
    cot_rows = swap(cot_send).reshape(experts * CAP, width)

    groups = HEADS // GROUP
    tiles = qkv_cols // 3 // GROUP_LANES
    weight_specs = [
        pl.BlockSpec((width, GROUP_LANES), functools.partial(lambda o, i: (0, o + i), part * tiles))
        for part in range(3)
    ]
    small_spec = pl.BlockSpec((width, LANES), lambda *_: (0, (qkv_cols + width) // LANES))
    wo_spec = pl.BlockSpec((width, width), lambda *_: (0, qkv_cols // width))
    table = whole_block((tok_count, LANES))
    full = whole_block((tok_count, width))
    group_spec = pl.BlockSpec((tok_count, GROUP_LANES), lambda i: (0, i))
    qkv_spec = pl.BlockSpec((3, tok_count, GROUP_LANES), lambda i: (0, 0, i))
    seg_specs = [whole_block((tok_count, 1)), whole_block((1, tok_count))]
    span = DOC_MAX + BLOCK
    head_rows = 16
    lse_spec = whole_block((head_rows, tok_count))
    qkv, attn_in, attn_out, lse = pl.pallas_call(
        functools.partial(attend_kernel, kinds + 6),
        grid=(groups,),
        in_specs=[full, *weight_specs, small_spec, table, table, *seg_specs],
        out_specs=[qkv_spec, full, group_spec, lse_spec],
        out_shape=[
            jax.ShapeDtypeStruct((3, tok_count, width), BF16),
            jax.ShapeDtypeStruct((tok_count, width), BF16),
            jax.ShapeDtypeStruct((tok_count, width), BF16),
            jax.ShapeDtypeStruct((head_rows, tok_count), F32),
        ],
        scratch_shapes=[
            pltpu.VMEM((1, width), F32),
            pltpu.VMEM((BLOCK, span), F32),
            pltpu.VMEM((tok_count, LANES), F32),
        ],
        compiler_params=params(),
        cost_estimate=cost(12e9, 16e6),
        name="attend",
    )(tokens, whole, whole, whole, whole, cosines, sines, seg_col, seg_row)

    payload = width + LANES
    resid_mid, scal, send = pl.pallas_call(
        functools.partial(middle_kernel, kinds),
        grid=(1,),
        in_specs=[
            full, wo_spec, full, small_spec, table, whole_block((tok_count, 2)),
            whole_block((2, tok_count)),
        ],
        out_specs=[full, table, whole_block((experts, CAP, payload))],
        out_shape=[
            jax.ShapeDtypeStruct((tok_count, width), F32),
            jax.ShapeDtypeStruct((tok_count, LANES), F32),
            jax.ShapeDtypeStruct((experts, CAP, payload), BF16),
        ],
        scratch_shapes=[
            pltpu.VMEM((tok_count, width), BF16),
            pltpu.VMEM((tok_count, LANES), BF16),
            pltpu.VMEM((tok_count, LANES), BF16),
        ],
        compiler_params=params(),
        cost_estimate=cost(3.5e9, 10e6),
        name="middle",
    )(attn_out, whole, tokens, whole, prev_mix, routes, target_row)
    w_in_one = w_in.reshape(width, 2 * ff)
    w_out_one = w_out.reshape(ff, width)
    if by_hand:
        expert_grads, returned = exchange_experts(send, cot_rows, w_in_one, w_out_one)
    else:
        expert_grads, returned = plain_experts(send, cot_rows, w_in_one, w_out_one, swap)
    returned, *expert_grads = lax.optimization_barrier((returned, *expert_grads))
    crossed = [cross(split_parts(grad)) for grad in expert_grads[:2]] if by_hand else None

    mix_turned = jnp.pad(gate_mix.T, ((0, LANES - kinds), (0, LANES - kinds)))
    indicator = (
        jnp.arange(width)[None, :] // HEAD_DIM == jnp.arange(head_rows)[:, None]
    ).astype(BF16)
    token_block = pl.BlockSpec((BLOCK, width), lambda i: (i, 0))
    table_block = pl.BlockSpec((BLOCK, LANES), lambda i: (i, 0))
    two_block = pl.BlockSpec((BLOCK, 2), lambda i: (i, 0))
    (
        mixed, grad_prev, mid_grad, proj_grad, attn_grad, delta, minor, vec, gain2_row, grad_mix,
    ) = pl.pallas_call(
        functools.partial(combine_kernel, kinds, experts),
        grid=(tok_count // BLOCK,),
        in_specs=[
            whole_block((experts, 2 * CAP, width)), two_block, two_block, table_block,
            token_block, token_block, token_block, small_spec, wo_spec,
            whole_block((LANES, LANES)),
            pl.BlockSpec((kinds, BLOCK), lambda i: (0, i)),
            whole_block((head_rows, width)),
        ],
        out_specs=[
            token_block, pl.BlockSpec((BLOCK, kinds), lambda i: (i, 0)), token_block, token_block,
            token_block, pl.BlockSpec((head_rows, BLOCK), lambda i: (0, i)),
            whole_block((LANES, width)), whole_block((LANES, width)), whole_block((1, width)),
            whole_block((kinds, LANES)),
        ],
        out_shape=[
            jax.ShapeDtypeStruct((tok_count, width), BF16),
            jax.ShapeDtypeStruct((tok_count, kinds), F32),
            jax.ShapeDtypeStruct((tok_count, width), F32),
            jax.ShapeDtypeStruct((tok_count, width), BF16),
            jax.ShapeDtypeStruct((tok_count, width), BF16),
            jax.ShapeDtypeStruct((head_rows, tok_count), F32),
            jax.ShapeDtypeStruct((LANES, width), F32),
            jax.ShapeDtypeStruct((LANES, width), F32),
            jax.ShapeDtypeStruct((1, width), F32),
            jax.ShapeDtypeStruct((kinds, LANES), F32),
        ],
        scratch_shapes=[pltpu.VMEM((LANES, width), F32)],
        compiler_params=params(),
        cost_estimate=cost(1e6, 1e5),
        name="combine",
    )(
        returned, target_col, routes, scal, resid_mid, cotangent, attn_out, whole, whole,
        mix_turned, prev_scores.T, indicator,
    )

    halves = GROUP_LANES // LANES
    weights, grad_tokens, gain1_row = pl.pallas_call(
        functools.partial(attend_back_kernel, kinds + 6),
        grid=(groups,),
        in_specs=[
            qkv_spec, group_spec, lse_spec, lse_spec, table, table, *seg_specs, *weight_specs,
            full, full, group_spec, full, full, small_spec,
        ],
        out_specs=[
            pl.BlockSpec((4 * halves, width, LANES), lambda i: (i, 0, 0)), full,
            whole_block((1, width)),
        ],
        out_shape=[
            jax.ShapeDtypeStruct((4 * halves * groups, width, LANES), BF16),
            jax.ShapeDtypeStruct((tok_count, width), F32),
            jax.ShapeDtypeStruct((1, width), F32),
        ],
        scratch_shapes=[
            pltpu.VMEM((tok_count, GROUP_LANES), F32),
            pltpu.VMEM((tok_count, GROUP_LANES), F32),
            pltpu.VMEM((tok_count, GROUP_LANES), BF16),
            pltpu.VMEM((BLOCK, span), F32),
            pltpu.VMEM((width, tok_count), BF16),
            pltpu.VMEM((width, tok_count), BF16),
            pltpu.VMEM((tok_count, width), F32),
        ],
        compiler_params=params(),
        cost_estimate=cost(1e6, 1e5),
        name="attend_back",
    )(
        qkv, attn_grad, lse, delta, cosines, sines, seg_col, seg_row, whole, whole, whole,
        attn_in, attn_out, proj_grad, tokens, mid_grad, whole,
    )

    minor_rows = jnp.concatenate([minor[: kinds + 4], vec[:2], gain1_row, gain2_row], axis=0)
    minor_all = jnp.concatenate(
        [minor_rows, jnp.pad(grad_mix[:, :kinds], ((0, 0), (0, width - kinds)))], axis=0
    )
    rows = width // parts
    if by_hand:
        crossed, weights = lax.optimization_barrier((crossed, weights))
        kept = [meet(halves_of) for halves_of in crossed]
        shares, weight_sum, minor_all = reduce_parts(
            kept, expert_grads[2], weights, minor_all
        )
    else:
        shares = [
            lax.psum_scatter(grad, "dp", scatter_dimension=0, tiled=True).astype(F32)
            for grad in expert_grads
        ]
        weight_part = lax.psum_scatter(weights, "expert", scatter_dimension=0, tiled=True)
        weight_part = lax.psum_scatter(weight_part, "dp", scatter_dimension=1, tiled=True)
        weight_sum = lax.all_gather(weight_part, "expert", axis=0, tiled=True)
        minor_all = lax.psum(minor_all, ("dp", "expert"))
    grad_gate_mix = minor_all[kinds + 8 :, :kinds]
    minor_sum = lax.dynamic_slice_in_dim(
        minor_all[: kinds + 8], lax.axis_index("dp") * rows, rows, 1
    ).T
    weight_sum = weight_sum.reshape(groups, 4, -1, rows, LANES)
    weight_sum = weight_sum.transpose(3, 1, 0, 2, 4).reshape(rows, 4 * width).astype(F32)
    return (
        mixed,
        grad_tokens,
        grad_prev,
        weight_sum[:, :qkv_cols],
        weight_sum[:, qkv_cols:],
        minor_sum[:, :kinds],
        minor_sum[:, kinds : kinds + 4],
        minor_sum[:, kinds + 4 : kinds + 6],
        minor_sum[:, kinds + 6],
        minor_sum[:, kinds + 7],
        grad_gate_mix,
        jnp.concatenate([shares[0], shares[1]], axis=1)[None],
        shares[2][None],
    )


def solution(mesh):
    rows = P(("dp", "expert"), None)
    in_specs = (
        rows, rows, rows, rows,
        P("dp", None), P("dp", None), P("dp", None), P("dp", None), P("dp", None), P("dp"), P("dp"),
        P(), P("expert", None, None), P("expert", None, None), rows,
    )
    out_specs = (
        rows, rows, rows,
        P("dp", None), P("dp", None), P("dp", None), P("dp", None), P("dp", None), P("dp"), P("dp"),
        P(), P("expert", "dp", None), P("expert", "dp", None),
    )
    return jax.shard_map(
        per_device, mesh=mesh, in_specs=in_specs, out_specs=out_specs, check_vma=False
    )
```

```python
import functools

import jax
import jax.numpy as jnp
from jax import lax
from jax.experimental import pallas as pl
from jax.experimental.pallas import tpu as pltpu
from jax.sharding import PartitionSpec as P


HEADS = 12
HEAD_DIM = 64
CAP = 256
DOC_MAX = 512
NORM_EPSILON = 1e-06
HIGHEST_PRECISION = lax.Precision.HIGHEST
NEGATIVE = -1e30
F32 = jnp.float32
BF16 = jnp.bfloat16
BLOCK = 256
GROUP = 4
GROUP_LANES = GROUP * HEAD_DIM
LANES = 128
MESH = pl.DeviceIdType.MESH
VMEM_BYTES = 62 * 1024 * 1024


def nn(left, right):
    return jnp.dot(left, right, preferred_element_type=F32)


def nt(left, right):
    return lax.dot_general(left, right, (((1,), (1,)), ((), ())), preferred_element_type=F32)


def tn(left, right):
    return lax.dot_general(left, right, (((0,), (0,)), ((), ())), preferred_element_type=F32)


def iota(shape, axis):
    return lax.broadcasted_iota(jnp.int32, shape, axis)


def split_low(values):
    high = values.astype(BF16)
    return high, (values - high.astype(F32)).astype(BF16)


def inverse_rms(values):
    return lax.rsqrt(jnp.mean(values * values, axis=-1, keepdims=True) + NORM_EPSILON)


def norm_back(upstream, normed, inverse):
    return inverse * (upstream - normed * jnp.mean(upstream * normed, axis=-1, keepdims=True))


def turn(values, cosines, signed_sines):
    pieces = []
    for start in range(0, values.shape[1], LANES):
        part = values[:, start : start + LANES]
        front = iota(part.shape, 1) % HEAD_DIM < HEAD_DIM // 2
        swapped = jnp.where(
            front,
            pltpu.roll(part, LANES - HEAD_DIM // 2, 1),
            pltpu.roll(part, HEAD_DIM // 2, 1),
        )
        pieces.append(part * cosines + swapped * signed_sines)
    return jnp.concatenate(pieces, axis=1)


def head_mask(head):
    return (iota((1, GROUP_LANES), 1) // HEAD_DIM == head).astype(F32).astype(BF16)


def params(**extra):
    return pltpu.CompilerParams(vmem_limit_bytes=VMEM_BYTES, **extra)


def whole_block(shape):
    return pl.BlockSpec(shape, lambda *_: (0,) * len(shape))


def cost(flops, moved):
    return pl.CostEstimate(flops=int(flops), bytes_accessed=int(moved), transcendentals=0)


def send_cotangent_kernel(experts, cot_ref, target_ref, out_ref):
    tokens = cot_ref.shape[0]

    @pl.loop(0, experts)
    def _(expert):
        slots = iota((CAP, tokens), 0) + expert * CAP
        hot = (target_ref[0:1, :] == slots) | (target_ref[1:2, :] == slots)
        out_ref[expert] = nn(hot.astype(F32).astype(BF16), cot_ref[...]).astype(BF16)


def attend_kernel(
    gain_row, tok_ref, wq_ref, wk_ref, wv_ref, small_ref, cos_ref, sin_ref, segc_ref, segr_ref,
    qkv_ref, attn_in_ref, out_ref, lse_ref, gain_ref, bias_ref, log_ref,
):
    step = pl.program_id(0)
    tokens = tok_ref.shape[0]
    blocks = tokens // BLOCK
    reach = DOC_MAX // BLOCK

    @pl.when(step == 0)
    def _():
        gain_ref[...] = small_ref[...].astype(F32).T[gain_row : gain_row + 1, :]
        log_ref[...] = jnp.zeros_like(log_ref)

        @pl.loop(0, blocks)
        def _(block):
            rows = pl.ds(pl.multiple_of(block * BLOCK, BLOCK), BLOCK)
            values = tok_ref[rows, :].astype(F32)
            attn_in_ref[rows, :] = (values * inverse_rms(values) * gain_ref[...]).astype(BF16)

    @pl.loop(0, blocks)
    def _(block):
        rows = pl.ds(pl.multiple_of(block * BLOCK, BLOCK), BLOCK)
        normed = attn_in_ref[rows, :]
        cosines = cos_ref[rows, :]
        sines = sin_ref[rows, :]
        query = turn(nn(normed, wq_ref[...]), cosines, sines) * HEAD_DIM**-0.5
        qkv_ref[0, rows, :] = query.astype(BF16)
        qkv_ref[1, rows, :] = turn(nn(normed, wk_ref[...]), cosines, sines).astype(BF16)
        qkv_ref[2, rows, :] = nn(normed, wv_ref[...]).astype(BF16)

    for block in range(blocks):
        first = max(0, block - reach) * BLOCK
        last = (block + 1) * BLOCK
        span = last - first
        rows = slice(block * BLOCK, last)
        row_ids = iota((BLOCK, span), 0) + block * BLOCK
        col_ids = iota((BLOCK, span), 1) + first
        seen = (col_ids <= row_ids) & (segc_ref[rows, :] == segr_ref[0:1, first:last])
        bias_ref[:, 0:span] = jnp.where(seen, 0.0, NEGATIVE)
        attended = []
        logs = log_ref[rows, :]
        for head in range(GROUP):
            mask = head_mask(head)
            scores = nt(qkv_ref[0, rows, :] * mask, qkv_ref[1, first:last, :]) + bias_ref[:, 0:span]
            top = jnp.max(scores, axis=1, keepdims=True)
            weights = jnp.exp(scores - top).astype(BF16)
            value = qkv_ref[2, first:last, :] * mask + (1 - mask)
            mixed = nn(weights, value)
            own = iota(mixed.shape, 1) // HEAD_DIM == head
            total = jnp.max(jnp.where(own, 0.0, mixed), axis=1, keepdims=True)
            attended.append(jnp.where(own, mixed / total, 0.0))
            logs = jnp.where(
                iota(logs.shape, 1) == step * GROUP + head, top + jnp.log(total), logs
            )
        log_ref[rows, :] = logs
        out_ref[rows, :] = (attended[0] + attended[1] + attended[2] + attended[3]).astype(BF16)

    @pl.when(step == pl.num_programs(0) - 1)
    def _():
        lse_ref[...] = log_ref[...].T[0 : lse_ref.shape[0], :]


def middle_kernel(
    kinds, ao_ref, wo_ref, tok_ref, small_ref, prev_ref, routes_ref, target_ref,
    resid_ref, scal_ref, send_ref, ffn_ref, first_ref, second_ref,
):
    tokens, width = tok_ref.shape
    gain = small_ref[...].astype(F32).T[kinds + 7 : kinds + 8, :]

    @pl.loop(0, tokens // BLOCK)
    def _(block):
        rows = pl.ds(pl.multiple_of(block * BLOCK, BLOCK), BLOCK)
        resid = tok_ref[rows, :].astype(F32) + nn(ao_ref[rows, :], wo_ref[...])
        resid_ref[rows, :] = resid
        inverse = inverse_rms(resid)
        low = (resid * inverse * gain).astype(BF16)
        ffn_ref[rows, :] = low
        logits = nn(low, small_ref[...]) + prev_ref[rows, :]
        lane = iota(logits.shape, 1)

        def pick(index):
            return jnp.sum(jnp.where(lane == index, logits, 0.0), axis=1, keepdims=True)

        def pair(left, right):
            top = jnp.maximum(left, right)
            left = jnp.exp(left - top)
            right = jnp.exp(right - top)
            total = left + right
            return left / total, right / total

        gates = pair(pick(routes_ref[rows, 0:1]), pick(routes_ref[rows, 1:2]))
        one = pair(pick(kinds), pick(kinds + 1))
        two = pair(pick(kinds + 2), pick(kinds + 3))
        scal = jnp.zeros_like(logits)
        for index, value in enumerate(gates + one + two + (inverse,)):
            scal = jnp.where(lane == index, value, scal)
        scal_ref[rows, :] = scal
        for gate, ref in zip(gates, (first_ref, second_ref)):
            high, rest = split_low(gate)
            ref[rows, :] = jnp.where(
                lane == 0, high.astype(F32), jnp.where(lane == 1, rest.astype(F32), 0.0)
            ).astype(BF16)

    @pl.loop(0, send_ref.shape[0])
    def _(expert):
        slots = iota((CAP, tokens), 0) + expert * CAP
        hot_one = (target_ref[0:1, :] == slots).astype(F32)
        hot_two = (target_ref[1:2, :] == slots).astype(F32)
        send_ref[expert, :, 0:width] = nn((hot_one + hot_two).astype(BF16), ffn_ref[...]).astype(
            BF16
        )
        send_ref[expert, :, width:] = (
            nn(hot_one.astype(BF16), first_ref[...]) + nn(hot_two.astype(BF16), second_ref[...])
        ).astype(BF16)


def expert_kernel(
    recv_ref, cot_ref, wg_ref, wu_ref, wo_ref, front_ref, ret_ref, out_acc, row_acc,
):
    step = pl.program_id(0)
    total, width = out_acc.shape
    tile = 512

    @pl.when(step == 0)
    def _():
        out_acc[...] = jnp.zeros_like(out_acc)
        row_acc[...] = jnp.zeros_like(row_acc)

    @pl.loop(0, total // tile)
    def _(block):
        rows = pl.ds(pl.multiple_of(block * tile, tile), tile)
        token = recv_ref[rows, 0:width]
        extra = recv_ref[rows, width:].astype(F32)
        gate_weight = extra[:, 0:1] + extra[:, 1:2]
        gate = nn(token, wg_ref[...])
        up = nn(token, wu_ref[...])
        grad = nt(cot_ref[rows, :], wo_ref[...]) * gate_weight
        sig = jax.nn.sigmoid(gate)
        act = gate * sig
        hidden = act * up
        out_acc[rows, :] += nn(hidden.astype(BF16), wo_ref[...])
        front_ref[2, rows, :] = (hidden * gate_weight).astype(BF16)
        gate_grad = (grad * up * sig * (1.0 + gate * (1.0 - sig))).astype(BF16)
        up_grad = (grad * act).astype(BF16)
        front_ref[0, rows, :] = gate_grad
        front_ref[1, rows, :] = up_grad
        row_acc[rows, :] += nt(gate_grad, wg_ref[...]) + nt(up_grad, wu_ref[...])

    @pl.when(step == pl.num_programs(0) - 1)
    def _():
        @pl.loop(0, total // CAP)
        def _(peer):
            rows = pl.ds(pl.multiple_of(peer * CAP, CAP), CAP)
            ret_ref[peer, 0:CAP, :] = out_acc[rows, :].astype(BF16)
            ret_ref[peer, CAP:, :] = row_acc[rows, :].astype(BF16)


def expert_grad_kernel(recv_ref, cot_ref, front_ref, gate_ref, up_ref, wout_ref, turned_ref):
    step = pl.program_id(0)
    width = turned_ref.shape[0]

    @pl.when(step == 0)
    def _():
        turned_ref[...] = recv_ref[:, 0:width].T

    wout_ref[...] = tn(front_ref[2], cot_ref[...]).astype(BF16)
    gate_ref[...] = nn(turned_ref[...], front_ref[0]).astype(BF16)
    up_ref[...] = nn(turned_ref[...], front_ref[1]).astype(BF16)


def combine_kernel(
    kinds, experts, ret_ref, target_ref, routes_ref, scal_ref, resid_ref, cot_ref, ao_ref,
    small_ref, wo_ref, mix_ref, prevt_ref, ind_ref,
    mixed_ref, prev_ref, mid_ref, proj_ref, attn_ref, delta_ref, minor_ref, vec_ref, gain_ref,
    gmix_ref, rows_ref,
):
    step = pl.program_id(0)

    @pl.when(step == 0)
    def _():
        rows_ref[...] = small_ref[...].astype(F32).T
        minor_ref[...] = jnp.zeros_like(minor_ref)
        vec_ref[...] = jnp.zeros_like(vec_ref)
        gain_ref[...] = jnp.zeros_like(gain_ref)
        gmix_ref[...] = jnp.zeros_like(gmix_ref)

    width = resid_ref.shape[1]
    slots = experts * CAP
    resid = resid_ref[...]
    cot = cot_ref[...]
    upstream = cot.astype(F32)
    scal = scal_ref[...]
    routes = (routes_ref[:, 0:1], routes_ref[:, 1:2])
    targets = (target_ref[:, 0:1], target_ref[:, 1:2])
    gates = (scal[:, 0:1], scal[:, 1:2])
    one_keep, one_vec = scal[:, 2:3], scal[:, 3:4]
    two_keep, two_vec = scal[:, 4:5], scal[:, 5:6]
    inverse = scal[:, 6:7]
    gain = rows_ref[kinds + 7 : kinds + 8, :]
    vec_one = rows_ref[kinds + 4 : kinds + 5, :]
    vec_two = rows_ref[kinds + 5 : kinds + 6, :]
    normed = resid * inverse
    ffn_norm = normed * gain
    low = ffn_norm.astype(BF16)
    slot_ids = iota((BLOCK, slots), 1)
    hots = [(target == slot_ids).astype(F32) for target in targets]
    outs = ret_ref[:, 0:CAP, :].reshape(slots, width)
    backs = ret_ref[:, CAP:, :].reshape(slots, width)
    branches = [nn(hot.astype(BF16), outs) for hot in hots]
    back = nn((hots[0] + hots[1]).astype(BF16), backs)

    def weight(kind):
        return sum(
            jnp.where(route == kind, gate, 0.0) for route, gate in zip(routes, gates)
        )

    weight_copy = weight(experts + 1)
    weight_one = weight(experts + 2)
    weight_two = weight(experts + 3)
    keep = weight_copy + weight_one * one_keep + weight_two * two_keep
    mixed_ref[...] = (
        resid
        + gates[0] * branches[0]
        + gates[1] * branches[1]
        + keep * ffn_norm
        + (weight_one * one_vec) * vec_one
        + (weight_two * two_vec) * vec_two
    ).astype(BF16)
    dot_norm = jnp.sum(upstream * ffn_norm, axis=1, keepdims=True)
    dot_one = jnp.sum(upstream * vec_one, axis=1, keepdims=True)
    dot_two = jnp.sum(upstream * vec_two, axis=1, keepdims=True)
    grads = []
    for route, branch in zip(routes, branches):
        grads.append(
            jnp.sum(branch * upstream, axis=1, keepdims=True)
            + jnp.where(route == experts + 1, dot_norm, 0.0)
            + jnp.where(route == experts + 2, one_keep * dot_norm + one_vec * dot_one, 0.0)
            + jnp.where(route == experts + 3, two_keep * dot_norm + two_vec * dot_two, 0.0)
        )
    mean_grad = gates[0] * grads[0] + gates[1] * grads[1]
    lane = iota((BLOCK, LANES), 1)
    wide = jnp.zeros((BLOCK, LANES), F32)
    for route, gate, grad in zip(routes, gates, grads):
        wide = jnp.where(lane == route, gate * (grad - mean_grad), wide)
    for index, keep_part, vec_part, grad_weight, dot in (
        (kinds, one_keep, one_vec, weight_one, dot_one),
        (kinds + 2, two_keep, two_vec, weight_two, dot_two),
    ):
        keep_grad = grad_weight * dot_norm
        vec_grad = grad_weight * dot
        both = keep_part * keep_grad + vec_part * vec_grad
        wide = jnp.where(lane == index, keep_part * (keep_grad - both), wide)
        wide = jnp.where(lane == index + 1, vec_part * (vec_grad - both), wide)
    wide_low = wide.astype(BF16)
    wide_back = wide_low.astype(F32)
    minor_ref[...] += nn(wide_back.T.astype(BF16), low)
    share = jnp.where(lane == 0, weight_one * one_vec, 0.0)
    share = jnp.where(lane == 1, weight_two * two_vec, share)
    high, rest = split_low(share.T)
    vec_ref[...] += nn(high, cot) + nn(rest, cot)
    prev_ref[...] = nn(wide_low, mix_ref[...])[:, 0:kinds]
    gmix_ref[...] += jnp.dot(
        prevt_ref[...], wide_back, precision=HIGHEST_PRECISION, preferred_element_type=F32
    )
    grad_two = back + nt(wide_low, small_ref[...]) + keep * upstream
    gain_ref[...] += jnp.sum(grad_two * normed, axis=0, keepdims=True)
    mid = upstream + norm_back(grad_two * gain, normed, inverse)
    mid_ref[...] = mid
    proj = mid.astype(BF16)
    proj_ref[...] = proj
    attn = nt(proj, wo_ref[...]).astype(BF16)
    attn_ref[...] = attn
    high, rest = split_low(attn.astype(F32) * ao_ref[...].astype(F32))
    delta_ref[...] = nt(ind_ref[...], high) + nt(ind_ref[...], rest)


def attend_back_kernel(
    gain_row, qkv_ref, grad_ref, lse_ref, delta_ref, cos_ref, sin_ref, segc_ref, segr_ref,
    wq_ref, wk_ref, wv_ref, attn_in_ref, ao_ref, proj_ref, tok_ref, mid_ref, small_ref,
    weight_ref, gtok_ref, gain_ref, dq_ref, dk_ref, dv_ref, bias_ref, in_t_ref, ao_t_ref, acc_ref,
):
    step = pl.program_id(0)
    tokens = tok_ref.shape[0]
    blocks = tokens // BLOCK
    reach = DOC_MAX // BLOCK

    @pl.when(step == 0)
    def _():
        in_t_ref[...] = attn_in_ref[...].T
        ao_t_ref[...] = ao_ref[...].T
        acc_ref[...] = jnp.zeros_like(acc_ref)

    dq_ref[...] = jnp.zeros_like(dq_ref)
    for block in range(blocks):
        first = block * BLOCK
        last = min(blocks, block + reach + 1) * BLOCK
        span = last - first
        keys = slice(first, first + BLOCK)
        key_ids = iota((BLOCK, span), 0) + first
        row_ids = iota((BLOCK, span), 1) + first
        seen = (key_ids <= row_ids) & (segc_ref[keys, :] == segr_ref[0:1, first:last])
        bias_ref[:, 0:span] = jnp.where(seen, 0.0, NEGATIVE)
        key = qkv_ref[1, keys, :]
        value = qkv_ref[2, keys, :]
        key_grad = None
        for head in range(GROUP):
            mask = head_mask(head)
            index = step * GROUP + head
            query = qkv_ref[0, first:last, :] * mask
            upstream = grad_ref[first:last, :] * mask
            scores = nt(key, query) + bias_ref[:, 0:span]
            probs = jnp.exp(scores - lse_ref[pl.ds(index, 1), first:last])
            prob_grad = nt(value, upstream)
            score_grad = (probs * (prob_grad - delta_ref[pl.ds(index, 1), first:last])).astype(BF16)
            dv = nn(probs.astype(BF16), upstream)
            dk = nn(score_grad, query)
            dq_ref[first:last, :] += tn(score_grad, key * mask)
            key_grad = dk if key_grad is None else key_grad + dk
            value_grad = dv if head == 0 else value_grad + dv
        dk_ref[keys, :] = key_grad
        dv_ref[keys, :] = value_grad.astype(BF16)

    @pl.loop(0, blocks)
    def _(block):
        rows = pl.ds(pl.multiple_of(block * BLOCK, BLOCK), BLOCK)
        cosines = cos_ref[rows, :]
        sines = -sin_ref[rows, :]
        dq = turn(dq_ref[rows, :] * HEAD_DIM**-0.5, cosines, sines)
        dk = turn(dk_ref[rows, :], cosines, sines)
        dq_ref[rows, :] = dq
        dk_ref[rows, :] = dk
        acc_ref[rows, :] += (
            nt(dq.astype(BF16), wq_ref[...])
            + nt(dk.astype(BF16), wk_ref[...])
            + nt(dv_ref[rows, :], wv_ref[...])
        )

    halves = GROUP_LANES // LANES
    for index, (turned, grads) in enumerate(
        ((in_t_ref, dq_ref), (in_t_ref, dk_ref), (in_t_ref, dv_ref), (ao_t_ref, proj_ref))
    ):
        product = nn(turned[...], grads[...].astype(BF16)).astype(BF16)
        for half in range(halves):
            weight_ref[index * halves + half] = product[:, half * LANES : (half + 1) * LANES]

    @pl.when(step == pl.num_programs(0) - 1)
    def _():
        gain = small_ref[...].astype(F32).T[gain_row : gain_row + 1, :]
        gain_ref[...] = jnp.zeros_like(gain_ref)

        @pl.loop(0, blocks)
        def _(block):
            rows = pl.ds(pl.multiple_of(block * BLOCK, BLOCK), BLOCK)
            values = tok_ref[rows, :].astype(F32)
            inverse = inverse_rms(values)
            normed = values * inverse
            grad = acc_ref[rows, :]
            gain_ref[...] += jnp.sum(grad * normed, axis=0, keepdims=True)
            gtok_ref[rows, :] = mid_ref[rows, :] + norm_back(grad * gain, normed, inverse)


def add_low(left, right):
    return (left.astype(F32) + right.astype(F32)).astype(BF16)


def over_parts(values, bit):
    return lax.ppermute(values, "dp", [(d, d ^ bit) for d in range(8)])


def greet(targets):
    barrier = pltpu.get_barrier_semaphore()
    for present, target in targets:
        @pl.when(present)
        def _():
            pl.semaphore_signal(barrier, inc=1, device_id=target, device_id_type=MESH)
    pl.semaphore_wait(barrier, sum(present.astype(jnp.int32) for present, _ in targets))


def gather_kernel(part_ref, out_ref, send_sem, recv_sem, local_sem):
    me = lax.axis_index("dp")
    owner = lax.axis_index("expert")
    here, side = me // 2, me % 2
    core = owner % 2
    up = ((2 * jnp.minimum(here + 1, 3) + side), here < 3)
    down = ((2 * jnp.maximum(here - 1, 0) + side), here > 0)
    across = 2 * here + 1 - side
    partner = owner + 1 - 2 * core
    always = here >= 0
    routes = (
        (up[1], {"dp": up[0]}),
        (down[1], {"dp": down[0]}),
        (always, {"dp": across}),
        (always, {"expert": partner}),
    )
    greet(routes)

    def copy(index, half, route, source=None):
        return pltpu.make_async_remote_copy(
            src_ref=out_ref.at[index, half] if source is None else source,
            dst_ref=out_ref.at[index, half],
            send_sem=send_sem.at[route, index],
            recv_sem=recv_sem.at[half, index],
            device_id=routes[route][1],
            device_id_type=MESH,
        )

    def arrive(index, half):
        copy(index, half, 2).wait_recv()

    local = pltpu.make_async_copy(part_ref, out_ref.at[me], local_sem)
    local.start()
    for route in range(3):
        @pl.when(routes[route][0])
        def _():
            copy(me, core, route, part_ref.at[core]).start()
    for distance in range(1, 5):
        for toward, forward, present in (
            (here - distance, 0, here >= distance),
            (here + distance, 1, here + distance <= 3),
        ):
            index = 2 * jnp.clip(toward, 0, 3) + side

            @pl.when(present)
            def _():
                arrive(index, core)
                copy(index, core, 2).start()
                copy(index, core, 3).start()

            @pl.when(present & routes[forward][0])
            def _():
                copy(index, core, forward).start()
        for sign in (-1, 1):
            if distance == 1 and sign == 1:
                continue
            toward = here + sign * (distance - 1)
            index = 2 * jnp.clip(toward, 0, 3) + 1 - side

            @pl.when((toward >= 0) & (toward <= 3))
            def _():
                arrive(index, core)
                copy(index, core, 3).start()
    for offset in range(1, 8):
        index = (me + offset) % 8
        arrive(index, 1 - core)
        copy(index, core, 3).wait_send()
    local.wait()
    for route in range(3):
        @pl.when(routes[route][0])
        def _():
            copy(me, core, route, part_ref.at[core]).wait_send()
    for distance in range(1, 4):
        for toward, forward, present in (
            (here - distance, 0, here >= distance),
            (here + distance, 1, here + distance <= 3),
        ):
            index = 2 * jnp.clip(toward, 0, 3) + side

            @pl.when(present)
            def _():
                copy(index, core, 2).wait_send()

            @pl.when(present & routes[forward][0])
            def _():
                copy(index, core, forward).wait_send()


def gather_parts(packed):
    rows, columns = packed.shape
    whole = pl.pallas_call(
        gather_kernel,
        in_specs=[pl.BlockSpec(memory_space=pltpu.VMEM)],
        out_specs=pl.BlockSpec(memory_space=pl.ANY),
        out_shape=jax.ShapeDtypeStruct((8, 2, rows // 2, columns), BF16),
        scratch_shapes=[
            pltpu.SemaphoreType.DMA((4, 8)),
            pltpu.SemaphoreType.DMA((2, 8)),
            pltpu.SemaphoreType.DMA,
        ],
        compiler_params=params(collective_id=0, has_side_effects=True),
        cost_estimate=cost(10e9, 10e6),
        name="gather_parts",
    )(packed.reshape(2, rows // 2, columns))
    return whole.reshape(8 * rows, columns)


def add_planes(target, left, right):
    @pl.loop(0, target.shape[0])
    def _(index):
        total = left[index].astype(F32) + right[index].astype(F32)
        target[index] = total.astype(target.dtype)


def reduce_kernel(
    gate_ref, up_ref, risen_ref, fallen_ref, pair_ref, weight_ref, minor_ref,
    gate_out, up_out, down_out, weight_out, minor_out,
    gate_in, up_in, line_in, gate_stage, up_stage, line_stage, pair_in, core_in, core_sum, side_in, side_sum, cross_in, line_ref, line_sum_ref,
    small_in, small_sum, piece_send, piece_recv, other_send, other_recv,
):
    me = lax.axis_index("dp")
    owner = lax.axis_index("expert")
    here, flank = me // 2, me % 2
    core, side = owner % 2, owner // 2
    rising = {"dp": 2 * jnp.minimum(here + 1, 3) + flank}
    falling = {"dp": 2 * jnp.maximum(here - 1, 0) + flank}
    across = {"dp": me + 1 - 2 * flank}
    partner = {"expert": owner + 1 - 2 * core}
    beside = {"expert": owner + 2 - 4 * side}
    always = here >= 0
    greet(((here < 3, rising), (here > 0, falling), (always, across), (always, partner),
           (always, beside)))
    pieces = (
        (gate_ref, gate_in, gate_stage),
        (up_ref, up_in, up_stage),
        (line_ref, line_in, line_stage),
    )

    def piece_copy(piece, turn_index, way, source):
        return pltpu.make_async_remote_copy(
            src_ref=source,
            dst_ref=pieces[piece][1].at[way, turn_index],
            send_sem=piece_send.at[piece, turn_index, way],
            recv_sem=piece_recv.at[piece, turn_index, way],
            device_id=(rising, falling)[way],
            device_id_type=MESH,
        )

    def other_copy(index, source, target, device):
        return pltpu.make_async_remote_copy(
            src_ref=source, dst_ref=target, send_sem=other_send.at[index],
            recv_sem=other_recv.at[index], device_id=device, device_id_type=MESH,
        )

    def direct(piece, turn_index):
        own = pieces[piece][0]

        @pl.when(here == 0)
        def _():
            piece_copy(piece, turn_index, 0, own.at[3 - turn_index]).start()

        @pl.when(here == 3)
        def _():
            piece_copy(piece, turn_index, 1, own.at[turn_index]).start()

    def relayed(turn_index):
        return (
            (0, (here > 0) & (here < 3 - turn_index), 3 - turn_index),
            (1, (here < 3) & (here > turn_index), turn_index),
        )

    def relay(piece, turn_index):
        own, landed, stage = pieces[piece]
        for way, present, chunk in relayed(turn_index):
            if piece == 0:
                present = present & ((here != 1) if way == 0 else (here != 2))

            @pl.when(present)
            def _():
                copy = piece_copy(piece, turn_index, way, stage.at[way, turn_index])
                copy.wait_recv()
                add_planes(
                    stage.at[way, turn_index], own.at[chunk], landed.at[way, turn_index]
                )
                copy.start()

    def early(turn_index):
        own, landed, stage = pieces[0]
        for way, place, chunk in ((0, 1, 3 - turn_index), (1, 2, turn_index)):
            @pl.when(here == place)
            def _():
                add_planes(
                    stage.at[way, turn_index], own.at[chunk], landed.at[way, turn_index]
                )
                piece_copy(0, turn_index, way, stage.at[way, turn_index]).start()

    def finish(piece, target):
        own, landed, stage = pieces[piece]
        lower = jnp.minimum(3 - here, 2)
        upper = jnp.minimum(here, 2)

        @pl.when((here > (1 if piece == 0 else 0)))
        def _():
            piece_copy(piece, lower, 0, stage.at[0, 0]).wait_recv()

        @pl.when(here < (2 if piece == 0 else 3))
        def _():
            piece_copy(piece, upper, 1, stage.at[0, 0]).wait_recv()

        @pl.when(here == 0)
        def _():
            add_planes(target, own.at[here], landed.at[1, upper])

        @pl.when(here == 3)
        def _():
            add_planes(target, own.at[here], landed.at[0, lower])

        @pl.when((here > 0) & (here < 3))
        def _():
            @pl.loop(0, target.shape[0])
            def _(index):
                total = (
                    own[here, index].astype(F32)
                    + landed[0, lower, index].astype(F32)
                    + landed[1, upper, index].astype(F32)
                )
                target[index] = total.astype(target.dtype)

    def drain(piece):
        own, _, stage = pieces[piece]
        for turn_index in range(0 if piece == 0 else 3):
            @pl.when(here == 0)
            def _():
                piece_copy(piece, turn_index, 0, own.at[3 - turn_index]).wait_send()

            @pl.when(here == 3)
            def _():
                piece_copy(piece, turn_index, 1, own.at[turn_index]).wait_send()
        for turn_index in range(2):
            for way, present, _ in relayed(turn_index):
                @pl.when(present)
                def _():
                    piece_copy(
                        piece, turn_index, way, stage.at[way, turn_index]
                    ).wait_send()

    half = core_in.shape[0]
    quarter = half // 2
    core_weight = other_copy(0, weight_ref.at[pl.ds(half * (1 - core), half)], core_in, partner)
    core_small = other_copy(1, minor_ref, small_in.at[0], partner)
    side_weight = other_copy(2, core_sum.at[pl.ds(quarter * (1 - side), quarter)], side_in, beside)
    side_small = other_copy(3, small_sum.at[0], small_in.at[1], beside)
    cross_weight = [
        other_copy(4 + z, side_sum.at[:, 2 * z + 1 - flank], cross_in.at[z], across)
        for z in range(4)
    ]
    cross_small = other_copy(8, small_sum.at[1], small_in.at[2], across)
    rise_small = other_copy(9, small_sum.at[3], small_in.at[3], rising)
    fall_small = other_copy(10, small_sum.at[4], small_in.at[4], falling)
    mine = half * core + quarter * side
    own_part = weight_out.at[pl.ds(mine, quarter)]
    own_half = weight_out.at[pl.ds(half * core, half)]
    side_back = other_copy(11, own_part, own_part, beside)
    core_back = other_copy(12, own_half, own_half, partner)

    pair_copy = other_copy(13, pair_ref.at[1 - flank], pair_in, across)
    core_weight.start()
    core_small.start()
    pair_copy.start()
    for turn_index in range(3):
        direct(1, turn_index)

    @pl.when(here == 1)
    def _():
        for turn_index in range(3):
            gate_in[0, turn_index] = risen_ref[2 - turn_index]

    @pl.when(here == 2)
    def _():
        for turn_index in range(3):
            gate_in[1, turn_index] = fallen_ref[turn_index]

    for turn_index in range(2):
        early(turn_index)
    core_weight.wait_recv()
    core_small.wait_recv()
    add_planes(core_sum, weight_ref.at[pl.ds(half * core, half)], core_in)
    small_sum[0] = minor_ref[...] + small_in[0]
    side_weight.start()
    side_small.start()
    for piece in (0, 1):
        relay(piece, 0)
    pair_copy.wait_recv()
    add_planes(down_out, pair_ref.at[flank], pair_in)
    side_weight.wait_recv()
    side_small.wait_recv()
    add_planes(side_sum, core_sum.at[pl.ds(quarter * side, quarter)], side_in)
    small_sum[1] = small_sum[0] + small_in[1]
    for copy in cross_weight:
        copy.start()
    cross_small.start()
    for piece in (0, 1):
        relay(piece, 1)
    for copy in cross_weight:
        copy.wait_recv()
    cross_small.wait_recv()
    for z in range(4):
        add_planes(line_ref.at[z], side_sum.at[:, 2 * z + flank], cross_in.at[z])
    small_sum[2] = small_sum[1] + small_in[2]
    small_sum[3] = small_sum[2]
    small_sum[4] = small_sum[2]
    for turn_index in range(3):
        direct(2, turn_index)

    @pl.when(here == 0)
    def _():
        rise_small.start()

    @pl.when(here == 3)
    def _():
        fall_small.start()

    for turn_index in range(2):
        relay(2, turn_index)

    @pl.when(here > 0)
    def _():
        rise_small.wait_recv()
        small_sum[3] = small_sum[2] + small_in[3]

    @pl.when((here > 0) & (here < 3))
    def _():
        rise_small.start()

    @pl.when(here < 3)
    def _():
        fall_small.wait_recv()
        small_sum[4] = small_sum[2] + small_in[4]

    @pl.when((here > 0) & (here < 3))
    def _():
        fall_small.start()

    minor_out[...] = small_sum[3] + small_sum[4] - small_sum[2]
    finish(2, line_sum_ref)
    for index in range(quarter):
        weight_out[mine + index] = line_sum_ref[index]
    side_back.start()
    finish(0, gate_out)
    side_back.wait_recv()
    core_back.start()
    finish(1, up_out)
    core_back.wait_recv()
    for piece in range(3):
        drain(piece)
    for copy in (core_weight, core_small, side_weight, side_small, *cross_weight, cross_small,
                 side_back, core_back, pair_copy):
        copy.wait_send()

    @pl.when(here < 3)
    def _():
        rise_small.wait_send()

    @pl.when(here > 0)
    def _():
        fall_small.wait_send()


def reduce_parts(kept, down, weights, minor):
    gate, up = kept[:2]
    kept = [piece.reshape(-1, piece.shape[1] // 32, 32, piece.shape[2]) for piece in kept]
    pair = down.reshape(2, down.shape[1] // 32, 32, down.shape[2])
    blocks, width, lanes = weights.shape
    rows = width // 8
    plane = (rows, lanes)
    chunks = [piece.shape[1:] for piece in kept[:2]]
    line = (blocks // 4,) + plane
    low = [pltpu.VMEM((2, 3) + chunk, BF16) for chunk in chunks + [line]]
    stages = [pltpu.VMEM((2, 2) + chunk, BF16) for chunk in chunks + [line]]
    outs = pl.pallas_call(
        reduce_kernel,
        in_specs=[pl.BlockSpec(memory_space=pltpu.VMEM)] * 7,
        out_specs=[pl.BlockSpec(memory_space=pltpu.VMEM)] * 5,
        out_shape=[jax.ShapeDtypeStruct(chunk, F32) for chunk in chunks + [pair.shape[1:]]]
        + [
            jax.ShapeDtypeStruct((blocks,) + plane, BF16),
            jax.ShapeDtypeStruct(minor.shape, F32),
        ],
        scratch_shapes=[
            *low,
            *stages,
            pltpu.VMEM(pair.shape[1:], BF16),
            pltpu.VMEM((blocks // 2, 8) + plane, BF16),
            pltpu.VMEM((blocks // 2, 8) + plane, BF16),
            pltpu.VMEM((blocks // 4, 8) + plane, BF16),
            pltpu.VMEM((blocks // 4, 8) + plane, BF16),
            pltpu.VMEM((4,) + line, BF16),
            pltpu.VMEM((4,) + line, BF16),
            pltpu.VMEM(line, BF16),
            pltpu.VMEM((5,) + minor.shape, F32),
            pltpu.VMEM((5,) + minor.shape, F32),
            pltpu.SemaphoreType.DMA((3, 3, 2)),
            pltpu.SemaphoreType.DMA((3, 3, 2)),
            pltpu.SemaphoreType.DMA((14,)),
            pltpu.SemaphoreType.DMA((14,)),
        ],
        compiler_params=params(collective_id=1, has_side_effects=True),
        name="reduce_parts",
    )(*kept, pair, weights.reshape(blocks, 8, rows, lanes), minor)
    shapes = (gate.shape[1:], up.shape[1:], down.shape[1:])
    shares = [out.reshape(shape) for out, shape in zip(outs, shapes)]
    return shares, outs[3], outs[4]


FF_TILE = 256


def exchange_kernel(
    send_ref, cot_ref, win_ref, wout_ref,
    gate_keep, gate_away, up_keep, up_away, own_down, one_down, two_down, three_down, return_out,
    recv, cot, gate_w, up_w, down_w, front, turned, out_acc, row_acc, ret, gate_g, up_g, down_g,
    token_send, token_recv, back_send, back_recv, load_sem, weight_sem, store_sem, down_sem, own_sem,
):
    me = lax.axis_index("expert")
    spot = lax.axis_index("dp")
    here, flank = spot // 2, spot % 2
    line_peers = (here, here + 1 - 2 * (here % 2), here + 2 - 4 * (here // 2), 3 - here)
    down_parts = (own_down, one_down, two_down, three_down)
    share = gate_w.shape[0] // 8
    core, side = me % 2, me // 2
    partner = me + 1 - 2 * core
    beside = me + 2 - 4 * side
    corner = partner + 2 - 4 * side
    peers = (me, beside, corner, partner)
    always = me >= 0
    width = out_acc.shape[1]
    ff = down_w.shape[0]
    tiles = ff // FF_TILE
    greet([(always, {"expert": peer}) for peer in peers[1:]])

    def token_copy(slot):
        return pltpu.make_async_remote_copy(
            src_ref=send_ref.at[peers[slot]], dst_ref=recv.at[slot],
            send_sem=token_send.at[slot], recv_sem=token_recv.at[slot],
            device_id={"expert": peers[slot]}, device_id_type=MESH,
        )

    def back_copy(slot):
        return pltpu.make_async_remote_copy(
            src_ref=ret.at[slot], dst_ref=return_out.at[me],
            send_sem=back_send.at[slot], recv_sem=back_recv.at[slot],
            device_id={"expert": peers[slot]}, device_id_type=MESH,
        )

    def tile_slice(tile):
        return pl.ds(pl.multiple_of(tile * FF_TILE, FF_TILE), FF_TILE)

    def weight_copies(tile):
        cols = tile_slice(tile)
        shifted = pl.ds(pl.multiple_of(ff + tile * FF_TILE, FF_TILE), FF_TILE)
        return (
            pltpu.make_async_copy(
                win_ref.at[:, cols], gate_w.at[:, cols], weight_sem.at[0, tile]
            ),
            pltpu.make_async_copy(
                win_ref.at[:, shifted], up_w.at[:, cols], weight_sem.at[1, tile]
            ),
            pltpu.make_async_copy(
                wout_ref.at[cols, :], down_w.at[cols, :], weight_sem.at[2, tile]
            ),
        )

    def side_copy(piece, index, kept):
        source = (gate_g, up_g)[piece].at[index * share : (index + 1) * share, :]
        target = ((gate_away, gate_keep), (up_away, up_keep))[piece][kept].at[index // 2]
        return pltpu.make_async_copy(source, target, store_sem.at[piece, index])

    def down_copy(tile, distance):
        return pltpu.make_async_copy(
            down_g.at[tile_slice(tile), :], down_parts[distance].at[tile % 2], down_sem.at[tile]
        )

    for slot in (1, 2, 3):
        token_copy(slot).start()
    loads = [pltpu.make_async_copy(send_ref.at[me], recv.at[0], load_sem.at[0])] + [
        pltpu.make_async_copy(cot_ref.at[peers[slot]], cot.at[slot], load_sem.at[1 + slot])
        for slot in range(4)
    ]
    for load in loads:
        load.start()

    @pl.loop(0, tiles)
    def _(tile):
        for copy in weight_copies(tile):
            copy.start()

    for load in loads:
        load.wait()

    def work(slot):
        extra = recv[slot, :, width:].astype(F32)
        gate_weight = extra[:, 0:1] + extra[:, 1:2]
        out_acc[...] = jnp.zeros_like(out_acc)
        row_acc[...] = jnp.zeros_like(row_acc)

        @pl.loop(0, tiles)
        def _(tile):
            cols = tile_slice(tile)
            if slot == 0:
                for copy in weight_copies(tile):
                    copy.wait()
            token = recv[slot, :, 0:width]
            gate = nn(token, gate_w[:, cols])
            up = nn(token, up_w[:, cols])
            grad = nt(cot[slot], down_w[cols, :]) * gate_weight
            sig = jax.nn.sigmoid(gate)
            act = gate * sig
            hidden = act * up
            out_acc[...] += nn(hidden.astype(BF16), down_w[cols, :])
            front[2, slot, :, cols] = (hidden * gate_weight).astype(BF16)
            gate_grad = (grad * up * sig * (1.0 + gate * (1.0 - sig))).astype(BF16)
            up_grad = (grad * act).astype(BF16)
            front[0, slot, :, cols] = gate_grad
            front[1, slot, :, cols] = up_grad
            row_acc[...] += nt(gate_grad, gate_w[:, cols]) + nt(up_grad, up_w[:, cols])

        ret[slot, 0:CAP, :] = out_acc[...].astype(BF16)
        ret[slot, CAP:, :] = row_acc[...].astype(BF16)
        turned[:, slot * CAP : (slot + 1) * CAP] = recv[slot, :, 0:width].T

    own_back = pltpu.make_async_copy(ret.at[0], return_out.at[me], own_sem)
    work(0)
    own_back.start()
    for slot in (1, 2, 3):
        token_copy(slot).wait_recv()
        work(slot)
        back_copy(slot).start()
    total = 4 * CAP

    @pl.loop(0, tiles)
    def _(tile):
        cols = tile_slice(tile)
        hidden = front[2, :, :, cols].reshape(total, FF_TILE)
        down_g[cols, :] = tn(hidden, cot[...].reshape(total, width)).astype(BF16)
        gate_g[:, cols] = nn(turned[...], front[0, :, :, cols].reshape(total, FF_TILE)).astype(BF16)
        up_g[:, cols] = nn(turned[...], front[1, :, :, cols].reshape(total, FF_TILE)).astype(BF16)
        for distance in range(4):
            @pl.when(tile // 2 == line_peers[distance])
            def _():
                down_copy(tile, distance).start()

    for piece in range(2):
        for index in range(8):
            for kept in range(2):
                @pl.when((flank == index % 2) if kept else (flank != index % 2))
                def _():
                    side_copy(piece, index, kept).start()

    for slot in (1, 2, 3):
        token_copy(slot).wait_send()
        back_copy(slot).wait_recv()
        back_copy(slot).wait_send()
    own_back.wait()

    for piece in range(2):
        for index in range(8):
            side_copy(piece, index, 1).wait()

    @pl.loop(0, tiles)
    def _(tile):
        down_copy(tile, 0).wait()


def exchange_experts(send, cot_rows, w_in, w_out):
    peers, cap, payload = send.shape
    ff, width = w_out.shape
    anywhere = pl.BlockSpec(memory_space=pl.ANY)
    tiles = ff // FF_TILE
    *grads, returned = pl.pallas_call(
        exchange_kernel,
        in_specs=[anywhere] * 4,
        out_specs=[anywhere] * 9,
        out_shape=[jax.ShapeDtypeStruct((4, width // 8, ff), BF16)] * 4
        + [jax.ShapeDtypeStruct((2, ff // 8, width), BF16)] * 4
        + [jax.ShapeDtypeStruct((peers, 2 * cap, width), BF16)],
        scratch_shapes=[
            pltpu.VMEM((peers, cap, payload), BF16),
            pltpu.VMEM((peers, cap, width), BF16),
            pltpu.VMEM((width, ff), BF16),
            pltpu.VMEM((width, ff), BF16),
            pltpu.VMEM((ff, width), BF16),
            pltpu.VMEM((3, peers, cap, ff), BF16),
            pltpu.VMEM((width, peers * cap), BF16),
            pltpu.VMEM((cap, width), F32),
            pltpu.VMEM((cap, width), F32),
            pltpu.VMEM((peers, 2 * cap, width), BF16),
            pltpu.VMEM((width, ff), BF16),
            pltpu.VMEM((width, ff), BF16),
            pltpu.VMEM((ff, width), BF16),
            pltpu.SemaphoreType.DMA((4,)),
            pltpu.SemaphoreType.DMA((4,)),
            pltpu.SemaphoreType.DMA((4,)),
            pltpu.SemaphoreType.DMA((4,)),
            pltpu.SemaphoreType.DMA((5,)),
            pltpu.SemaphoreType.DMA((3, tiles)),
            pltpu.SemaphoreType.DMA((2, 8)),
            pltpu.SemaphoreType.DMA((tiles,)),
            pltpu.SemaphoreType.DMA,
        ],
        compiler_params=params(collective_id=2, has_side_effects=True),
        cost_estimate=cost(18 * peers * cap * width * ff, 40e6),
        name="exchange_experts",
    )(send, cot_rows.reshape(peers, cap, width), w_in, w_out)
    return grads, returned


def plain_experts(send, cot_rows, w_in_one, w_out_one, swap):
    experts, _, payload = send.shape
    ff, width = w_out_one.shape
    recv = swap(send).reshape(experts * CAP, payload)

    slot_count = experts * CAP
    ff_tile = 256
    ff_tiles = ff // ff_tile
    slot_full = whole_block((slot_count, width))
    recv_full = whole_block((slot_count, payload))
    front_spec = pl.BlockSpec((3, slot_count, ff_tile), lambda j: (0, 0, j))
    front, ret = pl.pallas_call(
        expert_kernel,
        grid=(ff_tiles,),
        in_specs=[
            recv_full,
            slot_full,
            pl.BlockSpec((width, ff_tile), lambda j: (0, j)),
            pl.BlockSpec((width, ff_tile), lambda j: (0, ff_tiles + j)),
            pl.BlockSpec((ff_tile, width), lambda j: (j, 0)),
        ],
        out_specs=[front_spec, whole_block((experts, 2 * CAP, width))],
        out_shape=[
            jax.ShapeDtypeStruct((3, slot_count, ff), BF16),
            jax.ShapeDtypeStruct((experts, 2 * CAP, width), BF16),
        ],
        scratch_shapes=[pltpu.VMEM((slot_count, width), F32)] * 2,
        compiler_params=params(),
        cost_estimate=cost(12 * slot_count * width * ff, 26e6),
        name="expert",
    )(recv, cot_rows, w_in_one, w_in_one, w_out_one)
    returned = swap(ret)
    expert_grads = pl.pallas_call(
        expert_grad_kernel,
        grid=(ff_tiles,),
        in_specs=[recv_full, slot_full, front_spec],
        out_specs=[
            pl.BlockSpec((width, ff_tile), lambda j: (0, j)),
            pl.BlockSpec((width, ff_tile), lambda j: (0, j)),
            pl.BlockSpec((ff_tile, width), lambda j: (j, 0)),
        ],
        out_shape=[
            jax.ShapeDtypeStruct((width, ff), BF16),
            jax.ShapeDtypeStruct((width, ff), BF16),
            jax.ShapeDtypeStruct((ff, width), BF16),
        ],
        scratch_shapes=[pltpu.VMEM((width, slot_count), BF16)],
        compiler_params=params(),
        cost_estimate=cost(6 * slot_count * width * ff, 24e6),
        name="expert_grad",
    )(recv, cot_rows, front)
    return expert_grads, returned


def per_device(
    tokens, prev_scores, segments, routes, wqkv, wo, router, const_gate, const_vec, gain1, gain2,
    gate_mix, w_in, w_out, cotangent,
):
    tok_count, width = tokens.shape
    kinds = router.shape[1]
    experts = w_in.shape[0] * lax.axis_size("expert")
    ff = w_out.shape[1]
    qkv_cols = wqkv.shape[1]
    parts = lax.axis_size("dp")
    by_hand = parts == 8 and experts == 4
    small = jnp.concatenate(
        [router, const_gate, const_vec, gain1[:, None], gain2[:, None]], axis=1
    )
    packed = jnp.concatenate(
        [wqkv, wo, jnp.pad(small, ((0, 0), (0, LANES - small.shape[1])))], axis=1
    )
    if by_hand:
        whole = gather_parts(packed)
    else:
        whole = lax.all_gather(packed, "dp", axis=0, tiled=True)

    seq_len = segments.shape[1]
    positions = (jnp.arange(tok_count, dtype=jnp.int32) % seq_len).astype(F32)
    half = HEAD_DIM // 2
    frequency = 10000.0 ** (-jnp.arange(half).astype(F32) / half)
    angles = positions[:, None] * frequency[None, :]
    cosines = jnp.tile(jnp.cos(angles), (1, LANES // half))
    sines = jnp.tile(jnp.sin(angles), (1, LANES // half))
    signs = jnp.where(jnp.arange(LANES) % HEAD_DIM < half, -1.0, 1.0).astype(F32)
    sines = sines * signs[None, :]
    seg_col = segments.reshape(tok_count, 1)
    seg_row = segments.reshape(1, tok_count)

    names = jnp.arange(kinds, dtype=jnp.int32)
    hot = [routes[:, i : i + 1] == names[None, :] for i in range(2)]
    named = (hot[0] | hot[1]).astype(BF16)
    ids = jnp.arange(tok_count, dtype=jnp.int32)
    before = (ids[:, None] > ids[None, :]).astype(BF16)
    earlier = jnp.dot(before, named, preferred_element_type=F32)
    slots = [jnp.sum(jnp.where(h, earlier, 0.0), axis=1).astype(jnp.int32) for h in hot]
    targets = [
        jnp.where(routes[:, i] < experts, routes[:, i] * CAP + slots[i], experts * CAP)
        for i in range(2)
    ]
    target_row = jnp.stack(targets, axis=0)
    target_col = jnp.stack(targets, axis=1)
    prev_mix = jnp.dot(prev_scores, gate_mix.astype(F32), precision=HIGHEST_PRECISION)
    prev_mix = jnp.pad(prev_mix, ((0, 0), (0, LANES - kinds)))

    def swap(values):
        return lax.all_to_all(values, "expert", split_axis=0, concat_axis=0, tiled=True)

    cot_send = pl.pallas_call(
        functools.partial(send_cotangent_kernel, experts),
        out_shape=jax.ShapeDtypeStruct((experts, CAP, width), BF16),
        compiler_params=params(),
        cost_estimate=cost(2 * experts * CAP * tok_count * width, 4 * tok_count * width),
        name="send_cotangent",
    )(cotangent, target_row)
    cot_rows = swap(cot_send).reshape(experts * CAP, width)

    groups = HEADS // GROUP
    tiles = qkv_cols // 3 // GROUP_LANES
    weight_specs = [
        pl.BlockSpec((width, GROUP_LANES), functools.partial(lambda o, i: (0, o + i), part * tiles))
        for part in range(3)
    ]
    small_spec = pl.BlockSpec((width, LANES), lambda *_: (0, (qkv_cols + width) // LANES))
    wo_spec = pl.BlockSpec((width, width), lambda *_: (0, qkv_cols // width))
    table = whole_block((tok_count, LANES))
    full = whole_block((tok_count, width))
    group_spec = pl.BlockSpec((tok_count, GROUP_LANES), lambda i: (0, i))
    qkv_spec = pl.BlockSpec((3, tok_count, GROUP_LANES), lambda i: (0, 0, i))
    seg_specs = [whole_block((tok_count, 1)), whole_block((1, tok_count))]
    span = DOC_MAX + BLOCK
    head_rows = 16
    lse_spec = whole_block((head_rows, tok_count))
    qkv, attn_in, attn_out, lse = pl.pallas_call(
        functools.partial(attend_kernel, kinds + 6),
        grid=(groups,),
        in_specs=[full, *weight_specs, small_spec, table, table, *seg_specs],
        out_specs=[qkv_spec, full, group_spec, lse_spec],
        out_shape=[
            jax.ShapeDtypeStruct((3, tok_count, width), BF16),
            jax.ShapeDtypeStruct((tok_count, width), BF16),
            jax.ShapeDtypeStruct((tok_count, width), BF16),
            jax.ShapeDtypeStruct((head_rows, tok_count), F32),
        ],
        scratch_shapes=[
            pltpu.VMEM((1, width), F32),
            pltpu.VMEM((BLOCK, span), F32),
            pltpu.VMEM((tok_count, LANES), F32),
        ],
        compiler_params=params(),
        cost_estimate=cost(12e9, 16e6),
        name="attend",
    )(tokens, whole, whole, whole, whole, cosines, sines, seg_col, seg_row)

    payload = width + LANES
    resid_mid, scal, send = pl.pallas_call(
        functools.partial(middle_kernel, kinds),
        grid=(1,),
        in_specs=[
            full, wo_spec, full, small_spec, table, whole_block((tok_count, 2)),
            whole_block((2, tok_count)),
        ],
        out_specs=[full, table, whole_block((experts, CAP, payload))],
        out_shape=[
            jax.ShapeDtypeStruct((tok_count, width), F32),
            jax.ShapeDtypeStruct((tok_count, LANES), F32),
            jax.ShapeDtypeStruct((experts, CAP, payload), BF16),
        ],
        scratch_shapes=[
            pltpu.VMEM((tok_count, width), BF16),
            pltpu.VMEM((tok_count, LANES), BF16),
            pltpu.VMEM((tok_count, LANES), BF16),
        ],
        compiler_params=params(),
        cost_estimate=cost(3.5e9, 10e6),
        name="middle",
    )(attn_out, whole, tokens, whole, prev_mix, routes, target_row)
    w_in_one = w_in.reshape(width, 2 * ff)
    w_out_one = w_out.reshape(ff, width)
    if by_hand:
        expert_grads, returned = exchange_experts(send, cot_rows, w_in_one, w_out_one)
    else:
        expert_grads, returned = plain_experts(send, cot_rows, w_in_one, w_out_one, swap)
    returned, *expert_grads = lax.optimization_barrier((returned, *expert_grads))
    if by_hand:
        gate_keep, gate_away, up_keep, up_away, *down_parts = expert_grads
        gate_pair = (gate_keep, over_parts(gate_away, 1))
        up_pair = (up_keep, over_parts(up_away, 1))
        lined = [down_parts[0]]
        for i in (1, 2, 3):
            lined.append(over_parts(down_parts[i], 2 * i))

    mix_turned = jnp.pad(gate_mix.T, ((0, LANES - kinds), (0, LANES - kinds)))
    indicator = (
        jnp.arange(width)[None, :] // HEAD_DIM == jnp.arange(head_rows)[:, None]
    ).astype(BF16)
    token_block = pl.BlockSpec((BLOCK, width), lambda i: (i, 0))
    table_block = pl.BlockSpec((BLOCK, LANES), lambda i: (i, 0))
    two_block = pl.BlockSpec((BLOCK, 2), lambda i: (i, 0))
    (
        mixed, grad_prev, mid_grad, proj_grad, attn_grad, delta, minor, vec, gain2_row, grad_mix,
    ) = pl.pallas_call(
        functools.partial(combine_kernel, kinds, experts),
        grid=(tok_count // BLOCK,),
        in_specs=[
            whole_block((experts, 2 * CAP, width)), two_block, two_block, table_block,
            token_block, token_block, token_block, small_spec, wo_spec,
            whole_block((LANES, LANES)),
            pl.BlockSpec((kinds, BLOCK), lambda i: (0, i)),
            whole_block((head_rows, width)),
        ],
        out_specs=[
            token_block, pl.BlockSpec((BLOCK, kinds), lambda i: (i, 0)), token_block, token_block,
            token_block, pl.BlockSpec((head_rows, BLOCK), lambda i: (0, i)),
            whole_block((LANES, width)), whole_block((LANES, width)), whole_block((1, width)),
            whole_block((kinds, LANES)),
        ],
        out_shape=[
            jax.ShapeDtypeStruct((tok_count, width), BF16),
            jax.ShapeDtypeStruct((tok_count, kinds), F32),
            jax.ShapeDtypeStruct((tok_count, width), F32),
            jax.ShapeDtypeStruct((tok_count, width), BF16),
            jax.ShapeDtypeStruct((tok_count, width), BF16),
            jax.ShapeDtypeStruct((head_rows, tok_count), F32),
            jax.ShapeDtypeStruct((LANES, width), F32),
            jax.ShapeDtypeStruct((LANES, width), F32),
            jax.ShapeDtypeStruct((1, width), F32),
            jax.ShapeDtypeStruct((kinds, LANES), F32),
        ],
        scratch_shapes=[pltpu.VMEM((LANES, width), F32)],
        compiler_params=params(),
        cost_estimate=cost(1e6, 1e5),
        name="combine",
    )(
        returned, target_col, routes, scal, resid_mid, cotangent, attn_out, whole, whole,
        mix_turned, prev_scores.T, indicator,
    )

    if by_hand:
        gate_pair, attn_grad = lax.optimization_barrier((gate_pair, attn_grad))
        gate_met = add_low(*gate_pair)
        risen = lax.ppermute(gate_met[1:], "dp", [(0, 2), (1, 3)])
        fallen = lax.ppermute(gate_met[:3], "dp", [(6, 4), (7, 5)])
    halves = GROUP_LANES // LANES
    weights, grad_tokens, gain1_row = pl.pallas_call(
        functools.partial(attend_back_kernel, kinds + 6),
        grid=(groups,),
        in_specs=[
            qkv_spec, group_spec, lse_spec, lse_spec, table, table, *seg_specs, *weight_specs,
            full, full, group_spec, full, full, small_spec,
        ],
        out_specs=[
            pl.BlockSpec((4 * halves, width, LANES), lambda i: (i, 0, 0)), full,
            whole_block((1, width)),
        ],
        out_shape=[
            jax.ShapeDtypeStruct((4 * halves * groups, width, LANES), BF16),
            jax.ShapeDtypeStruct((tok_count, width), F32),
            jax.ShapeDtypeStruct((1, width), F32),
        ],
        scratch_shapes=[
            pltpu.VMEM((tok_count, GROUP_LANES), F32),
            pltpu.VMEM((tok_count, GROUP_LANES), F32),
            pltpu.VMEM((tok_count, GROUP_LANES), BF16),
            pltpu.VMEM((BLOCK, span), F32),
            pltpu.VMEM((width, tok_count), BF16),
            pltpu.VMEM((width, tok_count), BF16),
            pltpu.VMEM((tok_count, width), F32),
        ],
        compiler_params=params(),
        cost_estimate=cost(1e6, 1e5),
        name="attend_back",
    )(
        qkv, attn_grad, lse, delta, cosines, sines, seg_col, seg_row, whole, whole, whole,
        attn_in, attn_out, proj_grad, tokens, mid_grad, whole,
    )

    minor_rows = jnp.concatenate([minor[: kinds + 4], vec[:2], gain1_row, gain2_row], axis=0)
    minor_all = jnp.concatenate(
        [minor_rows, jnp.pad(grad_mix[:, :kinds], ((0, 0), (0, width - kinds)))], axis=0
    )
    rows = width // parts
    if by_hand:
        up_pair, lined, risen, fallen, weights = lax.optimization_barrier(
            (up_pair, lined, risen, fallen, weights)
        )
        kept = [gate_met, add_low(*up_pair), risen, fallen]
        shares, weight_sum, minor_all = reduce_parts(
            kept, sum(part.astype(F32) for part in lined).astype(BF16), weights, minor_all
        )
    else:
        shares = [
            lax.psum_scatter(grad, "dp", scatter_dimension=0, tiled=True).astype(F32)
            for grad in expert_grads
        ]
        weight_part = lax.psum_scatter(weights, "expert", scatter_dimension=0, tiled=True)
        weight_part = lax.psum_scatter(weight_part, "dp", scatter_dimension=1, tiled=True)
        weight_sum = lax.all_gather(weight_part, "expert", axis=0, tiled=True)
        minor_all = lax.psum(minor_all, ("dp", "expert"))
    grad_gate_mix = minor_all[kinds + 8 :, :kinds]
    minor_sum = lax.dynamic_slice_in_dim(
        minor_all[: kinds + 8], lax.axis_index("dp") * rows, rows, 1
    ).T
    weight_sum = weight_sum.reshape(groups, 4, -1, rows, LANES)
    weight_sum = weight_sum.transpose(3, 1, 0, 2, 4).reshape(rows, 4 * width).astype(F32)
    return (
        mixed,
        grad_tokens,
        grad_prev,
        weight_sum[:, :qkv_cols],
        weight_sum[:, qkv_cols:],
        minor_sum[:, :kinds],
        minor_sum[:, kinds : kinds + 4],
        minor_sum[:, kinds + 4 : kinds + 6],
        minor_sum[:, kinds + 6],
        minor_sum[:, kinds + 7],
        grad_gate_mix,
        jnp.concatenate([shares[0], shares[1]], axis=1)[None],
        shares[2][None],
    )


def solution(mesh):
    rows = P(("dp", "expert"), None)
    in_specs = (
        rows, rows, rows, rows,
        P("dp", None), P("dp", None), P("dp", None), P("dp", None), P("dp", None), P("dp"), P("dp"),
        P(), P("expert", None, None), P("expert", None, None), rows,
    )
    out_specs = (
        rows, rows, rows,
        P("dp", None), P("dp", None), P("dp", None), P("dp", None), P("dp", None), P("dp"), P("dp"),
        P(), P("expert", "dp", None), P("expert", "dp", None),
    )
    return jax.shard_map(
        per_device, mesh=mesh, in_specs=in_specs, out_specs=out_specs, check_vma=False
    )
```

```python
import functools

import jax
import jax.numpy as jnp
from jax import lax
from jax.experimental import pallas as pl
from jax.experimental.pallas import tpu as pltpu
from jax.sharding import PartitionSpec as P


HEADS = 12
HEAD_DIM = 64
CAP = 256
DOC_MAX = 512
NORM_EPSILON = 1e-06
HIGHEST_PRECISION = lax.Precision.HIGHEST
NEGATIVE = -1e30
F32 = jnp.float32
BF16 = jnp.bfloat16
BLOCK = 256
GROUP = 4
GROUP_LANES = GROUP * HEAD_DIM
LANES = 128
MESH = pl.DeviceIdType.MESH
VMEM_BYTES = 62 * 1024 * 1024


def nn(left, right):
    return jnp.dot(left, right, preferred_element_type=F32)


def nt(left, right):
    return lax.dot_general(left, right, (((1,), (1,)), ((), ())), preferred_element_type=F32)


def tn(left, right):
    return lax.dot_general(left, right, (((0,), (0,)), ((), ())), preferred_element_type=F32)


def iota(shape, axis):
    return lax.broadcasted_iota(jnp.int32, shape, axis)


def split_low(values):
    high = values.astype(BF16)
    return high, (values - high.astype(F32)).astype(BF16)


def inverse_rms(values):
    return lax.rsqrt(jnp.mean(values * values, axis=-1, keepdims=True) + NORM_EPSILON)


def norm_back(upstream, normed, inverse):
    return inverse * (upstream - normed * jnp.mean(upstream * normed, axis=-1, keepdims=True))


def turn(values, cosines, signed_sines):
    pieces = []
    for start in range(0, values.shape[1], LANES):
        part = values[:, start : start + LANES]
        front = iota(part.shape, 1) % HEAD_DIM < HEAD_DIM // 2
        swapped = jnp.where(
            front,
            pltpu.roll(part, LANES - HEAD_DIM // 2, 1),
            pltpu.roll(part, HEAD_DIM // 2, 1),
        )
        pieces.append(part * cosines + swapped * signed_sines)
    return jnp.concatenate(pieces, axis=1)


def head_mask(head):
    return (iota((1, GROUP_LANES), 1) // HEAD_DIM == head).astype(F32).astype(BF16)


def params(**extra):
    return pltpu.CompilerParams(vmem_limit_bytes=VMEM_BYTES, **extra)


def whole_block(shape):
    return pl.BlockSpec(shape, lambda *_: (0,) * len(shape))


def cost(flops, moved):
    return pl.CostEstimate(flops=int(flops), bytes_accessed=int(moved), transcendentals=0)


def send_cotangent_kernel(experts, cot_ref, target_ref, out_ref):
    tokens = cot_ref.shape[0]

    @pl.loop(0, experts)
    def _(expert):
        slots = iota((CAP, tokens), 0) + expert * CAP
        hot = (target_ref[0:1, :] == slots) | (target_ref[1:2, :] == slots)
        out_ref[expert] = nn(hot.astype(F32).astype(BF16), cot_ref[...]).astype(BF16)


def attend_kernel(
    gain_row, tok_ref, wq_ref, wk_ref, wv_ref, small_ref, cos_ref, sin_ref, segc_ref, segr_ref,
    qkv_ref, attn_in_ref, out_ref, lse_ref, gain_ref, bias_ref, log_ref,
):
    step = pl.program_id(0)
    tokens = tok_ref.shape[0]
    blocks = tokens // BLOCK
    reach = DOC_MAX // BLOCK

    @pl.when(step == 0)
    def _():
        gain_ref[...] = small_ref[...].astype(F32).T[gain_row : gain_row + 1, :]
        log_ref[...] = jnp.zeros_like(log_ref)

        @pl.loop(0, blocks)
        def _(block):
            rows = pl.ds(pl.multiple_of(block * BLOCK, BLOCK), BLOCK)
            values = tok_ref[rows, :].astype(F32)
            attn_in_ref[rows, :] = (values * inverse_rms(values) * gain_ref[...]).astype(BF16)

    @pl.loop(0, blocks)
    def _(block):
        rows = pl.ds(pl.multiple_of(block * BLOCK, BLOCK), BLOCK)
        normed = attn_in_ref[rows, :]
        cosines = cos_ref[rows, :]
        sines = sin_ref[rows, :]
        query = turn(nn(normed, wq_ref[...]), cosines, sines) * HEAD_DIM**-0.5
        qkv_ref[0, rows, :] = query.astype(BF16)
        qkv_ref[1, rows, :] = turn(nn(normed, wk_ref[...]), cosines, sines).astype(BF16)
        qkv_ref[2, rows, :] = nn(normed, wv_ref[...]).astype(BF16)

    for block in range(blocks):
        first = max(0, block - reach) * BLOCK
        last = (block + 1) * BLOCK
        span = last - first
        rows = slice(block * BLOCK, last)
        row_ids = iota((BLOCK, span), 0) + block * BLOCK
        col_ids = iota((BLOCK, span), 1) + first
        seen = (col_ids <= row_ids) & (segc_ref[rows, :] == segr_ref[0:1, first:last])
        bias_ref[:, 0:span] = jnp.where(seen, 0.0, NEGATIVE)
        attended = []
        logs = log_ref[rows, :]
        for head in range(GROUP):
            mask = head_mask(head)
            scores = nt(qkv_ref[0, rows, :] * mask, qkv_ref[1, first:last, :]) + bias_ref[:, 0:span]
            top = jnp.max(scores, axis=1, keepdims=True)
            weights = jnp.exp(scores - top).astype(BF16)
            value = qkv_ref[2, first:last, :] * mask + (1 - mask)
            mixed = nn(weights, value)
            own = iota(mixed.shape, 1) // HEAD_DIM == head
            total = jnp.max(jnp.where(own, 0.0, mixed), axis=1, keepdims=True)
            attended.append(jnp.where(own, mixed / total, 0.0))
            logs = jnp.where(
                iota(logs.shape, 1) == step * GROUP + head, top + jnp.log(total), logs
            )
        log_ref[rows, :] = logs
        out_ref[rows, :] = (attended[0] + attended[1] + attended[2] + attended[3]).astype(BF16)

    @pl.when(step == pl.num_programs(0) - 1)
    def _():
        lse_ref[...] = log_ref[...].T[0 : lse_ref.shape[0], :]


def middle_kernel(
    kinds, ao_ref, wo_ref, tok_ref, small_ref, prev_ref, routes_ref, target_ref,
    resid_ref, scal_ref, send_ref, ffn_ref, first_ref, second_ref,
):
    tokens, width = tok_ref.shape
    gain = small_ref[...].astype(F32).T[kinds + 7 : kinds + 8, :]

    @pl.loop(0, tokens // BLOCK)
    def _(block):
        rows = pl.ds(pl.multiple_of(block * BLOCK, BLOCK), BLOCK)
        resid = tok_ref[rows, :].astype(F32) + nn(ao_ref[rows, :], wo_ref[...])
        resid_ref[rows, :] = resid
        inverse = inverse_rms(resid)
        low = (resid * inverse * gain).astype(BF16)
        ffn_ref[rows, :] = low
        logits = nn(low, small_ref[...]) + prev_ref[rows, :]
        lane = iota(logits.shape, 1)

        def pick(index):
            return jnp.sum(jnp.where(lane == index, logits, 0.0), axis=1, keepdims=True)

        def pair(left, right):
            top = jnp.maximum(left, right)
            left = jnp.exp(left - top)
            right = jnp.exp(right - top)
            total = left + right
            return left / total, right / total

        gates = pair(pick(routes_ref[rows, 0:1]), pick(routes_ref[rows, 1:2]))
        one = pair(pick(kinds), pick(kinds + 1))
        two = pair(pick(kinds + 2), pick(kinds + 3))
        scal = jnp.zeros_like(logits)
        for index, value in enumerate(gates + one + two + (inverse,)):
            scal = jnp.where(lane == index, value, scal)
        scal_ref[rows, :] = scal
        for gate, ref in zip(gates, (first_ref, second_ref)):
            high, rest = split_low(gate)
            ref[rows, :] = jnp.where(
                lane == 0, high.astype(F32), jnp.where(lane == 1, rest.astype(F32), 0.0)
            ).astype(BF16)

    @pl.loop(0, send_ref.shape[0])
    def _(expert):
        slots = iota((CAP, tokens), 0) + expert * CAP
        hot_one = (target_ref[0:1, :] == slots).astype(F32)
        hot_two = (target_ref[1:2, :] == slots).astype(F32)
        send_ref[expert, :, 0:width] = nn((hot_one + hot_two).astype(BF16), ffn_ref[...]).astype(
            BF16
        )
        send_ref[expert, :, width:] = (
            nn(hot_one.astype(BF16), first_ref[...]) + nn(hot_two.astype(BF16), second_ref[...])
        ).astype(BF16)


def expert_kernel(
    recv_ref, cot_ref, wg_ref, wu_ref, wo_ref, front_ref, ret_ref, out_acc, row_acc,
):
    step = pl.program_id(0)
    total, width = out_acc.shape
    tile = 512

    @pl.when(step == 0)
    def _():
        out_acc[...] = jnp.zeros_like(out_acc)
        row_acc[...] = jnp.zeros_like(row_acc)

    @pl.loop(0, total // tile)
    def _(block):
        rows = pl.ds(pl.multiple_of(block * tile, tile), tile)
        token = recv_ref[rows, 0:width]
        extra = recv_ref[rows, width:].astype(F32)
        gate_weight = extra[:, 0:1] + extra[:, 1:2]
        gate = nn(token, wg_ref[...])
        up = nn(token, wu_ref[...])
        grad = nt(cot_ref[rows, :], wo_ref[...]) * gate_weight
        sig = jax.nn.sigmoid(gate)
        act = gate * sig
        hidden = act * up
        out_acc[rows, :] += nn(hidden.astype(BF16), wo_ref[...])
        front_ref[2, rows, :] = (hidden * gate_weight).astype(BF16)
        gate_grad = (grad * up * sig * (1.0 + gate * (1.0 - sig))).astype(BF16)
        up_grad = (grad * act).astype(BF16)
        front_ref[0, rows, :] = gate_grad
        front_ref[1, rows, :] = up_grad
        row_acc[rows, :] += nt(gate_grad, wg_ref[...]) + nt(up_grad, wu_ref[...])

    @pl.when(step == pl.num_programs(0) - 1)
    def _():
        @pl.loop(0, total // CAP)
        def _(peer):
            rows = pl.ds(pl.multiple_of(peer * CAP, CAP), CAP)
            ret_ref[peer, 0:CAP, :] = out_acc[rows, :].astype(BF16)
            ret_ref[peer, CAP:, :] = row_acc[rows, :].astype(BF16)


def expert_grad_kernel(recv_ref, cot_ref, front_ref, gate_ref, up_ref, wout_ref, turned_ref):
    step = pl.program_id(0)
    width = turned_ref.shape[0]

    @pl.when(step == 0)
    def _():
        turned_ref[...] = recv_ref[:, 0:width].T

    wout_ref[...] = tn(front_ref[2], cot_ref[...]).astype(BF16)
    gate_ref[...] = nn(turned_ref[...], front_ref[0]).astype(BF16)
    up_ref[...] = nn(turned_ref[...], front_ref[1]).astype(BF16)


def combine_kernel(
    kinds, experts, ret_ref, target_ref, routes_ref, scal_ref, resid_ref, cot_ref, ao_ref,
    small_ref, wo_ref, mix_ref, prevt_ref, ind_ref,
    mixed_ref, prev_ref, mid_ref, proj_ref, attn_ref, delta_ref, minor_ref, vec_ref, gain_ref,
    gmix_ref, rows_ref,
):
    step = pl.program_id(0)

    @pl.when(step == 0)
    def _():
        rows_ref[...] = small_ref[...].astype(F32).T
        minor_ref[...] = jnp.zeros_like(minor_ref)
        vec_ref[...] = jnp.zeros_like(vec_ref)
        gain_ref[...] = jnp.zeros_like(gain_ref)
        gmix_ref[...] = jnp.zeros_like(gmix_ref)

    width = resid_ref.shape[1]
    slots = experts * CAP
    resid = resid_ref[...]
    cot = cot_ref[...]
    upstream = cot.astype(F32)
    scal = scal_ref[...]
    routes = (routes_ref[:, 0:1], routes_ref[:, 1:2])
    targets = (target_ref[:, 0:1], target_ref[:, 1:2])
    gates = (scal[:, 0:1], scal[:, 1:2])
    one_keep, one_vec = scal[:, 2:3], scal[:, 3:4]
    two_keep, two_vec = scal[:, 4:5], scal[:, 5:6]
    inverse = scal[:, 6:7]
    gain = rows_ref[kinds + 7 : kinds + 8, :]
    vec_one = rows_ref[kinds + 4 : kinds + 5, :]
    vec_two = rows_ref[kinds + 5 : kinds + 6, :]
    normed = resid * inverse
    ffn_norm = normed * gain
    low = ffn_norm.astype(BF16)
    slot_ids = iota((BLOCK, slots), 1)
    hots = [(target == slot_ids).astype(F32) for target in targets]
    outs = ret_ref[:, 0:CAP, :].reshape(slots, width)
    backs = ret_ref[:, CAP:, :].reshape(slots, width)
    branches = [nn(hot.astype(BF16), outs) for hot in hots]
    back = nn((hots[0] + hots[1]).astype(BF16), backs)

    def weight(kind):
        return sum(
            jnp.where(route == kind, gate, 0.0) for route, gate in zip(routes, gates)
        )

    weight_copy = weight(experts + 1)
    weight_one = weight(experts + 2)
    weight_two = weight(experts + 3)
    keep = weight_copy + weight_one * one_keep + weight_two * two_keep
    mixed_ref[...] = (
        resid
        + gates[0] * branches[0]
        + gates[1] * branches[1]
        + keep * ffn_norm
        + (weight_one * one_vec) * vec_one
        + (weight_two * two_vec) * vec_two
    ).astype(BF16)
    dot_norm = jnp.sum(upstream * ffn_norm, axis=1, keepdims=True)
    dot_one = jnp.sum(upstream * vec_one, axis=1, keepdims=True)
    dot_two = jnp.sum(upstream * vec_two, axis=1, keepdims=True)
    grads = []
    for route, branch in zip(routes, branches):
        grads.append(
            jnp.sum(branch * upstream, axis=1, keepdims=True)
            + jnp.where(route == experts + 1, dot_norm, 0.0)
            + jnp.where(route == experts + 2, one_keep * dot_norm + one_vec * dot_one, 0.0)
            + jnp.where(route == experts + 3, two_keep * dot_norm + two_vec * dot_two, 0.0)
        )
    mean_grad = gates[0] * grads[0] + gates[1] * grads[1]
    lane = iota((BLOCK, LANES), 1)
    wide = jnp.zeros((BLOCK, LANES), F32)
    for route, gate, grad in zip(routes, gates, grads):
        wide = jnp.where(lane == route, gate * (grad - mean_grad), wide)
    for index, keep_part, vec_part, grad_weight, dot in (
        (kinds, one_keep, one_vec, weight_one, dot_one),
        (kinds + 2, two_keep, two_vec, weight_two, dot_two),
    ):
        keep_grad = grad_weight * dot_norm
        vec_grad = grad_weight * dot
        both = keep_part * keep_grad + vec_part * vec_grad
        wide = jnp.where(lane == index, keep_part * (keep_grad - both), wide)
        wide = jnp.where(lane == index + 1, vec_part * (vec_grad - both), wide)
    wide_low = wide.astype(BF16)
    wide_back = wide_low.astype(F32)
    minor_ref[...] += nn(wide_back.T.astype(BF16), low)
    share = jnp.where(lane == 0, weight_one * one_vec, 0.0)
    share = jnp.where(lane == 1, weight_two * two_vec, share)
    high, rest = split_low(share.T)
    vec_ref[...] += nn(high, cot) + nn(rest, cot)
    prev_ref[...] = nn(wide_low, mix_ref[...])[:, 0:kinds]
    gmix_ref[...] += jnp.dot(
        prevt_ref[...], wide_back, precision=HIGHEST_PRECISION, preferred_element_type=F32
    )
    grad_two = back + nt(wide_low, small_ref[...]) + keep * upstream
    gain_ref[...] += jnp.sum(grad_two * normed, axis=0, keepdims=True)
    mid = upstream + norm_back(grad_two * gain, normed, inverse)
    mid_ref[...] = mid
    proj = mid.astype(BF16)
    proj_ref[...] = proj
    attn = nt(proj, wo_ref[...]).astype(BF16)
    attn_ref[...] = attn
    high, rest = split_low(attn.astype(F32) * ao_ref[...].astype(F32))
    delta_ref[...] = nt(ind_ref[...], high) + nt(ind_ref[...], rest)


def attend_back_kernel(
    gain_row, qkv_ref, grad_ref, lse_ref, delta_ref, cos_ref, sin_ref, segc_ref, segr_ref,
    wq_ref, wk_ref, wv_ref, attn_in_ref, ao_ref, proj_ref, tok_ref, mid_ref, small_ref,
    weight_ref, gtok_ref, gain_ref, dq_ref, dk_ref, dv_ref, bias_ref, in_t_ref, ao_t_ref, acc_ref,
):
    step = pl.program_id(0)
    tokens = tok_ref.shape[0]
    blocks = tokens // BLOCK
    reach = DOC_MAX // BLOCK

    @pl.when(step == 0)
    def _():
        in_t_ref[...] = attn_in_ref[...].T
        ao_t_ref[...] = ao_ref[...].T
        acc_ref[...] = jnp.zeros_like(acc_ref)

    dq_ref[...] = jnp.zeros_like(dq_ref)
    for block in range(blocks):
        first = block * BLOCK
        last = min(blocks, block + reach + 1) * BLOCK
        span = last - first
        keys = slice(first, first + BLOCK)
        key_ids = iota((BLOCK, span), 0) + first
        row_ids = iota((BLOCK, span), 1) + first
        seen = (key_ids <= row_ids) & (segc_ref[keys, :] == segr_ref[0:1, first:last])
        bias_ref[:, 0:span] = jnp.where(seen, 0.0, NEGATIVE)
        key = qkv_ref[1, keys, :]
        value = qkv_ref[2, keys, :]
        key_grad = None
        for head in range(GROUP):
            mask = head_mask(head)
            index = step * GROUP + head
            query = qkv_ref[0, first:last, :] * mask
            upstream = grad_ref[first:last, :] * mask
            scores = nt(key, query) + bias_ref[:, 0:span]
            probs = jnp.exp(scores - lse_ref[pl.ds(index, 1), first:last])
            prob_grad = nt(value, upstream)
            score_grad = (probs * (prob_grad - delta_ref[pl.ds(index, 1), first:last])).astype(BF16)
            dv = nn(probs.astype(BF16), upstream)
            dk = nn(score_grad, query)
            dq_ref[first:last, :] += tn(score_grad, key * mask)
            key_grad = dk if key_grad is None else key_grad + dk
            value_grad = dv if head == 0 else value_grad + dv
        dk_ref[keys, :] = key_grad
        dv_ref[keys, :] = value_grad.astype(BF16)

    @pl.loop(0, blocks)
    def _(block):
        rows = pl.ds(pl.multiple_of(block * BLOCK, BLOCK), BLOCK)
        cosines = cos_ref[rows, :]
        sines = -sin_ref[rows, :]
        dq = turn(dq_ref[rows, :] * HEAD_DIM**-0.5, cosines, sines)
        dk = turn(dk_ref[rows, :], cosines, sines)
        dq_ref[rows, :] = dq
        dk_ref[rows, :] = dk
        acc_ref[rows, :] += (
            nt(dq.astype(BF16), wq_ref[...])
            + nt(dk.astype(BF16), wk_ref[...])
            + nt(dv_ref[rows, :], wv_ref[...])
        )

    halves = GROUP_LANES // LANES
    for index, (turned, grads) in enumerate(
        ((in_t_ref, dq_ref), (in_t_ref, dk_ref), (in_t_ref, dv_ref), (ao_t_ref, proj_ref))
    ):
        product = nn(turned[...], grads[...].astype(BF16)).astype(BF16)
        for half in range(halves):
            weight_ref[index * halves + half] = product[:, half * LANES : (half + 1) * LANES]

    @pl.when(step == pl.num_programs(0) - 1)
    def _():
        gain = small_ref[...].astype(F32).T[gain_row : gain_row + 1, :]
        gain_ref[...] = jnp.zeros_like(gain_ref)

        @pl.loop(0, blocks)
        def _(block):
            rows = pl.ds(pl.multiple_of(block * BLOCK, BLOCK), BLOCK)
            values = tok_ref[rows, :].astype(F32)
            inverse = inverse_rms(values)
            normed = values * inverse
            grad = acc_ref[rows, :]
            gain_ref[...] += jnp.sum(grad * normed, axis=0, keepdims=True)
            gtok_ref[rows, :] = mid_ref[rows, :] + norm_back(grad * gain, normed, inverse)


def add_low(left, right):
    return (left.astype(F32) + right.astype(F32)).astype(BF16)


def over_parts(values, bit):
    return lax.ppermute(values, "dp", [(d, d ^ bit) for d in range(8)])


def greet(targets):
    barrier = pltpu.get_barrier_semaphore()
    for present, target in targets:
        @pl.when(present)
        def _():
            pl.semaphore_signal(barrier, inc=1, device_id=target, device_id_type=MESH)
    pl.semaphore_wait(barrier, sum(present.astype(jnp.int32) for present, _ in targets))


def gather_kernel(
    part_ref, cot_ref, target_ref, out_ref, rows_ref, outgoing, send_sem, recv_sem, local_sem,
    row_send, row_recv, own_sem,
):
    me = lax.axis_index("dp")
    owner = lax.axis_index("expert")
    here, flank = me // 2, me % 2
    core = owner % 2
    up = ((2 * jnp.minimum(here + 1, 3) + flank), here < 3)
    down = ((2 * jnp.maximum(here - 1, 0) + flank), here > 0)
    across = 2 * here + 1 - flank
    partner = owner + 1 - 2 * core
    always = here >= 0
    routes = (
        (up[1], {"dp": up[0]}),
        (down[1], {"dp": down[0]}),
        (always, {"dp": across}),
        (always, {"expert": partner}),
    )
    side = owner // 2
    beside = owner + 2 - 4 * side
    corner = partner + 2 - 4 * side
    peers = (beside, corner, partner, owner)
    greet((*routes, (always, {"expert": beside}), (always, {"expert": corner})))

    def row_copy(slot):
        return pltpu.make_async_remote_copy(
            src_ref=outgoing.at[slot],
            dst_ref=rows_ref.at[owner],
            send_sem=row_send.at[slot],
            recv_sem=row_recv.at[slot],
            device_id={"expert": peers[slot]},
            device_id_type=MESH,
        )

    def copy(index, half, route, source=None):
        return pltpu.make_async_remote_copy(
            src_ref=out_ref.at[index, half] if source is None else source,
            dst_ref=out_ref.at[index, half],
            send_sem=send_sem.at[route, index],
            recv_sem=recv_sem.at[half, index],
            device_id=routes[route][1],
            device_id_type=MESH,
        )

    def arrive(index, half):
        copy(index, half, 2).wait_recv()

    local = pltpu.make_async_copy(part_ref, out_ref.at[me], local_sem)
    local.start()
    for route in range(3):
        @pl.when(routes[route][0])
        def _():
            copy(me, core, route, part_ref.at[core]).start()
    tokens = cot_ref.shape[0]
    for slot, peer in enumerate(peers):
        slots = iota((CAP, tokens), 0) + peer * CAP
        hot = (target_ref[0:1, :] == slots) | (target_ref[1:2, :] == slots)
        outgoing[slot] = nn(hot.astype(F32).astype(BF16), cot_ref[...]).astype(BF16)
        if slot > 0:
            row_copy(slot - 1).start()
    own_rows = pltpu.make_async_copy(outgoing.at[3], rows_ref.at[owner], own_sem)
    own_rows.start()
    for distance in range(1, 5):
        for toward, forward, present in (
            (here - distance, 0, here >= distance),
            (here + distance, 1, here + distance <= 3),
        ):
            index = 2 * jnp.clip(toward, 0, 3) + flank

            @pl.when(present)
            def _():
                arrive(index, core)
                copy(index, core, 2).start()
                copy(index, core, 3).start()

            @pl.when(present & routes[forward][0])
            def _():
                copy(index, core, forward).start()
        for sign in (-1, 1):
            if distance == 1 and sign == 1:
                continue
            toward = here + sign * (distance - 1)
            index = 2 * jnp.clip(toward, 0, 3) + 1 - flank

            @pl.when((toward >= 0) & (toward <= 3))
            def _():
                arrive(index, core)
                copy(index, core, 3).start()
    for offset in range(1, 8):
        index = (me + offset) % 8
        arrive(index, 1 - core)
        copy(index, core, 3).wait_send()
    local.wait()
    for route in range(3):
        @pl.when(routes[route][0])
        def _():
            copy(me, core, route, part_ref.at[core]).wait_send()
    for distance in range(1, 4):
        for toward, forward, present in (
            (here - distance, 0, here >= distance),
            (here + distance, 1, here + distance <= 3),
        ):
            index = 2 * jnp.clip(toward, 0, 3) + flank

            @pl.when(present)
            def _():
                copy(index, core, 2).wait_send()

            @pl.when(present & routes[forward][0])
            def _():
                copy(index, core, forward).wait_send()
    for slot in range(3):
        row_copy(slot).wait_recv()
        row_copy(slot).wait_send()
    own_rows.wait()


def gather_parts(packed, cotangent, target_row):
    rows, columns = packed.shape
    width = cotangent.shape[1]
    whole, cot_rows = pl.pallas_call(
        gather_kernel,
        in_specs=[pl.BlockSpec(memory_space=pltpu.VMEM)] * 3,
        out_specs=[pl.BlockSpec(memory_space=pl.ANY)] * 2,
        out_shape=[
            jax.ShapeDtypeStruct((8, 2, rows // 2, columns), BF16),
            jax.ShapeDtypeStruct((4, CAP, width), BF16),
        ],
        scratch_shapes=[
            pltpu.VMEM((4, CAP, width), BF16),
            pltpu.SemaphoreType.DMA((4, 8)),
            pltpu.SemaphoreType.DMA((2, 8)),
            pltpu.SemaphoreType.DMA,
            pltpu.SemaphoreType.DMA((3,)),
            pltpu.SemaphoreType.DMA((3,)),
            pltpu.SemaphoreType.DMA,
        ],
        compiler_params=params(collective_id=0, has_side_effects=True),
        cost_estimate=cost(10e9, 10e6),
        name="gather_parts",
    )(packed.reshape(2, rows // 2, columns), cotangent, target_row)
    return whole.reshape(8 * rows, columns), cot_rows


def add_planes(target, left, right):
    @pl.loop(0, target.shape[0])
    def _(index):
        total = left[index].astype(F32) + right[index].astype(F32)
        target[index] = total.astype(target.dtype)


def reduce_kernel(
    gate_ref, up_ref, risen_ref, fallen_ref, pair_ref, weight_ref, minor_ref,
    gate_out, up_out, down_out, weight_out, minor_out,
    gate_in, up_in, line_in, gate_stage, up_stage, line_stage, pair_in, core_in, core_sum, side_in, side_sum, cross_in, line_ref, line_sum_ref,
    small_in, small_sum, piece_send, piece_recv, other_send, other_recv,
):
    me = lax.axis_index("dp")
    owner = lax.axis_index("expert")
    here, flank = me // 2, me % 2
    core, side = owner % 2, owner // 2
    rising = {"dp": 2 * jnp.minimum(here + 1, 3) + flank}
    falling = {"dp": 2 * jnp.maximum(here - 1, 0) + flank}
    across = {"dp": me + 1 - 2 * flank}
    partner = {"expert": owner + 1 - 2 * core}
    beside = {"expert": owner + 2 - 4 * side}
    always = here >= 0
    greet(((here < 3, rising), (here > 0, falling), (always, across), (always, partner),
           (always, beside)))
    pieces = (
        (gate_ref, gate_in, gate_stage),
        (up_ref, up_in, up_stage),
        (line_ref, line_in, line_stage),
    )

    def piece_copy(piece, turn_index, way, source):
        return pltpu.make_async_remote_copy(
            src_ref=source,
            dst_ref=pieces[piece][1].at[way, turn_index],
            send_sem=piece_send.at[piece, turn_index, way],
            recv_sem=piece_recv.at[piece, turn_index, way],
            device_id=(rising, falling)[way],
            device_id_type=MESH,
        )

    def other_copy(index, source, target, device):
        return pltpu.make_async_remote_copy(
            src_ref=source, dst_ref=target, send_sem=other_send.at[index],
            recv_sem=other_recv.at[index], device_id=device, device_id_type=MESH,
        )

    def direct(piece, turn_index):
        own = pieces[piece][0]

        @pl.when(here == 0)
        def _():
            piece_copy(piece, turn_index, 0, own.at[3 - turn_index]).start()

        @pl.when(here == 3)
        def _():
            piece_copy(piece, turn_index, 1, own.at[turn_index]).start()

    def relayed(turn_index):
        return (
            (0, (here > 0) & (here < 3 - turn_index), 3 - turn_index),
            (1, (here < 3) & (here > turn_index), turn_index),
        )

    def relay(piece, turn_index):
        own, landed, stage = pieces[piece]
        for way, present, chunk in relayed(turn_index):
            if piece == 0:
                present = present & ((here != 1) if way == 0 else (here != 2))

            @pl.when(present)
            def _():
                copy = piece_copy(piece, turn_index, way, stage.at[way, turn_index])
                copy.wait_recv()
                add_planes(
                    stage.at[way, turn_index], own.at[chunk], landed.at[way, turn_index]
                )
                copy.start()

    def early(turn_index):
        own, landed, stage = pieces[0]
        for way, place, chunk in ((0, 1, 3 - turn_index), (1, 2, turn_index)):
            @pl.when(here == place)
            def _():
                add_planes(
                    stage.at[way, turn_index], own.at[chunk], landed.at[way, turn_index]
                )
                piece_copy(0, turn_index, way, stage.at[way, turn_index]).start()

    def finish(piece, target):
        own, landed, stage = pieces[piece]
        lower = jnp.minimum(3 - here, 2)
        upper = jnp.minimum(here, 2)

        @pl.when((here > (1 if piece == 0 else 0)))
        def _():
            piece_copy(piece, lower, 0, stage.at[0, 0]).wait_recv()

        @pl.when(here < (2 if piece == 0 else 3))
        def _():
            piece_copy(piece, upper, 1, stage.at[0, 0]).wait_recv()

        @pl.when(here == 0)
        def _():
            add_planes(target, own.at[here], landed.at[1, upper])

        @pl.when(here == 3)
        def _():
            add_planes(target, own.at[here], landed.at[0, lower])

        @pl.when((here > 0) & (here < 3))
        def _():
            @pl.loop(0, target.shape[0])
            def _(index):
                total = (
                    own[here, index].astype(F32)
                    + landed[0, lower, index].astype(F32)
                    + landed[1, upper, index].astype(F32)
                )
                target[index] = total.astype(target.dtype)

    def drain(piece):
        own, _, stage = pieces[piece]
        for turn_index in range(0 if piece == 0 else 3):
            @pl.when(here == 0)
            def _():
                piece_copy(piece, turn_index, 0, own.at[3 - turn_index]).wait_send()

            @pl.when(here == 3)
            def _():
                piece_copy(piece, turn_index, 1, own.at[turn_index]).wait_send()
        for turn_index in range(2):
            for way, present, _ in relayed(turn_index):
                @pl.when(present)
                def _():
                    piece_copy(
                        piece, turn_index, way, stage.at[way, turn_index]
                    ).wait_send()

    half = core_in.shape[0]
    quarter = half // 2
    core_weight = other_copy(0, weight_ref.at[pl.ds(half * (1 - core), half)], core_in, partner)
    core_small = other_copy(1, minor_ref, small_in.at[0], partner)
    side_weight = other_copy(2, core_sum.at[pl.ds(quarter * (1 - side), quarter)], side_in, beside)
    side_small = other_copy(3, small_sum.at[0], small_in.at[1], beside)
    cross_weight = [
        other_copy(4 + z, side_sum.at[:, 2 * z + 1 - flank], cross_in.at[z], across)
        for z in range(4)
    ]
    cross_small = other_copy(8, small_sum.at[1], small_in.at[2], across)
    rise_small = other_copy(9, small_sum.at[3], small_in.at[3], rising)
    fall_small = other_copy(10, small_sum.at[4], small_in.at[4], falling)
    mine = half * core + quarter * side
    own_part = weight_out.at[pl.ds(mine, quarter)]
    own_half = weight_out.at[pl.ds(half * core, half)]
    side_back = other_copy(11, own_part, own_part, beside)
    core_back = other_copy(12, own_half, own_half, partner)

    pair_copy = other_copy(13, pair_ref.at[1 - flank], pair_in, across)
    core_weight.start()
    core_small.start()
    pair_copy.start()
    for turn_index in range(3):
        direct(1, turn_index)

    @pl.when(here == 1)
    def _():
        for turn_index in range(3):
            gate_in[0, turn_index] = risen_ref[2 - turn_index]

    @pl.when(here == 2)
    def _():
        for turn_index in range(3):
            gate_in[1, turn_index] = fallen_ref[turn_index]

    for turn_index in range(2):
        early(turn_index)
    core_weight.wait_recv()
    core_small.wait_recv()
    add_planes(core_sum, weight_ref.at[pl.ds(half * core, half)], core_in)
    small_sum[0] = minor_ref[...] + small_in[0]
    side_weight.start()
    side_small.start()
    for piece in (0, 1):
        relay(piece, 0)
    pair_copy.wait_recv()
    add_planes(down_out, pair_ref.at[flank], pair_in)
    side_weight.wait_recv()
    side_small.wait_recv()
    add_planes(side_sum, core_sum.at[pl.ds(quarter * side, quarter)], side_in)
    small_sum[1] = small_sum[0] + small_in[1]
    for copy in cross_weight:
        copy.start()
    cross_small.start()
    for piece in (0, 1):
        relay(piece, 1)
    for copy in cross_weight:
        copy.wait_recv()
    cross_small.wait_recv()
    for z in range(4):
        add_planes(line_ref.at[z], side_sum.at[:, 2 * z + flank], cross_in.at[z])
    small_sum[2] = small_sum[1] + small_in[2]
    small_sum[3] = small_sum[2]
    small_sum[4] = small_sum[2]
    for turn_index in range(3):
        direct(2, turn_index)

    @pl.when(here == 0)
    def _():
        rise_small.start()

    @pl.when(here == 3)
    def _():
        fall_small.start()

    for turn_index in range(2):
        relay(2, turn_index)

    @pl.when(here > 0)
    def _():
        rise_small.wait_recv()
        small_sum[3] = small_sum[2] + small_in[3]

    @pl.when((here > 0) & (here < 3))
    def _():
        rise_small.start()

    @pl.when(here < 3)
    def _():
        fall_small.wait_recv()
        small_sum[4] = small_sum[2] + small_in[4]

    @pl.when((here > 0) & (here < 3))
    def _():
        fall_small.start()

    minor_out[...] = small_sum[3] + small_sum[4] - small_sum[2]
    finish(2, line_sum_ref)
    for index in range(quarter):
        weight_out[mine + index] = line_sum_ref[index]
    side_back.start()
    finish(0, gate_out)
    side_back.wait_recv()
    core_back.start()
    finish(1, up_out)
    core_back.wait_recv()
    for piece in range(3):
        drain(piece)
    for copy in (core_weight, core_small, side_weight, side_small, *cross_weight, cross_small,
                 side_back, core_back, pair_copy):
        copy.wait_send()

    @pl.when(here < 3)
    def _():
        rise_small.wait_send()

    @pl.when(here > 0)
    def _():
        fall_small.wait_send()


def reduce_parts(kept, down, weights, minor):
    gate, up = kept[:2]
    kept = [piece.reshape(-1, piece.shape[1] // 32, 32, piece.shape[2]) for piece in kept]
    pair = down.reshape(2, down.shape[1] // 32, 32, down.shape[2])
    blocks, width, lanes = weights.shape
    rows = width // 8
    plane = (rows, lanes)
    chunks = [piece.shape[1:] for piece in kept[:2]]
    line = (blocks // 4,) + plane
    low = [pltpu.VMEM((2, 3) + chunk, BF16) for chunk in chunks + [line]]
    stages = [pltpu.VMEM((2, 2) + chunk, BF16) for chunk in chunks + [line]]
    outs = pl.pallas_call(
        reduce_kernel,
        in_specs=[pl.BlockSpec(memory_space=pltpu.VMEM)] * 7,
        out_specs=[pl.BlockSpec(memory_space=pltpu.VMEM)] * 5,
        out_shape=[jax.ShapeDtypeStruct(chunk, F32) for chunk in chunks + [pair.shape[1:]]]
        + [
            jax.ShapeDtypeStruct((blocks,) + plane, BF16),
            jax.ShapeDtypeStruct(minor.shape, F32),
        ],
        scratch_shapes=[
            *low,
            *stages,
            pltpu.VMEM(pair.shape[1:], BF16),
            pltpu.VMEM((blocks // 2, 8) + plane, BF16),
            pltpu.VMEM((blocks // 2, 8) + plane, BF16),
            pltpu.VMEM((blocks // 4, 8) + plane, BF16),
            pltpu.VMEM((blocks // 4, 8) + plane, BF16),
            pltpu.VMEM((4,) + line, BF16),
            pltpu.VMEM((4,) + line, BF16),
            pltpu.VMEM(line, BF16),
            pltpu.VMEM((5,) + minor.shape, F32),
            pltpu.VMEM((5,) + minor.shape, F32),
            pltpu.SemaphoreType.DMA((3, 3, 2)),
            pltpu.SemaphoreType.DMA((3, 3, 2)),
            pltpu.SemaphoreType.DMA((14,)),
            pltpu.SemaphoreType.DMA((14,)),
        ],
        compiler_params=params(collective_id=1, has_side_effects=True),
        name="reduce_parts",
    )(*kept, pair, weights.reshape(blocks, 8, rows, lanes), minor)
    shapes = (gate.shape[1:], up.shape[1:], down.shape[1:])
    shares = [out.reshape(shape) for out, shape in zip(outs, shapes)]
    return shares, outs[3], outs[4]


FF_TILE = 256


def exchange_kernel(
    send_ref, cot_ref, win_ref, wout_ref,
    gate_keep, gate_away, up_keep, up_away, own_down, one_down, two_down, three_down, return_out,
    recv, cot, gate_w, up_w, down_w, front, turned, out_acc, row_acc, ret, gate_g, up_g, down_g,
    token_send, token_recv, back_send, back_recv, load_sem, weight_sem, store_sem, down_sem, own_sem,
):
    me = lax.axis_index("expert")
    spot = lax.axis_index("dp")
    here, flank = spot // 2, spot % 2
    line_peers = (here, here + 1 - 2 * (here % 2), here + 2 - 4 * (here // 2), 3 - here)
    down_parts = (own_down, one_down, two_down, three_down)
    share = gate_w.shape[0] // 8
    core, side = me % 2, me // 2
    partner = me + 1 - 2 * core
    beside = me + 2 - 4 * side
    corner = partner + 2 - 4 * side
    peers = (me, beside, corner, partner)
    always = me >= 0
    width = out_acc.shape[1]
    ff = down_w.shape[0]
    tiles = ff // FF_TILE
    greet([(always, {"expert": peer}) for peer in peers[1:]])

    def token_copy(slot):
        return pltpu.make_async_remote_copy(
            src_ref=send_ref.at[peers[slot]], dst_ref=recv.at[slot],
            send_sem=token_send.at[slot], recv_sem=token_recv.at[slot],
            device_id={"expert": peers[slot]}, device_id_type=MESH,
        )

    def back_copy(slot):
        return pltpu.make_async_remote_copy(
            src_ref=ret.at[slot], dst_ref=return_out.at[me],
            send_sem=back_send.at[slot], recv_sem=back_recv.at[slot],
            device_id={"expert": peers[slot]}, device_id_type=MESH,
        )

    def tile_slice(tile):
        return pl.ds(pl.multiple_of(tile * FF_TILE, FF_TILE), FF_TILE)

    def weight_copies(tile):
        cols = tile_slice(tile)
        shifted = pl.ds(pl.multiple_of(ff + tile * FF_TILE, FF_TILE), FF_TILE)
        return (
            pltpu.make_async_copy(
                win_ref.at[:, cols], gate_w.at[:, cols], weight_sem.at[0, tile]
            ),
            pltpu.make_async_copy(
                win_ref.at[:, shifted], up_w.at[:, cols], weight_sem.at[1, tile]
            ),
            pltpu.make_async_copy(
                wout_ref.at[cols, :], down_w.at[cols, :], weight_sem.at[2, tile]
            ),
        )

    def side_copy(piece, index, kept):
        source = (gate_g, up_g)[piece].at[index * share : (index + 1) * share, :]
        target = ((gate_away, gate_keep), (up_away, up_keep))[piece][kept].at[index // 2]
        return pltpu.make_async_copy(source, target, store_sem.at[piece, index])

    def down_copy(tile, distance):
        return pltpu.make_async_copy(
            down_g.at[tile_slice(tile), :], down_parts[distance].at[tile % 2], down_sem.at[tile]
        )

    for slot in (1, 2, 3):
        token_copy(slot).start()
    loads = [pltpu.make_async_copy(send_ref.at[me], recv.at[0], load_sem.at[0])] + [
        pltpu.make_async_copy(cot_ref.at[peers[slot]], cot.at[slot], load_sem.at[1 + slot])
        for slot in range(4)
    ]
    for load in loads:
        load.start()

    @pl.loop(0, tiles)
    def _(tile):
        for copy in weight_copies(tile):
            copy.start()

    for load in loads:
        load.wait()

    def work(slot):
        extra = recv[slot, :, width:].astype(F32)
        gate_weight = extra[:, 0:1] + extra[:, 1:2]
        out_acc[...] = jnp.zeros_like(out_acc)
        row_acc[...] = jnp.zeros_like(row_acc)

        @pl.loop(0, tiles)
        def _(tile):
            cols = tile_slice(tile)
            if slot == 0:
                for copy in weight_copies(tile):
                    copy.wait()
            token = recv[slot, :, 0:width]
            gate = nn(token, gate_w[:, cols])
            up = nn(token, up_w[:, cols])
            grad = nt(cot[slot], down_w[cols, :]) * gate_weight
            sig = jax.nn.sigmoid(gate)
            act = gate * sig
            hidden = act * up
            out_acc[...] += nn(hidden.astype(BF16), down_w[cols, :])
            front[2, slot, :, cols] = (hidden * gate_weight).astype(BF16)
            gate_grad = (grad * up * sig * (1.0 + gate * (1.0 - sig))).astype(BF16)
            up_grad = (grad * act).astype(BF16)
            front[0, slot, :, cols] = gate_grad
            front[1, slot, :, cols] = up_grad
            row_acc[...] += nt(gate_grad, gate_w[:, cols]) + nt(up_grad, up_w[:, cols])

        ret[slot, 0:CAP, :] = out_acc[...].astype(BF16)
        ret[slot, CAP:, :] = row_acc[...].astype(BF16)
        turned[:, slot * CAP : (slot + 1) * CAP] = recv[slot, :, 0:width].T

    own_back = pltpu.make_async_copy(ret.at[0], return_out.at[me], own_sem)
    work(0)
    own_back.start()
    for slot in (1, 2, 3):
        token_copy(slot).wait_recv()
        work(slot)
        back_copy(slot).start()
    total = 4 * CAP

    @pl.loop(0, tiles)
    def _(tile):
        cols = tile_slice(tile)
        hidden = front[2, :, :, cols].reshape(total, FF_TILE)
        down_g[cols, :] = tn(hidden, cot[...].reshape(total, width)).astype(BF16)
        gate_g[:, cols] = nn(turned[...], front[0, :, :, cols].reshape(total, FF_TILE)).astype(BF16)
        up_g[:, cols] = nn(turned[...], front[1, :, :, cols].reshape(total, FF_TILE)).astype(BF16)
        for distance in range(4):
            @pl.when(tile // 2 == line_peers[distance])
            def _():
                down_copy(tile, distance).start()

    for piece in range(2):
        for index in range(8):
            for kept in range(2):
                @pl.when((flank == index % 2) if kept else (flank != index % 2))
                def _():
                    side_copy(piece, index, kept).start()

    for slot in (1, 2, 3):
        token_copy(slot).wait_send()
        back_copy(slot).wait_recv()
        back_copy(slot).wait_send()
    own_back.wait()

    for piece in range(2):
        for index in range(8):
            side_copy(piece, index, 1).wait()

    @pl.loop(0, tiles)
    def _(tile):
        down_copy(tile, 0).wait()


def exchange_experts(send, cot_rows, w_in, w_out):
    peers, cap, payload = send.shape
    ff, width = w_out.shape
    anywhere = pl.BlockSpec(memory_space=pl.ANY)
    tiles = ff // FF_TILE
    *grads, returned = pl.pallas_call(
        exchange_kernel,
        in_specs=[anywhere] * 4,
        out_specs=[anywhere] * 9,
        out_shape=[jax.ShapeDtypeStruct((4, width // 8, ff), BF16)] * 4
        + [jax.ShapeDtypeStruct((2, ff // 8, width), BF16)] * 4
        + [jax.ShapeDtypeStruct((peers, 2 * cap, width), BF16)],
        scratch_shapes=[
            pltpu.VMEM((peers, cap, payload), BF16),
            pltpu.VMEM((peers, cap, width), BF16),
            pltpu.VMEM((width, ff), BF16),
            pltpu.VMEM((width, ff), BF16),
            pltpu.VMEM((ff, width), BF16),
            pltpu.VMEM((3, peers, cap, ff), BF16),
            pltpu.VMEM((width, peers * cap), BF16),
            pltpu.VMEM((cap, width), F32),
            pltpu.VMEM((cap, width), F32),
            pltpu.VMEM((peers, 2 * cap, width), BF16),
            pltpu.VMEM((width, ff), BF16),
            pltpu.VMEM((width, ff), BF16),
            pltpu.VMEM((ff, width), BF16),
            pltpu.SemaphoreType.DMA((4,)),
            pltpu.SemaphoreType.DMA((4,)),
            pltpu.SemaphoreType.DMA((4,)),
            pltpu.SemaphoreType.DMA((4,)),
            pltpu.SemaphoreType.DMA((5,)),
            pltpu.SemaphoreType.DMA((3, tiles)),
            pltpu.SemaphoreType.DMA((2, 8)),
            pltpu.SemaphoreType.DMA((tiles,)),
            pltpu.SemaphoreType.DMA,
        ],
        compiler_params=params(collective_id=2, has_side_effects=True),
        cost_estimate=cost(18 * peers * cap * width * ff, 40e6),
        name="exchange_experts",
    )(send, cot_rows.reshape(peers, cap, width), w_in, w_out)
    return grads, returned


def plain_experts(send, cot_rows, w_in_one, w_out_one, swap):
    experts, _, payload = send.shape
    ff, width = w_out_one.shape
    recv = swap(send).reshape(experts * CAP, payload)

    slot_count = experts * CAP
    ff_tile = 256
    ff_tiles = ff // ff_tile
    slot_full = whole_block((slot_count, width))
    recv_full = whole_block((slot_count, payload))
    front_spec = pl.BlockSpec((3, slot_count, ff_tile), lambda j: (0, 0, j))
    front, ret = pl.pallas_call(
        expert_kernel,
        grid=(ff_tiles,),
        in_specs=[
            recv_full,
            slot_full,
            pl.BlockSpec((width, ff_tile), lambda j: (0, j)),
            pl.BlockSpec((width, ff_tile), lambda j: (0, ff_tiles + j)),
            pl.BlockSpec((ff_tile, width), lambda j: (j, 0)),
        ],
        out_specs=[front_spec, whole_block((experts, 2 * CAP, width))],
        out_shape=[
            jax.ShapeDtypeStruct((3, slot_count, ff), BF16),
            jax.ShapeDtypeStruct((experts, 2 * CAP, width), BF16),
        ],
        scratch_shapes=[pltpu.VMEM((slot_count, width), F32)] * 2,
        compiler_params=params(),
        cost_estimate=cost(12 * slot_count * width * ff, 26e6),
        name="expert",
    )(recv, cot_rows, w_in_one, w_in_one, w_out_one)
    returned = swap(ret)
    expert_grads = pl.pallas_call(
        expert_grad_kernel,
        grid=(ff_tiles,),
        in_specs=[recv_full, slot_full, front_spec],
        out_specs=[
            pl.BlockSpec((width, ff_tile), lambda j: (0, j)),
            pl.BlockSpec((width, ff_tile), lambda j: (0, j)),
            pl.BlockSpec((ff_tile, width), lambda j: (j, 0)),
        ],
        out_shape=[
            jax.ShapeDtypeStruct((width, ff), BF16),
            jax.ShapeDtypeStruct((width, ff), BF16),
            jax.ShapeDtypeStruct((ff, width), BF16),
        ],
        scratch_shapes=[pltpu.VMEM((width, slot_count), BF16)],
        compiler_params=params(),
        cost_estimate=cost(6 * slot_count * width * ff, 24e6),
        name="expert_grad",
    )(recv, cot_rows, front)
    return expert_grads, returned


def per_device(
    tokens, prev_scores, segments, routes, wqkv, wo, router, const_gate, const_vec, gain1, gain2,
    gate_mix, w_in, w_out, cotangent,
):
    tok_count, width = tokens.shape
    kinds = router.shape[1]
    experts = w_in.shape[0] * lax.axis_size("expert")
    ff = w_out.shape[1]
    qkv_cols = wqkv.shape[1]
    parts = lax.axis_size("dp")
    by_hand = parts == 8 and experts == 4
    small = jnp.concatenate(
        [router, const_gate, const_vec, gain1[:, None], gain2[:, None]], axis=1
    )
    packed = jnp.concatenate(
        [wqkv, wo, jnp.pad(small, ((0, 0), (0, LANES - small.shape[1])))], axis=1
    )

    seq_len = segments.shape[1]
    positions = (jnp.arange(tok_count, dtype=jnp.int32) % seq_len).astype(F32)
    half = HEAD_DIM // 2
    frequency = 10000.0 ** (-jnp.arange(half).astype(F32) / half)
    angles = positions[:, None] * frequency[None, :]
    cosines = jnp.tile(jnp.cos(angles), (1, LANES // half))
    sines = jnp.tile(jnp.sin(angles), (1, LANES // half))
    signs = jnp.where(jnp.arange(LANES) % HEAD_DIM < half, -1.0, 1.0).astype(F32)
    sines = sines * signs[None, :]
    seg_col = segments.reshape(tok_count, 1)
    seg_row = segments.reshape(1, tok_count)

    names = jnp.arange(kinds, dtype=jnp.int32)
    hot = [routes[:, i : i + 1] == names[None, :] for i in range(2)]
    named = (hot[0] | hot[1]).astype(BF16)
    ids = jnp.arange(tok_count, dtype=jnp.int32)
    before = (ids[:, None] > ids[None, :]).astype(BF16)
    earlier = jnp.dot(before, named, preferred_element_type=F32)
    slots = [jnp.sum(jnp.where(h, earlier, 0.0), axis=1).astype(jnp.int32) for h in hot]
    targets = [
        jnp.where(routes[:, i] < experts, routes[:, i] * CAP + slots[i], experts * CAP)
        for i in range(2)
    ]
    target_row = jnp.stack(targets, axis=0)
    target_col = jnp.stack(targets, axis=1)
    prev_mix = jnp.dot(prev_scores, gate_mix.astype(F32), precision=HIGHEST_PRECISION)
    prev_mix = jnp.pad(prev_mix, ((0, 0), (0, LANES - kinds)))

    def swap(values):
        return lax.all_to_all(values, "expert", split_axis=0, concat_axis=0, tiled=True)

    if by_hand:
        whole, cot_rows = gather_parts(packed, cotangent, target_row)
    else:
        whole = lax.all_gather(packed, "dp", axis=0, tiled=True)
        cot_send = pl.pallas_call(
            functools.partial(send_cotangent_kernel, experts),
            out_shape=jax.ShapeDtypeStruct((experts, CAP, width), BF16),
            compiler_params=params(),
            cost_estimate=cost(2 * experts * CAP * tok_count * width, 4 * tok_count * width),
            name="send_cotangent",
        )(cotangent, target_row)
        cot_rows = swap(cot_send)
    cot_rows = cot_rows.reshape(experts * CAP, width)

    groups = HEADS // GROUP
    tiles = qkv_cols // 3 // GROUP_LANES
    weight_specs = [
        pl.BlockSpec((width, GROUP_LANES), functools.partial(lambda o, i: (0, o + i), part * tiles))
        for part in range(3)
    ]
    small_spec = pl.BlockSpec((width, LANES), lambda *_: (0, (qkv_cols + width) // LANES))
    wo_spec = pl.BlockSpec((width, width), lambda *_: (0, qkv_cols // width))
    table = whole_block((tok_count, LANES))
    full = whole_block((tok_count, width))
    group_spec = pl.BlockSpec((tok_count, GROUP_LANES), lambda i: (0, i))
    qkv_spec = pl.BlockSpec((3, tok_count, GROUP_LANES), lambda i: (0, 0, i))
    seg_specs = [whole_block((tok_count, 1)), whole_block((1, tok_count))]
    span = DOC_MAX + BLOCK
    head_rows = 16
    lse_spec = whole_block((head_rows, tok_count))
    qkv, attn_in, attn_out, lse = pl.pallas_call(
        functools.partial(attend_kernel, kinds + 6),
        grid=(groups,),
        in_specs=[full, *weight_specs, small_spec, table, table, *seg_specs],
        out_specs=[qkv_spec, full, group_spec, lse_spec],
        out_shape=[
            jax.ShapeDtypeStruct((3, tok_count, width), BF16),
            jax.ShapeDtypeStruct((tok_count, width), BF16),
            jax.ShapeDtypeStruct((tok_count, width), BF16),
            jax.ShapeDtypeStruct((head_rows, tok_count), F32),
        ],
        scratch_shapes=[
            pltpu.VMEM((1, width), F32),
            pltpu.VMEM((BLOCK, span), F32),
            pltpu.VMEM((tok_count, LANES), F32),
        ],
        compiler_params=params(),
        cost_estimate=cost(12e9, 16e6),
        name="attend",
    )(tokens, whole, whole, whole, whole, cosines, sines, seg_col, seg_row)

    payload = width + LANES
    resid_mid, scal, send = pl.pallas_call(
        functools.partial(middle_kernel, kinds),
        grid=(1,),
        in_specs=[
            full, wo_spec, full, small_spec, table, whole_block((tok_count, 2)),
            whole_block((2, tok_count)),
        ],
        out_specs=[full, table, whole_block((experts, CAP, payload))],
        out_shape=[
            jax.ShapeDtypeStruct((tok_count, width), F32),
            jax.ShapeDtypeStruct((tok_count, LANES), F32),
            jax.ShapeDtypeStruct((experts, CAP, payload), BF16),
        ],
        scratch_shapes=[
            pltpu.VMEM((tok_count, width), BF16),
            pltpu.VMEM((tok_count, LANES), BF16),
            pltpu.VMEM((tok_count, LANES), BF16),
        ],
        compiler_params=params(),
        cost_estimate=cost(3.5e9, 10e6),
        name="middle",
    )(attn_out, whole, tokens, whole, prev_mix, routes, target_row)
    w_in_one = w_in.reshape(width, 2 * ff)
    w_out_one = w_out.reshape(ff, width)
    if by_hand:
        expert_grads, returned = exchange_experts(send, cot_rows, w_in_one, w_out_one)
    else:
        expert_grads, returned = plain_experts(send, cot_rows, w_in_one, w_out_one, swap)
    returned, *expert_grads = lax.optimization_barrier((returned, *expert_grads))
    if by_hand:
        gate_keep, gate_away, up_keep, up_away, *down_parts = expert_grads
        gate_pair = (gate_keep, over_parts(gate_away, 1))
        up_pair = (up_keep, over_parts(up_away, 1))
        lined = [down_parts[0]]
        for i in (1, 2, 3):
            lined.append(over_parts(down_parts[i], 2 * i))

    mix_turned = jnp.pad(gate_mix.T, ((0, LANES - kinds), (0, LANES - kinds)))
    indicator = (
        jnp.arange(width)[None, :] // HEAD_DIM == jnp.arange(head_rows)[:, None]
    ).astype(BF16)
    token_block = pl.BlockSpec((BLOCK, width), lambda i: (i, 0))
    table_block = pl.BlockSpec((BLOCK, LANES), lambda i: (i, 0))
    two_block = pl.BlockSpec((BLOCK, 2), lambda i: (i, 0))
    (
        mixed, grad_prev, mid_grad, proj_grad, attn_grad, delta, minor, vec, gain2_row, grad_mix,
    ) = pl.pallas_call(
        functools.partial(combine_kernel, kinds, experts),
        grid=(tok_count // BLOCK,),
        in_specs=[
            whole_block((experts, 2 * CAP, width)), two_block, two_block, table_block,
            token_block, token_block, token_block, small_spec, wo_spec,
            whole_block((LANES, LANES)),
            pl.BlockSpec((kinds, BLOCK), lambda i: (0, i)),
            whole_block((head_rows, width)),
        ],
        out_specs=[
            token_block, pl.BlockSpec((BLOCK, kinds), lambda i: (i, 0)), token_block, token_block,
            token_block, pl.BlockSpec((head_rows, BLOCK), lambda i: (0, i)),
            whole_block((LANES, width)), whole_block((LANES, width)), whole_block((1, width)),
            whole_block((kinds, LANES)),
        ],
        out_shape=[
            jax.ShapeDtypeStruct((tok_count, width), BF16),
            jax.ShapeDtypeStruct((tok_count, kinds), F32),
            jax.ShapeDtypeStruct((tok_count, width), F32),
            jax.ShapeDtypeStruct((tok_count, width), BF16),
            jax.ShapeDtypeStruct((tok_count, width), BF16),
            jax.ShapeDtypeStruct((head_rows, tok_count), F32),
            jax.ShapeDtypeStruct((LANES, width), F32),
            jax.ShapeDtypeStruct((LANES, width), F32),
            jax.ShapeDtypeStruct((1, width), F32),
            jax.ShapeDtypeStruct((kinds, LANES), F32),
        ],
        scratch_shapes=[pltpu.VMEM((LANES, width), F32)],
        compiler_params=params(),
        cost_estimate=cost(1e6, 1e5),
        name="combine",
    )(
        returned, target_col, routes, scal, resid_mid, cotangent, attn_out, whole, whole,
        mix_turned, prev_scores.T, indicator,
    )

    if by_hand:
        gate_pair, attn_grad = lax.optimization_barrier((gate_pair, attn_grad))
        gate_met = add_low(*gate_pair)
        risen = lax.ppermute(gate_met[1:], "dp", [(0, 2), (1, 3)])
        fallen = lax.ppermute(gate_met[:3], "dp", [(6, 4), (7, 5)])
    halves = GROUP_LANES // LANES
    weights, grad_tokens, gain1_row = pl.pallas_call(
        functools.partial(attend_back_kernel, kinds + 6),
        grid=(groups,),
        in_specs=[
            qkv_spec, group_spec, lse_spec, lse_spec, table, table, *seg_specs, *weight_specs,
            full, full, group_spec, full, full, small_spec,
        ],
        out_specs=[
            pl.BlockSpec((4 * halves, width, LANES), lambda i: (i, 0, 0)), full,
            whole_block((1, width)),
        ],
        out_shape=[
            jax.ShapeDtypeStruct((4 * halves * groups, width, LANES), BF16),
            jax.ShapeDtypeStruct((tok_count, width), F32),
            jax.ShapeDtypeStruct((1, width), F32),
        ],
        scratch_shapes=[
            pltpu.VMEM((tok_count, GROUP_LANES), F32),
            pltpu.VMEM((tok_count, GROUP_LANES), F32),
            pltpu.VMEM((tok_count, GROUP_LANES), BF16),
            pltpu.VMEM((BLOCK, span), F32),
            pltpu.VMEM((width, tok_count), BF16),
            pltpu.VMEM((width, tok_count), BF16),
            pltpu.VMEM((tok_count, width), F32),
        ],
        compiler_params=params(),
        cost_estimate=cost(1e6, 1e5),
        name="attend_back",
    )(
        qkv, attn_grad, lse, delta, cosines, sines, seg_col, seg_row, whole, whole, whole,
        attn_in, attn_out, proj_grad, tokens, mid_grad, whole,
    )

    minor_rows = jnp.concatenate([minor[: kinds + 4], vec[:2], gain1_row, gain2_row], axis=0)
    minor_all = jnp.concatenate(
        [minor_rows, jnp.pad(grad_mix[:, :kinds], ((0, 0), (0, width - kinds)))], axis=0
    )
    rows = width // parts
    if by_hand:
        up_pair, lined, risen, fallen, weights = lax.optimization_barrier(
            (up_pair, lined, risen, fallen, weights)
        )
        kept = [gate_met, add_low(*up_pair), risen, fallen]
        shares, weight_sum, minor_all = reduce_parts(
            kept, sum(part.astype(F32) for part in lined).astype(BF16), weights, minor_all
        )
    else:
        shares = [
            lax.psum_scatter(grad, "dp", scatter_dimension=0, tiled=True).astype(F32)
            for grad in expert_grads
        ]
        weight_part = lax.psum_scatter(weights, "expert", scatter_dimension=0, tiled=True)
        weight_part = lax.psum_scatter(weight_part, "dp", scatter_dimension=1, tiled=True)
        weight_sum = lax.all_gather(weight_part, "expert", axis=0, tiled=True)
        minor_all = lax.psum(minor_all, ("dp", "expert"))
    grad_gate_mix = minor_all[kinds + 8 :, :kinds]
    minor_sum = lax.dynamic_slice_in_dim(
        minor_all[: kinds + 8], lax.axis_index("dp") * rows, rows, 1
    ).T
    weight_sum = weight_sum.reshape(groups, 4, -1, rows, LANES)
    weight_sum = weight_sum.transpose(3, 1, 0, 2, 4).reshape(rows, 4 * width).astype(F32)
    return (
        mixed,
        grad_tokens,
        grad_prev,
        weight_sum[:, :qkv_cols],
        weight_sum[:, qkv_cols:],
        minor_sum[:, :kinds],
        minor_sum[:, kinds : kinds + 4],
        minor_sum[:, kinds + 4 : kinds + 6],
        minor_sum[:, kinds + 6],
        minor_sum[:, kinds + 7],
        grad_gate_mix,
        jnp.concatenate([shares[0], shares[1]], axis=1)[None],
        shares[2][None],
    )


def solution(mesh):
    rows = P(("dp", "expert"), None)
    in_specs = (
        rows, rows, rows, rows,
        P("dp", None), P("dp", None), P("dp", None), P("dp", None), P("dp", None), P("dp"), P("dp"),
        P(), P("expert", None, None), P("expert", None, None), rows,
    )
    out_specs = (
        rows, rows, rows,
        P("dp", None), P("dp", None), P("dp", None), P("dp", None), P("dp", None), P("dp"), P("dp"),
        P(), P("expert", "dp", None), P("expert", "dp", None),
    )
    return jax.shard_map(
        per_device, mesh=mesh, in_specs=in_specs, out_specs=out_specs, check_vma=False
    )
```

```python
import functools

import jax
import jax.numpy as jnp
from jax import lax
from jax.experimental import pallas as pl
from jax.experimental.pallas import tpu as pltpu
from jax.sharding import PartitionSpec as P


HEADS = 12
HEAD_DIM = 64
CAP = 256
DOC_MAX = 512
NORM_EPSILON = 1e-06
HIGHEST_PRECISION = lax.Precision.HIGHEST
NEGATIVE = -1e30
F32 = jnp.float32
BF16 = jnp.bfloat16
BLOCK = 256
GROUP = 4
GROUP_LANES = GROUP * HEAD_DIM
LANES = 128
MESH = pl.DeviceIdType.MESH
VMEM_BYTES = 62 * 1024 * 1024


def nn(left, right):
    return jnp.dot(left, right, preferred_element_type=F32)


def nt(left, right):
    return lax.dot_general(left, right, (((1,), (1,)), ((), ())), preferred_element_type=F32)


def tn(left, right):
    return lax.dot_general(left, right, (((0,), (0,)), ((), ())), preferred_element_type=F32)


def iota(shape, axis):
    return lax.broadcasted_iota(jnp.int32, shape, axis)


def split_low(values):
    high = values.astype(BF16)
    return high, (values - high.astype(F32)).astype(BF16)


def inverse_rms(values):
    return lax.rsqrt(jnp.mean(values * values, axis=-1, keepdims=True) + NORM_EPSILON)


def norm_back(upstream, normed, inverse):
    return inverse * (upstream - normed * jnp.mean(upstream * normed, axis=-1, keepdims=True))


def turn(values, cosines, signed_sines):
    pieces = []
    for start in range(0, values.shape[1], LANES):
        part = values[:, start : start + LANES]
        front = iota(part.shape, 1) % HEAD_DIM < HEAD_DIM // 2
        swapped = jnp.where(
            front,
            pltpu.roll(part, LANES - HEAD_DIM // 2, 1),
            pltpu.roll(part, HEAD_DIM // 2, 1),
        )
        pieces.append(part * cosines + swapped * signed_sines)
    return jnp.concatenate(pieces, axis=1)


def head_mask(head):
    return (iota((1, GROUP_LANES), 1) // HEAD_DIM == head).astype(F32).astype(BF16)


def params(**extra):
    return pltpu.CompilerParams(vmem_limit_bytes=VMEM_BYTES, **extra)


def whole_block(shape):
    return pl.BlockSpec(shape, lambda *_: (0,) * len(shape))


def cost(flops, moved):
    return pl.CostEstimate(flops=int(flops), bytes_accessed=int(moved), transcendentals=0)


def send_cotangent_kernel(experts, cot_ref, target_ref, out_ref):
    tokens = cot_ref.shape[0]

    @pl.loop(0, experts)
    def _(expert):
        slots = iota((CAP, tokens), 0) + expert * CAP
        hot = (target_ref[0:1, :] == slots) | (target_ref[1:2, :] == slots)
        out_ref[expert] = nn(hot.astype(F32).astype(BF16), cot_ref[...]).astype(BF16)


def attend_kernel(
    gain_row, tok_ref, wq_ref, wk_ref, wv_ref, small_ref, cos_ref, sin_ref, segc_ref, segr_ref,
    qkv_ref, attn_in_ref, out_ref, lse_ref, gain_ref, bias_ref, log_ref,
):
    step = pl.program_id(0)
    tokens = tok_ref.shape[0]
    blocks = tokens // BLOCK
    reach = DOC_MAX // BLOCK

    @pl.when(step == 0)
    def _():
        gain_ref[...] = small_ref[...].astype(F32).T[gain_row : gain_row + 1, :]
        log_ref[...] = jnp.zeros_like(log_ref)

        @pl.loop(0, blocks)
        def _(block):
            rows = pl.ds(pl.multiple_of(block * BLOCK, BLOCK), BLOCK)
            values = tok_ref[rows, :].astype(F32)
            attn_in_ref[rows, :] = (values * inverse_rms(values) * gain_ref[...]).astype(BF16)

    @pl.loop(0, blocks)
    def _(block):
        rows = pl.ds(pl.multiple_of(block * BLOCK, BLOCK), BLOCK)
        normed = attn_in_ref[rows, :]
        cosines = cos_ref[rows, :]
        sines = sin_ref[rows, :]
        query = turn(nn(normed, wq_ref[...]), cosines, sines) * HEAD_DIM**-0.5
        qkv_ref[0, rows, :] = query.astype(BF16)
        qkv_ref[1, rows, :] = turn(nn(normed, wk_ref[...]), cosines, sines).astype(BF16)
        qkv_ref[2, rows, :] = nn(normed, wv_ref[...]).astype(BF16)

    for block in range(blocks):
        first = max(0, block - reach) * BLOCK
        last = (block + 1) * BLOCK
        span = last - first
        rows = slice(block * BLOCK, last)
        row_ids = iota((BLOCK, span), 0) + block * BLOCK
        col_ids = iota((BLOCK, span), 1) + first
        seen = (col_ids <= row_ids) & (segc_ref[rows, :] == segr_ref[0:1, first:last])
        bias_ref[:, 0:span] = jnp.where(seen, 0.0, NEGATIVE)
        attended = []
        logs = log_ref[rows, :]
        for head in range(GROUP):
            mask = head_mask(head)
            scores = nt(qkv_ref[0, rows, :] * mask, qkv_ref[1, first:last, :]) + bias_ref[:, 0:span]
            top = jnp.max(scores, axis=1, keepdims=True)
            weights = jnp.exp(scores - top).astype(BF16)
            value = qkv_ref[2, first:last, :] * mask + (1 - mask)
            mixed = nn(weights, value)
            own = iota(mixed.shape, 1) // HEAD_DIM == head
            total = jnp.max(jnp.where(own, 0.0, mixed), axis=1, keepdims=True)
            attended.append(jnp.where(own, mixed / total, 0.0))
            logs = jnp.where(
                iota(logs.shape, 1) == step * GROUP + head, top + jnp.log(total), logs
            )
        log_ref[rows, :] = logs
        out_ref[rows, :] = (attended[0] + attended[1] + attended[2] + attended[3]).astype(BF16)

    @pl.when(step == pl.num_programs(0) - 1)
    def _():
        lse_ref[...] = log_ref[...].T[0 : lse_ref.shape[0], :]


def middle_kernel(
    kinds, ao_ref, wo_ref, tok_ref, small_ref, prev_ref, routes_ref, target_ref,
    resid_ref, scal_ref, send_ref, ffn_ref, first_ref, second_ref,
):
    tokens, width = tok_ref.shape
    gain = small_ref[...].astype(F32).T[kinds + 7 : kinds + 8, :]

    @pl.loop(0, tokens // BLOCK)
    def _(block):
        rows = pl.ds(pl.multiple_of(block * BLOCK, BLOCK), BLOCK)
        resid = tok_ref[rows, :].astype(F32) + nn(ao_ref[rows, :], wo_ref[...])
        resid_ref[rows, :] = resid
        inverse = inverse_rms(resid)
        low = (resid * inverse * gain).astype(BF16)
        ffn_ref[rows, :] = low
        logits = nn(low, small_ref[...]) + prev_ref[rows, :]
        lane = iota(logits.shape, 1)

        def pick(index):
            return jnp.sum(jnp.where(lane == index, logits, 0.0), axis=1, keepdims=True)

        def pair(left, right):
            top = jnp.maximum(left, right)
            left = jnp.exp(left - top)
            right = jnp.exp(right - top)
            total = left + right
            return left / total, right / total

        gates = pair(pick(routes_ref[rows, 0:1]), pick(routes_ref[rows, 1:2]))
        one = pair(pick(kinds), pick(kinds + 1))
        two = pair(pick(kinds + 2), pick(kinds + 3))
        scal = jnp.zeros_like(logits)
        for index, value in enumerate(gates + one + two + (inverse,)):
            scal = jnp.where(lane == index, value, scal)
        scal_ref[rows, :] = scal
        for gate, ref in zip(gates, (first_ref, second_ref)):
            high, rest = split_low(gate)
            ref[rows, :] = jnp.where(
                lane == 0, high.astype(F32), jnp.where(lane == 1, rest.astype(F32), 0.0)
            ).astype(BF16)

    @pl.loop(0, send_ref.shape[0])
    def _(expert):
        slots = iota((CAP, tokens), 0) + expert * CAP
        hot_one = (target_ref[0:1, :] == slots).astype(F32)
        hot_two = (target_ref[1:2, :] == slots).astype(F32)
        send_ref[expert, :, 0:width] = nn((hot_one + hot_two).astype(BF16), ffn_ref[...]).astype(
            BF16
        )
        send_ref[expert, :, width:] = (
            nn(hot_one.astype(BF16), first_ref[...]) + nn(hot_two.astype(BF16), second_ref[...])
        ).astype(BF16)


def expert_kernel(
    recv_ref, cot_ref, wg_ref, wu_ref, wo_ref, front_ref, ret_ref, out_acc, row_acc,
):
    step = pl.program_id(0)
    total, width = out_acc.shape
    tile = 512

    @pl.when(step == 0)
    def _():
        out_acc[...] = jnp.zeros_like(out_acc)
        row_acc[...] = jnp.zeros_like(row_acc)

    @pl.loop(0, total // tile)
    def _(block):
        rows = pl.ds(pl.multiple_of(block * tile, tile), tile)
        token = recv_ref[rows, 0:width]
        extra = recv_ref[rows, width:].astype(F32)
        gate_weight = extra[:, 0:1] + extra[:, 1:2]
        gate = nn(token, wg_ref[...])
        up = nn(token, wu_ref[...])
        grad = nt(cot_ref[rows, :], wo_ref[...]) * gate_weight
        sig = jax.nn.sigmoid(gate)
        act = gate * sig
        hidden = act * up
        out_acc[rows, :] += nn(hidden.astype(BF16), wo_ref[...])
        front_ref[2, rows, :] = (hidden * gate_weight).astype(BF16)
        gate_grad = (grad * up * sig * (1.0 + gate * (1.0 - sig))).astype(BF16)
        up_grad = (grad * act).astype(BF16)
        front_ref[0, rows, :] = gate_grad
        front_ref[1, rows, :] = up_grad
        row_acc[rows, :] += nt(gate_grad, wg_ref[...]) + nt(up_grad, wu_ref[...])

    @pl.when(step == pl.num_programs(0) - 1)
    def _():
        @pl.loop(0, total // CAP)
        def _(peer):
            rows = pl.ds(pl.multiple_of(peer * CAP, CAP), CAP)
            ret_ref[peer, 0:CAP, :] = out_acc[rows, :].astype(BF16)
            ret_ref[peer, CAP:, :] = row_acc[rows, :].astype(BF16)


def expert_grad_kernel(recv_ref, cot_ref, front_ref, gate_ref, up_ref, wout_ref, turned_ref):
    step = pl.program_id(0)
    width = turned_ref.shape[0]

    @pl.when(step == 0)
    def _():
        turned_ref[...] = recv_ref[:, 0:width].T

    wout_ref[...] = tn(front_ref[2], cot_ref[...]).astype(BF16)
    gate_ref[...] = nn(turned_ref[...], front_ref[0]).astype(BF16)
    up_ref[...] = nn(turned_ref[...], front_ref[1]).astype(BF16)


def combine_kernel(
    kinds, experts, ret_ref, target_ref, routes_ref, scal_ref, resid_ref, cot_ref, ao_ref,
    small_ref, wo_ref, mix_ref, prevt_ref, ind_ref,
    mixed_ref, prev_ref, mid_ref, proj_ref, attn_ref, delta_ref, minor_ref, vec_ref, gain_ref,
    gmix_ref, rows_ref,
):
    step = pl.program_id(0)

    @pl.when(step == 0)
    def _():
        rows_ref[...] = small_ref[...].astype(F32).T
        minor_ref[...] = jnp.zeros_like(minor_ref)
        vec_ref[...] = jnp.zeros_like(vec_ref)
        gain_ref[...] = jnp.zeros_like(gain_ref)
        gmix_ref[...] = jnp.zeros_like(gmix_ref)

    width = resid_ref.shape[1]
    slots = experts * CAP
    resid = resid_ref[...]
    cot = cot_ref[...]
    upstream = cot.astype(F32)
    scal = scal_ref[...]
    routes = (routes_ref[:, 0:1], routes_ref[:, 1:2])
    targets = (target_ref[:, 0:1], target_ref[:, 1:2])
    gates = (scal[:, 0:1], scal[:, 1:2])
    one_keep, one_vec = scal[:, 2:3], scal[:, 3:4]
    two_keep, two_vec = scal[:, 4:5], scal[:, 5:6]
    inverse = scal[:, 6:7]
    gain = rows_ref[kinds + 7 : kinds + 8, :]
    vec_one = rows_ref[kinds + 4 : kinds + 5, :]
    vec_two = rows_ref[kinds + 5 : kinds + 6, :]
    normed = resid * inverse
    ffn_norm = normed * gain
    low = ffn_norm.astype(BF16)
    slot_ids = iota((BLOCK, slots), 1)
    hots = [(target == slot_ids).astype(F32) for target in targets]
    outs = ret_ref[:, 0:CAP, :].reshape(slots, width)
    backs = ret_ref[:, CAP:, :].reshape(slots, width)
    branches = [nn(hot.astype(BF16), outs) for hot in hots]
    back = nn((hots[0] + hots[1]).astype(BF16), backs)

    def weight(kind):
        return sum(
            jnp.where(route == kind, gate, 0.0) for route, gate in zip(routes, gates)
        )

    weight_copy = weight(experts + 1)
    weight_one = weight(experts + 2)
    weight_two = weight(experts + 3)
    keep = weight_copy + weight_one * one_keep + weight_two * two_keep
    mixed_ref[...] = (
        resid
        + gates[0] * branches[0]
        + gates[1] * branches[1]
        + keep * ffn_norm
        + (weight_one * one_vec) * vec_one
        + (weight_two * two_vec) * vec_two
    ).astype(BF16)
    dot_norm = jnp.sum(upstream * ffn_norm, axis=1, keepdims=True)
    dot_one = jnp.sum(upstream * vec_one, axis=1, keepdims=True)
    dot_two = jnp.sum(upstream * vec_two, axis=1, keepdims=True)
    grads = []
    for route, branch in zip(routes, branches):
        grads.append(
            jnp.sum(branch * upstream, axis=1, keepdims=True)
            + jnp.where(route == experts + 1, dot_norm, 0.0)
            + jnp.where(route == experts + 2, one_keep * dot_norm + one_vec * dot_one, 0.0)
            + jnp.where(route == experts + 3, two_keep * dot_norm + two_vec * dot_two, 0.0)
        )
    mean_grad = gates[0] * grads[0] + gates[1] * grads[1]
    lane = iota((BLOCK, LANES), 1)
    wide = jnp.zeros((BLOCK, LANES), F32)
    for route, gate, grad in zip(routes, gates, grads):
        wide = jnp.where(lane == route, gate * (grad - mean_grad), wide)
    for index, keep_part, vec_part, grad_weight, dot in (
        (kinds, one_keep, one_vec, weight_one, dot_one),
        (kinds + 2, two_keep, two_vec, weight_two, dot_two),
    ):
        keep_grad = grad_weight * dot_norm
        vec_grad = grad_weight * dot
        both = keep_part * keep_grad + vec_part * vec_grad
        wide = jnp.where(lane == index, keep_part * (keep_grad - both), wide)
        wide = jnp.where(lane == index + 1, vec_part * (vec_grad - both), wide)
    wide_low = wide.astype(BF16)
    wide_back = wide_low.astype(F32)
    minor_ref[...] += nn(wide_back.T.astype(BF16), low)
    share = jnp.where(lane == 0, weight_one * one_vec, 0.0)
    share = jnp.where(lane == 1, weight_two * two_vec, share)
    high, rest = split_low(share.T)
    vec_ref[...] += nn(high, cot) + nn(rest, cot)
    prev_ref[...] = nn(wide_low, mix_ref[...])[:, 0:kinds]
    gmix_ref[...] += jnp.dot(
        prevt_ref[...], wide_back, precision=HIGHEST_PRECISION, preferred_element_type=F32
    )
    grad_two = back + nt(wide_low, small_ref[...]) + keep * upstream
    gain_ref[...] += jnp.sum(grad_two * normed, axis=0, keepdims=True)
    mid = upstream + norm_back(grad_two * gain, normed, inverse)
    mid_ref[...] = mid
    proj = mid.astype(BF16)
    proj_ref[...] = proj
    attn = nt(proj, wo_ref[...]).astype(BF16)
    attn_ref[...] = attn
    high, rest = split_low(attn.astype(F32) * ao_ref[...].astype(F32))
    delta_ref[...] = nt(ind_ref[...], high) + nt(ind_ref[...], rest)


def attend_back_kernel(
    gain_row, qkv_ref, grad_ref, lse_ref, delta_ref, cos_ref, sin_ref, segc_ref, segr_ref,
    wq_ref, wk_ref, wv_ref, attn_in_ref, ao_ref, proj_ref, tok_ref, mid_ref, small_ref,
    weight_ref, gtok_ref, gain_ref, dq_ref, dk_ref, dv_ref, bias_ref, in_t_ref, ao_t_ref, acc_ref,
):
    step = pl.program_id(0)
    tokens = tok_ref.shape[0]
    blocks = tokens // BLOCK
    reach = DOC_MAX // BLOCK

    @pl.when(step == 0)
    def _():
        in_t_ref[...] = attn_in_ref[...].T
        ao_t_ref[...] = ao_ref[...].T
        acc_ref[...] = jnp.zeros_like(acc_ref)

    dq_ref[...] = jnp.zeros_like(dq_ref)
    for block in range(blocks):
        first = block * BLOCK
        last = min(blocks, block + reach + 1) * BLOCK
        span = last - first
        keys = slice(first, first + BLOCK)
        key_ids = iota((BLOCK, span), 0) + first
        row_ids = iota((BLOCK, span), 1) + first
        seen = (key_ids <= row_ids) & (segc_ref[keys, :] == segr_ref[0:1, first:last])
        bias_ref[:, 0:span] = jnp.where(seen, 0.0, NEGATIVE)
        key = qkv_ref[1, keys, :]
        value = qkv_ref[2, keys, :]
        key_grad = None
        for head in range(GROUP):
            mask = head_mask(head)
            index = step * GROUP + head
            query = qkv_ref[0, first:last, :] * mask
            upstream = grad_ref[first:last, :] * mask
            scores = nt(key, query) + bias_ref[:, 0:span]
            probs = jnp.exp(scores - lse_ref[pl.ds(index, 1), first:last])
            prob_grad = nt(value, upstream)
            score_grad = (probs * (prob_grad - delta_ref[pl.ds(index, 1), first:last])).astype(BF16)
            dv = nn(probs.astype(BF16), upstream)
            dk = nn(score_grad, query)
            dq_ref[first:last, :] += tn(score_grad, key * mask)
            key_grad = dk if key_grad is None else key_grad + dk
            value_grad = dv if head == 0 else value_grad + dv
        dk_ref[keys, :] = key_grad
        dv_ref[keys, :] = value_grad.astype(BF16)

    @pl.loop(0, blocks)
    def _(block):
        rows = pl.ds(pl.multiple_of(block * BLOCK, BLOCK), BLOCK)
        cosines = cos_ref[rows, :]
        sines = -sin_ref[rows, :]
        dq = turn(dq_ref[rows, :] * HEAD_DIM**-0.5, cosines, sines)
        dk = turn(dk_ref[rows, :], cosines, sines)
        dq_ref[rows, :] = dq
        dk_ref[rows, :] = dk
        acc_ref[rows, :] += (
            nt(dq.astype(BF16), wq_ref[...])
            + nt(dk.astype(BF16), wk_ref[...])
            + nt(dv_ref[rows, :], wv_ref[...])
        )

    halves = GROUP_LANES // LANES
    for index, (turned, grads) in enumerate(
        ((in_t_ref, dq_ref), (in_t_ref, dk_ref), (in_t_ref, dv_ref), (ao_t_ref, proj_ref))
    ):
        product = nn(turned[...], grads[...].astype(BF16)).astype(BF16)
        for half in range(halves):
            weight_ref[index * halves + half] = product[:, half * LANES : (half + 1) * LANES]

    @pl.when(step == pl.num_programs(0) - 1)
    def _():
        gain = small_ref[...].astype(F32).T[gain_row : gain_row + 1, :]
        gain_ref[...] = jnp.zeros_like(gain_ref)

        @pl.loop(0, blocks)
        def _(block):
            rows = pl.ds(pl.multiple_of(block * BLOCK, BLOCK), BLOCK)
            values = tok_ref[rows, :].astype(F32)
            inverse = inverse_rms(values)
            normed = values * inverse
            grad = acc_ref[rows, :]
            gain_ref[...] += jnp.sum(grad * normed, axis=0, keepdims=True)
            gtok_ref[rows, :] = mid_ref[rows, :] + norm_back(grad * gain, normed, inverse)


def add_low(left, right):
    return (left.astype(F32) + right.astype(F32)).astype(BF16)


def over_parts(values, bit):
    return lax.ppermute(values, "dp", [(d, d ^ bit) for d in range(8)])


def greet(targets):
    barrier = pltpu.get_barrier_semaphore()
    for present, target in targets:
        @pl.when(present)
        def _():
            pl.semaphore_signal(barrier, inc=1, device_id=target, device_id_type=MESH)
    pl.semaphore_wait(barrier, sum(present.astype(jnp.int32) for present, _ in targets))


def gather_kernel(
    part_ref, cot_ref, target_ref, out_ref, rows_ref, outgoing, send_sem, recv_sem, local_sem,
    row_send, row_recv, own_sem,
):
    me = lax.axis_index("dp")
    owner = lax.axis_index("expert")
    here, flank = me // 2, me % 2
    core = owner % 2
    up = ((2 * jnp.minimum(here + 1, 3) + flank), here < 3)
    down = ((2 * jnp.maximum(here - 1, 0) + flank), here > 0)
    across = 2 * here + 1 - flank
    partner = owner + 1 - 2 * core
    always = here >= 0
    routes = (
        (up[1], {"dp": up[0]}),
        (down[1], {"dp": down[0]}),
        (always, {"dp": across}),
        (always, {"expert": partner}),
    )
    side = owner // 2
    beside = owner + 2 - 4 * side
    corner = partner + 2 - 4 * side
    peers = (beside, corner, partner, owner)
    greet((*routes, (always, {"expert": beside}), (always, {"expert": corner})))

    def row_copy(slot):
        return pltpu.make_async_remote_copy(
            src_ref=outgoing.at[slot],
            dst_ref=rows_ref.at[owner],
            send_sem=row_send.at[slot],
            recv_sem=row_recv.at[slot],
            device_id={"expert": peers[slot]},
            device_id_type=MESH,
        )

    def copy(index, half, route, source=None):
        return pltpu.make_async_remote_copy(
            src_ref=out_ref.at[index, half] if source is None else source,
            dst_ref=out_ref.at[index, half],
            send_sem=send_sem.at[route, index],
            recv_sem=recv_sem.at[half, index],
            device_id=routes[route][1],
            device_id_type=MESH,
        )

    def arrive(index, half):
        copy(index, half, 2).wait_recv()

    local = pltpu.make_async_copy(part_ref, out_ref.at[me], local_sem)
    local.start()
    for route in range(3):
        @pl.when(routes[route][0])
        def _():
            copy(me, core, route, part_ref.at[core]).start()
    tokens = cot_ref.shape[0]
    for slot, peer in enumerate(peers):
        slots = iota((CAP, tokens), 0) + peer * CAP
        hot = (target_ref[0:1, :] == slots) | (target_ref[1:2, :] == slots)
        outgoing[slot] = nn(hot.astype(F32).astype(BF16), cot_ref[...]).astype(BF16)
        if slot > 0:
            row_copy(slot - 1).start()
    own_rows = pltpu.make_async_copy(outgoing.at[3], rows_ref.at[owner], own_sem)
    own_rows.start()
    for distance in range(1, 5):
        for toward, forward, present in (
            (here - distance, 0, here >= distance),
            (here + distance, 1, here + distance <= 3),
        ):
            index = 2 * jnp.clip(toward, 0, 3) + flank

            @pl.when(present)
            def _():
                arrive(index, core)
                copy(index, core, 2).start()
                copy(index, core, 3).start()

            @pl.when(present & routes[forward][0])
            def _():
                copy(index, core, forward).start()
        for sign in (-1, 1):
            if distance == 1 and sign == 1:
                continue
            toward = here + sign * (distance - 1)
            index = 2 * jnp.clip(toward, 0, 3) + 1 - flank

            @pl.when((toward >= 0) & (toward <= 3))
            def _():
                arrive(index, core)
                copy(index, core, 3).start()
    for offset in range(1, 8):
        index = (me + offset) % 8
        arrive(index, 1 - core)
        copy(index, core, 3).wait_send()
    local.wait()
    for route in range(3):
        @pl.when(routes[route][0])
        def _():
            copy(me, core, route, part_ref.at[core]).wait_send()
    for distance in range(1, 4):
        for toward, forward, present in (
            (here - distance, 0, here >= distance),
            (here + distance, 1, here + distance <= 3),
        ):
            index = 2 * jnp.clip(toward, 0, 3) + flank

            @pl.when(present)
            def _():
                copy(index, core, 2).wait_send()

            @pl.when(present & routes[forward][0])
            def _():
                copy(index, core, forward).wait_send()
    for slot in range(3):
        row_copy(slot).wait_recv()
        row_copy(slot).wait_send()
    own_rows.wait()


def gather_parts(packed, cotangent, target_row):
    rows, columns = packed.shape
    width = cotangent.shape[1]
    whole, cot_rows = pl.pallas_call(
        gather_kernel,
        in_specs=[pl.BlockSpec(memory_space=pltpu.VMEM)] * 3,
        out_specs=[pl.BlockSpec(memory_space=pl.ANY)] * 2,
        out_shape=[
            jax.ShapeDtypeStruct((8, 2, rows // 2, columns), BF16),
            jax.ShapeDtypeStruct((4, CAP, width), BF16),
        ],
        scratch_shapes=[
            pltpu.VMEM((4, CAP, width), BF16),
            pltpu.SemaphoreType.DMA((4, 8)),
            pltpu.SemaphoreType.DMA((2, 8)),
            pltpu.SemaphoreType.DMA,
            pltpu.SemaphoreType.DMA((3,)),
            pltpu.SemaphoreType.DMA((3,)),
            pltpu.SemaphoreType.DMA,
        ],
        compiler_params=params(collective_id=0, has_side_effects=True),
        cost_estimate=cost(10e9, 10e6),
        name="gather_parts",
    )(packed.reshape(2, rows // 2, columns), cotangent, target_row)
    return whole.reshape(8 * rows, columns), cot_rows


def add_planes(target, left, right):
    @pl.loop(0, target.shape[0])
    def _(index):
        total = left[index].astype(F32) + right[index].astype(F32)
        target[index] = total.astype(target.dtype)


def reduce_kernel(
    gate_ref, up_ref, risen_ref, fallen_ref, pair_ref, weight_ref, minor_ref,
    gate_out, up_out, down_out, weight_out, minor_out,
    gate_in, up_in, line_in, gate_stage, up_stage, line_stage, pair_in, core_in, core_sum, side_in, side_sum, cross_in, line_ref, line_sum_ref,
    small_in, small_sum, piece_send, piece_recv, other_send, other_recv,
):
    me = lax.axis_index("dp")
    owner = lax.axis_index("expert")
    here, flank = me // 2, me % 2
    core, side = owner % 2, owner // 2
    rising = {"dp": 2 * jnp.minimum(here + 1, 3) + flank}
    falling = {"dp": 2 * jnp.maximum(here - 1, 0) + flank}
    across = {"dp": me + 1 - 2 * flank}
    partner = {"expert": owner + 1 - 2 * core}
    beside = {"expert": owner + 2 - 4 * side}
    always = here >= 0
    greet(((here < 3, rising), (here > 0, falling), (always, across), (always, partner),
           (always, beside)))
    pieces = (
        (gate_ref, gate_in, gate_stage),
        (up_ref, up_in, up_stage),
        (line_ref, line_in, line_stage),
    )

    def piece_copy(piece, turn_index, way, source):
        return pltpu.make_async_remote_copy(
            src_ref=source,
            dst_ref=pieces[piece][1].at[way, turn_index],
            send_sem=piece_send.at[piece, turn_index, way],
            recv_sem=piece_recv.at[piece, turn_index, way],
            device_id=(rising, falling)[way],
            device_id_type=MESH,
        )

    def other_copy(index, source, target, device):
        return pltpu.make_async_remote_copy(
            src_ref=source, dst_ref=target, send_sem=other_send.at[index],
            recv_sem=other_recv.at[index], device_id=device, device_id_type=MESH,
        )

    def direct(piece, turn_index):
        own = pieces[piece][0]

        @pl.when(here == 0)
        def _():
            piece_copy(piece, turn_index, 0, own.at[3 - turn_index]).start()

        @pl.when(here == 3)
        def _():
            piece_copy(piece, turn_index, 1, own.at[turn_index]).start()

    def relayed(turn_index):
        return (
            (0, (here > 0) & (here < 3 - turn_index), 3 - turn_index),
            (1, (here < 3) & (here > turn_index), turn_index),
        )

    def relay(piece, turn_index):
        own, landed, stage = pieces[piece]
        for way, present, chunk in relayed(turn_index):
            if piece == 0:
                present = present & ((here != 1) if way == 0 else (here != 2))

            @pl.when(present)
            def _():
                copy = piece_copy(piece, turn_index, way, stage.at[way, turn_index])
                copy.wait_recv()
                add_planes(
                    stage.at[way, turn_index], own.at[chunk], landed.at[way, turn_index]
                )
                copy.start()

    def early(turn_index):
        own, landed, stage = pieces[0]
        for way, place, chunk in ((0, 1, 3 - turn_index), (1, 2, turn_index)):
            @pl.when(here == place)
            def _():
                add_planes(
                    stage.at[way, turn_index], own.at[chunk], landed.at[way, turn_index]
                )
                piece_copy(0, turn_index, way, stage.at[way, turn_index]).start()

    def finish(piece, target):
        own, landed, stage = pieces[piece]
        lower = jnp.minimum(3 - here, 2)
        upper = jnp.minimum(here, 2)

        @pl.when((here > (1 if piece == 0 else 0)))
        def _():
            piece_copy(piece, lower, 0, stage.at[0, 0]).wait_recv()

        @pl.when(here < (2 if piece == 0 else 3))
        def _():
            piece_copy(piece, upper, 1, stage.at[0, 0]).wait_recv()

        @pl.when(here == 0)
        def _():
            add_planes(target, own.at[here], landed.at[1, upper])

        @pl.when(here == 3)
        def _():
            add_planes(target, own.at[here], landed.at[0, lower])

        @pl.when((here > 0) & (here < 3))
        def _():
            @pl.loop(0, target.shape[0])
            def _(index):
                total = (
                    own[here, index].astype(F32)
                    + landed[0, lower, index].astype(F32)
                    + landed[1, upper, index].astype(F32)
                )
                target[index] = total.astype(target.dtype)

    def drain(piece):
        own, _, stage = pieces[piece]
        for turn_index in range(0 if piece == 0 else 3):
            @pl.when(here == 0)
            def _():
                piece_copy(piece, turn_index, 0, own.at[3 - turn_index]).wait_send()

            @pl.when(here == 3)
            def _():
                piece_copy(piece, turn_index, 1, own.at[turn_index]).wait_send()
        for turn_index in range(2):
            for way, present, _ in relayed(turn_index):
                @pl.when(present)
                def _():
                    piece_copy(
                        piece, turn_index, way, stage.at[way, turn_index]
                    ).wait_send()

    half = core_in.shape[0]
    quarter = half // 2
    eighth = quarter // 2
    core_weight = [
        other_copy(
            14 * order,
            weight_ref.at[pl.ds(half * (1 - core) + quarter * which, quarter)],
            core_in.at[pl.ds(quarter * which, quarter)],
            partner,
        )
        for order, which in enumerate((1 - side, side))
    ]
    core_small = other_copy(1, minor_ref, small_in.at[0], partner)
    side_weight = [
        other_copy(
            2 + 13 * order,
            core_sum.at[pl.ds(quarter * (1 - side) + eighth * order, eighth)],
            side_in.at[pl.ds(eighth * order, eighth)],
            beside,
        )
        for order in range(2)
    ]
    side_small = other_copy(3, small_sum.at[0], small_in.at[1], beside)
    cross_weight = [
        other_copy(
            4 + 12 * order + z,
            side_sum.at[pl.ds(eighth * order, eighth), 2 * z + 1 - flank],
            cross_in.at[z, pl.ds(eighth * order, eighth)],
            across,
        )
        for order in range(2)
        for z in range(4)
    ]
    cross_small = other_copy(8, small_sum.at[1], small_in.at[2], across)
    rise_small = other_copy(9, small_sum.at[3], small_in.at[3], rising)
    fall_small = other_copy(10, small_sum.at[4], small_in.at[4], falling)
    mine = half * core + quarter * side
    own_part = weight_out.at[pl.ds(mine, quarter)]
    own_half = weight_out.at[pl.ds(half * core, half)]
    side_back = other_copy(11, own_part, own_part, beside)
    core_back = other_copy(12, own_half, own_half, partner)

    pair_copy = other_copy(13, pair_ref.at[1 - flank], pair_in, across)
    for copy in core_weight:
        copy.start()
    core_small.start()
    pair_copy.start()
    for turn_index in range(3):
        direct(1, turn_index)

    @pl.when(here == 1)
    def _():
        for turn_index in range(3):
            gate_in[0, turn_index] = risen_ref[2 - turn_index]

    @pl.when(here == 2)
    def _():
        for turn_index in range(3):
            gate_in[1, turn_index] = fallen_ref[turn_index]

    for turn_index in range(2):
        early(turn_index)
    for order, which in enumerate((1 - side, side)):
        core_weight[order].wait_recv()
        add_planes(
            core_sum.at[pl.ds(quarter * which, quarter)],
            weight_ref.at[pl.ds(half * core + quarter * which, quarter)],
            core_in.at[pl.ds(quarter * which, quarter)],
        )
        if order == 0:
            for copy in side_weight:
                copy.start()
    core_small.wait_recv()
    small_sum[0] = minor_ref[...] + small_in[0]
    side_small.start()
    for piece in (0, 1):
        relay(piece, 0)
    pair_copy.wait_recv()
    add_planes(down_out, pair_ref.at[flank], pair_in)
    for order in range(2):
        span = pl.ds(eighth * order, eighth)
        side_weight[order].wait_recv()
        add_planes(
            side_sum.at[span],
            core_sum.at[pl.ds(quarter * side + eighth * order, eighth)],
            side_in.at[span],
        )
        for copy in cross_weight[4 * order : 4 * order + 4]:
            copy.start()
    side_small.wait_recv()
    small_sum[1] = small_sum[0] + small_in[1]
    cross_small.start()
    for piece in (0, 1):
        relay(piece, 1)
    for copy in cross_weight:
        copy.wait_recv()
    cross_small.wait_recv()
    for z in range(4):
        add_planes(line_ref.at[z], side_sum.at[:, 2 * z + flank], cross_in.at[z])
    small_sum[2] = small_sum[1] + small_in[2]
    small_sum[3] = small_sum[2]
    small_sum[4] = small_sum[2]
    for turn_index in range(3):
        direct(2, turn_index)

    @pl.when(here == 0)
    def _():
        rise_small.start()

    @pl.when(here == 3)
    def _():
        fall_small.start()

    for turn_index in range(2):
        relay(2, turn_index)

    finish(2, line_sum_ref)
    for index in range(quarter):
        weight_out[mine + index] = line_sum_ref[index]
    side_back.start()

    @pl.when(here > 0)
    def _():
        rise_small.wait_recv()
        small_sum[3] = small_sum[2] + small_in[3]

    @pl.when((here > 0) & (here < 3))
    def _():
        rise_small.start()

    @pl.when(here < 3)
    def _():
        fall_small.wait_recv()
        small_sum[4] = small_sum[2] + small_in[4]

    @pl.when((here > 0) & (here < 3))
    def _():
        fall_small.start()

    minor_out[...] = small_sum[3] + small_sum[4] - small_sum[2]
    finish(0, gate_out)
    side_back.wait_recv()
    core_back.start()
    finish(1, up_out)
    core_back.wait_recv()
    for piece in range(3):
        drain(piece)
    for copy in (*core_weight, core_small, *side_weight, side_small, *cross_weight, cross_small,
                 side_back, core_back, pair_copy):
        copy.wait_send()

    @pl.when(here < 3)
    def _():
        rise_small.wait_send()

    @pl.when(here > 0)
    def _():
        fall_small.wait_send()


def reduce_parts(kept, down, weights, minor):
    gate, up = kept[:2]
    kept = [piece.reshape(-1, piece.shape[1] // 32, 32, piece.shape[2]) for piece in kept]
    pair = down.reshape(2, down.shape[1] // 32, 32, down.shape[2])
    blocks, width, lanes = weights.shape
    rows = width // 8
    plane = (rows, lanes)
    chunks = [piece.shape[1:] for piece in kept[:2]]
    line = (blocks // 4,) + plane
    low = [pltpu.VMEM((2, 3) + chunk, BF16) for chunk in chunks + [line]]
    stages = [pltpu.VMEM((2, 2) + chunk, BF16) for chunk in chunks + [line]]
    outs = pl.pallas_call(
        reduce_kernel,
        in_specs=[pl.BlockSpec(memory_space=pltpu.VMEM)] * 7,
        out_specs=[pl.BlockSpec(memory_space=pltpu.VMEM)] * 5,
        out_shape=[jax.ShapeDtypeStruct(chunk, F32) for chunk in chunks + [pair.shape[1:]]]
        + [
            jax.ShapeDtypeStruct((blocks,) + plane, BF16),
            jax.ShapeDtypeStruct(minor.shape, F32),
        ],
        scratch_shapes=[
            *low,
            *stages,
            pltpu.VMEM(pair.shape[1:], BF16),
            pltpu.VMEM((blocks // 2, 8) + plane, BF16),
            pltpu.VMEM((blocks // 2, 8) + plane, BF16),
            pltpu.VMEM((blocks // 4, 8) + plane, BF16),
            pltpu.VMEM((blocks // 4, 8) + plane, BF16),
            pltpu.VMEM((4,) + line, BF16),
            pltpu.VMEM((4,) + line, BF16),
            pltpu.VMEM(line, BF16),
            pltpu.VMEM((5,) + minor.shape, F32),
            pltpu.VMEM((5,) + minor.shape, F32),
            pltpu.SemaphoreType.DMA((3, 3, 2)),
            pltpu.SemaphoreType.DMA((3, 3, 2)),
            pltpu.SemaphoreType.DMA((20,)),
            pltpu.SemaphoreType.DMA((20,)),
        ],
        compiler_params=params(collective_id=1, has_side_effects=True),
        name="reduce_parts",
    )(*kept, pair, weights.reshape(blocks, 8, rows, lanes), minor)
    shapes = (gate.shape[1:], up.shape[1:], down.shape[1:])
    shares = [out.reshape(shape) for out, shape in zip(outs, shapes)]
    return shares, outs[3], outs[4]


FF_TILE = 256


def exchange_kernel(
    send_ref, cot_ref, win_ref, wout_ref,
    gate_keep, gate_away, up_keep, up_away, own_down, one_down, two_down, three_down, return_out,
    recv, cot, gate_w, up_w, down_w, front, turned, out_acc, row_acc, ret, gate_g, up_g, down_g,
    token_send, token_recv, back_send, back_recv, load_sem, weight_sem, store_sem, down_sem, own_sem,
):
    me = lax.axis_index("expert")
    spot = lax.axis_index("dp")
    here, flank = spot // 2, spot % 2
    line_peers = (here, here + 1 - 2 * (here % 2), here + 2 - 4 * (here // 2), 3 - here)
    down_parts = (own_down, one_down, two_down, three_down)
    share = gate_w.shape[0] // 8
    core, side = me % 2, me // 2
    partner = me + 1 - 2 * core
    beside = me + 2 - 4 * side
    corner = partner + 2 - 4 * side
    peers = (me, beside, corner, partner)
    always = me >= 0
    width = out_acc.shape[1]
    ff = down_w.shape[0]
    tiles = ff // FF_TILE
    greet([(always, {"expert": peer}) for peer in peers[1:]])

    def token_copy(slot):
        return pltpu.make_async_remote_copy(
            src_ref=send_ref.at[peers[slot]], dst_ref=recv.at[slot],
            send_sem=token_send.at[slot], recv_sem=token_recv.at[slot],
            device_id={"expert": peers[slot]}, device_id_type=MESH,
        )

    def back_copy(slot):
        return pltpu.make_async_remote_copy(
            src_ref=ret.at[slot], dst_ref=return_out.at[me],
            send_sem=back_send.at[slot], recv_sem=back_recv.at[slot],
            device_id={"expert": peers[slot]}, device_id_type=MESH,
        )

    def tile_slice(tile):
        return pl.ds(pl.multiple_of(tile * FF_TILE, FF_TILE), FF_TILE)

    def weight_copies(tile):
        cols = tile_slice(tile)
        shifted = pl.ds(pl.multiple_of(ff + tile * FF_TILE, FF_TILE), FF_TILE)
        return (
            pltpu.make_async_copy(
                win_ref.at[:, cols], gate_w.at[:, cols], weight_sem.at[0, tile]
            ),
            pltpu.make_async_copy(
                win_ref.at[:, shifted], up_w.at[:, cols], weight_sem.at[1, tile]
            ),
            pltpu.make_async_copy(
                wout_ref.at[cols, :], down_w.at[cols, :], weight_sem.at[2, tile]
            ),
        )

    def side_copy(piece, index, kept):
        source = (gate_g, up_g)[piece].at[index * share : (index + 1) * share, :]
        target = ((gate_away, gate_keep), (up_away, up_keep))[piece][kept].at[index // 2]
        return pltpu.make_async_copy(source, target, store_sem.at[piece, index])

    def down_copy(tile, distance):
        return pltpu.make_async_copy(
            down_g.at[tile_slice(tile), :], down_parts[distance].at[tile % 2], down_sem.at[tile]
        )

    for slot in (1, 2, 3):
        token_copy(slot).start()
    loads = [pltpu.make_async_copy(send_ref.at[me], recv.at[0], load_sem.at[0])] + [
        pltpu.make_async_copy(cot_ref.at[peers[slot]], cot.at[slot], load_sem.at[1 + slot])
        for slot in range(4)
    ]
    for load in loads:
        load.start()

    @pl.loop(0, tiles)
    def _(tile):
        for copy in weight_copies(tile):
            copy.start()

    for load in loads:
        load.wait()

    def work(slot):
        extra = recv[slot, :, width:].astype(F32)
        gate_weight = extra[:, 0:1] + extra[:, 1:2]
        out_acc[...] = jnp.zeros_like(out_acc)
        row_acc[...] = jnp.zeros_like(row_acc)

        @pl.loop(0, tiles)
        def _(tile):
            cols = tile_slice(tile)
            if slot == 0:
                for copy in weight_copies(tile):
                    copy.wait()
            token = recv[slot, :, 0:width]
            gate = nn(token, gate_w[:, cols])
            up = nn(token, up_w[:, cols])
            grad = nt(cot[slot], down_w[cols, :]) * gate_weight
            sig = jax.nn.sigmoid(gate)
            act = gate * sig
            hidden = act * up
            out_acc[...] += nn(hidden.astype(BF16), down_w[cols, :])
            front[2, slot, :, cols] = (hidden * gate_weight).astype(BF16)
            gate_grad = (grad * up * sig * (1.0 + gate * (1.0 - sig))).astype(BF16)
            up_grad = (grad * act).astype(BF16)
            front[0, slot, :, cols] = gate_grad
            front[1, slot, :, cols] = up_grad
            row_acc[...] += nt(gate_grad, gate_w[:, cols]) + nt(up_grad, up_w[:, cols])

        ret[slot, 0:CAP, :] = out_acc[...].astype(BF16)
        ret[slot, CAP:, :] = row_acc[...].astype(BF16)
        turned[:, slot * CAP : (slot + 1) * CAP] = recv[slot, :, 0:width].T

    own_back = pltpu.make_async_copy(ret.at[0], return_out.at[me], own_sem)
    work(0)
    own_back.start()
    for slot in (1, 2, 3):
        token_copy(slot).wait_recv()
        work(slot)
        back_copy(slot).start()
    total = 4 * CAP

    @pl.loop(0, tiles)
    def _(tile):
        cols = tile_slice(tile)
        hidden = front[2, :, :, cols].reshape(total, FF_TILE)
        down_g[cols, :] = tn(hidden, cot[...].reshape(total, width)).astype(BF16)
        gate_g[:, cols] = nn(turned[...], front[0, :, :, cols].reshape(total, FF_TILE)).astype(BF16)
        up_g[:, cols] = nn(turned[...], front[1, :, :, cols].reshape(total, FF_TILE)).astype(BF16)
        for distance in range(4):
            @pl.when(tile // 2 == line_peers[distance])
            def _():
                down_copy(tile, distance).start()

    for piece in range(2):
        for index in range(8):
            for kept in range(2):
                @pl.when((flank == index % 2) if kept else (flank != index % 2))
                def _():
                    side_copy(piece, index, kept).start()

    for slot in (1, 2, 3):
        token_copy(slot).wait_send()
        back_copy(slot).wait_recv()
        back_copy(slot).wait_send()
    own_back.wait()

    for piece in range(2):
        for index in range(8):
            side_copy(piece, index, 1).wait()

    @pl.loop(0, tiles)
    def _(tile):
        down_copy(tile, 0).wait()


def exchange_experts(send, cot_rows, w_in, w_out):
    peers, cap, payload = send.shape
    ff, width = w_out.shape
    anywhere = pl.BlockSpec(memory_space=pl.ANY)
    tiles = ff // FF_TILE
    *grads, returned = pl.pallas_call(
        exchange_kernel,
        in_specs=[anywhere] * 4,
        out_specs=[anywhere] * 9,
        out_shape=[jax.ShapeDtypeStruct((4, width // 8, ff), BF16)] * 4
        + [jax.ShapeDtypeStruct((2, ff // 8, width), BF16)] * 4
        + [jax.ShapeDtypeStruct((peers, 2 * cap, width), BF16)],
        scratch_shapes=[
            pltpu.VMEM((peers, cap, payload), BF16),
            pltpu.VMEM((peers, cap, width), BF16),
            pltpu.VMEM((width, ff), BF16),
            pltpu.VMEM((width, ff), BF16),
            pltpu.VMEM((ff, width), BF16),
            pltpu.VMEM((3, peers, cap, ff), BF16),
            pltpu.VMEM((width, peers * cap), BF16),
            pltpu.VMEM((cap, width), F32),
            pltpu.VMEM((cap, width), F32),
            pltpu.VMEM((peers, 2 * cap, width), BF16),
            pltpu.VMEM((width, ff), BF16),
            pltpu.VMEM((width, ff), BF16),
            pltpu.VMEM((ff, width), BF16),
            pltpu.SemaphoreType.DMA((4,)),
            pltpu.SemaphoreType.DMA((4,)),
            pltpu.SemaphoreType.DMA((4,)),
            pltpu.SemaphoreType.DMA((4,)),
            pltpu.SemaphoreType.DMA((5,)),
            pltpu.SemaphoreType.DMA((3, tiles)),
            pltpu.SemaphoreType.DMA((2, 8)),
            pltpu.SemaphoreType.DMA((tiles,)),
            pltpu.SemaphoreType.DMA,
        ],
        compiler_params=params(collective_id=2, has_side_effects=True),
        cost_estimate=cost(18 * peers * cap * width * ff, 40e6),
        name="exchange_experts",
    )(send, cot_rows.reshape(peers, cap, width), w_in, w_out)
    return grads, returned


def plain_experts(send, cot_rows, w_in_one, w_out_one, swap):
    experts, _, payload = send.shape
    ff, width = w_out_one.shape
    recv = swap(send).reshape(experts * CAP, payload)

    slot_count = experts * CAP
    ff_tile = 256
    ff_tiles = ff // ff_tile
    slot_full = whole_block((slot_count, width))
    recv_full = whole_block((slot_count, payload))
    front_spec = pl.BlockSpec((3, slot_count, ff_tile), lambda j: (0, 0, j))
    front, ret = pl.pallas_call(
        expert_kernel,
        grid=(ff_tiles,),
        in_specs=[
            recv_full,
            slot_full,
            pl.BlockSpec((width, ff_tile), lambda j: (0, j)),
            pl.BlockSpec((width, ff_tile), lambda j: (0, ff_tiles + j)),
            pl.BlockSpec((ff_tile, width), lambda j: (j, 0)),
        ],
        out_specs=[front_spec, whole_block((experts, 2 * CAP, width))],
        out_shape=[
            jax.ShapeDtypeStruct((3, slot_count, ff), BF16),
            jax.ShapeDtypeStruct((experts, 2 * CAP, width), BF16),
        ],
        scratch_shapes=[pltpu.VMEM((slot_count, width), F32)] * 2,
        compiler_params=params(),
        cost_estimate=cost(12 * slot_count * width * ff, 26e6),
        name="expert",
    )(recv, cot_rows, w_in_one, w_in_one, w_out_one)
    returned = swap(ret)
    expert_grads = pl.pallas_call(
        expert_grad_kernel,
        grid=(ff_tiles,),
        in_specs=[recv_full, slot_full, front_spec],
        out_specs=[
            pl.BlockSpec((width, ff_tile), lambda j: (0, j)),
            pl.BlockSpec((width, ff_tile), lambda j: (0, j)),
            pl.BlockSpec((ff_tile, width), lambda j: (j, 0)),
        ],
        out_shape=[
            jax.ShapeDtypeStruct((width, ff), BF16),
            jax.ShapeDtypeStruct((width, ff), BF16),
            jax.ShapeDtypeStruct((ff, width), BF16),
        ],
        scratch_shapes=[pltpu.VMEM((width, slot_count), BF16)],
        compiler_params=params(),
        cost_estimate=cost(6 * slot_count * width * ff, 24e6),
        name="expert_grad",
    )(recv, cot_rows, front)
    return expert_grads, returned


def per_device(
    tokens, prev_scores, segments, routes, wqkv, wo, router, const_gate, const_vec, gain1, gain2,
    gate_mix, w_in, w_out, cotangent,
):
    tok_count, width = tokens.shape
    kinds = router.shape[1]
    experts = w_in.shape[0] * lax.axis_size("expert")
    ff = w_out.shape[1]
    qkv_cols = wqkv.shape[1]
    parts = lax.axis_size("dp")
    by_hand = parts == 8 and experts == 4
    small = jnp.concatenate(
        [router, const_gate, const_vec, gain1[:, None], gain2[:, None]], axis=1
    )
    packed = jnp.concatenate(
        [wqkv, wo, jnp.pad(small, ((0, 0), (0, LANES - small.shape[1])))], axis=1
    )

    seq_len = segments.shape[1]
    positions = (jnp.arange(tok_count, dtype=jnp.int32) % seq_len).astype(F32)
    half = HEAD_DIM // 2
    frequency = 10000.0 ** (-jnp.arange(half).astype(F32) / half)
    angles = positions[:, None] * frequency[None, :]
    cosines = jnp.tile(jnp.cos(angles), (1, LANES // half))
    sines = jnp.tile(jnp.sin(angles), (1, LANES // half))
    signs = jnp.where(jnp.arange(LANES) % HEAD_DIM < half, -1.0, 1.0).astype(F32)
    sines = sines * signs[None, :]
    seg_col = segments.reshape(tok_count, 1)
    seg_row = segments.reshape(1, tok_count)

    names = jnp.arange(kinds, dtype=jnp.int32)
    hot = [routes[:, i : i + 1] == names[None, :] for i in range(2)]
    named = (hot[0] | hot[1]).astype(BF16)
    ids = jnp.arange(tok_count, dtype=jnp.int32)
    before = (ids[:, None] > ids[None, :]).astype(BF16)
    earlier = jnp.dot(before, named, preferred_element_type=F32)
    slots = [jnp.sum(jnp.where(h, earlier, 0.0), axis=1).astype(jnp.int32) for h in hot]
    targets = [
        jnp.where(routes[:, i] < experts, routes[:, i] * CAP + slots[i], experts * CAP)
        for i in range(2)
    ]
    target_row = jnp.stack(targets, axis=0)
    target_col = jnp.stack(targets, axis=1)
    prev_mix = jnp.dot(prev_scores, gate_mix.astype(F32), precision=HIGHEST_PRECISION)
    prev_mix = jnp.pad(prev_mix, ((0, 0), (0, LANES - kinds)))

    def swap(values):
        return lax.all_to_all(values, "expert", split_axis=0, concat_axis=0, tiled=True)

    if by_hand:
        whole, cot_rows = gather_parts(packed, cotangent, target_row)
    else:
        whole = lax.all_gather(packed, "dp", axis=0, tiled=True)
        cot_send = pl.pallas_call(
            functools.partial(send_cotangent_kernel, experts),
            out_shape=jax.ShapeDtypeStruct((experts, CAP, width), BF16),
            compiler_params=params(),
            cost_estimate=cost(2 * experts * CAP * tok_count * width, 4 * tok_count * width),
            name="send_cotangent",
        )(cotangent, target_row)
        cot_rows = swap(cot_send)
    cot_rows = cot_rows.reshape(experts * CAP, width)

    groups = HEADS // GROUP
    tiles = qkv_cols // 3 // GROUP_LANES
    weight_specs = [
        pl.BlockSpec((width, GROUP_LANES), functools.partial(lambda o, i: (0, o + i), part * tiles))
        for part in range(3)
    ]
    small_spec = pl.BlockSpec((width, LANES), lambda *_: (0, (qkv_cols + width) // LANES))
    wo_spec = pl.BlockSpec((width, width), lambda *_: (0, qkv_cols // width))
    table = whole_block((tok_count, LANES))
    full = whole_block((tok_count, width))
    group_spec = pl.BlockSpec((tok_count, GROUP_LANES), lambda i: (0, i))
    qkv_spec = pl.BlockSpec((3, tok_count, GROUP_LANES), lambda i: (0, 0, i))
    seg_specs = [whole_block((tok_count, 1)), whole_block((1, tok_count))]
    span = DOC_MAX + BLOCK
    head_rows = 16
    lse_spec = whole_block((head_rows, tok_count))
    qkv, attn_in, attn_out, lse = pl.pallas_call(
        functools.partial(attend_kernel, kinds + 6),
        grid=(groups,),
        in_specs=[full, *weight_specs, small_spec, table, table, *seg_specs],
        out_specs=[qkv_spec, full, group_spec, lse_spec],
        out_shape=[
            jax.ShapeDtypeStruct((3, tok_count, width), BF16),
            jax.ShapeDtypeStruct((tok_count, width), BF16),
            jax.ShapeDtypeStruct((tok_count, width), BF16),
            jax.ShapeDtypeStruct((head_rows, tok_count), F32),
        ],
        scratch_shapes=[
            pltpu.VMEM((1, width), F32),
            pltpu.VMEM((BLOCK, span), F32),
            pltpu.VMEM((tok_count, LANES), F32),
        ],
        compiler_params=params(),
        cost_estimate=cost(12e9, 16e6),
        name="attend",
    )(tokens, whole, whole, whole, whole, cosines, sines, seg_col, seg_row)

    payload = width + LANES
    resid_mid, scal, send = pl.pallas_call(
        functools.partial(middle_kernel, kinds),
        grid=(1,),
        in_specs=[
            full, wo_spec, full, small_spec, table, whole_block((tok_count, 2)),
            whole_block((2, tok_count)),
        ],
        out_specs=[full, table, whole_block((experts, CAP, payload))],
        out_shape=[
            jax.ShapeDtypeStruct((tok_count, width), F32),
            jax.ShapeDtypeStruct((tok_count, LANES), F32),
            jax.ShapeDtypeStruct((experts, CAP, payload), BF16),
        ],
        scratch_shapes=[
            pltpu.VMEM((tok_count, width), BF16),
            pltpu.VMEM((tok_count, LANES), BF16),
            pltpu.VMEM((tok_count, LANES), BF16),
        ],
        compiler_params=params(),
        cost_estimate=cost(3.5e9, 10e6),
        name="middle",
    )(attn_out, whole, tokens, whole, prev_mix, routes, target_row)
    w_in_one = w_in.reshape(width, 2 * ff)
    w_out_one = w_out.reshape(ff, width)
    if by_hand:
        expert_grads, returned = exchange_experts(send, cot_rows, w_in_one, w_out_one)
    else:
        expert_grads, returned = plain_experts(send, cot_rows, w_in_one, w_out_one, swap)
    returned, *expert_grads = lax.optimization_barrier((returned, *expert_grads))
    if by_hand:
        gate_keep, gate_away, up_keep, up_away, *down_parts = expert_grads
        gate_pair = (gate_keep, over_parts(gate_away, 1))
        up_pair = (up_keep, over_parts(up_away, 1))
        lined = [down_parts[0]]
        for i in (1, 2, 3):
            lined.append(over_parts(down_parts[i], 2 * i))

    mix_turned = jnp.pad(gate_mix.T, ((0, LANES - kinds), (0, LANES - kinds)))
    indicator = (
        jnp.arange(width)[None, :] // HEAD_DIM == jnp.arange(head_rows)[:, None]
    ).astype(BF16)
    token_block = pl.BlockSpec((BLOCK, width), lambda i: (i, 0))
    table_block = pl.BlockSpec((BLOCK, LANES), lambda i: (i, 0))
    two_block = pl.BlockSpec((BLOCK, 2), lambda i: (i, 0))
    (
        mixed, grad_prev, mid_grad, proj_grad, attn_grad, delta, minor, vec, gain2_row, grad_mix,
    ) = pl.pallas_call(
        functools.partial(combine_kernel, kinds, experts),
        grid=(tok_count // BLOCK,),
        in_specs=[
            whole_block((experts, 2 * CAP, width)), two_block, two_block, table_block,
            token_block, token_block, token_block, small_spec, wo_spec,
            whole_block((LANES, LANES)),
            pl.BlockSpec((kinds, BLOCK), lambda i: (0, i)),
            whole_block((head_rows, width)),
        ],
        out_specs=[
            token_block, pl.BlockSpec((BLOCK, kinds), lambda i: (i, 0)), token_block, token_block,
            token_block, pl.BlockSpec((head_rows, BLOCK), lambda i: (0, i)),
            whole_block((LANES, width)), whole_block((LANES, width)), whole_block((1, width)),
            whole_block((kinds, LANES)),
        ],
        out_shape=[
            jax.ShapeDtypeStruct((tok_count, width), BF16),
            jax.ShapeDtypeStruct((tok_count, kinds), F32),
            jax.ShapeDtypeStruct((tok_count, width), F32),
            jax.ShapeDtypeStruct((tok_count, width), BF16),
            jax.ShapeDtypeStruct((tok_count, width), BF16),
            jax.ShapeDtypeStruct((head_rows, tok_count), F32),
            jax.ShapeDtypeStruct((LANES, width), F32),
            jax.ShapeDtypeStruct((LANES, width), F32),
            jax.ShapeDtypeStruct((1, width), F32),
            jax.ShapeDtypeStruct((kinds, LANES), F32),
        ],
        scratch_shapes=[pltpu.VMEM((LANES, width), F32)],
        compiler_params=params(),
        cost_estimate=cost(1e6, 1e5),
        name="combine",
    )(
        returned, target_col, routes, scal, resid_mid, cotangent, attn_out, whole, whole,
        mix_turned, prev_scores.T, indicator,
    )

    if by_hand:
        gate_pair, attn_grad = lax.optimization_barrier((gate_pair, attn_grad))
        gate_met = add_low(*gate_pair)
        risen = lax.ppermute(gate_met[1:], "dp", [(0, 2), (1, 3)])
        fallen = lax.ppermute(gate_met[:3], "dp", [(6, 4), (7, 5)])
    halves = GROUP_LANES // LANES
    weights, grad_tokens, gain1_row = pl.pallas_call(
        functools.partial(attend_back_kernel, kinds + 6),
        grid=(groups,),
        in_specs=[
            qkv_spec, group_spec, lse_spec, lse_spec, table, table, *seg_specs, *weight_specs,
            full, full, group_spec, full, full, small_spec,
        ],
        out_specs=[
            pl.BlockSpec((4 * halves, width, LANES), lambda i: (i, 0, 0)), full,
            whole_block((1, width)),
        ],
        out_shape=[
            jax.ShapeDtypeStruct((4 * halves * groups, width, LANES), BF16),
            jax.ShapeDtypeStruct((tok_count, width), F32),
            jax.ShapeDtypeStruct((1, width), F32),
        ],
        scratch_shapes=[
            pltpu.VMEM((tok_count, GROUP_LANES), F32),
            pltpu.VMEM((tok_count, GROUP_LANES), F32),
            pltpu.VMEM((tok_count, GROUP_LANES), BF16),
            pltpu.VMEM((BLOCK, span), F32),
            pltpu.VMEM((width, tok_count), BF16),
            pltpu.VMEM((width, tok_count), BF16),
            pltpu.VMEM((tok_count, width), F32),
        ],
        compiler_params=params(),
        cost_estimate=cost(1e6, 1e5),
        name="attend_back",
    )(
        qkv, attn_grad, lse, delta, cosines, sines, seg_col, seg_row, whole, whole, whole,
        attn_in, attn_out, proj_grad, tokens, mid_grad, whole,
    )

    minor_rows = jnp.concatenate([minor[: kinds + 4], vec[:2], gain1_row, gain2_row], axis=0)
    minor_all = jnp.concatenate(
        [minor_rows, jnp.pad(grad_mix[:, :kinds], ((0, 0), (0, width - kinds)))], axis=0
    )
    rows = width // parts
    if by_hand:
        up_pair, lined, risen, fallen, weights = lax.optimization_barrier(
            (up_pair, lined, risen, fallen, weights)
        )
        kept = [gate_met, add_low(*up_pair), risen, fallen]
        shares, weight_sum, minor_all = reduce_parts(
            kept, sum(part.astype(F32) for part in lined).astype(BF16), weights, minor_all
        )
    else:
        shares = [
            lax.psum_scatter(grad, "dp", scatter_dimension=0, tiled=True).astype(F32)
            for grad in expert_grads
        ]
        weight_part = lax.psum_scatter(weights, "expert", scatter_dimension=0, tiled=True)
        weight_part = lax.psum_scatter(weight_part, "dp", scatter_dimension=1, tiled=True)
        weight_sum = lax.all_gather(weight_part, "expert", axis=0, tiled=True)
        minor_all = lax.psum(minor_all, ("dp", "expert"))
    grad_gate_mix = minor_all[kinds + 8 :, :kinds]
    minor_sum = lax.dynamic_slice_in_dim(
        minor_all[: kinds + 8], lax.axis_index("dp") * rows, rows, 1
    ).T
    weight_sum = weight_sum.reshape(groups, 4, -1, rows, LANES)
    weight_sum = weight_sum.transpose(3, 1, 0, 2, 4).reshape(rows, 4 * width).astype(F32)
    return (
        mixed,
        grad_tokens,
        grad_prev,
        weight_sum[:, :qkv_cols],
        weight_sum[:, qkv_cols:],
        minor_sum[:, :kinds],
        minor_sum[:, kinds : kinds + 4],
        minor_sum[:, kinds + 4 : kinds + 6],
        minor_sum[:, kinds + 6],
        minor_sum[:, kinds + 7],
        grad_gate_mix,
        jnp.concatenate([shares[0], shares[1]], axis=1)[None],
        shares[2][None],
    )


def solution(mesh):
    rows = P(("dp", "expert"), None)
    in_specs = (
        rows, rows, rows, rows,
        P("dp", None), P("dp", None), P("dp", None), P("dp", None), P("dp", None), P("dp"), P("dp"),
        P(), P("expert", None, None), P("expert", None, None), rows,
    )
    out_specs = (
        rows, rows, rows,
        P("dp", None), P("dp", None), P("dp", None), P("dp", None), P("dp", None), P("dp"), P("dp"),
        P(), P("expert", "dp", None), P("expert", "dp", None),
    )
    return jax.shard_map(
        per_device, mesh=mesh, in_specs=in_specs, out_specs=out_specs, check_vma=False
    )
```

```python
import functools

import jax
import jax.numpy as jnp
from jax import lax
from jax.experimental import pallas as pl
from jax.experimental.pallas import tpu as pltpu
from jax.sharding import PartitionSpec as P


HEADS = 12
HEAD_DIM = 64
CAP = 256
DOC_MAX = 512
NORM_EPSILON = 1e-06
HIGHEST_PRECISION = lax.Precision.HIGHEST
NEGATIVE = -1e30
F32 = jnp.float32
BF16 = jnp.bfloat16
BLOCK = 256
GROUP = 4
GROUP_LANES = GROUP * HEAD_DIM
LANES = 128
MESH = pl.DeviceIdType.MESH
VMEM_BYTES = 62 * 1024 * 1024


def nn(left, right):
    return jnp.dot(left, right, preferred_element_type=F32)


def nt(left, right):
    return lax.dot_general(left, right, (((1,), (1,)), ((), ())), preferred_element_type=F32)


def tn(left, right):
    return lax.dot_general(left, right, (((0,), (0,)), ((), ())), preferred_element_type=F32)


def iota(shape, axis):
    return lax.broadcasted_iota(jnp.int32, shape, axis)


def split_low(values):
    high = values.astype(BF16)
    return high, (values - high.astype(F32)).astype(BF16)


def inverse_rms(values):
    return lax.rsqrt(jnp.mean(values * values, axis=-1, keepdims=True) + NORM_EPSILON)


def norm_back(upstream, normed, inverse):
    return inverse * (upstream - normed * jnp.mean(upstream * normed, axis=-1, keepdims=True))


def turn(values, cosines, signed_sines):
    pieces = []
    for start in range(0, values.shape[1], LANES):
        part = values[:, start : start + LANES]
        front = iota(part.shape, 1) % HEAD_DIM < HEAD_DIM // 2
        swapped = jnp.where(
            front,
            pltpu.roll(part, LANES - HEAD_DIM // 2, 1),
            pltpu.roll(part, HEAD_DIM // 2, 1),
        )
        pieces.append(part * cosines + swapped * signed_sines)
    return jnp.concatenate(pieces, axis=1)


def head_mask(head):
    return (iota((1, GROUP_LANES), 1) // HEAD_DIM == head).astype(F32).astype(BF16)


def params(**extra):
    return pltpu.CompilerParams(vmem_limit_bytes=VMEM_BYTES, **extra)


def whole_block(shape):
    return pl.BlockSpec(shape, lambda *_: (0,) * len(shape))


def cost(flops, moved):
    return pl.CostEstimate(flops=int(flops), bytes_accessed=int(moved), transcendentals=0)


def send_cotangent_kernel(experts, cot_ref, target_ref, out_ref):
    tokens = cot_ref.shape[0]

    @pl.loop(0, experts)
    def _(expert):
        slots = iota((CAP, tokens), 0) + expert * CAP
        hot = (target_ref[0:1, :] == slots) | (target_ref[1:2, :] == slots)
        out_ref[expert] = nn(hot.astype(F32).astype(BF16), cot_ref[...]).astype(BF16)


def attend_kernel(
    gain_row, tok_ref, wq_ref, wk_ref, wv_ref, small_ref, cos_ref, sin_ref, segc_ref, segr_ref,
    qkv_ref, attn_in_ref, out_ref, lse_ref, gain_ref, bias_ref, log_ref,
):
    step = pl.program_id(0)
    tokens = tok_ref.shape[0]
    blocks = tokens // BLOCK
    reach = DOC_MAX // BLOCK

    @pl.when(step == 0)
    def _():
        gain_ref[...] = small_ref[...].astype(F32).T[gain_row : gain_row + 1, :]
        log_ref[...] = jnp.zeros_like(log_ref)

        @pl.loop(0, blocks)
        def _(block):
            rows = pl.ds(pl.multiple_of(block * BLOCK, BLOCK), BLOCK)
            values = tok_ref[rows, :].astype(F32)
            attn_in_ref[rows, :] = (values * inverse_rms(values) * gain_ref[...]).astype(BF16)

    @pl.loop(0, blocks)
    def _(block):
        rows = pl.ds(pl.multiple_of(block * BLOCK, BLOCK), BLOCK)
        normed = attn_in_ref[rows, :]
        cosines = cos_ref[rows, :]
        sines = sin_ref[rows, :]
        query = turn(nn(normed, wq_ref[...]), cosines, sines) * HEAD_DIM**-0.5
        qkv_ref[0, rows, :] = query.astype(BF16)
        qkv_ref[1, rows, :] = turn(nn(normed, wk_ref[...]), cosines, sines).astype(BF16)
        qkv_ref[2, rows, :] = nn(normed, wv_ref[...]).astype(BF16)

    for block in range(blocks):
        first = max(0, block - reach) * BLOCK
        last = (block + 1) * BLOCK
        span = last - first
        rows = slice(block * BLOCK, last)
        row_ids = iota((BLOCK, span), 0) + block * BLOCK
        col_ids = iota((BLOCK, span), 1) + first
        seen = (col_ids <= row_ids) & (segc_ref[rows, :] == segr_ref[0:1, first:last])
        bias_ref[:, 0:span] = jnp.where(seen, 0.0, NEGATIVE)
        attended = []
        logs = log_ref[rows, :]
        for head in range(GROUP):
            mask = head_mask(head)
            scores = nt(qkv_ref[0, rows, :] * mask, qkv_ref[1, first:last, :]) + bias_ref[:, 0:span]
            top = jnp.max(scores, axis=1, keepdims=True)
            weights = jnp.exp(scores - top).astype(BF16)
            value = qkv_ref[2, first:last, :] * mask + (1 - mask)
            mixed = nn(weights, value)
            own = iota(mixed.shape, 1) // HEAD_DIM == head
            total = jnp.max(jnp.where(own, 0.0, mixed), axis=1, keepdims=True)
            attended.append(jnp.where(own, mixed / total, 0.0))
            logs = jnp.where(
                iota(logs.shape, 1) == step * GROUP + head, top + jnp.log(total), logs
            )
        log_ref[rows, :] = logs
        out_ref[rows, :] = (attended[0] + attended[1] + attended[2] + attended[3]).astype(BF16)

    @pl.when(step == pl.num_programs(0) - 1)
    def _():
        lse_ref[...] = log_ref[...].T[0 : lse_ref.shape[0], :]


def middle_kernel(
    kinds, ao_ref, wo_ref, tok_ref, small_ref, prev_ref, routes_ref, target_ref,
    resid_ref, scal_ref, send_ref, ffn_ref, first_ref, second_ref,
):
    tokens, width = tok_ref.shape
    gain = small_ref[...].astype(F32).T[kinds + 7 : kinds + 8, :]

    @pl.loop(0, tokens // BLOCK)
    def _(block):
        rows = pl.ds(pl.multiple_of(block * BLOCK, BLOCK), BLOCK)
        resid = tok_ref[rows, :].astype(F32) + nn(ao_ref[rows, :], wo_ref[...])
        resid_ref[rows, :] = resid
        inverse = inverse_rms(resid)
        low = (resid * inverse * gain).astype(BF16)
        ffn_ref[rows, :] = low
        logits = nn(low, small_ref[...]) + prev_ref[rows, :]
        lane = iota(logits.shape, 1)

        def pick(index):
            return jnp.sum(jnp.where(lane == index, logits, 0.0), axis=1, keepdims=True)

        def pair(left, right):
            top = jnp.maximum(left, right)
            left = jnp.exp(left - top)
            right = jnp.exp(right - top)
            total = left + right
            return left / total, right / total

        gates = pair(pick(routes_ref[rows, 0:1]), pick(routes_ref[rows, 1:2]))
        one = pair(pick(kinds), pick(kinds + 1))
        two = pair(pick(kinds + 2), pick(kinds + 3))
        scal = jnp.zeros_like(logits)
        for index, value in enumerate(gates + one + two + (inverse,)):
            scal = jnp.where(lane == index, value, scal)
        scal_ref[rows, :] = scal
        for gate, ref in zip(gates, (first_ref, second_ref)):
            high, rest = split_low(gate)
            ref[rows, :] = jnp.where(
                lane == 0, high.astype(F32), jnp.where(lane == 1, rest.astype(F32), 0.0)
            ).astype(BF16)

    @pl.loop(0, send_ref.shape[0])
    def _(expert):
        slots = iota((CAP, tokens), 0) + expert * CAP
        hot_one = (target_ref[0:1, :] == slots).astype(F32)
        hot_two = (target_ref[1:2, :] == slots).astype(F32)
        send_ref[expert, :, 0:width] = nn((hot_one + hot_two).astype(BF16), ffn_ref[...]).astype(
            BF16
        )
        send_ref[expert, :, width:] = (
            nn(hot_one.astype(BF16), first_ref[...]) + nn(hot_two.astype(BF16), second_ref[...])
        ).astype(BF16)


def expert_kernel(
    recv_ref, cot_ref, wg_ref, wu_ref, wo_ref, front_ref, ret_ref, out_acc, row_acc,
):
    step = pl.program_id(0)
    total, width = out_acc.shape
    tile = 512

    @pl.when(step == 0)
    def _():
        out_acc[...] = jnp.zeros_like(out_acc)
        row_acc[...] = jnp.zeros_like(row_acc)

    @pl.loop(0, total // tile)
    def _(block):
        rows = pl.ds(pl.multiple_of(block * tile, tile), tile)
        token = recv_ref[rows, 0:width]
        extra = recv_ref[rows, width:].astype(F32)
        gate_weight = extra[:, 0:1] + extra[:, 1:2]
        gate = nn(token, wg_ref[...])
        up = nn(token, wu_ref[...])
        grad = nt(cot_ref[rows, :], wo_ref[...]) * gate_weight
        sig = jax.nn.sigmoid(gate)
        act = gate * sig
        hidden = act * up
        out_acc[rows, :] += nn(hidden.astype(BF16), wo_ref[...])
        front_ref[2, rows, :] = (hidden * gate_weight).astype(BF16)
        gate_grad = (grad * up * sig * (1.0 + gate * (1.0 - sig))).astype(BF16)
        up_grad = (grad * act).astype(BF16)
        front_ref[0, rows, :] = gate_grad
        front_ref[1, rows, :] = up_grad
        row_acc[rows, :] += nt(gate_grad, wg_ref[...]) + nt(up_grad, wu_ref[...])

    @pl.when(step == pl.num_programs(0) - 1)
    def _():
        @pl.loop(0, total // CAP)
        def _(peer):
            rows = pl.ds(pl.multiple_of(peer * CAP, CAP), CAP)
            ret_ref[peer, 0:CAP, :] = out_acc[rows, :].astype(BF16)
            ret_ref[peer, CAP:, :] = row_acc[rows, :].astype(BF16)


def expert_grad_kernel(recv_ref, cot_ref, front_ref, gate_ref, up_ref, wout_ref, turned_ref):
    step = pl.program_id(0)
    width = turned_ref.shape[0]

    @pl.when(step == 0)
    def _():
        turned_ref[...] = recv_ref[:, 0:width].T

    wout_ref[...] = tn(front_ref[2], cot_ref[...]).astype(BF16)
    gate_ref[...] = nn(turned_ref[...], front_ref[0]).astype(BF16)
    up_ref[...] = nn(turned_ref[...], front_ref[1]).astype(BF16)


def combine_kernel(
    kinds, experts, ret_ref, target_ref, routes_ref, scal_ref, resid_ref, cot_ref, ao_ref,
    small_ref, wo_ref, mix_ref, prevt_ref, ind_ref,
    mixed_ref, prev_ref, mid_ref, proj_ref, attn_ref, delta_ref, minor_ref, vec_ref, gain_ref,
    gmix_ref, rows_ref,
):
    step = pl.program_id(0)

    @pl.when(step == 0)
    def _():
        rows_ref[...] = small_ref[...].astype(F32).T
        minor_ref[...] = jnp.zeros_like(minor_ref)
        vec_ref[...] = jnp.zeros_like(vec_ref)
        gain_ref[...] = jnp.zeros_like(gain_ref)
        gmix_ref[...] = jnp.zeros_like(gmix_ref)

    width = resid_ref.shape[1]
    slots = experts * CAP
    resid = resid_ref[...]
    cot = cot_ref[...]
    upstream = cot.astype(F32)
    scal = scal_ref[...]
    routes = (routes_ref[:, 0:1], routes_ref[:, 1:2])
    targets = (target_ref[:, 0:1], target_ref[:, 1:2])
    gates = (scal[:, 0:1], scal[:, 1:2])
    one_keep, one_vec = scal[:, 2:3], scal[:, 3:4]
    two_keep, two_vec = scal[:, 4:5], scal[:, 5:6]
    inverse = scal[:, 6:7]
    gain = rows_ref[kinds + 7 : kinds + 8, :]
    vec_one = rows_ref[kinds + 4 : kinds + 5, :]
    vec_two = rows_ref[kinds + 5 : kinds + 6, :]
    normed = resid * inverse
    ffn_norm = normed * gain
    low = ffn_norm.astype(BF16)
    slot_ids = iota((BLOCK, slots), 1)
    hots = [(target == slot_ids).astype(F32) for target in targets]
    outs = ret_ref[:, 0:CAP, :].reshape(slots, width)
    backs = ret_ref[:, CAP:, :].reshape(slots, width)
    branches = [nn(hot.astype(BF16), outs) for hot in hots]
    back = nn((hots[0] + hots[1]).astype(BF16), backs)

    def weight(kind):
        return sum(
            jnp.where(route == kind, gate, 0.0) for route, gate in zip(routes, gates)
        )

    weight_copy = weight(experts + 1)
    weight_one = weight(experts + 2)
    weight_two = weight(experts + 3)
    keep = weight_copy + weight_one * one_keep + weight_two * two_keep
    mixed_ref[...] = (
        resid
        + gates[0] * branches[0]
        + gates[1] * branches[1]
        + keep * ffn_norm
        + (weight_one * one_vec) * vec_one
        + (weight_two * two_vec) * vec_two
    ).astype(BF16)
    dot_norm = jnp.sum(upstream * ffn_norm, axis=1, keepdims=True)
    dot_one = jnp.sum(upstream * vec_one, axis=1, keepdims=True)
    dot_two = jnp.sum(upstream * vec_two, axis=1, keepdims=True)
    grads = []
    for route, branch in zip(routes, branches):
        grads.append(
            jnp.sum(branch * upstream, axis=1, keepdims=True)
            + jnp.where(route == experts + 1, dot_norm, 0.0)
            + jnp.where(route == experts + 2, one_keep * dot_norm + one_vec * dot_one, 0.0)
            + jnp.where(route == experts + 3, two_keep * dot_norm + two_vec * dot_two, 0.0)
        )
    mean_grad = gates[0] * grads[0] + gates[1] * grads[1]
    lane = iota((BLOCK, LANES), 1)
    wide = jnp.zeros((BLOCK, LANES), F32)
    for route, gate, grad in zip(routes, gates, grads):
        wide = jnp.where(lane == route, gate * (grad - mean_grad), wide)
    for index, keep_part, vec_part, grad_weight, dot in (
        (kinds, one_keep, one_vec, weight_one, dot_one),
        (kinds + 2, two_keep, two_vec, weight_two, dot_two),
    ):
        keep_grad = grad_weight * dot_norm
        vec_grad = grad_weight * dot
        both = keep_part * keep_grad + vec_part * vec_grad
        wide = jnp.where(lane == index, keep_part * (keep_grad - both), wide)
        wide = jnp.where(lane == index + 1, vec_part * (vec_grad - both), wide)
    wide_low = wide.astype(BF16)
    wide_back = wide_low.astype(F32)
    minor_ref[...] += nn(wide_back.T.astype(BF16), low)
    share = jnp.where(lane == 0, weight_one * one_vec, 0.0)
    share = jnp.where(lane == 1, weight_two * two_vec, share)
    high, rest = split_low(share.T)
    vec_ref[...] += nn(high, cot) + nn(rest, cot)
    prev_ref[...] = nn(wide_low, mix_ref[...])[:, 0:kinds]
    gmix_ref[...] += jnp.dot(
        prevt_ref[...], wide_back, precision=HIGHEST_PRECISION, preferred_element_type=F32
    )
    grad_two = back + nt(wide_low, small_ref[...]) + keep * upstream
    gain_ref[...] += jnp.sum(grad_two * normed, axis=0, keepdims=True)
    mid = upstream + norm_back(grad_two * gain, normed, inverse)
    mid_ref[...] = mid
    proj = mid.astype(BF16)
    proj_ref[...] = proj
    attn = nt(proj, wo_ref[...]).astype(BF16)
    attn_ref[...] = attn
    high, rest = split_low(attn.astype(F32) * ao_ref[...].astype(F32))
    delta_ref[...] = nt(ind_ref[...], high) + nt(ind_ref[...], rest)


def attend_back_kernel(
    gain_row, qkv_ref, grad_ref, lse_ref, delta_ref, cos_ref, sin_ref, segc_ref, segr_ref,
    wq_ref, wk_ref, wv_ref, attn_in_ref, ao_ref, proj_ref, tok_ref, mid_ref, small_ref,
    weight_ref, gtok_ref, gain_ref, dq_ref, dk_ref, dv_ref, bias_ref, in_t_ref, ao_t_ref, acc_ref,
):
    step = pl.program_id(0)
    tokens = tok_ref.shape[0]
    blocks = tokens // BLOCK
    reach = DOC_MAX // BLOCK

    @pl.when(step == 0)
    def _():
        in_t_ref[...] = attn_in_ref[...].T
        ao_t_ref[...] = ao_ref[...].T
        acc_ref[...] = jnp.zeros_like(acc_ref)

    dq_ref[...] = jnp.zeros_like(dq_ref)
    for block in range(blocks):
        first = block * BLOCK
        last = min(blocks, block + reach + 1) * BLOCK
        span = last - first
        keys = slice(first, first + BLOCK)
        key_ids = iota((BLOCK, span), 0) + first
        row_ids = iota((BLOCK, span), 1) + first
        seen = (key_ids <= row_ids) & (segc_ref[keys, :] == segr_ref[0:1, first:last])
        bias_ref[:, 0:span] = jnp.where(seen, 0.0, NEGATIVE)
        key = qkv_ref[1, keys, :]
        value = qkv_ref[2, keys, :]
        key_grad = None
        for head in range(GROUP):
            mask = head_mask(head)
            index = step * GROUP + head
            query = qkv_ref[0, first:last, :] * mask
            upstream = grad_ref[first:last, :] * mask
            scores = nt(key, query) + bias_ref[:, 0:span]
            probs = jnp.exp(scores - lse_ref[pl.ds(index, 1), first:last])
            prob_grad = nt(value, upstream)
            score_grad = (probs * (prob_grad - delta_ref[pl.ds(index, 1), first:last])).astype(BF16)
            dv = nn(probs.astype(BF16), upstream)
            dk = nn(score_grad, query)
            dq_ref[first:last, :] += tn(score_grad, key * mask)
            key_grad = dk if key_grad is None else key_grad + dk
            value_grad = dv if head == 0 else value_grad + dv
        dk_ref[keys, :] = key_grad
        dv_ref[keys, :] = value_grad.astype(BF16)

    @pl.loop(0, blocks)
    def _(block):
        rows = pl.ds(pl.multiple_of(block * BLOCK, BLOCK), BLOCK)
        cosines = cos_ref[rows, :]
        sines = -sin_ref[rows, :]
        dq = turn(dq_ref[rows, :] * HEAD_DIM**-0.5, cosines, sines)
        dk = turn(dk_ref[rows, :], cosines, sines)
        dq_ref[rows, :] = dq
        dk_ref[rows, :] = dk
        acc_ref[rows, :] += (
            nt(dq.astype(BF16), wq_ref[...])
            + nt(dk.astype(BF16), wk_ref[...])
            + nt(dv_ref[rows, :], wv_ref[...])
        )

    halves = GROUP_LANES // LANES
    for index, (turned, grads) in enumerate(
        ((in_t_ref, dq_ref), (in_t_ref, dk_ref), (in_t_ref, dv_ref), (ao_t_ref, proj_ref))
    ):
        product = nn(turned[...], grads[...].astype(BF16)).astype(BF16)
        for half in range(halves):
            weight_ref[index * halves + half] = product[:, half * LANES : (half + 1) * LANES]

    @pl.when(step == pl.num_programs(0) - 1)
    def _():
        gain = small_ref[...].astype(F32).T[gain_row : gain_row + 1, :]
        gain_ref[...] = jnp.zeros_like(gain_ref)

        @pl.loop(0, blocks)
        def _(block):
            rows = pl.ds(pl.multiple_of(block * BLOCK, BLOCK), BLOCK)
            values = tok_ref[rows, :].astype(F32)
            inverse = inverse_rms(values)
            normed = values * inverse
            grad = acc_ref[rows, :]
            gain_ref[...] += jnp.sum(grad * normed, axis=0, keepdims=True)
            gtok_ref[rows, :] = mid_ref[rows, :] + norm_back(grad * gain, normed, inverse)


def add_low(left, right):
    return (left.astype(F32) + right.astype(F32)).astype(BF16)


def over_parts(values, bit):
    return lax.ppermute(values, "dp", [(d, d ^ bit) for d in range(8)])


def greet(targets):
    barrier = pltpu.get_barrier_semaphore()
    for present, target in targets:
        @pl.when(present)
        def _():
            pl.semaphore_signal(barrier, inc=1, device_id=target, device_id_type=MESH)
    pl.semaphore_wait(barrier, sum(present.astype(jnp.int32) for present, _ in targets))


def gather_kernel(
    part_ref, cot_ref, target_ref, out_ref, rows_ref, outgoing, send_sem, recv_sem, local_sem,
    row_send, row_recv, own_sem,
):
    me = lax.axis_index("dp")
    owner = lax.axis_index("expert")
    here, flank = me // 2, me % 2
    core = owner % 2
    up = ((2 * jnp.minimum(here + 1, 3) + flank), here < 3)
    down = ((2 * jnp.maximum(here - 1, 0) + flank), here > 0)
    across = 2 * here + 1 - flank
    partner = owner + 1 - 2 * core
    always = here >= 0
    routes = (
        (up[1], {"dp": up[0]}),
        (down[1], {"dp": down[0]}),
        (always, {"dp": across}),
        (always, {"expert": partner}),
    )
    side = owner // 2
    beside = owner + 2 - 4 * side
    corner = partner + 2 - 4 * side
    peers = (beside, corner, partner, owner)
    greet((*routes, (always, {"expert": beside}), (always, {"expert": corner})))

    def row_copy(slot):
        return pltpu.make_async_remote_copy(
            src_ref=outgoing.at[slot],
            dst_ref=rows_ref.at[owner],
            send_sem=row_send.at[slot],
            recv_sem=row_recv.at[slot],
            device_id={"expert": peers[slot]},
            device_id_type=MESH,
        )

    def copy(index, half, route, source=None):
        return pltpu.make_async_remote_copy(
            src_ref=out_ref.at[index, half] if source is None else source,
            dst_ref=out_ref.at[index, half],
            send_sem=send_sem.at[route, index],
            recv_sem=recv_sem.at[half, index],
            device_id=routes[route][1],
            device_id_type=MESH,
        )

    def arrive(index, half):
        copy(index, half, 2).wait_recv()

    local = pltpu.make_async_copy(part_ref, out_ref.at[me], local_sem)
    local.start()
    for route in range(3):
        @pl.when(routes[route][0])
        def _():
            copy(me, core, route, part_ref.at[core]).start()
    tokens = cot_ref.shape[0]

    @pl.loop(0, 4)
    def _(slot):
        turn_core, turn_side = (slot + 1) // 2 % 2, 1 - slot // 2
        peer = (
            core + turn_core - 2 * core * turn_core
            + 2 * (side + turn_side - 2 * side * turn_side)
        )
        slots = iota((CAP, tokens), 0) + peer * CAP
        hot = (target_ref[0:1, :] == slots) | (target_ref[1:2, :] == slots)
        outgoing[slot] = nn(hot.astype(F32).astype(BF16), cot_ref[...]).astype(BF16)

    for slot in range(3):
        row_copy(slot).start()
    own_rows = pltpu.make_async_copy(outgoing.at[3], rows_ref.at[owner], own_sem)
    own_rows.start()
    for distance in range(1, 5):
        for toward, forward, present in (
            (here - distance, 0, here >= distance),
            (here + distance, 1, here + distance <= 3),
        ):
            index = 2 * jnp.clip(toward, 0, 3) + flank

            @pl.when(present)
            def _():
                arrive(index, core)
                copy(index, core, 2).start()
                copy(index, core, 3).start()

            @pl.when(present & routes[forward][0])
            def _():
                copy(index, core, forward).start()
        for sign in (-1, 1):
            if distance == 1 and sign == 1:
                continue
            toward = here + sign * (distance - 1)
            index = 2 * jnp.clip(toward, 0, 3) + 1 - flank

            @pl.when((toward >= 0) & (toward <= 3))
            def _():
                arrive(index, core)
                copy(index, core, 3).start()
    for offset in range(1, 8):
        index = (me + offset) % 8
        arrive(index, 1 - core)
        copy(index, core, 3).wait_send()
    local.wait()
    for route in range(3):
        @pl.when(routes[route][0])
        def _():
            copy(me, core, route, part_ref.at[core]).wait_send()
    for distance in range(1, 4):
        for toward, forward, present in (
            (here - distance, 0, here >= distance),
            (here + distance, 1, here + distance <= 3),
        ):
            index = 2 * jnp.clip(toward, 0, 3) + flank

            @pl.when(present)
            def _():
                copy(index, core, 2).wait_send()

            @pl.when(present & routes[forward][0])
            def _():
                copy(index, core, forward).wait_send()
    for slot in range(3):
        row_copy(slot).wait_recv()
        row_copy(slot).wait_send()
    own_rows.wait()


def gather_parts(packed, cotangent, target_row):
    rows, columns = packed.shape
    width = cotangent.shape[1]
    whole, cot_rows = pl.pallas_call(
        gather_kernel,
        in_specs=[pl.BlockSpec(memory_space=pltpu.VMEM)] * 3,
        out_specs=[pl.BlockSpec(memory_space=pl.ANY)] * 2,
        out_shape=[
            jax.ShapeDtypeStruct((8, 2, rows // 2, columns), BF16),
            jax.ShapeDtypeStruct((4, CAP, width), BF16),
        ],
        scratch_shapes=[
            pltpu.VMEM((4, CAP, width), BF16),
            pltpu.SemaphoreType.DMA((4, 8)),
            pltpu.SemaphoreType.DMA((2, 8)),
            pltpu.SemaphoreType.DMA,
            pltpu.SemaphoreType.DMA((3,)),
            pltpu.SemaphoreType.DMA((3,)),
            pltpu.SemaphoreType.DMA,
        ],
        compiler_params=params(collective_id=0, has_side_effects=True),
        cost_estimate=cost(10e9, 10e6),
        name="gather_parts",
    )(packed.reshape(2, rows // 2, columns), cotangent, target_row)
    return whole.reshape(8 * rows, columns), cot_rows


def add_planes(target, left, right):
    @pl.loop(0, target.shape[0])
    def _(index):
        total = left[index].astype(F32) + right[index].astype(F32)
        target[index] = total.astype(target.dtype)


def reduce_kernel(
    gate_ref, up_ref, risen_ref, fallen_ref, pair_ref, weight_ref, minor_ref,
    gate_out, up_out, down_out, weight_out, minor_out,
    gate_in, up_in, line_in, gate_stage, up_stage, line_stage, pair_in, core_in, core_sum, side_in, side_sum, cross_in, line_ref, line_sum_ref,
    small_in, small_sum, piece_send, piece_recv, other_send, other_recv,
):
    me = lax.axis_index("dp")
    owner = lax.axis_index("expert")
    here, flank = me // 2, me % 2
    core, side = owner % 2, owner // 2
    rising = {"dp": 2 * jnp.minimum(here + 1, 3) + flank}
    falling = {"dp": 2 * jnp.maximum(here - 1, 0) + flank}
    across = {"dp": me + 1 - 2 * flank}
    partner = {"expert": owner + 1 - 2 * core}
    beside = {"expert": owner + 2 - 4 * side}
    always = here >= 0
    greet(((here < 3, rising), (here > 0, falling), (always, across), (always, partner),
           (always, beside)))
    pieces = (
        (gate_ref, gate_in, gate_stage),
        (up_ref, up_in, up_stage),
        (line_ref, line_in, line_stage),
    )

    def piece_copy(piece, turn_index, way, source):
        return pltpu.make_async_remote_copy(
            src_ref=source,
            dst_ref=pieces[piece][1].at[way, turn_index],
            send_sem=piece_send.at[piece, turn_index, way],
            recv_sem=piece_recv.at[piece, turn_index, way],
            device_id=(rising, falling)[way],
            device_id_type=MESH,
        )

    def other_copy(index, source, target, device):
        return pltpu.make_async_remote_copy(
            src_ref=source, dst_ref=target, send_sem=other_send.at[index],
            recv_sem=other_recv.at[index], device_id=device, device_id_type=MESH,
        )

    def direct(piece, turn_index):
        own = pieces[piece][0]

        @pl.when(here == 0)
        def _():
            piece_copy(piece, turn_index, 0, own.at[3 - turn_index]).start()

        @pl.when(here == 3)
        def _():
            piece_copy(piece, turn_index, 1, own.at[turn_index]).start()

    def relayed(turn_index):
        return (
            (0, (here > 0) & (here < 3 - turn_index), 3 - turn_index),
            (1, (here < 3) & (here > turn_index), turn_index),
        )

    def relay(piece, turn_index):
        own, landed, stage = pieces[piece]
        for way, present, chunk in relayed(turn_index):
            if piece == 0:
                present = present & ((here != 1) if way == 0 else (here != 2))

            @pl.when(present)
            def _():
                copy = piece_copy(piece, turn_index, way, stage.at[way, turn_index])
                copy.wait_recv()
                add_planes(
                    stage.at[way, turn_index], own.at[chunk], landed.at[way, turn_index]
                )
                copy.start()

    def early(turn_index):
        own, landed, stage = pieces[0]
        for way, place, chunk in ((0, 1, 3 - turn_index), (1, 2, turn_index)):
            @pl.when(here == place)
            def _():
                add_planes(
                    stage.at[way, turn_index], own.at[chunk], landed.at[way, turn_index]
                )
                piece_copy(0, turn_index, way, stage.at[way, turn_index]).start()

    def finish(piece, target):
        own, landed, stage = pieces[piece]
        lower = jnp.minimum(3 - here, 2)
        upper = jnp.minimum(here, 2)

        @pl.when((here > (1 if piece == 0 else 0)))
        def _():
            piece_copy(piece, lower, 0, stage.at[0, 0]).wait_recv()

        @pl.when(here < (2 if piece == 0 else 3))
        def _():
            piece_copy(piece, upper, 1, stage.at[0, 0]).wait_recv()

        @pl.when(here == 0)
        def _():
            add_planes(target, own.at[here], landed.at[1, upper])

        @pl.when(here == 3)
        def _():
            add_planes(target, own.at[here], landed.at[0, lower])

        @pl.when((here > 0) & (here < 3))
        def _():
            @pl.loop(0, target.shape[0])
            def _(index):
                total = (
                    own[here, index].astype(F32)
                    + landed[0, lower, index].astype(F32)
                    + landed[1, upper, index].astype(F32)
                )
                target[index] = total.astype(target.dtype)

    def drain(piece):
        own, _, stage = pieces[piece]
        for turn_index in range(0 if piece == 0 else 3):
            @pl.when(here == 0)
            def _():
                piece_copy(piece, turn_index, 0, own.at[3 - turn_index]).wait_send()

            @pl.when(here == 3)
            def _():
                piece_copy(piece, turn_index, 1, own.at[turn_index]).wait_send()
        for turn_index in range(2):
            for way, present, _ in relayed(turn_index):
                @pl.when(present)
                def _():
                    piece_copy(
                        piece, turn_index, way, stage.at[way, turn_index]
                    ).wait_send()

    half = core_in.shape[0]
    quarter = half // 2
    eighth = quarter // 2
    core_weight = [
        other_copy(
            14 * order,
            weight_ref.at[pl.ds(half * (1 - core) + quarter * which, quarter)],
            core_in.at[pl.ds(quarter * which, quarter)],
            partner,
        )
        for order, which in enumerate((1 - side, side))
    ]
    core_small = other_copy(1, minor_ref, small_in.at[0], partner)
    side_weight = [
        other_copy(
            2 + 13 * order,
            core_sum.at[pl.ds(quarter * (1 - side) + eighth * order, eighth)],
            side_in.at[pl.ds(eighth * order, eighth)],
            beside,
        )
        for order in range(2)
    ]
    side_small = other_copy(3, small_sum.at[0], small_in.at[1], beside)
    cross_weight = [
        other_copy(
            4 + 12 * order + z,
            side_sum.at[pl.ds(eighth * order, eighth), 2 * z + 1 - flank],
            cross_in.at[z, pl.ds(eighth * order, eighth)],
            across,
        )
        for order in range(2)
        for z in range(4)
    ]
    cross_small = other_copy(8, small_sum.at[1], small_in.at[2], across)
    rise_small = other_copy(9, small_sum.at[3], small_in.at[3], rising)
    fall_small = other_copy(10, small_sum.at[4], small_in.at[4], falling)
    mine = half * core + quarter * side
    own_part = weight_out.at[pl.ds(mine, quarter)]
    own_half = weight_out.at[pl.ds(half * core, half)]
    side_back = other_copy(11, own_part, own_part, beside)
    core_back = other_copy(12, own_half, own_half, partner)

    pair_copy = other_copy(13, pair_ref.at[1 - flank], pair_in, across)
    for copy in core_weight:
        copy.start()
    core_small.start()
    pair_copy.start()
    for turn_index in range(3):
        direct(1, turn_index)

    @pl.when(here == 1)
    def _():
        for turn_index in range(3):
            gate_in[0, turn_index] = risen_ref[2 - turn_index]

    @pl.when(here == 2)
    def _():
        for turn_index in range(3):
            gate_in[1, turn_index] = fallen_ref[turn_index]

    for turn_index in range(2):
        early(turn_index)
    for order, which in enumerate((1 - side, side)):
        core_weight[order].wait_recv()
        add_planes(
            core_sum.at[pl.ds(quarter * which, quarter)],
            weight_ref.at[pl.ds(half * core + quarter * which, quarter)],
            core_in.at[pl.ds(quarter * which, quarter)],
        )
        if order == 0:
            for copy in side_weight:
                copy.start()
    core_small.wait_recv()
    small_sum[0] = minor_ref[...] + small_in[0]
    side_small.start()
    for piece in (0, 1):
        relay(piece, 0)
    pair_copy.wait_recv()
    add_planes(down_out, pair_ref.at[flank], pair_in)
    for order in range(2):
        span = pl.ds(eighth * order, eighth)
        side_weight[order].wait_recv()
        add_planes(
            side_sum.at[span],
            core_sum.at[pl.ds(quarter * side + eighth * order, eighth)],
            side_in.at[span],
        )
        for copy in cross_weight[4 * order : 4 * order + 4]:
            copy.start()
    side_small.wait_recv()
    small_sum[1] = small_sum[0] + small_in[1]
    cross_small.start()
    for piece in (0, 1):
        relay(piece, 1)
    for copy in cross_weight:
        copy.wait_recv()
    cross_small.wait_recv()
    for z in range(4):
        add_planes(line_ref.at[z], side_sum.at[:, 2 * z + flank], cross_in.at[z])
    small_sum[2] = small_sum[1] + small_in[2]
    small_sum[3] = small_sum[2]
    small_sum[4] = small_sum[2]
    for turn_index in range(3):
        direct(2, turn_index)

    @pl.when(here == 0)
    def _():
        rise_small.start()

    @pl.when(here == 3)
    def _():
        fall_small.start()

    for turn_index in range(2):
        relay(2, turn_index)

    finish(2, line_sum_ref)
    for index in range(quarter):
        weight_out[mine + index] = line_sum_ref[index]
    side_back.start()

    @pl.when(here > 0)
    def _():
        rise_small.wait_recv()
        small_sum[3] = small_sum[2] + small_in[3]

    @pl.when((here > 0) & (here < 3))
    def _():
        rise_small.start()

    @pl.when(here < 3)
    def _():
        fall_small.wait_recv()
        small_sum[4] = small_sum[2] + small_in[4]

    @pl.when((here > 0) & (here < 3))
    def _():
        fall_small.start()

    minor_out[...] = small_sum[3] + small_sum[4] - small_sum[2]
    finish(0, gate_out)
    side_back.wait_recv()
    core_back.start()
    finish(1, up_out)
    core_back.wait_recv()
    for piece in range(3):
        drain(piece)
    for copy in (*core_weight, core_small, *side_weight, side_small, *cross_weight, cross_small,
                 side_back, core_back, pair_copy):
        copy.wait_send()

    @pl.when(here < 3)
    def _():
        rise_small.wait_send()

    @pl.when(here > 0)
    def _():
        fall_small.wait_send()


def reduce_parts(kept, down, weights, minor):
    gate, up = kept[:2]
    kept = [piece.reshape(-1, piece.shape[1] // 8, 8, piece.shape[2]) for piece in kept]
    pair = down.reshape(2, down.shape[1] // 8, 8, down.shape[2])
    blocks, width, lanes = weights.shape
    rows = width // 8
    plane = (rows, lanes)
    chunks = [piece.shape[1:] for piece in kept[:2]]
    line = (blocks // 4,) + plane
    low = [pltpu.VMEM((2, 3) + chunk, BF16) for chunk in chunks + [line]]
    stages = [pltpu.VMEM((2, 2) + chunk, BF16) for chunk in chunks + [line]]
    outs = pl.pallas_call(
        reduce_kernel,
        in_specs=[pl.BlockSpec(memory_space=pltpu.VMEM)] * 7,
        out_specs=[pl.BlockSpec(memory_space=pltpu.VMEM)] * 5,
        out_shape=[jax.ShapeDtypeStruct(chunk, F32) for chunk in chunks + [pair.shape[1:]]]
        + [
            jax.ShapeDtypeStruct((blocks,) + plane, BF16),
            jax.ShapeDtypeStruct(minor.shape, F32),
        ],
        scratch_shapes=[
            *low,
            *stages,
            pltpu.VMEM(pair.shape[1:], BF16),
            pltpu.VMEM((blocks // 2, 8) + plane, BF16),
            pltpu.VMEM((blocks // 2, 8) + plane, BF16),
            pltpu.VMEM((blocks // 4, 8) + plane, BF16),
            pltpu.VMEM((blocks // 4, 8) + plane, BF16),
            pltpu.VMEM((4,) + line, BF16),
            pltpu.VMEM((4,) + line, BF16),
            pltpu.VMEM(line, BF16),
            pltpu.VMEM((5,) + minor.shape, F32),
            pltpu.VMEM((5,) + minor.shape, F32),
            pltpu.SemaphoreType.DMA((3, 3, 2)),
            pltpu.SemaphoreType.DMA((3, 3, 2)),
            pltpu.SemaphoreType.DMA((20,)),
            pltpu.SemaphoreType.DMA((20,)),
        ],
        compiler_params=params(collective_id=1, has_side_effects=True),
        name="reduce_parts",
    )(*kept, pair, weights.reshape(blocks, 8, rows, lanes), minor)
    shapes = (gate.shape[1:], up.shape[1:], down.shape[1:])
    shares = [out.reshape(shape) for out, shape in zip(outs, shapes)]
    return shares, outs[3], outs[4]


FF_TILE = 256


def exchange_kernel(
    send_ref, cot_ref, win_ref, wout_ref,
    gate_keep, gate_away, up_keep, up_away, own_down, one_down, two_down, three_down, return_out,
    recv, cot, gate_w, up_w, down_w, front, turned, out_acc, row_acc, ret, gate_g, up_g, down_g,
    token_send, token_recv, back_send, back_recv, load_sem, weight_sem, store_sem, down_sem, own_sem,
):
    me = lax.axis_index("expert")
    spot = lax.axis_index("dp")
    here, flank = spot // 2, spot % 2
    line_peers = (here, here + 1 - 2 * (here % 2), here + 2 - 4 * (here // 2), 3 - here)
    down_parts = (own_down, one_down, two_down, three_down)
    share = gate_w.shape[0] // 8
    core, side = me % 2, me // 2
    partner = me + 1 - 2 * core
    beside = me + 2 - 4 * side
    corner = partner + 2 - 4 * side
    peers = (me, beside, corner, partner)
    always = me >= 0
    width = out_acc.shape[1]
    ff = down_w.shape[0]
    tiles = ff // FF_TILE
    greet([(always, {"expert": peer}) for peer in peers[1:]])

    def peer_of(slot):
        turn_core, turn_side = slot // 2, 1 - slot // 3
        return (
            core + turn_core - 2 * core * turn_core
            + 2 * (side + turn_side - 2 * side * turn_side)
        )

    def token_copy(slot):
        return pltpu.make_async_remote_copy(
            src_ref=send_ref.at[peer_of(slot)], dst_ref=recv.at[slot],
            send_sem=token_send.at[slot], recv_sem=token_recv.at[slot],
            device_id={"expert": peer_of(slot)}, device_id_type=MESH,
        )

    def back_copy(slot):
        return pltpu.make_async_remote_copy(
            src_ref=ret.at[slot], dst_ref=return_out.at[me],
            send_sem=back_send.at[slot], recv_sem=back_recv.at[slot],
            device_id={"expert": peer_of(slot)}, device_id_type=MESH,
        )

    def tile_slice(tile):
        return pl.ds(pl.multiple_of(tile * FF_TILE, FF_TILE), FF_TILE)

    def weight_copies(tile):
        cols = tile_slice(tile)
        shifted = pl.ds(pl.multiple_of(ff + tile * FF_TILE, FF_TILE), FF_TILE)
        return (
            pltpu.make_async_copy(
                win_ref.at[:, cols], gate_w.at[:, cols], weight_sem.at[0, tile]
            ),
            pltpu.make_async_copy(
                win_ref.at[:, shifted], up_w.at[:, cols], weight_sem.at[1, tile]
            ),
            pltpu.make_async_copy(
                wout_ref.at[cols, :], down_w.at[cols, :], weight_sem.at[2, tile]
            ),
        )

    def side_copy(piece, index, kept):
        source = (gate_g, up_g)[piece].at[index * share : (index + 1) * share, :]
        target = ((gate_away, gate_keep), (up_away, up_keep))[piece][kept].at[index // 2]
        return pltpu.make_async_copy(source, target, store_sem.at[piece, index])

    def down_copy(tile, distance):
        return pltpu.make_async_copy(
            down_g.at[tile_slice(tile), :], down_parts[distance].at[tile % 2], down_sem.at[tile]
        )

    for slot in (1, 2, 3):
        token_copy(slot).start()
    loads = [pltpu.make_async_copy(send_ref.at[me], recv.at[0], load_sem.at[0])] + [
        pltpu.make_async_copy(cot_ref.at[peers[slot]], cot.at[slot], load_sem.at[1 + slot])
        for slot in range(4)
    ]
    for load in loads:
        load.start()

    @pl.loop(0, tiles)
    def _(tile):
        for copy in weight_copies(tile):
            copy.start()

    for load in loads:
        load.wait()

    def work(slot):
        extra = recv[slot, :, width:].astype(F32)
        gate_weight = extra[:, 0:1] + extra[:, 1:2]
        out_acc[...] = jnp.zeros_like(out_acc)
        row_acc[...] = jnp.zeros_like(row_acc)

        @pl.loop(0, tiles)
        def _(tile):
            cols = tile_slice(tile)

            @pl.when(slot == 0)
            def _():
                for copy in weight_copies(tile):
                    copy.wait()

            token = recv[slot, :, 0:width]
            gate = nn(token, gate_w[:, cols])
            up = nn(token, up_w[:, cols])
            grad = nt(cot[slot], down_w[cols, :]) * gate_weight
            sig = jax.nn.sigmoid(gate)
            act = gate * sig
            hidden = act * up
            out_acc[...] += nn(hidden.astype(BF16), down_w[cols, :])
            front[2, slot, :, cols] = (hidden * gate_weight).astype(BF16)
            gate_grad = (grad * up * sig * (1.0 + gate * (1.0 - sig))).astype(BF16)
            up_grad = (grad * act).astype(BF16)
            front[0, slot, :, cols] = gate_grad
            front[1, slot, :, cols] = up_grad
            row_acc[...] += nt(gate_grad, gate_w[:, cols]) + nt(up_grad, up_w[:, cols])

        ret[slot, 0:CAP, :] = out_acc[...].astype(BF16)
        ret[slot, CAP:, :] = row_acc[...].astype(BF16)
        turned[:, pl.ds(pl.multiple_of(slot * CAP, CAP), CAP)] = recv[slot, :, 0:width].T

    own_back = pltpu.make_async_copy(ret.at[0], return_out.at[me], own_sem)


    @pl.loop(0, 4)
    def _(slot):
        @pl.when(slot > 0)
        def _():
            token_copy(slot).wait_recv()

        work(slot)

        @pl.when(slot > 0)
        def _():
            back_copy(slot).start()

        @pl.when(slot == 0)
        def _():
            own_back.start()

    total = 4 * CAP

    @pl.loop(0, tiles)
    def _(tile):
        cols = tile_slice(tile)
        hidden = front[2, :, :, cols].reshape(total, FF_TILE)
        down_g[cols, :] = tn(hidden, cot[...].reshape(total, width)).astype(BF16)
        gate_g[:, cols] = nn(turned[...], front[0, :, :, cols].reshape(total, FF_TILE)).astype(BF16)
        up_g[:, cols] = nn(turned[...], front[1, :, :, cols].reshape(total, FF_TILE)).astype(BF16)
        for distance in range(4):
            @pl.when(tile // 2 == line_peers[distance])
            def _():
                down_copy(tile, distance).start()

    for piece in range(2):
        for index in range(8):
            for kept in range(2):
                @pl.when((flank == index % 2) if kept else (flank != index % 2))
                def _():
                    side_copy(piece, index, kept).start()

    for slot in (1, 2, 3):
        token_copy(slot).wait_send()
        back_copy(slot).wait_recv()
        back_copy(slot).wait_send()
    own_back.wait()

    for piece in range(2):
        for index in range(8):
            side_copy(piece, index, 1).wait()

    @pl.loop(0, tiles)
    def _(tile):
        down_copy(tile, 0).wait()


def exchange_experts(send, cot_rows, w_in, w_out):
    peers, cap, payload = send.shape
    ff, width = w_out.shape
    anywhere = pl.BlockSpec(memory_space=pl.ANY)
    tiles = ff // FF_TILE
    *grads, returned = pl.pallas_call(
        exchange_kernel,
        in_specs=[anywhere] * 4,
        out_specs=[anywhere] * 9,
        out_shape=[jax.ShapeDtypeStruct((4, width // 8, ff), BF16)] * 4
        + [jax.ShapeDtypeStruct((2, ff // 8, width), BF16)] * 4
        + [jax.ShapeDtypeStruct((peers, 2 * cap, width), BF16)],
        scratch_shapes=[
            pltpu.VMEM((peers, cap, payload), BF16),
            pltpu.VMEM((peers, cap, width), BF16),
            pltpu.VMEM((width, ff), BF16),
            pltpu.VMEM((width, ff), BF16),
            pltpu.VMEM((ff, width), BF16),
            pltpu.VMEM((3, peers, cap, ff), BF16),
            pltpu.VMEM((width, peers * cap), BF16),
            pltpu.VMEM((cap, width), F32),
            pltpu.VMEM((cap, width), F32),
            pltpu.VMEM((peers, 2 * cap, width), BF16),
            pltpu.VMEM((width, ff), BF16),
            pltpu.VMEM((width, ff), BF16),
            pltpu.VMEM((ff, width), BF16),
            pltpu.SemaphoreType.DMA((4,)),
            pltpu.SemaphoreType.DMA((4,)),
            pltpu.SemaphoreType.DMA((4,)),
            pltpu.SemaphoreType.DMA((4,)),
            pltpu.SemaphoreType.DMA((5,)),
            pltpu.SemaphoreType.DMA((3, tiles)),
            pltpu.SemaphoreType.DMA((2, 8)),
            pltpu.SemaphoreType.DMA((tiles,)),
            pltpu.SemaphoreType.DMA,
        ],
        compiler_params=params(collective_id=2, has_side_effects=True),
        cost_estimate=cost(18 * peers * cap * width * ff, 40e6),
        name="exchange_experts",
    )(send, cot_rows.reshape(peers, cap, width), w_in, w_out)
    return grads, returned


def plain_experts(send, cot_rows, w_in_one, w_out_one, swap):
    experts, _, payload = send.shape
    ff, width = w_out_one.shape
    recv = swap(send).reshape(experts * CAP, payload)

    slot_count = experts * CAP
    ff_tile = 256
    ff_tiles = ff // ff_tile
    slot_full = whole_block((slot_count, width))
    recv_full = whole_block((slot_count, payload))
    front_spec = pl.BlockSpec((3, slot_count, ff_tile), lambda j: (0, 0, j))
    front, ret = pl.pallas_call(
        expert_kernel,
        grid=(ff_tiles,),
        in_specs=[
            recv_full,
            slot_full,
            pl.BlockSpec((width, ff_tile), lambda j: (0, j)),
            pl.BlockSpec((width, ff_tile), lambda j: (0, ff_tiles + j)),
            pl.BlockSpec((ff_tile, width), lambda j: (j, 0)),
        ],
        out_specs=[front_spec, whole_block((experts, 2 * CAP, width))],
        out_shape=[
            jax.ShapeDtypeStruct((3, slot_count, ff), BF16),
            jax.ShapeDtypeStruct((experts, 2 * CAP, width), BF16),
        ],
        scratch_shapes=[pltpu.VMEM((slot_count, width), F32)] * 2,
        compiler_params=params(),
        cost_estimate=cost(12 * slot_count * width * ff, 26e6),
        name="expert",
    )(recv, cot_rows, w_in_one, w_in_one, w_out_one)
    returned = swap(ret)
    expert_grads = pl.pallas_call(
        expert_grad_kernel,
        grid=(ff_tiles,),
        in_specs=[recv_full, slot_full, front_spec],
        out_specs=[
            pl.BlockSpec((width, ff_tile), lambda j: (0, j)),
            pl.BlockSpec((width, ff_tile), lambda j: (0, j)),
            pl.BlockSpec((ff_tile, width), lambda j: (j, 0)),
        ],
        out_shape=[
            jax.ShapeDtypeStruct((width, ff), BF16),
            jax.ShapeDtypeStruct((width, ff), BF16),
            jax.ShapeDtypeStruct((ff, width), BF16),
        ],
        scratch_shapes=[pltpu.VMEM((width, slot_count), BF16)],
        compiler_params=params(),
        cost_estimate=cost(6 * slot_count * width * ff, 24e6),
        name="expert_grad",
    )(recv, cot_rows, front)
    return expert_grads, returned


def per_device(
    tokens, prev_scores, segments, routes, wqkv, wo, router, const_gate, const_vec, gain1, gain2,
    gate_mix, w_in, w_out, cotangent,
):
    tok_count, width = tokens.shape
    kinds = router.shape[1]
    experts = w_in.shape[0] * lax.axis_size("expert")
    ff = w_out.shape[1]
    qkv_cols = wqkv.shape[1]
    parts = lax.axis_size("dp")
    by_hand = parts == 8 and experts == 4
    small = jnp.concatenate(
        [router, const_gate, const_vec, gain1[:, None], gain2[:, None]], axis=1
    )
    packed = jnp.concatenate(
        [wqkv, wo, jnp.pad(small, ((0, 0), (0, LANES - small.shape[1])))], axis=1
    )

    seq_len = segments.shape[1]
    positions = (jnp.arange(tok_count, dtype=jnp.int32) % seq_len).astype(F32)
    half = HEAD_DIM // 2
    frequency = 10000.0 ** (-jnp.arange(half).astype(F32) / half)
    angles = positions[:, None] * frequency[None, :]
    cosines = jnp.tile(jnp.cos(angles), (1, LANES // half))
    sines = jnp.tile(jnp.sin(angles), (1, LANES // half))
    signs = jnp.where(jnp.arange(LANES) % HEAD_DIM < half, -1.0, 1.0).astype(F32)
    sines = sines * signs[None, :]
    seg_col = segments.reshape(tok_count, 1)
    seg_row = segments.reshape(1, tok_count)

    names = jnp.arange(kinds, dtype=jnp.int32)
    hot = [routes[:, i : i + 1] == names[None, :] for i in range(2)]
    named = (hot[0] | hot[1]).astype(BF16)
    ids = jnp.arange(tok_count, dtype=jnp.int32)
    before = (ids[:, None] > ids[None, :]).astype(BF16)
    earlier = jnp.dot(before, named, preferred_element_type=F32)
    slots = [jnp.sum(jnp.where(h, earlier, 0.0), axis=1).astype(jnp.int32) for h in hot]
    targets = [
        jnp.where(routes[:, i] < experts, routes[:, i] * CAP + slots[i], experts * CAP)
        for i in range(2)
    ]
    target_row = jnp.stack(targets, axis=0)
    target_col = jnp.stack(targets, axis=1)
    prev_mix = jnp.dot(prev_scores, gate_mix.astype(F32), precision=HIGHEST_PRECISION)
    prev_mix = jnp.pad(prev_mix, ((0, 0), (0, LANES - kinds)))

    def swap(values):
        return lax.all_to_all(values, "expert", split_axis=0, concat_axis=0, tiled=True)

    if by_hand:
        whole, cot_rows = gather_parts(packed, cotangent, target_row)
    else:
        whole = lax.all_gather(packed, "dp", axis=0, tiled=True)
        cot_send = pl.pallas_call(
            functools.partial(send_cotangent_kernel, experts),
            out_shape=jax.ShapeDtypeStruct((experts, CAP, width), BF16),
            compiler_params=params(),
            cost_estimate=cost(2 * experts * CAP * tok_count * width, 4 * tok_count * width),
            name="send_cotangent",
        )(cotangent, target_row)
        cot_rows = swap(cot_send)
    cot_rows = cot_rows.reshape(experts * CAP, width)

    groups = HEADS // GROUP
    tiles = qkv_cols // 3 // GROUP_LANES
    weight_specs = [
        pl.BlockSpec((width, GROUP_LANES), functools.partial(lambda o, i: (0, o + i), part * tiles))
        for part in range(3)
    ]
    small_spec = pl.BlockSpec((width, LANES), lambda *_: (0, (qkv_cols + width) // LANES))
    wo_spec = pl.BlockSpec((width, width), lambda *_: (0, qkv_cols // width))
    table = whole_block((tok_count, LANES))
    full = whole_block((tok_count, width))
    group_spec = pl.BlockSpec((tok_count, GROUP_LANES), lambda i: (0, i))
    qkv_spec = pl.BlockSpec((3, tok_count, GROUP_LANES), lambda i: (0, 0, i))
    seg_specs = [whole_block((tok_count, 1)), whole_block((1, tok_count))]
    span = DOC_MAX + BLOCK
    head_rows = 16
    lse_spec = whole_block((head_rows, tok_count))
    qkv, attn_in, attn_out, lse = pl.pallas_call(
        functools.partial(attend_kernel, kinds + 6),
        grid=(groups,),
        in_specs=[full, *weight_specs, small_spec, table, table, *seg_specs],
        out_specs=[qkv_spec, full, group_spec, lse_spec],
        out_shape=[
            jax.ShapeDtypeStruct((3, tok_count, width), BF16),
            jax.ShapeDtypeStruct((tok_count, width), BF16),
            jax.ShapeDtypeStruct((tok_count, width), BF16),
            jax.ShapeDtypeStruct((head_rows, tok_count), F32),
        ],
        scratch_shapes=[
            pltpu.VMEM((1, width), F32),
            pltpu.VMEM((BLOCK, span), F32),
            pltpu.VMEM((tok_count, LANES), F32),
        ],
        compiler_params=params(),
        cost_estimate=cost(12e9, 16e6),
        name="attend",
    )(tokens, whole, whole, whole, whole, cosines, sines, seg_col, seg_row)

    payload = width + LANES
    resid_mid, scal, send = pl.pallas_call(
        functools.partial(middle_kernel, kinds),
        grid=(1,),
        in_specs=[
            full, wo_spec, full, small_spec, table, whole_block((tok_count, 2)),
            whole_block((2, tok_count)),
        ],
        out_specs=[full, table, whole_block((experts, CAP, payload))],
        out_shape=[
            jax.ShapeDtypeStruct((tok_count, width), F32),
            jax.ShapeDtypeStruct((tok_count, LANES), F32),
            jax.ShapeDtypeStruct((experts, CAP, payload), BF16),
        ],
        scratch_shapes=[
            pltpu.VMEM((tok_count, width), BF16),
            pltpu.VMEM((tok_count, LANES), BF16),
            pltpu.VMEM((tok_count, LANES), BF16),
        ],
        compiler_params=params(),
        cost_estimate=cost(3.5e9, 10e6),
        name="middle",
    )(attn_out, whole, tokens, whole, prev_mix, routes, target_row)
    w_in_one = w_in.reshape(width, 2 * ff)
    w_out_one = w_out.reshape(ff, width)
    if by_hand:
        expert_grads, returned = exchange_experts(send, cot_rows, w_in_one, w_out_one)
    else:
        expert_grads, returned = plain_experts(send, cot_rows, w_in_one, w_out_one, swap)
    returned, *expert_grads = lax.optimization_barrier((returned, *expert_grads))
    if by_hand:
        gate_keep, gate_away, up_keep, up_away, *down_parts = expert_grads
        gate_pair = (gate_keep, over_parts(gate_away, 1))
        up_pair = (up_keep, over_parts(up_away, 1))
        lined = [down_parts[0]]
        for i in (1, 2, 3):
            lined.append(over_parts(down_parts[i], 2 * i))

    mix_turned = jnp.pad(gate_mix.T, ((0, LANES - kinds), (0, LANES - kinds)))
    indicator = (
        jnp.arange(width)[None, :] // HEAD_DIM == jnp.arange(head_rows)[:, None]
    ).astype(BF16)
    token_block = pl.BlockSpec((BLOCK, width), lambda i: (i, 0))
    table_block = pl.BlockSpec((BLOCK, LANES), lambda i: (i, 0))
    two_block = pl.BlockSpec((BLOCK, 2), lambda i: (i, 0))
    (
        mixed, grad_prev, mid_grad, proj_grad, attn_grad, delta, minor, vec, gain2_row, grad_mix,
    ) = pl.pallas_call(
        functools.partial(combine_kernel, kinds, experts),
        grid=(tok_count // BLOCK,),
        in_specs=[
            whole_block((experts, 2 * CAP, width)), two_block, two_block, table_block,
            token_block, token_block, token_block, small_spec, wo_spec,
            whole_block((LANES, LANES)),
            pl.BlockSpec((kinds, BLOCK), lambda i: (0, i)),
            whole_block((head_rows, width)),
        ],
        out_specs=[
            token_block, pl.BlockSpec((BLOCK, kinds), lambda i: (i, 0)), token_block, token_block,
            token_block, pl.BlockSpec((head_rows, BLOCK), lambda i: (0, i)),
            whole_block((LANES, width)), whole_block((LANES, width)), whole_block((1, width)),
            whole_block((kinds, LANES)),
        ],
        out_shape=[
            jax.ShapeDtypeStruct((tok_count, width), BF16),
            jax.ShapeDtypeStruct((tok_count, kinds), F32),
            jax.ShapeDtypeStruct((tok_count, width), F32),
            jax.ShapeDtypeStruct((tok_count, width), BF16),
            jax.ShapeDtypeStruct((tok_count, width), BF16),
            jax.ShapeDtypeStruct((head_rows, tok_count), F32),
            jax.ShapeDtypeStruct((LANES, width), F32),
            jax.ShapeDtypeStruct((LANES, width), F32),
            jax.ShapeDtypeStruct((1, width), F32),
            jax.ShapeDtypeStruct((kinds, LANES), F32),
        ],
        scratch_shapes=[pltpu.VMEM((LANES, width), F32)],
        compiler_params=params(),
        cost_estimate=cost(1e6, 1e5),
        name="combine",
    )(
        returned, target_col, routes, scal, resid_mid, cotangent, attn_out, whole, whole,
        mix_turned, prev_scores.T, indicator,
    )

    if by_hand:
        gate_pair, attn_grad = lax.optimization_barrier((gate_pair, attn_grad))
        gate_met = add_low(*gate_pair)
        risen = lax.ppermute(gate_met[1:], "dp", [(0, 2), (1, 3)])
        fallen = lax.ppermute(gate_met[:3], "dp", [(6, 4), (7, 5)])
    halves = GROUP_LANES // LANES
    weights, grad_tokens, gain1_row = pl.pallas_call(
        functools.partial(attend_back_kernel, kinds + 6),
        grid=(groups,),
        in_specs=[
            qkv_spec, group_spec, lse_spec, lse_spec, table, table, *seg_specs, *weight_specs,
            full, full, group_spec, full, full, small_spec,
        ],
        out_specs=[
            pl.BlockSpec((4 * halves, width, LANES), lambda i: (i, 0, 0)), full,
            whole_block((1, width)),
        ],
        out_shape=[
            jax.ShapeDtypeStruct((4 * halves * groups, width, LANES), BF16),
            jax.ShapeDtypeStruct((tok_count, width), F32),
            jax.ShapeDtypeStruct((1, width), F32),
        ],
        scratch_shapes=[
            pltpu.VMEM((tok_count, GROUP_LANES), F32),
            pltpu.VMEM((tok_count, GROUP_LANES), F32),
            pltpu.VMEM((tok_count, GROUP_LANES), BF16),
            pltpu.VMEM((BLOCK, span), F32),
            pltpu.VMEM((width, tok_count), BF16),
            pltpu.VMEM((width, tok_count), BF16),
            pltpu.VMEM((tok_count, width), F32),
        ],
        compiler_params=params(),
        cost_estimate=cost(1e6, 1e5),
        name="attend_back",
    )(
        qkv, attn_grad, lse, delta, cosines, sines, seg_col, seg_row, whole, whole, whole,
        attn_in, attn_out, proj_grad, tokens, mid_grad, whole,
    )

    minor_rows = jnp.concatenate([minor[: kinds + 4], vec[:2], gain1_row, gain2_row], axis=0)
    minor_all = jnp.concatenate(
        [minor_rows, jnp.pad(grad_mix[:, :kinds], ((0, 0), (0, width - kinds)))], axis=0
    )
    rows = width // parts
    if by_hand:
        up_pair, lined, risen, fallen, weights = lax.optimization_barrier(
            (up_pair, lined, risen, fallen, weights)
        )
        kept = [gate_met, add_low(*up_pair), risen, fallen]
        shares, weight_sum, minor_all = reduce_parts(
            kept, sum(part.astype(F32) for part in lined).astype(BF16), weights, minor_all
        )
    else:
        shares = [
            lax.psum_scatter(grad, "dp", scatter_dimension=0, tiled=True).astype(F32)
            for grad in expert_grads
        ]
        weight_part = lax.psum_scatter(weights, "expert", scatter_dimension=0, tiled=True)
        weight_part = lax.psum_scatter(weight_part, "dp", scatter_dimension=1, tiled=True)
        weight_sum = lax.all_gather(weight_part, "expert", axis=0, tiled=True)
        minor_all = lax.psum(minor_all, ("dp", "expert"))
    grad_gate_mix = minor_all[kinds + 8 :, :kinds]
    minor_sum = lax.dynamic_slice_in_dim(
        minor_all[: kinds + 8], lax.axis_index("dp") * rows, rows, 1
    ).T
    weight_sum = weight_sum.reshape(groups, 4, -1, rows, LANES)
    weight_sum = weight_sum.transpose(3, 1, 0, 2, 4).reshape(rows, 4 * width).astype(F32)
    return (
        mixed,
        grad_tokens,
        grad_prev,
        weight_sum[:, :qkv_cols],
        weight_sum[:, qkv_cols:],
        minor_sum[:, :kinds],
        minor_sum[:, kinds : kinds + 4],
        minor_sum[:, kinds + 4 : kinds + 6],
        minor_sum[:, kinds + 6],
        minor_sum[:, kinds + 7],
        grad_gate_mix,
        jnp.concatenate([shares[0], shares[1]], axis=1)[None],
        shares[2][None],
    )


def solution(mesh):
    rows = P(("dp", "expert"), None)
    in_specs = (
        rows, rows, rows, rows,
        P("dp", None), P("dp", None), P("dp", None), P("dp", None), P("dp", None), P("dp"), P("dp"),
        P(), P("expert", None, None), P("expert", None, None), rows,
    )
    out_specs = (
        rows, rows, rows,
        P("dp", None), P("dp", None), P("dp", None), P("dp", None), P("dp", None), P("dp"), P("dp"),
        P(), P("expert", "dp", None), P("expert", "dp", None),
    )
    return jax.shard_map(
        per_device, mesh=mesh, in_specs=in_specs, out_specs=out_specs, check_vma=False
    )
```
